32 devices in a mesh: dp: 8 (over y, x, core), tensor: 4 (over z).
Axes of the slice: x: 2, y: 2, z: 4, core: 2. Of those that a mesh axis runs over, the one named last changes fastest.
Arguments:
- layer_input: bfloat16 [1024, 8, 2048], P('tensor', 'dp'), may hold values from -6 to 6
- first_gain: bfloat16 [2048], replicated, may hold values from 0.25 to 1.75
- query_weight: bfloat16 [2048, 2048], P('dp', 'tensor'), may hold values from -0.125 to 0.125
- key_matrix: bfloat16 [2048, 1024], P('dp', 'tensor'), may hold values from -0.125 to 0.125
- value_matrix: bfloat16 [2048, 1024], P('dp', 'tensor'), may hold values from -0.125 to 0.125
- query_gain: bfloat16 [128], replicated, may hold values from 0.6 to 7
- key_gain: bfloat16 [128], replicated, may hold values from 0.6 to 7
- output_weight: bfloat16 [2048, 2048], P('dp', 'tensor'), may hold values from -0.75 to 0.75
- second_gain: bfloat16 [2048], replicated, may hold values from 0.25 to 1.75
- gate_weight: bfloat16 [2048, 6144], P('dp', 'tensor'), may hold values from -0.125 to 0.125
- up_weight: bfloat16 [2048, 6144], P('dp', 'tensor'), may hold values from -0.125 to 0.125
- down_weight: bfloat16 [2048, 6144], P('dp', 'tensor'), may hold values from -0.078125 to 0.078125
- segments: int32 [8, 1024], P('dp'), may hold values from 0 to 3, never falling along the last dimension, each value on 1 to 512 neighbouring positions
- cotangent: bfloat16 [1024, 8, 2048], P('tensor', 'dp'), may hold values from -6 to 6
Outputs:
- layer_output: bfloat16 [1024, 8, 2048], P('tensor', 'dp')
- input_grad: bfloat16 [1024, 8, 2048], P('tensor', 'dp')
- first_gain_grad: float32 [2048], replicated
- query_weight_grad: float32 [2048, 2048], P('dp', 'tensor')
- key_weight_grad: float32 [2048, 1024], P('dp', 'tensor')
- value_weight_grad: float32 [2048, 1024], P('dp', 'tensor')
- query_gain_grad: float32 [128], replicated
- key_gain_grad: float32 [128], replicated
- output_weight_grad: float32 [2048, 2048], P('dp', 'tensor')
- second_gain_grad: float32 [2048], replicated
- gate_weight_grad: float32 [2048, 6144], P('dp', 'tensor')
- up_weight_grad: float32 [2048, 6144], P('dp', 'tensor')
- down_weight_grad: float32 [2048, 6144], P('dp', 'tensor')
The draws below stay inside these ranges and needn't reach their ends.
Inputs may be any that keep to these rules, and one draw needn't show every extreme that they name: `segments`: along each sequence the segment numbers never fall; every number appears, each document holds 1 to 512 positions and one holds exactly 512.
All inputs are finite; a program needn't handle non-finite values.
Results may differ from the reference program's by a relative error of at most 0.025.
The reference program's roundings to bfloat16 on the way count: a program that leaves them out, or rounds other values in their place, can miss the bound.
Values may be sent and summed in bfloat16 or wider, within the bound.
A program may use at most 192 MiB of HBM per device.

```python
import math
import jax
import jax.numpy as jnp
import numpy as np
from jax import lax

MODEL_WIDTH = 2048
QUERY_HEADS_COUNT = 16
KEY_VALUE_HEADS = 8
HEAD_WIDTH = 128
FF = 6144
SEQ_LEN = 1024
NSEQ = 8


def head_gains(key, constant_tag):
    local_key = jax.random.fold_in(key, constant_tag)
    return jnp.exp(jax.random.uniform(local_key, (HEAD_WIDTH,), jnp.float32, -0.4, 0.6))


def draw_query_gain(key, part):
    return head_gains(key, 11).astype(jnp.bfloat16)


def draw_key_gain(key, part):
    return head_gains(key, 23).astype(jnp.bfloat16)


def spiked(drawn, rng, source, target, shards_of, factor):
    def block_of(dim):
        return (jnp.arange(drawn.shape[dim]) // (drawn.shape[dim] // shards_of)).reshape((-1,) + (1,) * (drawn.ndim - 1 - dim))

    near = jax.random.permutation(rng, shards_of)[block_of(target)]
    other_side = (block_of(target) + shards_of // 2) % shards_of
    return jnp.where((block_of(source) == near) | (block_of(source) == other_side), factor * drawn, drawn)


def level_of(stream_key, dims, pieces, low, top_value):
    level = 1.0
    for axis_at, parts in pieces:
        heights = jax.random.uniform(jax.random.fold_in(jax.random.fold_in(stream_key, 6), axis_at), (parts,), jnp.float32, low / len(pieces), top_value / len(pieces))
        level = level * jnp.repeat(jnp.exp(heights), dims[axis_at] // parts).reshape((-1,) + (1,) * (len(dims) - 1 - axis_at))
    return level


def length_profile(number_of, total, bound, slope):
    portions = [(1 << 20) // math.isqrt(grade ** slope) + 1 for grade in range(2, number_of + 1)]
    rest, counts = total - bound - (number_of - 1), [1] * (number_of - 1)
    while rest > 0:
        candidates = [i for i in range(number_of - 1) if counts[i] < bound]
        mass, remaining = sum([portions[i] for i in candidates]), rest
        for i in candidates:
            extra = min(bound - counts[i], max(1, remaining * portions[i] // mass), rest)
            counts[i] = counts[i] + extra
            rest = rest - extra
    return np.array([bound] + counts)


def uneven(own_key, amount, total, limit, lean):
    if amount == 2:
        one = jax.random.randint(own_key, (), max(1, total - limit), min(limit, total - 1) + 1)
        return jnp.stack([one, total - one])
    tallies = jnp.asarray(length_profile(amount, total, limit, lean), jnp.int32)
    couples = (amount - 1) // 2
    giver, taker = tallies[1:1 + 2 * couples:2], tallies[2:2 + 2 * couples:2]
    slack = jnp.minimum(giver - 1, limit - taker)
    moved = jax.random.randint(jax.random.fold_in(own_key, 1), (couples,), 0, 1 << 20) % (slack + 1)
    tallies = tallies.at[1:1 + 2 * couples:2].set(giver - moved).at[2:2 + 2 * couples:2].set(taker + moved)
    return tallies[jax.random.permutation(jax.random.fold_in(own_key, 2), amount)]


def normal_values(stream_key, extent, deviation, limit, pieces=(), kind=jnp.bfloat16):
    level = level_of(stream_key, extent, pieces, -0.22, 0.18) if pieces else 1.0
    array = jax.random.normal(stream_key, extent, jnp.float32) * deviation * level
    return jnp.minimum(jnp.maximum(array, -limit), limit).astype(kind)


def heavy_noise(key, shape, spread, bound, shards, heavy, kind=jnp.bfloat16):
    drawn = spread * jax.random.normal(key, shape, jnp.float32)
    if shards:
        drawn = drawn * level_of(key, shape, shards, -0.22, 0.18)
    return jnp.clip(spiked(drawn, jax.random.fold_in(key, 3), *heavy), -bound, bound).astype(kind)


def setup_inputs(seed: int = 0) -> dict:
    streams_of = jax.random.split(jax.random.key(seed), 15)
    return {
        "layer_input": heavy_noise(streams_of[0], (SEQ_LEN, NSEQ, MODEL_WIDTH), 1.0, 6.0, ((0, 4), (1, 8)), (1, 2, 8, 2.0)),
        "first_gain": jnp.clip(1.0 + 0.15 * jax.random.normal(streams_of[1], (MODEL_WIDTH,), jnp.float32), 0.25, 1.75).astype(jnp.bfloat16),
        "query_weight": normal_values(streams_of[2], (MODEL_WIDTH, QUERY_HEADS_COUNT * HEAD_WIDTH), MODEL_WIDTH ** -0.5, 0.125, ((0, 8), (1, 4))),
        "key_matrix": normal_values(streams_of[3], (MODEL_WIDTH, KEY_VALUE_HEADS * HEAD_WIDTH), MODEL_WIDTH ** -0.5, 0.125, ((0, 8), (1, 4))),
        "value_matrix": normal_values(streams_of[4], (MODEL_WIDTH, KEY_VALUE_HEADS * HEAD_WIDTH), MODEL_WIDTH ** -0.5, 0.125, ((0, 8), (1, 4))),
        "query_gain": draw_query_gain(jax.random.fold_in(streams_of[14], 71), 0),
        "key_gain": draw_key_gain(jax.random.fold_in(streams_of[14], 71), 0),
        "output_weight": normal_values(streams_of[7], (MODEL_WIDTH, QUERY_HEADS_COUNT * HEAD_WIDTH), (max(QUERY_HEADS_COUNT * HEAD_WIDTH // 32, 16)) ** -0.5, 0.75, ((0, 8), (1, 4))),
        "second_gain": jnp.clip(1.0 + 0.15 * jax.random.normal(streams_of[8], (MODEL_WIDTH,), jnp.float32), 0.25, 1.75).astype(jnp.bfloat16),
        "gate_weight": normal_values(streams_of[9], (MODEL_WIDTH, FF), MODEL_WIDTH ** -0.5, 0.125, ((0, 8), (1, 4))),
        "up_weight": normal_values(streams_of[10], (MODEL_WIDTH, FF), MODEL_WIDTH ** -0.5, 0.125, ((0, 8), (1, 4))),
        "down_weight": normal_values(streams_of[11], (MODEL_WIDTH, FF), FF ** -0.5, 0.078125, ((0, 8), (1, 4))),
        "segments": jax.vmap(lambda own: jnp.searchsorted(jnp.cumsum(uneven(own, 4, SEQ_LEN, SEQ_LEN // 2, 0)), jnp.arange(SEQ_LEN), side="right"))(jax.random.split(streams_of[12], NSEQ)).reshape((NSEQ, SEQ_LEN)).astype(jnp.int32),
        "cotangent": heavy_noise(streams_of[13], (SEQ_LEN, NSEQ, MODEL_WIDTH), 1.0, 6.0, ((0, 4), (1, 8)), (1, 2, 8, 2.0)),
    }


@jax.custom_vjp
def low(v):
    return lax.optimization_barrier(v.astype(jnp.bfloat16)).astype(jnp.float32)

@jax.custom_vjp
def lowered_backward(v):
    return v

def low_keep(v):
    return (low(v), None)

def low_pass(kept, grad):
    return (grad,)

def back_keep(v):
    return (v, None)

def back_low(kept, grad):
    return (low(grad),)
low.defvjp(low_keep, low_pass)
lowered_backward.defvjp(back_keep, back_low)
epsilon = 1e-06
rope_base = 1000000.0
highest_precision = lax.Precision.HIGHEST

def rms_scale(values, gain):
    return values * lax.rsqrt(lax.optimization_barrier(jnp.mean(values * values, axis=-1, keepdims=True)) + epsilon) * gain

def rope_tables(sequence_length, head_size):
    half_width = head_size // 2
    frequency = rope_base ** (-(2.0 * jnp.arange(half_width, dtype=jnp.float32)) / head_size)
    angles = jnp.arange(sequence_length, dtype=jnp.float32)[:, None] * frequency[None, :]
    angles = jnp.concatenate([angles, angles], axis=1)
    return (jnp.cos(angles), jnp.sin(angles))

def rotate(values, cosine_table, sine_table):
    half_width = values.shape[-1] // 2
    turned = jnp.concatenate([-values[..., half_width:], values[..., :half_width]], axis=-1)
    return values * cosine_table + turned * sine_table

def one_sequence(source, segment_row, params, cosine_table, sine_table):
    first_gain, query_weight, key_matrix, value_matrix, query_gain, key_gain, output_weight, second_gain, gate_weight, up_weight, down_weight = params
    sequence_length = source.shape[0]
    head_groups = QUERY_HEADS_COUNT // KEY_VALUE_HEADS
    first_normalized = low(rms_scale(source, first_gain))
    proj_query = lowered_backward(jnp.dot(first_normalized, query_weight, precision=highest_precision)).reshape(sequence_length, QUERY_HEADS_COUNT, HEAD_WIDTH)
    projected_key = lowered_backward(jnp.dot(first_normalized, key_matrix, precision=highest_precision)).reshape(sequence_length, KEY_VALUE_HEADS, HEAD_WIDTH)
    projected_value = lowered_backward(jnp.dot(first_normalized, value_matrix, precision=highest_precision)).reshape(sequence_length, KEY_VALUE_HEADS, HEAD_WIDTH)
    cos_heads = cosine_table[:, None, :]
    sin_heads = sine_table[:, None, :]
    query_row_block = lowered_backward(low(rotate(rms_scale(proj_query, query_gain), cos_heads, sin_heads)))
    key_rows = lowered_backward(low(rotate(rms_scale(projected_key, key_gain), cos_heads, sin_heads)))
    value_rows = low(projected_value)
    query_row_block = query_row_block.reshape(sequence_length, KEY_VALUE_HEADS, head_groups, HEAD_WIDTH)
    scores = jnp.einsum('qhgd,khd->hgqk', query_row_block, key_rows, precision=highest_precision) * (1.0 / math.sqrt(HEAD_WIDTH))
    scores = lowered_backward(scores)
    position = jnp.arange(sequence_length)
    allowed = (segment_row[:, None] == segment_row[None, :]) & (position[None, :] <= position[:, None])
    masked = jnp.where(allowed, scores, -1e+30)
    row_max = lax.optimization_barrier(jnp.max(masked, axis=-1, keepdims=True))
    weights = jnp.exp(masked - row_max)
    attention = low(weights / lax.optimization_barrier(jnp.sum(weights, axis=-1, keepdims=True)))
    attended = jnp.einsum('hgqk,khd->qhgd', attention, value_rows, precision=highest_precision).reshape(sequence_length, QUERY_HEADS_COUNT * HEAD_WIDTH)
    attended = lowered_backward(low(attended))
    middle = source + lowered_backward(jnp.dot(attended, output_weight.T, precision=highest_precision))
    normed_two = low(rms_scale(middle, second_gain))
    gate_projected = lowered_backward(jnp.dot(normed_two, gate_weight, precision=highest_precision))
    up_projected = lowered_backward(jnp.dot(normed_two, up_weight, precision=highest_precision))
    hidden = low(gate_projected * jax.nn.sigmoid(gate_projected) * up_projected)
    return middle + lowered_backward(jnp.dot(hidden, down_weight.T, precision=highest_precision))

def reference(layer_input, first_gain, query_weight, key_matrix, value_matrix, query_gain, key_gain, output_weight, second_gain, gate_weight, up_weight, down_weight, segments, cotangent):
    params = tuple((argument.astype(jnp.float32) for argument in (first_gain, query_weight, key_matrix, value_matrix, query_gain, key_gain, output_weight, second_gain, gate_weight, up_weight, down_weight)))
    sequences = jnp.transpose(layer_input.astype(jnp.float32), (1, 0, 2))
    cosine_table, sine_table = rope_tables(SEQ_LEN, HEAD_WIDTH)

    def forward(inputs, weights_all):

        def one_step(pair_item):
            return one_sequence(pair_item[0], pair_item[1], weights_all, cosine_table, sine_table)
        return lax.map(jax.checkpoint(one_step), (inputs, segments))
    outputs, pullback = jax.vjp(forward, sequences, params)
    grad_input, grad_params = pullback(jnp.transpose(cotangent.astype(jnp.float32), (1, 0, 2)))
    layer_output = jnp.transpose(outputs, (1, 0, 2)).astype(jnp.bfloat16)
    input_grad = jnp.transpose(grad_input, (1, 0, 2)).astype(jnp.bfloat16)
    return (layer_output, input_grad, grad_params[0], grad_params[1], grad_params[2], grad_params[3], grad_params[4], grad_params[5], grad_params[6], grad_params[7], grad_params[8], grad_params[9], grad_params[10])
```

```python
import functools

import jax
import jax.numpy as jnp
from jax import lax
from jax.experimental import pallas as pl
from jax.experimental.pallas import tpu as pltpu
from jax.sharding import PartitionSpec as P

epsilon = 1e-06
rope_base = 1000000.0
longest_document = 512
bf16 = jnp.bfloat16
f32 = jnp.float32


def mm(eq, a, b):
    return jnp.einsum(eq, a, b, preferred_element_type=f32)


def rms_parts(values, gain):
    inverse = lax.rsqrt(jnp.mean(values * values, axis=-1, keepdims=True) + epsilon)
    return values * inverse * gain, inverse


def rms_back(values, inverse, gain, upstream):
    normed = values * inverse
    inner = upstream * gain
    grad = inverse * (inner - normed * jnp.mean(inner * normed, axis=-1, keepdims=True))
    return grad, upstream * normed


def rope_tables(positions, head_size):
    half = head_size // 2
    frequency = rope_base ** (-(2.0 * jnp.arange(half, dtype=f32)) / head_size)
    angles = positions.astype(f32)[:, None] * frequency[None, :]
    sine = jnp.sin(angles)
    return (
        jnp.concatenate([jnp.cos(angles)] * 2, axis=1),
        jnp.concatenate([-sine, sine], axis=1),
    )


def rotate_back(upstream, cosine, sine):
    half = upstream.shape[-1] // 2
    shifted = upstream * sine
    return upstream * cosine + jnp.concatenate(
        [shifted[..., half:], shifted[..., :half]], axis=-1
    )


class Plan:
    def __init__(self):
        self.size = lax.axis_size("dp")
        self.index = lax.axis_index("dp")
        self.place = lax.axis_index("tensor")
        self.line = lax.axis_size("tensor")
        assert self.line == 4
        self.others = [1 << i for i in range(1, self.size.bit_length() - 1)]
        evens = [0]
        for bit in self.others:
            evens = evens + [m ^ bit for m in evens]
        self.evens = evens
        self.masks = evens + [m ^ 1 for m in evens]
        self.forward = self.others
        self.backward = self.others[::-1]

    def swap(self, value, bit):
        return lax.ppermute(value, "dp", [(i, i ^ bit) for i in range(self.size)])

    def move(self, value, pairs):
        return lax.ppermute(value, "tensor", pairs)

    def xor_blocks(self, blocks):
        bit = 1
        while bit < self.size:
            on = (self.index & bit) != 0
            blocks = [jnp.where(on, blocks[i ^ bit], blocks[i]) for i in range(self.size)]
            bit *= 2
        return blocks

    def to_masks(self, value):
        blocks = self.xor_blocks(jnp.split(value, self.size, axis=-1))
        return jnp.concatenate([blocks[m] for m in self.masks], axis=-1)

    def from_masks(self, value):
        parts = jnp.split(value, self.size, axis=-1)
        blocks = [parts[self.masks.index(m)] for m in range(self.size)]
        return jnp.concatenate(self.xor_blocks(blocks), axis=-1)

    def gather(self, shard, order):
        rows = shard.shape[0]
        held, masks = shard, [0]
        for bit in order:
            arrived = self.swap(held, bit)
            held = jnp.concatenate([held, arrived], axis=0)
            masks = masks + [m ^ bit for m in masks]
        if masks != self.evens:
            held = jnp.concatenate(
                [lax.slice_in_dim(held, masks.index(m) * rows, (masks.index(m) + 1) * rows) for m in self.evens],
                axis=0,
            )
        return held, self.swap(held, 1)

    def reduce(self, even, odd, order):
        rows = even.shape[0] // len(self.evens)
        total = even.astype(f32) + self.swap(odd.astype(bf16), 1).astype(f32)
        pieces = {
            m: lax.slice_in_dim(total, i * rows, (i + 1) * rows) for i, m in enumerate(self.evens)
        }
        for bit in order:
            leaving = [m for m in pieces if m & bit]
            sent = jnp.concatenate([pieces[m].astype(bf16) for m in leaving], axis=0)
            arrived = self.swap(sent, bit)
            kept = {m: v for m, v in pieces.items() if not m & bit}
            for i, m in enumerate(leaving):
                kept[m ^ bit] = kept[m ^ bit] + lax.slice_in_dim(
                    arrived, i * rows, (i + 1) * rows
                ).astype(f32)
            pieces = kept
        return pieces[0]

    def gather_line(self, own):
        from_right = self.move(own, [(1, 0), (2, 1), (3, 2)])
        from_left = self.move(own, [(0, 1), (1, 2), (2, 3)])
        right_two = self.move(from_right, [(1, 0), (2, 1)])
        left_two = self.move(from_left, [(1, 2), (2, 3)])
        slot_two = jnp.where(self.place < 2, right_two, left_two)
        last = self.move(slot_two, [(1, 0), (2, 3)])
        slot_one = jnp.where(self.place < 3, from_right, last)
        slot_three = jnp.where(self.place > 0, from_left, last)
        return [own, slot_one, slot_two, slot_three]

    def scatter_line(self, slots):
        zero, one, two, three = slots
        first = self.move(
            jnp.where(self.place == 3, one, three).astype(bf16), [(3, 2), (0, 1)]
        )
        middle = (two + first.astype(f32)).astype(bf16)
        leftward = self.move(middle, [(3, 2), (2, 1)])
        rightward = self.move(middle, [(0, 1), (1, 2)])
        leftward = self.move(
            (three + leftward.astype(f32)).astype(bf16), [(3, 2), (2, 1), (1, 0)]
        )
        rightward = self.move(
            (one + rightward.astype(f32)).astype(bf16), [(0, 1), (1, 2), (2, 3)]
        )
        return zero + leftward.astype(f32) + rightward.astype(f32)

    def total(self, value):
        bit = 1
        while bit < self.size:
            value = value + self.swap(value, bit)
            bit *= 2
        for bit in (1, 2):
            value = value + self.move(value, [(i, i ^ bit) for i in range(self.line)])
        return value


def after(value, *others):
    return lax.optimization_barrier((value,) + others)[0]


def mesh_copy(src, dst, send, recv, device):
    return pltpu.make_async_remote_copy(
        src_ref=src, dst_ref=dst, send_sem=send, recv_sem=recv, device_id=device,
        device_id_type=pl.DeviceIdType.MESH,
    )


class Links:
    def __init__(self, size):
        bits = [1 << i for i in range(1, size.bit_length() - 1)]
        self.orders = (bits, bits[::-1])
        evens = [0]
        for bit in bits:
            evens = evens + [m ^ bit for m in evens]
        self.evens = evens
        self.masks = evens + [m ^ 1 for m in evens]
        self.bits = bits

    def onward(self, half, mask):
        order = self.orders[half]
        last = max([i for i, bit in enumerate(order) if mask & bit], default=-1)
        return order[last + 1 :]


def greet(links, d, t, line):
    barrier = pltpu.get_barrier_semaphore()
    for bit in [1] + links.bits:
        pl.semaphore_signal(barrier, inc=1, device_id=(d ^ bit, t), device_id_type=pl.DeviceIdType.MESH)

    @pl.when(t > 0)
    def _():
        pl.semaphore_signal(barrier, inc=1, device_id=(d, t - 1), device_id_type=pl.DeviceIdType.MESH)

    @pl.when(t < line - 1)
    def _():
        pl.semaphore_signal(barrier, inc=1, device_id=(d, t + 1), device_id_type=pl.DeviceIdType.MESH)

    pl.semaphore_wait(
        barrier,
        1 + len(links.bits) + jnp.where(t > 0, 1, 0) + jnp.where(t < line - 1, 1, 0),
    )


def nt(a, b):
    return lax.dot_general(a, b, (((1,), (1,)), ((), ())), preferred_element_type=f32)


def tn(a, b):
    return lax.dot_general(a, b, (((0,), (0,)), ((), ())), preferred_element_type=f32)


def nn(a, b):
    return jnp.dot(a, b, preferred_element_type=f32)


def head_norm(values, gain):
    inverse = lax.rsqrt(jnp.mean(values * values, axis=-1, keepdims=True) + epsilon)
    return values * inverse * gain


def forward_kernel(
    size, line, head,
    shard, rows_in, source, gain_q, gain_k, gain_two, cosine, sine, key_seg, query_seg,
    weights_out, proj_q, proj_k, q_out, k_out, v_out, lse_out, att_out, middle, normed_out,
    full, rows_all, acc,
    z_send, z_recv, send, recv, row_send, row_recv, keep,
):
    links = Links(size)
    d, t = lax.axis_index("dp"), lax.axis_index("tensor")
    block = shard.shape[1]
    rows, width = rows_in.shape
    span = rows_all.shape[0]
    factor = head**-0.5

    def place(mask):
        return pl.ds(links.masks.index(mask) * block, block)

    def slot_of(i):
        far = jnp.where(t < line - 1, 1, 3)
        near = jnp.where(t < line - 1, 3, 1)
        return jnp.where(i == 0, 0, jnp.where(i == 1, far, jnp.where(i == 2, 2, near)))

    def across(slot, half, mask, bit):
        piece = mask ^ bit
        return mesh_copy(
            full.at[half, slot, place(mask)],
            full.at[half, slot, place(piece)],
            send.at[slot, half, links.masks.index(piece)],
            recv.at[slot, half, links.masks.index(piece)],
            (d ^ bit, t),
        )

    def along(number, source_slot, target_slot, to):
        return mesh_copy(
            full.at[:, source_slot, place(0)],
            full.at[:, target_slot, place(0)],
            z_send.at[number],
            z_recv.at[target_slot],
            (d, to),
        )

    own = pltpu.make_async_copy(shard, full.at[:, 0, place(0)], z_recv.at[0])
    own.start()
    rows_all[pl.ds(span - rows, rows), :] = rows_in[...]

    @pl.when(t == 0)
    def _():
        rows_all[pl.ds(0, 2 * rows), :] = jnp.zeros((2 * rows, width), bf16)

    @pl.when(t == 1)
    def _():
        rows_all[pl.ds(0, rows), :] = jnp.zeros((rows, width), bf16)

    greet(links, d, t, line)
    own.wait()

    row_one = mesh_copy(
        rows_in, rows_all.at[pl.ds(rows, rows)], row_send.at[0], row_recv.at[0], (d, t + 1)
    )
    row_two = mesh_copy(
        rows_all.at[pl.ds(rows, rows)], rows_all.at[pl.ds(0, rows)], row_send.at[1],
        row_recv.at[1], (d, t + 1),
    )

    def launch(slot):
        for step in range(len(links.bits)):
            for half in (0, 1):
                across(slot, half, 0, links.orders[half][step]).start()
        for half in (0, 1):
            across(slot, half, 0, 1).start()

    def arrive(slot, half, mask):
        bit = [b for b in links.orders[half] if b & mask][-1]
        across(slot, half, mask ^ bit, bit).wait_recv()
        for other in links.onward(half, mask):
            across(slot, half, mask, other).start()
        across(slot, half, mask, 1).start()

    def onward(slot):
        for mask in links.evens[1:]:
            for half in (0, 1):
                if links.onward(half, mask):
                    arrive(slot, half, mask)

    def complete(slot):
        for mask in links.evens[1:]:
            for half in (0, 1):
                if not links.onward(half, mask):
                    arrive(slot, half, mask)
        for mask in links.evens:
            for half in (0, 1):
                across(slot, half, mask, 1).wait_recv()

    inner = (t > 0) & (t < line - 1)

    def wait_line(slot):
        along(0, 0, slot, t).wait_recv()

    @pl.when(t > 0)
    def _():
        along(0, 0, 1, t - 1).start()

    @pl.when(t < line - 1)
    def _():
        along(1, 0, 3, t + 1).start()
        row_one.start()

    launch(0)
    onward(0)
    wait_line(slot_of(1))
    launch(slot_of(1))

    @pl.when(inner)
    def _():
        along(2, 1, 2, t - 1).start()
        wait_line(3)
        along(3, 3, 2, t + 1).start()

    @pl.when(t > 0)
    def _():
        row_one.wait_recv()

    @pl.when(inner)
    def _():
        row_two.start()

    wait_line(2)
    launch(2)

    @pl.when(t == 1)
    def _():
        along(4, 2, 3, t - 1).start()

    @pl.when(t == 2)
    def _():
        along(5, 2, 1, t + 1).start()

    onward(slot_of(1))

    @pl.when(t > 1)
    def _():
        row_two.wait_recv()

    acc[...] = source[...]

    lane = lax.broadcasted_iota(jnp.int32, (rows, 128), 1)
    q_index = lax.broadcasted_iota(jnp.int32, (rows, span), 0) + (span - rows)
    k_index = lax.broadcasted_iota(jnp.int32, (rows, span), 1)

    def step(i, carry):
        slot = slot_of(i)

        @pl.when(i == 1)
        def _():
            @pl.when(t == 0)
            def _():
                wait_line(3)

            @pl.when(t == line - 1)
            def _():
                wait_line(1)

            launch(slot_of(3))

        @pl.when(i >= 2)
        def _():
            onward(slot)

        complete(slot)
        for half in (0, 1):
            pltpu.make_async_copy(
                full.at[half, slot], weights_out.at[half, slot], keep.at[slot, half]
            ).start()

        own_rows = pl.ds(span - rows, rows)
        allowed = (query_seg[...] == key_seg[...]) & (k_index <= q_index)
        lse_acc = jnp.zeros((rows, 128), f32)
        for g in (0, 1):
            key_cols = slice(g * head, (g + 1) * head)
            if g == 0:
                for r in range(span // rows):
                    part = pl.ds(r * rows, rows)
                    both = nn(rows_all[part, :], full[1, slot, :, 0 : 4 * head])
                    if r == span // rows - 1:
                        proj_k[slot] = both[:, : 2 * head]
                    for h in (0, 1):
                        unit = head_norm(both[:, h * head : (h + 1) * head], gain_k[...])
                        turned = unit * cosine[part, :] + pltpu.roll(unit, head // 2, 1) * sine[part, :]
                        k_out[slot, part, h * head : (h + 1) * head] = turned.astype(bf16)
                    v_out[slot, part, :] = both[:, 2 * head :].astype(bf16)
            for j in (0, 1):
                h = 2 * g + j
                cols = slice(h * head, (h + 1) * head)
                raw = nn(rows_in[...], full[0, slot, :, cols])
                proj_q[slot, :, cols] = raw
                unit = head_norm(raw, gain_q[...])
                turned = unit * cosine[own_rows, :] + pltpu.roll(unit, head // 2, 1) * sine[own_rows, :]
                query = turned.astype(bf16)
                q_out[slot, :, cols] = query
                scores = nt(query, k_out[slot, :, key_cols]) * factor
                scores = jnp.where(allowed, scores, -1e30)
                top = jnp.max(scores, axis=-1, keepdims=True)
                weight = jnp.exp(scores - top)
                total = jnp.sum(weight, axis=-1, keepdims=True)
                probs = (weight / total).astype(bf16)
                att_out[slot, :, cols] = nn(probs, v_out[slot, :, key_cols]).astype(bf16)
                lse_acc = jnp.where(lane == h, top + jnp.log(total), lse_acc)
        lse_out[slot] = lse_acc
        for half in (0, 1):
            acc[...] += nt(
                att_out[slot, :, half * 2 * head : (half + 1) * 2 * head],
                full[half, slot, :, 4 * head : 6 * head],
            )
        return carry

    lax.fori_loop(0, line, step, 0)
    values = acc[...]
    middle[...] = values
    normed_out[...] = head_norm(values, gain_two[...]).astype(bf16)

    def finish(i, carry):
        for half in (0, 1):
            for mask in links.masks[1:]:
                index = links.masks.index(mask)
                mesh_copy(
                    full.at[half, i, place(0)], full.at[half, i, place(mask)],
                    send.at[i, half, index], recv.at[i, half, index], (d, t),
                ).wait_send()
            pltpu.make_async_copy(full.at[half, i], weights_out.at[half, i], keep.at[i, half]).wait()
        return carry

    lax.fori_loop(0, line, finish, 0)

    @pl.when(t > 0)
    def _():
        along(0, 0, 1, t - 1).wait_send()

    @pl.when(t < line - 1)
    def _():
        along(1, 0, 3, t + 1).wait_send()
        row_one.wait_send()

    @pl.when(inner)
    def _():
        along(2, 1, 2, t - 1).wait_send()
        along(3, 3, 2, t + 1).wait_send()
        row_two.wait_send()

    @pl.when(t == 1)
    def _():
        along(4, 2, 3, t - 1).wait_send()

    @pl.when(t == 2)
    def _():
        along(5, 2, 1, t + 1).wait_send()


def attention_forward(shard, rows_one, source, gain_q, gain_k, gain_two, cosine, sine, key_seg, query_seg, size, line):
    _, block, cols = shard.shape
    rows, width = rows_one.shape
    span = cosine.shape[0]
    head = gain_q.shape[1]
    pieces = 2 * (size // 2)
    vmem = pl.BlockSpec(memory_space=pltpu.VMEM)
    hbm = pl.BlockSpec(memory_space=pl.ANY)
    shape = jax.ShapeDtypeStruct
    return pl.pallas_call(
        functools.partial(forward_kernel, size, line, head),
        out_shape=(
            shape((2, line, width, cols), bf16),
            shape((line, rows, 4 * head), f32),
            shape((line, rows, 2 * head), f32),
            shape((line, rows, 4 * head), bf16),
            shape((line, span, 2 * head), bf16),
            shape((line, span, 2 * head), bf16),
            shape((line, rows, 128), f32),
            shape((line, rows, 4 * head), bf16),
            shape((rows, width), f32),
            shape((rows, width), bf16),
        ),
        in_specs=[hbm] + [vmem] * 9,
        out_specs=[hbm] + [vmem] * 9,
        scratch_shapes=[
            pltpu.VMEM((2, line, width, cols), bf16),
            pltpu.VMEM((span, width), bf16),
            pltpu.VMEM((rows, width), f32),
            pltpu.SemaphoreType.DMA((6,)),
            pltpu.SemaphoreType.DMA((line,)),
            pltpu.SemaphoreType.DMA((line, 2, pieces)),
            pltpu.SemaphoreType.DMA((line, 2, pieces)),
            pltpu.SemaphoreType.DMA((2,)),
            pltpu.SemaphoreType.DMA((2,)),
            pltpu.SemaphoreType.DMA((line, 2)),
        ],
        compiler_params=pltpu.CompilerParams(
            collective_id=0, has_side_effects=True, vmem_limit_bytes=62 << 20
        ),
        cost_estimate=pl.CostEstimate(flops=40 << 30, bytes_accessed=200 << 20, transcendentals=4 << 20),
    )(shard, rows_one, source, gain_q, gain_k, gain_two, cosine, sine, key_seg, query_seg)


def body(
    layer_input,
    first_gain,
    query_weight,
    key_matrix,
    value_matrix,
    query_gain,
    key_gain,
    output_weight,
    second_gain,
    gate_weight,
    up_weight,
    down_weight,
    segments,
    cotangent,
):
    plan = Plan()
    line, place = plan.line, plan.place
    rows, seq_count, width = layer_input.shape
    head = query_gain.shape[0]
    kv_heads = key_matrix.shape[1] // head
    query_heads = query_weight.shape[1] // head
    groups = query_heads // kv_heads
    all_kv = line * kv_heads
    half = width // 2
    hops = -(-(longest_document - 1) // rows)
    assert seq_count == 1 and hops == 2
    factor = head**-0.5

    gain_one = plan.to_masks(first_gain.astype(f32))
    gain_two = plan.to_masks(second_gain.astype(f32))
    gain_query = query_gain.astype(f32)
    gain_key = key_gain.astype(f32)
    source = plan.to_masks(layer_input[:, 0, :]).astype(f32)
    upstream = plan.to_masks(cotangent[:, 0, :])

    q_cols = query_weight.shape[1]
    kv_cols = key_matrix.shape[1]
    o_half = output_weight.shape[1] // 2
    shard = jnp.stack(
        [
            jnp.concatenate([query_weight, output_weight[:, :o_half]], axis=1),
            jnp.concatenate([key_matrix, value_matrix, output_weight[:, o_half:]], axis=1),
        ]
    )
    normed, inverse_one = rms_parts(source, gain_one)
    rows_one = normed.astype(bf16)
    span = (hops + 1) * rows
    positions = (place - hops) * rows + jnp.arange(span)
    cosine, sine = rope_tables(positions, head)
    padded = jnp.concatenate([jnp.full((hops * rows,), -1, segments.dtype), segments[0]], axis=0)
    key_segments = lax.dynamic_slice(padded, (place * rows,), (span,))
    query_segments = key_segments[hops * rows :]
    (
        weights, proj_query, proj_key, query_rows, key_rows, value_rows, lse, attended, middle, rows_two_own,
    ) = attention_forward(
        shard, rows_one, source, gain_query[None], gain_key[None], gain_two[None], cosine, sine,
        key_segments[None, :], query_segments[:, None], plan.size, line,
    )
    inverse_two = lax.rsqrt(jnp.mean(middle * middle, axis=-1, keepdims=True) + epsilon)

    gate_in, up_in = after((gate_weight, up_weight), rows_two_own)
    gate_full = plan.gather(gate_in, plan.forward)
    up_full = plan.gather(up_in, plan.backward)
    hidden_half = down_weight.shape[1] // 2
    down_in = after(down_weight, gate_full[0], up_full[0])
    down_full = [
        plan.gather(down_in[:, :hidden_half], plan.forward),
        plan.gather(down_in[:, hidden_half:], plan.backward),
    ]
    upstream_all = lax.all_gather(upstream, "tensor", axis=0, tiled=True)

    def project(values, full):
        return mm("ld,dc->lc", values[:, :half], full[0]) + mm(
            "ld,dc->lc", values[:, half:], full[1]
        )

    def spread(values, full):
        return jnp.concatenate(
            [mm("lc,dc->ld", values, full[0]), mm("lc,dc->ld", values, full[1])], axis=1
        )

    rows_two = lax.all_gather(rows_two_own, "tensor", axis=0, tiled=True)

    gate_proj = project(rows_two, gate_full)
    up_proj = project(rows_two, up_full)
    sigmoid = jax.nn.sigmoid(gate_proj)
    activated = gate_proj * sigmoid
    hidden = (activated * up_proj).astype(bf16)
    grad_hidden = jnp.concatenate([project(upstream_all, f) for f in down_full], axis=1)
    grad_gate = (
        grad_hidden * up_proj * sigmoid * (1.0 + gate_proj * (1.0 - sigmoid))
    ).astype(bf16)
    grad_up = (grad_hidden * activated).astype(bf16)
    grad_two_part = (spread(grad_gate, gate_full) + spread(grad_up, up_full)).astype(bf16)
    grad_two = lax.psum_scatter(
        grad_two_part, "tensor", scatter_dimension=0, tiled=True
    ).astype(f32)
    mixed_part = spread(hidden[:, :hidden_half], down_full[0]) + spread(
        hidden[:, hidden_half:], down_full[1]
    )
    mixed_in = after(mixed_part.astype(bf16), grad_two_part)
    mixed = lax.psum_scatter(mixed_in, "tensor", scatter_dimension=0, tiled=True).astype(f32)
    layer_output = plan.from_masks((middle + mixed).astype(bf16))[:, None, :]

    def weight_term(left, right):
        return (
            mm("ld,lc->dc", left[:, :half], right).astype(bf16),
            mm("ld,lc->dc", left[:, half:], right).astype(bf16),
        )

    gate_grad = plan.reduce(*weight_term(rows_two, grad_gate), plan.forward)
    up_grad = plan.reduce(*weight_term(rows_two, grad_up), plan.backward)
    down_grad = jnp.concatenate(
        [
            plan.reduce(*weight_term(upstream_all, hidden[:, :hidden_half]), plan.forward),
            plan.reduce(*weight_term(upstream_all, hidden[:, hidden_half:]), plan.backward),
        ],
        axis=1,
    )

    grad_mid_norm, gain_two_terms = rms_back(middle, inverse_two, gain_two, grad_two)
    grad_middle = upstream.astype(f32) + grad_mid_norm
    grad_branch = grad_middle.astype(bf16)
    o_weights = weights[:, :, :, q_cols:]
    grad_attended = jnp.stack(
        [
            jnp.concatenate([mm("ld,dc->lc", grad_branch, o_weights[h, s]) for h in (0, 1)], axis=1)
            for s in range(line)
        ]
    ).astype(bf16)
    attended_flat = jnp.concatenate([attended[s] for s in range(line)], axis=1)
    output_cols = attended_flat.shape[1] // 2
    output_sum = jnp.concatenate(
        [
            plan.reduce(*weight_term(grad_branch, attended_flat[:, :output_cols]), plan.forward),
            plan.reduce(*weight_term(grad_branch, attended_flat[:, output_cols:]), plan.backward),
        ],
        axis=1,
    )
    output_grad = plan.scatter_line(jnp.split(output_sum, line, axis=1))

    allowed = (query_segments[:, None] == key_segments[None, :]) & (
        positions[None, :] <= positions[hops * rows :][:, None]
    )

    def heads_of(values, count):
        return values.reshape(values.shape[0], values.shape[1], -1, *count)

    grouped = heads_of(query_rows, (groups, head))
    grad_out = heads_of(grad_attended, (groups, head))
    keys = heads_of(key_rows, (head,))
    values_all = heads_of(value_rows, (head,))
    log_total = lse[:, :, :query_heads].reshape(line, rows, kv_heads, groups)
    log_total = jnp.transpose(log_total, (0, 2, 3, 1))[..., None]
    scores = jnp.where(allowed, mm("sqhgd,skhd->shgqk", grouped, keys) * factor, -1e30)
    probs32 = jnp.exp(scores - log_total)
    grad_probs = mm("sqhgd,skhd->shgqk", grad_out, values_all)
    delta = jnp.sum(probs32 * grad_probs, axis=-1, keepdims=True)
    grad_scores = (probs32 * (grad_probs - delta)).astype(bf16)
    grad_query = (mm("shgqk,skhd->sqhgd", grad_scores, keys) * factor).astype(bf16)
    grad_key_part = mm("shgqk,sqhgd->skhd", grad_scores, grouped) * factor
    grad_value_part = mm("shgqk,sqhgd->skhd", probs32.astype(bf16), grad_out)

    def flat(values):
        return jnp.concatenate([values[s].reshape(values.shape[1], -1) for s in range(line)], axis=1)

    grad_kv_part = jnp.concatenate([flat(grad_key_part), flat(grad_value_part)], axis=1)
    key_width = all_kv * head
    def turn_slots(values):
        slot = key_width // line
        return jnp.concatenate(
            [
                values[:, key_width - slot : key_width],
                values[:, : key_width - slot],
                values[:, 2 * key_width - slot :],
                values[:, key_width : 2 * key_width - slot],
            ],
            axis=1,
        )

    far = plan.move(grad_kv_part[:rows].astype(bf16), [(2, 1), (3, 2)])
    near = plan.move(
        (grad_kv_part[rows : 2 * rows] + turn_slots(far).astype(f32)).astype(bf16),
        [(1, 0), (2, 1), (3, 2)],
    )
    grad_kv = (grad_kv_part[2 * rows :] + turn_slots(near).astype(f32)).astype(bf16)
    grad_key = grad_kv[:, :key_width].reshape(rows, all_kv, head)
    grad_value_low = grad_kv[:, key_width:]

    cos_own = cosine[hops * rows :][:, None, :]
    sin_own = sine[hops * rows :][:, None, :]
    raw_query = flat(proj_query).reshape(rows, -1, head)
    raw_key = flat(proj_key).reshape(rows, -1, head)

    def head_back(raw, gain, upstream_rows):
        inverse = lax.rsqrt(jnp.mean(raw * raw, axis=-1, keepdims=True) + epsilon)
        return rms_back(raw, inverse, gain, rotate_back(upstream_rows, cos_own, sin_own))

    grad_proj_query, query_terms = head_back(
        raw_query, gain_query, flat(grad_query).reshape(rows, -1, head).astype(f32)
    )
    grad_proj_key, key_terms = head_back(raw_key, gain_key, grad_key.astype(f32))
    grad_query_low = grad_proj_query.reshape(rows, -1).astype(bf16)
    grad_key_low = grad_proj_key.reshape(rows, -1).astype(bf16)
    query_sum = plan.reduce(*weight_term(rows_one, grad_query_low), plan.forward)
    query_weight_grad = plan.scatter_line(jnp.split(query_sum, line, axis=1))
    kv_terms = [weight_term(rows_one, v) for v in (grad_key_low, grad_value_low)]
    key_sum = plan.reduce(*kv_terms[0], plan.forward)
    value_sum = plan.reduce(*kv_terms[1], plan.backward)
    kv_grad = plan.scatter_line(
        [
            jnp.concatenate([a, b], axis=1)
            for a, b in zip(jnp.split(key_sum, line, axis=1), jnp.split(value_sum, line, axis=1))
        ]
    )
    grad_one = 0.0
    for s in range(line):
        q_part = grad_query_low[:, s * q_cols : (s + 1) * q_cols]
        kv_part = jnp.concatenate(
            [
                grad_key_low[:, s * kv_cols : (s + 1) * kv_cols],
                grad_value_low[:, s * kv_cols : (s + 1) * kv_cols],
            ],
            axis=1,
        )
        grad_one = grad_one + mm("lc,dc->ld", q_part, weights[0, s, :, :q_cols])
        grad_one = grad_one + mm("lc,dc->ld", kv_part, weights[1, s, :, : 2 * kv_cols])
    grad_src_norm, gain_one_terms = rms_back(source, inverse_one, gain_one, grad_one)
    input_grad = plan.from_masks((grad_middle + grad_src_norm).astype(bf16))[:, None, :]

    gains = plan.total(
        jnp.concatenate(
            [
                plan.from_masks(jnp.sum(gain_one_terms, axis=0)),
                plan.from_masks(jnp.sum(gain_two_terms, axis=0)),
                jnp.sum(query_terms, axis=(0, 1)),
                jnp.sum(key_terms, axis=(0, 1)),
            ]
        )
    )
    return (
        layer_output,
        input_grad,
        gains[:width],
        query_weight_grad,
        kv_grad[:, :kv_cols],
        kv_grad[:, kv_cols:],
        gains[2 * width : 2 * width + head],
        gains[2 * width + head :],
        output_grad,
        gains[width : 2 * width],
        gate_grad,
        up_grad,
        down_grad,
    )


def solution(mesh):
    positions = P("tensor", "dp", None)
    weight = P("dp", "tensor")
    return jax.shard_map(
        body,
        mesh=mesh,
        in_specs=(
            positions,
            P(),
            weight,
            weight,
            weight,
            P(),
            P(),
            weight,
            P(),
            weight,
            weight,
            weight,
            P("dp", None),
            positions,
        ),
        out_specs=(
            positions,
            positions,
            P(),
            weight,
            weight,
            weight,
            P(),
            P(),
            weight,
            P(),
            weight,
            weight,
            weight,
        ),
        check_vma=False,
    )
```

```python
import functools

import jax
import jax.numpy as jnp
from jax import lax
from jax.experimental import pallas as pl
from jax.experimental.pallas import tpu as pltpu
from jax.sharding import PartitionSpec as P

epsilon = 1e-06
rope_base = 1000000.0
longest_document = 512
bf16 = jnp.bfloat16
f32 = jnp.float32


def mm(eq, a, b):
    return jnp.einsum(eq, a, b, preferred_element_type=f32)


def rms_parts(values, gain):
    inverse = lax.rsqrt(jnp.mean(values * values, axis=-1, keepdims=True) + epsilon)
    return values * inverse * gain, inverse


def rms_back(values, inverse, gain, upstream):
    normed = values * inverse
    inner = upstream * gain
    grad = inverse * (inner - normed * jnp.mean(inner * normed, axis=-1, keepdims=True))
    return grad, upstream * normed


def rope_tables(positions, head_size):
    half = head_size // 2
    frequency = rope_base ** (-(2.0 * jnp.arange(half, dtype=f32)) / head_size)
    angles = positions.astype(f32)[:, None] * frequency[None, :]
    sine = jnp.sin(angles)
    return (
        jnp.concatenate([jnp.cos(angles)] * 2, axis=1),
        jnp.concatenate([-sine, sine], axis=1),
    )


def rotate_back(upstream, cosine, sine):
    half = upstream.shape[-1] // 2
    shifted = upstream * sine
    return upstream * cosine + jnp.concatenate(
        [shifted[..., half:], shifted[..., :half]], axis=-1
    )


class Plan:
    def __init__(self):
        self.size = lax.axis_size("dp")
        self.index = lax.axis_index("dp")
        self.place = lax.axis_index("tensor")
        self.line = lax.axis_size("tensor")
        assert self.line == 4
        self.others = [1 << i for i in range(1, self.size.bit_length() - 1)]
        evens = [0]
        for bit in self.others:
            evens = evens + [m ^ bit for m in evens]
        self.evens = evens
        self.masks = evens + [m ^ 1 for m in evens]
        self.forward = self.others
        self.backward = self.others[::-1]

    def swap(self, value, bit):
        return lax.ppermute(value, "dp", [(i, i ^ bit) for i in range(self.size)])

    def move(self, value, pairs):
        return lax.ppermute(value, "tensor", pairs)

    def xor_blocks(self, blocks):
        bit = 1
        while bit < self.size:
            on = (self.index & bit) != 0
            blocks = [jnp.where(on, blocks[i ^ bit], blocks[i]) for i in range(self.size)]
            bit *= 2
        return blocks

    def to_masks(self, value):
        blocks = self.xor_blocks(jnp.split(value, self.size, axis=-1))
        return jnp.concatenate([blocks[m] for m in self.masks], axis=-1)

    def from_masks(self, value):
        parts = jnp.split(value, self.size, axis=-1)
        blocks = [parts[self.masks.index(m)] for m in range(self.size)]
        return jnp.concatenate(self.xor_blocks(blocks), axis=-1)

    def gather(self, shard, order):
        rows = shard.shape[0]
        held, masks = shard, [0]
        for bit in order:
            arrived = self.swap(held, bit)
            held = jnp.concatenate([held, arrived], axis=0)
            masks = masks + [m ^ bit for m in masks]
        if masks != self.evens:
            held = jnp.concatenate(
                [lax.slice_in_dim(held, masks.index(m) * rows, (masks.index(m) + 1) * rows) for m in self.evens],
                axis=0,
            )
        return held, self.swap(held, 1)

    def reduce(self, even, odd, order):
        rows = even.shape[0] // len(self.evens)
        total = even.astype(f32) + self.swap(odd.astype(bf16), 1).astype(f32)
        pieces = {
            m: lax.slice_in_dim(total, i * rows, (i + 1) * rows) for i, m in enumerate(self.evens)
        }
        for bit in order:
            leaving = [m for m in pieces if m & bit]
            sent = jnp.concatenate([pieces[m].astype(bf16) for m in leaving], axis=0)
            arrived = self.swap(sent, bit)
            kept = {m: v for m, v in pieces.items() if not m & bit}
            for i, m in enumerate(leaving):
                kept[m ^ bit] = kept[m ^ bit] + lax.slice_in_dim(
                    arrived, i * rows, (i + 1) * rows
                ).astype(f32)
            pieces = kept
        return pieces[0]

    def gather_line(self, own):
        from_right = self.move(own, [(1, 0), (2, 1), (3, 2)])
        from_left = self.move(own, [(0, 1), (1, 2), (2, 3)])
        right_two = self.move(from_right, [(1, 0), (2, 1)])
        left_two = self.move(from_left, [(1, 2), (2, 3)])
        slot_two = jnp.where(self.place < 2, right_two, left_two)
        last = self.move(slot_two, [(1, 0), (2, 3)])
        slot_one = jnp.where(self.place < 3, from_right, last)
        slot_three = jnp.where(self.place > 0, from_left, last)
        return [own, slot_one, slot_two, slot_three]

    def scatter_line(self, slots):
        zero, one, two, three = slots
        first = self.move(
            jnp.where(self.place == 3, one, three).astype(bf16), [(3, 2), (0, 1)]
        )
        middle = (two + first.astype(f32)).astype(bf16)
        leftward = self.move(middle, [(3, 2), (2, 1)])
        rightward = self.move(middle, [(0, 1), (1, 2)])
        leftward = self.move(
            (three + leftward.astype(f32)).astype(bf16), [(3, 2), (2, 1), (1, 0)]
        )
        rightward = self.move(
            (one + rightward.astype(f32)).astype(bf16), [(0, 1), (1, 2), (2, 3)]
        )
        return zero + leftward.astype(f32) + rightward.astype(f32)

    def total(self, value):
        bit = 1
        while bit < self.size:
            value = value + self.swap(value, bit)
            bit *= 2
        for bit in (1, 2):
            value = value + self.move(value, [(i, i ^ bit) for i in range(self.line)])
        return value


def after(value, *others):
    return lax.optimization_barrier((value,) + others)[0]


def mesh_copy(src, dst, send, recv, device):
    return pltpu.make_async_remote_copy(
        src_ref=src, dst_ref=dst, send_sem=send, recv_sem=recv, device_id=device,
        device_id_type=pl.DeviceIdType.MESH,
    )


class Links:
    def __init__(self, size):
        bits = [1 << i for i in range(1, size.bit_length() - 1)]
        self.orders = (bits, bits[::-1])
        evens = [0]
        for bit in bits:
            evens = evens + [m ^ bit for m in evens]
        self.evens = evens
        self.masks = evens + [m ^ 1 for m in evens]
        self.bits = bits

    def onward(self, half, mask):
        order = self.orders[half]
        last = max([i for i, bit in enumerate(order) if mask & bit], default=-1)
        return order[last + 1 :]


class Gather:
    def __init__(self, links, d, t, piece, send, recv):
        self.links, self.d, self.t = links, d, t
        self.piece, self.send, self.recv = piece, send, recv

    def copy(self, half, mask, bit):
        index = self.links.masks.index(mask ^ bit)
        return mesh_copy(
            self.piece(half, mask), self.piece(half, mask ^ bit), self.send(half, index),
            self.recv(half, index), (self.d ^ bit, self.t),
        )

    def launch(self):
        for step in range(len(self.links.bits)):
            for half in (0, 1):
                self.copy(half, 0, self.links.orders[half][step]).start()
        for half in (0, 1):
            self.copy(half, 0, 1).start()

    def arrive(self, half, mask):
        bit = [b for b in self.links.orders[half] if b & mask][-1]
        self.copy(half, mask ^ bit, bit).wait_recv()
        for other in self.links.onward(half, mask):
            self.copy(half, mask, other).start()
        self.copy(half, mask, 1).start()

    def onward(self):
        for mask in self.links.evens[1:]:
            for half in (0, 1):
                if self.links.onward(half, mask):
                    self.arrive(half, mask)

    def complete(self):
        for mask in self.links.evens[1:]:
            for half in (0, 1):
                if not self.links.onward(half, mask):
                    self.arrive(half, mask)
        for mask in self.links.evens:
            for half in (0, 1):
                self.copy(half, mask, 1).wait_recv()

    def finish(self):
        for mask in self.links.masks[1:]:
            for half in (0, 1):
                self.copy(half, mask ^ 1 if mask & 1 else 0, 1 if mask & 1 else mask).wait_send()


class Relay:
    def __init__(self, d, t, line, slot, send, recv):
        self.d, self.t, self.line = d, t, line
        self.slot, self.send, self.recv = slot, send, recv
        self.inner = (t > 0) & (t < line - 1)

    def copy(self, number, source, target, to):
        return mesh_copy(
            self.slot(source), self.slot(target), self.send.at[number], self.recv.at[target],
            (self.d, to),
        )

    def moves(self):
        t = self.t
        return (
            (t > 0, (0, 0, 1, t - 1)),
            (t < self.line - 1, (1, 0, 3, t + 1)),
            (self.inner, (2, 1, 2, t - 1)),
            (self.inner, (3, 3, 2, t + 1)),
            (t == 1, (4, 2, 3, t - 1)),
            (t == 2, (5, 2, 1, t + 1)),
        )

    def start(self, *numbers):
        for number in numbers:
            condition, route = self.moves()[number]

            @pl.when(condition)
            def _(route=route):
                self.copy(*route).start()

    def wait(self, slot):
        self.copy(0, 0, slot, self.t).wait_recv()

    def finish(self):
        for condition, route in self.moves():

            @pl.when(condition)
            def _(route=route):
                self.copy(*route).wait_send()

    def first(self):
        self.start(0, 1)

    def second(self):
        t, line = self.t, self.line

        @pl.when(t < line - 1)
        def _():
            self.wait(1)

        self.start(2)

        @pl.when(t > 0)
        def _():
            self.wait(3)

        self.start(3)

    def third(self):
        self.wait(2)
        self.start(4, 5)

    def ends(self):
        @pl.when(self.t == 0)
        def _():
            self.wait(3)

        @pl.when(self.t == self.line - 1)
        def _():
            self.wait(1)


def slot_of(i, t, line):
    far = jnp.where(t < line - 1, 1, 3)
    near = jnp.where(t < line - 1, 3, 1)
    return jnp.where(i == 0, 0, jnp.where(i == 1, far, jnp.where(i == 2, 2, near)))


def greet(links, d, t, line):
    barrier = pltpu.get_barrier_semaphore()
    for bit in [1] + links.bits:
        pl.semaphore_signal(barrier, inc=1, device_id=(d ^ bit, t), device_id_type=pl.DeviceIdType.MESH)

    @pl.when(t > 0)
    def _():
        pl.semaphore_signal(barrier, inc=1, device_id=(d, t - 1), device_id_type=pl.DeviceIdType.MESH)

    @pl.when(t < line - 1)
    def _():
        pl.semaphore_signal(barrier, inc=1, device_id=(d, t + 1), device_id_type=pl.DeviceIdType.MESH)

    pl.semaphore_wait(
        barrier,
        1 + len(links.bits) + jnp.where(t > 0, 1, 0) + jnp.where(t < line - 1, 1, 0),
    )


def nt(a, b):
    return lax.dot_general(a, b, (((1,), (1,)), ((), ())), preferred_element_type=f32)


def tn(a, b):
    return lax.dot_general(a, b, (((0,), (0,)), ((), ())), preferred_element_type=f32)


def nn(a, b):
    return jnp.dot(a, b, preferred_element_type=f32)


def head_norm(values, gain):
    inverse = lax.rsqrt(jnp.mean(values * values, axis=-1, keepdims=True) + epsilon)
    return values * inverse * gain


def forward_kernel(
    size, line, head,
    shard, mlp_shard, rows_in, upstream, source, gain_q, gain_k, gain_two, cosine, sine, key_seg, query_seg,
    weights_out, mlp_out, upstream_all, proj_q, proj_k, q_out, k_out, v_out, lse_out, att_out, middle, normed_out,
    full, rows_all, acc,
    z_send, z_recv, send, recv, row_send, row_recv, keep, mlp_send, mlp_recv, up_send, up_recv, local,
):
    links = Links(size)
    d, t = lax.axis_index("dp"), lax.axis_index("tensor")
    block = shard.shape[1]
    rows, width = rows_in.shape
    span = rows_all.shape[0]
    factor = head**-0.5

    def place(mask):
        return pl.ds(links.masks.index(mask) * block, block)

    def gather(slot):
        return Gather(
            links, d, t,
            lambda half, mask: full.at[half, slot, place(mask)],
            lambda half, index: send.at[slot, half, index],
            lambda half, index: recv.at[slot, half, index],
        )

    feed = Gather(
        links, d, t,
        lambda half, mask: mlp_out.at[half, place(mask)],
        lambda half, index: mlp_send.at[half, index],
        lambda half, index: mlp_recv.at[half, index],
    )
    relay = Relay(d, t, line, lambda slot: full.at[:, slot, place(0)], z_send, z_recv)
    upward = Relay(d, t, line, lambda slot: upstream_all.at[slot], up_send, up_recv)

    own = (
        pltpu.make_async_copy(shard, full.at[:, 0, place(0)], local.at[0]),
        pltpu.make_async_copy(mlp_shard, mlp_out.at[:, place(0)], local.at[1]),
        pltpu.make_async_copy(upstream, upstream_all.at[0], local.at[2]),
    )
    for copy in own:
        copy.start()
    rows_all[pl.ds(span - rows, rows), :] = rows_in[...]

    @pl.when(t == 0)
    def _():
        rows_all[pl.ds(0, 2 * rows), :] = jnp.zeros((2 * rows, width), bf16)

    @pl.when(t == 1)
    def _():
        rows_all[pl.ds(0, rows), :] = jnp.zeros((rows, width), bf16)

    greet(links, d, t, line)
    own[0].wait()

    row_one = mesh_copy(
        rows_in, rows_all.at[pl.ds(rows, rows)], row_send.at[0], row_recv.at[0], (d, t + 1)
    )
    row_two = mesh_copy(
        rows_all.at[pl.ds(rows, rows)], rows_all.at[pl.ds(0, rows)], row_send.at[1],
        row_recv.at[1], (d, t + 1),
    )
    inner = relay.inner
    relay.first()

    @pl.when(t < line - 1)
    def _():
        row_one.start()

    gather(0).launch()
    gather(0).onward()
    relay.second()
    second = slot_of(1, t, line)

    @pl.when(t < line - 1)
    def _():
        gather(1).launch()

    @pl.when(t == line - 1)
    def _():
        gather(3).launch()

    @pl.when(t > 0)
    def _():
        row_one.wait_recv()

    @pl.when(inner)
    def _():
        row_two.start()

    relay.third()
    gather(2).launch()
    gather(second).onward()

    @pl.when(t > 1)
    def _():
        row_two.wait_recv()

    own[1].wait()
    own[2].wait()
    acc[...] = source[...]

    lane = lax.broadcasted_iota(jnp.int32, (rows, 128), 1)
    q_index = lax.broadcasted_iota(jnp.int32, (rows, span), 0) + (span - rows)
    k_index = lax.broadcasted_iota(jnp.int32, (rows, span), 1)

    def step(i, carry):
        slot = slot_of(i, t, line)

        @pl.when(i == 1)
        def _():
            relay.ends()
            gather(slot_of(3, t, line)).launch()
            upward.first()

        @pl.when(i >= 2)
        def _():
            gather(slot).onward()

        @pl.when(i == 3)
        def _():
            feed.launch()

        gather(slot).complete()
        for half in (0, 1):
            pltpu.make_async_copy(
                full.at[half, slot], weights_out.at[half, slot], keep.at[slot, half]
            ).start()

        own_rows = pl.ds(span - rows, rows)
        allowed = (query_seg[...] == key_seg[...]) & (k_index <= q_index)
        lse_acc = jnp.zeros((rows, 128), f32)
        for g in (0, 1):
            key_cols = slice(g * head, (g + 1) * head)
            if g == 0:
                for r in range(span // rows):
                    part = pl.ds(r * rows, rows)
                    both = nn(rows_all[part, :], full[1, slot, :, 0 : 4 * head])
                    if r == span // rows - 1:
                        proj_k[slot] = both[:, : 2 * head]
                    for h in (0, 1):
                        unit = head_norm(both[:, h * head : (h + 1) * head], gain_k[...])
                        turned = unit * cosine[part, :] + pltpu.roll(unit, head // 2, 1) * sine[part, :]
                        k_out[slot, part, h * head : (h + 1) * head] = turned.astype(bf16)
                    v_out[slot, part, :] = both[:, 2 * head :].astype(bf16)
            for j in (0, 1):
                h = 2 * g + j
                cols = slice(h * head, (h + 1) * head)
                raw = nn(rows_in[...], full[0, slot, :, cols])
                proj_q[slot, :, cols] = raw
                unit = head_norm(raw, gain_q[...])
                turned = unit * cosine[own_rows, :] + pltpu.roll(unit, head // 2, 1) * sine[own_rows, :]
                query = turned.astype(bf16)
                q_out[slot, :, cols] = query
                scores = nt(query, k_out[slot, :, key_cols]) * factor
                scores = jnp.where(allowed, scores, -1e30)
                top = jnp.max(scores, axis=-1, keepdims=True)
                weight = jnp.exp(scores - top)
                total = jnp.sum(weight, axis=-1, keepdims=True)
                probs = (weight / total).astype(bf16)
                att_out[slot, :, cols] = nn(probs, v_out[slot, :, key_cols]).astype(bf16)
                lse_acc = jnp.where(lane == h, top + jnp.log(total), lse_acc)
        lse_out[slot] = lse_acc
        for half in (0, 1):
            acc[...] += nt(
                att_out[slot, :, half * 2 * head : (half + 1) * 2 * head],
                full[half, slot, :, 4 * head : 6 * head],
            )
        return carry

    lax.fori_loop(0, line, step, 0)
    upward.second()
    feed.onward()
    values = acc[...]
    middle[...] = values
    normed_out[...] = head_norm(values, gain_two[...]).astype(bf16)
    upward.third()
    feed.complete()

    def finish(i, carry):
        gather(i).finish()
        for half in (0, 1):
            pltpu.make_async_copy(full.at[half, i], weights_out.at[half, i], keep.at[i, half]).wait()
        return carry

    lax.fori_loop(0, line, finish, 0)
    feed.finish()
    relay.finish()

    @pl.when(t < line - 1)
    def _():
        row_one.wait_send()

    @pl.when(inner)
    def _():
        row_two.wait_send()

    upward.ends()
    upward.finish()


def attention_forward(shard, mlp_shard, rows_one, upstream, source, gain_q, gain_k, gain_two, cosine, sine, key_seg, query_seg, size, line):
    _, block, cols = shard.shape
    rows, width = rows_one.shape
    span = cosine.shape[0]
    head = gain_q.shape[1]
    pieces = 2 * (size // 2)
    vmem = pl.BlockSpec(memory_space=pltpu.VMEM)
    hbm = pl.BlockSpec(memory_space=pl.ANY)
    shape = jax.ShapeDtypeStruct
    return pl.pallas_call(
        functools.partial(forward_kernel, size, line, head),
        out_shape=(
            shape((2, line, width, cols), bf16),
            shape((2, width, mlp_shard.shape[2]), bf16),
            shape((line, rows, width), bf16),
            shape((line, rows, 4 * head), f32),
            shape((line, rows, 2 * head), f32),
            shape((line, rows, 4 * head), bf16),
            shape((line, span, 2 * head), bf16),
            shape((line, span, 2 * head), bf16),
            shape((line, rows, 128), f32),
            shape((line, rows, 4 * head), bf16),
            shape((rows, width), f32),
            shape((rows, width), bf16),
        ),
        in_specs=[hbm, hbm, vmem, hbm] + [vmem] * 8,
        out_specs=[hbm] * 3 + [vmem] * 9,
        scratch_shapes=[
            pltpu.VMEM((2, line, width, cols), bf16),
            pltpu.VMEM((span, width), bf16),
            pltpu.VMEM((rows, width), f32),
            pltpu.SemaphoreType.DMA((6,)),
            pltpu.SemaphoreType.DMA((line,)),
            pltpu.SemaphoreType.DMA((line, 2, pieces)),
            pltpu.SemaphoreType.DMA((line, 2, pieces)),
            pltpu.SemaphoreType.DMA((2,)),
            pltpu.SemaphoreType.DMA((2,)),
            pltpu.SemaphoreType.DMA((line, 2)),
            pltpu.SemaphoreType.DMA((2, pieces)),
            pltpu.SemaphoreType.DMA((2, pieces)),
            pltpu.SemaphoreType.DMA((6,)),
            pltpu.SemaphoreType.DMA((line,)),
            pltpu.SemaphoreType.DMA((3,)),
        ],
        compiler_params=pltpu.CompilerParams(
            collective_id=0, has_side_effects=True, vmem_limit_bytes=62 << 20
        ),
        cost_estimate=pl.CostEstimate(flops=40 << 30, bytes_accessed=200 << 20, transcendentals=4 << 20),
    )(shard, mlp_shard, rows_one, upstream, source, gain_q, gain_k, gain_two, cosine, sine, key_seg, query_seg)


def feed_kernel(
    size, line,
    rows_in, upstream_in, pair_in, down_in,
    rows_out, hidden_out, gate_out, up_out, grad_out, mixed_out,
    rows_v, upstream_v, pair, down, gate_f, up_f, hidden_v, gate_v, up_v, grad_v, mixed_v,
    z_send, z_recv, send, recv, local, leave,
):
    links = Links(size)
    d, t = lax.axis_index("dp"), lax.axis_index("tensor")
    block = down_in.shape[1]
    _, rows, width = rows_v.shape
    units = hidden_v.shape[2]
    chunk = units // 4
    piece = width // 4

    def place(mask):
        return pl.ds(links.masks.index(mask) * block, block)

    gather = Gather(
        links, d, t,
        lambda half, mask: down.at[half, place(mask)],
        lambda half, index: send.at[half, index],
        lambda half, index: recv.at[half, index],
    )
    relay = Relay(d, t, line, lambda slot: rows_v.at[slot], z_send, z_recv)
    arrivals = (
        pltpu.make_async_copy(rows_in, rows_v.at[0], local.at[0]),
        pltpu.make_async_copy(down_in, down.at[:, place(0)], local.at[1]),
        pltpu.make_async_copy(pair_in, pair, local.at[2]),
        pltpu.make_async_copy(upstream_in, upstream_v, local.at[3]),
    )
    for copy in arrivals:
        copy.start()
    greet(links, d, t, line)
    arrivals[0].wait()
    relay.first()
    arrivals[1].wait()
    gather.launch()
    gather.onward()
    arrivals[2].wait()
    arrivals[3].wait()

    def departures(slot):
        position = lax.rem(slot + t, line)
        natural = pl.ds(pl.multiple_of(position * rows, rows), rows)
        return [
            pltpu.make_async_copy(rows_v.at[slot], rows_out.at[slot], leave.at[0, slot]),
            pltpu.make_async_copy(hidden_v.at[slot], hidden_out.at[slot], leave.at[1, slot]),
            pltpu.make_async_copy(gate_v.at[slot], gate_out.at[slot], leave.at[2, slot]),
            pltpu.make_async_copy(up_v.at[slot], up_out.at[slot], leave.at[3, slot]),
            pltpu.make_async_copy(grad_v.at[slot], grad_out.at[natural], leave.at[4, slot]),
            pltpu.make_async_copy(mixed_v.at[slot], mixed_out.at[natural], leave.at[5, slot]),
        ]

    def step(i, carry):
        slot = slot_of(i, t, line)
        for c in range(4):
            cols = slice(c * chunk, (c + 1) * chunk)
            gate = nn(rows_v[slot], pair[0, :, cols])
            up = nn(rows_v[slot], pair[1, :, cols])
            gate_f[:, cols] = gate
            up_f[:, cols] = up
            hidden_v[slot, :, cols] = (gate * jax.nn.sigmoid(gate) * up).astype(bf16)

        @pl.when(i == 0)
        def _():
            relay.second()
            gather.complete()

        @pl.when(i == 1)
        def _():
            relay.third()

        @pl.when(i == 2)
        def _():
            relay.ends()

        for c in range(4):
            cols = slice(c * chunk, (c + 1) * chunk)
            inner = slice((c % 2) * chunk, (c % 2 + 1) * chunk)
            grad_hidden = nn(upstream_v[slot], down[c // 2, :, inner])
            gate, up = gate_f[:, cols], up_f[:, cols]
            sigmoid = jax.nn.sigmoid(gate)
            gate_v[slot, :, cols] = (
                grad_hidden * up * sigmoid * (1.0 + gate * (1.0 - sigmoid))
            ).astype(bf16)
            up_v[slot, :, cols] = (grad_hidden * (gate * sigmoid)).astype(bf16)
        for n in range(4):
            out = slice(n * piece, (n + 1) * piece)
            grad_v[slot, :, out] = (
                nt(gate_v[slot], pair[0, out, :]) + nt(up_v[slot], pair[1, out, :])
            ).astype(bf16)
            mixed_v[slot, :, out] = (
                nt(hidden_v[slot, :, : units // 2], down[0, out, :])
                + nt(hidden_v[slot, :, units // 2 :], down[1, out, :])
            ).astype(bf16)
        for copy in departures(slot):
            copy.start()
        return carry

    lax.fori_loop(0, line, step, 0)

    def finish(i, carry):
        for copy in departures(i):
            copy.wait()
        return carry

    lax.fori_loop(0, line, finish, 0)
    gather.finish()
    relay.finish()


def feed_forward(rows_own, upstream_all, pair_full, down_shard, size, line):
    rows, width = rows_own.shape
    units = pair_full.shape[2]
    hbm = pl.BlockSpec(memory_space=pl.ANY)
    shape = jax.ShapeDtypeStruct
    dma = pltpu.SemaphoreType.DMA
    return pl.pallas_call(
        functools.partial(feed_kernel, size, line),
        out_shape=(
            shape((line, rows, width), bf16),
            shape((line, rows, units), bf16),
            shape((line, rows, units), bf16),
            shape((line, rows, units), bf16),
            shape((line * rows, width), bf16),
            shape((line * rows, width), bf16),
        ),
        in_specs=[hbm] * 4,
        out_specs=[hbm] * 6,
        scratch_shapes=[
            pltpu.VMEM((line, rows, width), bf16),
            pltpu.VMEM((line, rows, width), bf16),
            pltpu.VMEM((2, width, units), bf16),
            pltpu.VMEM((2, width, units // 2), bf16),
            pltpu.VMEM((rows, units), f32),
            pltpu.VMEM((rows, units), f32),
            pltpu.VMEM((line, rows, units), bf16),
            pltpu.VMEM((line, rows, units), bf16),
            pltpu.VMEM((line, rows, units), bf16),
            pltpu.VMEM((line, rows, width), bf16),
            pltpu.VMEM((line, rows, width), bf16),
            dma((6,)),
            dma((line,)),
            dma((2, size)),
            dma((2, size)),
            dma((4,)),
            dma((6, line)),
        ],
        compiler_params=pltpu.CompilerParams(
            collective_id=1, has_side_effects=True, vmem_limit_bytes=62 << 20
        ),
        cost_estimate=pl.CostEstimate(flops=40 << 30, bytes_accessed=60 << 20, transcendentals=3 << 20),
    )(rows_own, upstream_all, pair_full, down_shard)


class Scatter:
    def __init__(self, links, d, t, block, refs, semaphores):
        self.links, self.d, self.t, self.block = links, d, t, block
        self.odd, self.core, self.sums, self.arrived, self.out = refs
        self.core_send, self.core_recv, self.send, self.recv = semaphores

    @staticmethod
    def pieces(links):
        return max(1, len(links.evens) - 1)

    def steps(self, half):
        masks, number, found = self.links.evens, 0, []
        for bit in self.links.orders[half][::-1]:
            masks = [m for m in masks if not m & bit]
            found.append((bit, [(m, number + i) for i, m in enumerate(masks)]))
            number += len(masks)
        return found

    def rows(self, mask):
        return pl.ds(self.links.evens.index(mask) * self.block, self.block)

    def core_copy(self, j):
        return mesh_copy(
            self.odd(j), self.core(j), self.core_send(j), self.core_recv(j), (self.d ^ 1, self.t)
        )

    def piece_copy(self, j, mask, number, bit):
        return mesh_copy(
            self.sums(j, self.rows(mask ^ bit)), self.arrived(j, number), self.send(j, number),
            self.recv(j, number), (self.d ^ bit, self.t),
        )

    def launch(self, j, half, step):
        steps = self.steps(half)
        if step < len(steps):
            bit, pairs = steps[step]
            for mask, number in pairs:
                self.piece_copy(j, mask, number, bit).start()

    def add(self, j, mask, value):
        if mask == 0:
            out = self.out(j)
            out[...] = out[...] + value[...].astype(f32)
        else:
            total = self.sums(j, self.rows(mask))
            total[...] = (total[...].astype(f32) + value[...].astype(f32)).astype(bf16)

    def stage(self, j, half, stage):
        if stage == 0:
            self.core_copy(j).wait_recv()
            steps = self.steps(half)
            first = steps[0][0] if steps else 0
            for mask in sorted(self.links.evens, key=lambda m: not m & first):
                self.add(j, mask, self.core(j, self.rows(mask)))
        else:
            bit, pairs = self.steps(half)[stage - 1]
            for mask, number in pairs[::-1]:
                self.piece_copy(j, mask, number, bit).wait_recv()
                self.add(j, mask, self.arrived(j, number))
        self.launch(j, half, stage)

    def finish(self, j, half):
        self.core_copy(j).wait_send()
        for bit, pairs in self.steps(half):
            for mask, number in pairs:
                self.piece_copy(j, mask, number, bit).wait_send()


def greet_dp(links, d, t):
    barrier = pltpu.get_barrier_semaphore()
    for bit in [1] + links.bits:
        pl.semaphore_signal(barrier, inc=1, device_id=(d ^ bit, t), device_id_type=pl.DeviceIdType.MESH)
    pl.semaphore_wait(barrier, 1 + len(links.bits))


def weight_kernel(
    size, line,
    rows_in, upstream_in, gate_in, up_in, hidden_in,
    gate_out, up_out, down_out,
    raw, left, right, odd, core, sums, arrived, out,
    core_send, core_recv, send, recv, local, raw_sem, leave,
):
    links = Links(size)
    d, t = lax.axis_index("dp"), lax.axis_index("tensor")
    width = left.shape[1]
    rows = raw.shape[1]
    count, tokens, chunk = right.shape
    middle = width // 2
    block = out.shape[1]
    pairs = count // 2
    wide = gate_in.shape[1] // chunk

    def load(j):
        p, h = j // 2, j % 2
        if p < wide:
            source, at = (gate_in, up_in)[h], p
        else:
            source, at = hidden_in, p - wide + h * (wide // 2)
        return pltpu.make_async_copy(
            source.at[:, at * chunk : (at + 1) * chunk], right.at[j], local.at[j]
        )

    def store(j):
        p, h = j // 2, j % 2
        if p < wide:
            target, at = (gate_out, up_out)[h], p
        else:
            target, at = down_out, p - wide + h * (wide // 2)
        return pltpu.make_async_copy(
            out.at[j], target.at[:, at * chunk : (at + 1) * chunk], leave.at[j]
        )

    def fetch(k, r):
        source = (rows_in, upstream_in)[k]
        slot = (k * line + r) % 2
        return pltpu.make_async_copy(source.at[r], raw.at[slot], raw_sem.at[slot]), slot

    fetch(0, 0)[0].start()
    for j in range(count):
        load(j).start()
    greet_dp(links, d, t)

    def turn(k):
        for r in range(line):
            copy, slot = fetch(k, r)
            copy.wait()
            following = k * line + r + 1
            if following < 2 * line:
                fetch(following // line, following % line)[0].start()
            left[k, :, r * rows : (r + 1) * rows] = raw[slot].T

    engine = Scatter(
        links, d, t, block,
        (
            lambda j: odd.at[j],
            lambda j, at=pl.ds(0, middle): core.at[j, at],
            lambda j, at: sums.at[j, at],
            lambda j, number: arrived.at[j, number],
            lambda j: out.at[j],
        ),
        (
            lambda j: core_send.at[j],
            lambda j: core_recv.at[j],
            lambda j, number: send.at[j, number],
            lambda j, number: recv.at[j, number],
        ),
    )
    for j in range(count):
        load(j).wait()
    turn(0)

    def step(p, carry):
        @pl.when(p == wide // 2)
        def _():
            turn(1)

        @pl.when(p < pairs)
        def _():
            k = jnp.where(p < wide, 0, 1)
            for h in (0, 1):
                j = 2 * p + h
                for r in range(middle // 256):
                    at = pl.ds(middle + r * 256, 256)
                    odd[j, pl.ds(r * 256, 256), :] = nn(left[k, at, :], right[j]).astype(bf16)
                engine.core_copy(j).start()
            for h in (0, 1):
                j = 2 * p + h
                for r in range(middle // 256):
                    at = pl.ds(r * 256, 256)
                    value = nn(left[k, at, :], right[j])
                    sums[j, at, :] = value.astype(bf16)
                    if r == 0:
                        out[j] = value[:block]

        for stage in range(len(links.bits) + 1):
            @pl.when((p >= stage + 1) & (p < pairs + stage + 1))
            def _(stage=stage):
                for h in (0, 1):
                    engine.stage(2 * (p - stage - 1) + h, h, stage)

        return carry

    lax.fori_loop(0, pairs + len(links.bits) + 1, step, 0)
    for j in range(count):
        store(j).start()

    def finish(p, carry):
        for h in (0, 1):
            engine.finish(2 * p + h, h)
        return carry

    lax.fori_loop(0, pairs, finish, 0)
    for j in range(count):
        store(j).wait()


def feed_weights(rows_all, upstream_all, gate, up, hidden, size):
    line, rows, width = rows_all.shape
    tokens, units = gate.shape
    chunk = units // 4
    count = 3 * 4
    block = width // size
    middle = width // 2
    pieces = Scatter.pieces(Links(size))
    hbm = pl.BlockSpec(memory_space=pl.ANY)
    shape = jax.ShapeDtypeStruct
    dma = pltpu.SemaphoreType.DMA
    return pl.pallas_call(
        functools.partial(weight_kernel, size, line),
        out_shape=(shape((block, units), f32),) * 3,
        in_specs=[hbm] * 5,
        out_specs=[hbm] * 3,
        scratch_shapes=[
            pltpu.VMEM((2, rows, width), bf16),
            pltpu.VMEM((2, width, tokens), bf16),
            pltpu.VMEM((count, tokens, chunk), bf16),
            pltpu.VMEM((count, middle, chunk), bf16),
            pltpu.VMEM((count, middle, chunk), bf16),
            pltpu.VMEM((count, middle, chunk), bf16),
            pltpu.VMEM((count, pieces, block, chunk), bf16),
            pltpu.VMEM((count, block, chunk), f32),
            dma((count,)),
            dma((count,)),
            dma((count, pieces)),
            dma((count, pieces)),
            dma((count,)),
            dma((2,)),
            dma((count,)),
        ],
        compiler_params=pltpu.CompilerParams(
            collective_id=2, has_side_effects=True, vmem_limit_bytes=63 << 20
        ),
        cost_estimate=pl.CostEstimate(flops=20 << 30, bytes_accessed=60 << 20, transcendentals=0),
    )(rows_all, upstream_all, gate, up, hidden)


def body(
    layer_input,
    first_gain,
    query_weight,
    key_matrix,
    value_matrix,
    query_gain,
    key_gain,
    output_weight,
    second_gain,
    gate_weight,
    up_weight,
    down_weight,
    segments,
    cotangent,
):
    plan = Plan()
    line, place = plan.line, plan.place
    rows, seq_count, width = layer_input.shape
    head = query_gain.shape[0]
    kv_heads = key_matrix.shape[1] // head
    query_heads = query_weight.shape[1] // head
    groups = query_heads // kv_heads
    all_kv = line * kv_heads
    half = width // 2
    hops = -(-(longest_document - 1) // rows)
    assert seq_count == 1 and hops == 2
    factor = head**-0.5

    gain_one = plan.to_masks(first_gain.astype(f32))
    gain_two = plan.to_masks(second_gain.astype(f32))
    gain_query = query_gain.astype(f32)
    gain_key = key_gain.astype(f32)
    source = plan.to_masks(layer_input[:, 0, :]).astype(f32)
    upstream = plan.to_masks(cotangent[:, 0, :])

    q_cols = query_weight.shape[1]
    kv_cols = key_matrix.shape[1]
    o_half = output_weight.shape[1] // 2
    shard = jnp.stack(
        [
            jnp.concatenate([query_weight, output_weight[:, :o_half]], axis=1),
            jnp.concatenate([key_matrix, value_matrix, output_weight[:, o_half:]], axis=1),
        ]
    )
    normed, inverse_one = rms_parts(source, gain_one)
    rows_one = normed.astype(bf16)
    span = (hops + 1) * rows
    positions = (place - hops) * rows + jnp.arange(span)
    cosine, sine = rope_tables(positions, head)
    padded = jnp.concatenate([jnp.full((hops * rows,), -1, segments.dtype), segments[0]], axis=0)
    key_segments = lax.dynamic_slice(padded, (place * rows,), (span,))
    query_segments = key_segments[hops * rows :]
    mlp_shard = jnp.stack([gate_weight, up_weight])
    (
        weights, pair_full, upstream_all, proj_query, proj_key, query_rows, key_rows, value_rows, lse, attended, middle, rows_two_own,
    ) = attention_forward(
        shard, mlp_shard, rows_one, upstream, source, gain_query[None], gain_key[None], gain_two[None], cosine, sine,
        key_segments[None, :], query_segments[:, None], plan.size, line,
    )
    inverse_two = lax.rsqrt(jnp.mean(middle * middle, axis=-1, keepdims=True) + epsilon)

    hidden_half = down_weight.shape[1] // 2
    down_shard = jnp.stack([down_weight[:, :hidden_half], down_weight[:, hidden_half:]])
    rows_two, hidden, grad_gate, grad_up, grad_two_part, mixed_part = feed_forward(
        rows_two_own, upstream_all, pair_full, down_shard, plan.size, line
    )

    def unslot(values):
        return values.reshape(-1, values.shape[2])

    hidden, grad_gate, grad_up = map(unslot, (hidden, grad_gate, grad_up))
    grad_two = lax.psum_scatter(
        grad_two_part, "tensor", scatter_dimension=0, tiled=True
    ).astype(f32)
    mixed_in = after(mixed_part, grad_two)
    mixed = lax.psum_scatter(mixed_in, "tensor", scatter_dimension=0, tiled=True).astype(f32)
    layer_output = plan.from_masks((middle + mixed).astype(bf16))[:, None, :]

    def weight_term(left, right):
        return (
            mm("ld,lc->dc", left[:, :half], right).astype(bf16),
            mm("ld,lc->dc", left[:, half:], right).astype(bf16),
        )

    gate_grad, up_grad, down_grad = feed_weights(
        rows_two, upstream_all, grad_gate, grad_up, hidden, plan.size
    )

    grad_mid_norm, gain_two_terms = rms_back(middle, inverse_two, gain_two, grad_two)
    grad_middle = upstream.astype(f32) + grad_mid_norm
    grad_branch = grad_middle.astype(bf16)
    o_weights = weights[:, :, :, q_cols:]
    grad_attended = jnp.stack(
        [
            jnp.concatenate([mm("ld,dc->lc", grad_branch, o_weights[h, s]) for h in (0, 1)], axis=1)
            for s in range(line)
        ]
    ).astype(bf16)
    attended_flat = jnp.concatenate([attended[s] for s in range(line)], axis=1)
    output_cols = attended_flat.shape[1] // 2
    output_sum = jnp.concatenate(
        [
            plan.reduce(*weight_term(grad_branch, attended_flat[:, :output_cols]), plan.forward),
            plan.reduce(*weight_term(grad_branch, attended_flat[:, output_cols:]), plan.backward),
        ],
        axis=1,
    )
    output_grad = plan.scatter_line(jnp.split(output_sum, line, axis=1))

    allowed = (query_segments[:, None] == key_segments[None, :]) & (
        positions[None, :] <= positions[hops * rows :][:, None]
    )

    def heads_of(values, count):
        return values.reshape(values.shape[0], values.shape[1], -1, *count)

    grouped = heads_of(query_rows, (groups, head))
    grad_out = heads_of(grad_attended, (groups, head))
    keys = heads_of(key_rows, (head,))
    values_all = heads_of(value_rows, (head,))
    log_total = lse[:, :, :query_heads].reshape(line, rows, kv_heads, groups)
    log_total = jnp.transpose(log_total, (0, 2, 3, 1))[..., None]
    scores = jnp.where(allowed, mm("sqhgd,skhd->shgqk", grouped, keys) * factor, -1e30)
    probs32 = jnp.exp(scores - log_total)
    grad_probs = mm("sqhgd,skhd->shgqk", grad_out, values_all)
    delta = jnp.sum(probs32 * grad_probs, axis=-1, keepdims=True)
    grad_scores = (probs32 * (grad_probs - delta)).astype(bf16)
    grad_query = (mm("shgqk,skhd->sqhgd", grad_scores, keys) * factor).astype(bf16)
    grad_key_part = mm("shgqk,sqhgd->skhd", grad_scores, grouped) * factor
    grad_value_part = mm("shgqk,sqhgd->skhd", probs32.astype(bf16), grad_out)

    def flat(values):
        return jnp.concatenate([values[s].reshape(values.shape[1], -1) for s in range(line)], axis=1)

    grad_kv_part = jnp.concatenate([flat(grad_key_part), flat(grad_value_part)], axis=1)
    key_width = all_kv * head
    def turn_slots(values):
        slot = key_width // line
        return jnp.concatenate(
            [
                values[:, key_width - slot : key_width],
                values[:, : key_width - slot],
                values[:, 2 * key_width - slot :],
                values[:, key_width : 2 * key_width - slot],
            ],
            axis=1,
        )

    far = plan.move(grad_kv_part[:rows].astype(bf16), [(2, 1), (3, 2)])
    near = plan.move(
        (grad_kv_part[rows : 2 * rows] + turn_slots(far).astype(f32)).astype(bf16),
        [(1, 0), (2, 1), (3, 2)],
    )
    grad_kv = (grad_kv_part[2 * rows :] + turn_slots(near).astype(f32)).astype(bf16)
    grad_key = grad_kv[:, :key_width].reshape(rows, all_kv, head)
    grad_value_low = grad_kv[:, key_width:]

    cos_own = cosine[hops * rows :][:, None, :]
    sin_own = sine[hops * rows :][:, None, :]
    raw_query = flat(proj_query).reshape(rows, -1, head)
    raw_key = flat(proj_key).reshape(rows, -1, head)

    def head_back(raw, gain, upstream_rows):
        inverse = lax.rsqrt(jnp.mean(raw * raw, axis=-1, keepdims=True) + epsilon)
        return rms_back(raw, inverse, gain, rotate_back(upstream_rows, cos_own, sin_own))

    grad_proj_query, query_terms = head_back(
        raw_query, gain_query, flat(grad_query).reshape(rows, -1, head).astype(f32)
    )
    grad_proj_key, key_terms = head_back(raw_key, gain_key, grad_key.astype(f32))
    grad_query_low = grad_proj_query.reshape(rows, -1).astype(bf16)
    grad_key_low = grad_proj_key.reshape(rows, -1).astype(bf16)
    query_sum = plan.reduce(*weight_term(rows_one, grad_query_low), plan.forward)
    query_weight_grad = plan.scatter_line(jnp.split(query_sum, line, axis=1))
    kv_terms = [weight_term(rows_one, v) for v in (grad_key_low, grad_value_low)]
    key_sum = plan.reduce(*kv_terms[0], plan.forward)
    value_sum = plan.reduce(*kv_terms[1], plan.backward)
    kv_grad = plan.scatter_line(
        [
            jnp.concatenate([a, b], axis=1)
            for a, b in zip(jnp.split(key_sum, line, axis=1), jnp.split(value_sum, line, axis=1))
        ]
    )
    grad_one = 0.0
    for s in range(line):
        q_part = grad_query_low[:, s * q_cols : (s + 1) * q_cols]
        kv_part = jnp.concatenate(
            [
                grad_key_low[:, s * kv_cols : (s + 1) * kv_cols],
                grad_value_low[:, s * kv_cols : (s + 1) * kv_cols],
            ],
            axis=1,
        )
        grad_one = grad_one + mm("lc,dc->ld", q_part, weights[0, s, :, :q_cols])
        grad_one = grad_one + mm("lc,dc->ld", kv_part, weights[1, s, :, : 2 * kv_cols])
    grad_src_norm, gain_one_terms = rms_back(source, inverse_one, gain_one, grad_one)
    input_grad = plan.from_masks((grad_middle + grad_src_norm).astype(bf16))[:, None, :]

    gains = plan.total(
        jnp.concatenate(
            [
                plan.from_masks(jnp.sum(gain_one_terms, axis=0)),
                plan.from_masks(jnp.sum(gain_two_terms, axis=0)),
                jnp.sum(query_terms, axis=(0, 1)),
                jnp.sum(key_terms, axis=(0, 1)),
            ]
        )
    )
    return (
        layer_output,
        input_grad,
        gains[:width],
        query_weight_grad,
        kv_grad[:, :kv_cols],
        kv_grad[:, kv_cols:],
        gains[2 * width : 2 * width + head],
        gains[2 * width + head :],
        output_grad,
        gains[width : 2 * width],
        gate_grad,
        up_grad,
        down_grad,
    )


def solution(mesh):
    positions = P("tensor", "dp", None)
    weight = P("dp", "tensor")
    return jax.shard_map(
        body,
        mesh=mesh,
        in_specs=(
            positions,
            P(),
            weight,
            weight,
            weight,
            P(),
            P(),
            weight,
            P(),
            weight,
            weight,
            weight,
            P("dp", None),
            positions,
        ),
        out_specs=(
            positions,
            positions,
            P(),
            weight,
            weight,
            weight,
            P(),
            P(),
            weight,
            P(),
            weight,
            weight,
            weight,
        ),
        check_vma=False,
    )
```

```python
import functools

import jax
import jax.numpy as jnp
from jax import lax
from jax.experimental import pallas as pl
from jax.experimental.pallas import tpu as pltpu
from jax.sharding import PartitionSpec as P

epsilon = 1e-06
rope_base = 1000000.0
longest_document = 512
bf16 = jnp.bfloat16
f32 = jnp.float32


def mm(eq, a, b):
    return jnp.einsum(eq, a, b, preferred_element_type=f32)


def rms_parts(values, gain):
    inverse = lax.rsqrt(jnp.mean(values * values, axis=-1, keepdims=True) + epsilon)
    return values * inverse * gain, inverse


def rms_back(values, inverse, gain, upstream):
    normed = values * inverse
    inner = upstream * gain
    grad = inverse * (inner - normed * jnp.mean(inner * normed, axis=-1, keepdims=True))
    return grad, upstream * normed


def rope_tables(positions, head_size):
    half = head_size // 2
    frequency = rope_base ** (-(2.0 * jnp.arange(half, dtype=f32)) / head_size)
    angles = positions.astype(f32)[:, None] * frequency[None, :]
    sine = jnp.sin(angles)
    return (
        jnp.concatenate([jnp.cos(angles)] * 2, axis=1),
        jnp.concatenate([-sine, sine], axis=1),
    )


def rotate_back(upstream, cosine, sine):
    half = upstream.shape[-1] // 2
    shifted = upstream * sine
    return upstream * cosine + jnp.concatenate(
        [shifted[..., half:], shifted[..., :half]], axis=-1
    )


class Plan:
    def __init__(self):
        self.size = lax.axis_size("dp")
        self.index = lax.axis_index("dp")
        self.place = lax.axis_index("tensor")
        self.line = lax.axis_size("tensor")
        assert self.line == 4
        self.others = [1 << i for i in range(1, self.size.bit_length() - 1)]
        evens = [0]
        for bit in self.others:
            evens = evens + [m ^ bit for m in evens]
        self.evens = evens
        self.masks = evens + [m ^ 1 for m in evens]
        self.forward = self.others
        self.backward = self.others[::-1]

    def swap(self, value, bit):
        return lax.ppermute(value, "dp", [(i, i ^ bit) for i in range(self.size)])

    def move(self, value, pairs):
        return lax.ppermute(value, "tensor", pairs)

    def xor_blocks(self, blocks):
        bit = 1
        while bit < self.size:
            on = (self.index & bit) != 0
            blocks = [jnp.where(on, blocks[i ^ bit], blocks[i]) for i in range(self.size)]
            bit *= 2
        return blocks

    def to_masks(self, value):
        blocks = self.xor_blocks(jnp.split(value, self.size, axis=-1))
        return jnp.concatenate([blocks[m] for m in self.masks], axis=-1)

    def from_masks(self, value):
        parts = jnp.split(value, self.size, axis=-1)
        blocks = [parts[self.masks.index(m)] for m in range(self.size)]
        return jnp.concatenate(self.xor_blocks(blocks), axis=-1)

    def gather(self, shard, order):
        rows = shard.shape[0]
        held, masks = shard, [0]
        for bit in order:
            arrived = self.swap(held, bit)
            held = jnp.concatenate([held, arrived], axis=0)
            masks = masks + [m ^ bit for m in masks]
        if masks != self.evens:
            held = jnp.concatenate(
                [lax.slice_in_dim(held, masks.index(m) * rows, (masks.index(m) + 1) * rows) for m in self.evens],
                axis=0,
            )
        return held, self.swap(held, 1)

    def reduce(self, even, odd, order):
        rows = even.shape[0] // len(self.evens)
        total = even.astype(f32) + self.swap(odd.astype(bf16), 1).astype(f32)
        pieces = {
            m: lax.slice_in_dim(total, i * rows, (i + 1) * rows) for i, m in enumerate(self.evens)
        }
        for bit in order:
            leaving = [m for m in pieces if m & bit]
            sent = jnp.concatenate([pieces[m].astype(bf16) for m in leaving], axis=0)
            arrived = self.swap(sent, bit)
            kept = {m: v for m, v in pieces.items() if not m & bit}
            for i, m in enumerate(leaving):
                kept[m ^ bit] = kept[m ^ bit] + lax.slice_in_dim(
                    arrived, i * rows, (i + 1) * rows
                ).astype(f32)
            pieces = kept
        return pieces[0]

    def gather_line(self, own):
        from_right = self.move(own, [(1, 0), (2, 1), (3, 2)])
        from_left = self.move(own, [(0, 1), (1, 2), (2, 3)])
        right_two = self.move(from_right, [(1, 0), (2, 1)])
        left_two = self.move(from_left, [(1, 2), (2, 3)])
        slot_two = jnp.where(self.place < 2, right_two, left_two)
        last = self.move(slot_two, [(1, 0), (2, 3)])
        slot_one = jnp.where(self.place < 3, from_right, last)
        slot_three = jnp.where(self.place > 0, from_left, last)
        return [own, slot_one, slot_two, slot_three]

    def scatter_line(self, slots):
        zero, one, two, three = slots
        first = self.move(
            jnp.where(self.place == 3, one, three).astype(bf16), [(3, 2), (0, 1)]
        )
        middle = (two + first.astype(f32)).astype(bf16)
        leftward = self.move(middle, [(3, 2), (2, 1)])
        rightward = self.move(middle, [(0, 1), (1, 2)])
        leftward = self.move(
            (three + leftward.astype(f32)).astype(bf16), [(3, 2), (2, 1), (1, 0)]
        )
        rightward = self.move(
            (one + rightward.astype(f32)).astype(bf16), [(0, 1), (1, 2), (2, 3)]
        )
        return zero + leftward.astype(f32) + rightward.astype(f32)

    def total(self, value):
        bit = 1
        while bit < self.size:
            value = value + self.swap(value, bit)
            bit *= 2
        for bit in (1, 2):
            value = value + self.move(value, [(i, i ^ bit) for i in range(self.line)])
        return value


def after(value, *others):
    return lax.optimization_barrier((value,) + others)[0]


def mesh_copy(src, dst, send, recv, device):
    return pltpu.make_async_remote_copy(
        src_ref=src, dst_ref=dst, send_sem=send, recv_sem=recv, device_id=device,
        device_id_type=pl.DeviceIdType.MESH,
    )


class Links:
    def __init__(self, size):
        bits = [1 << i for i in range(1, size.bit_length() - 1)]
        self.orders = (bits, bits[::-1])
        evens = [0]
        for bit in bits:
            evens = evens + [m ^ bit for m in evens]
        self.evens = evens
        self.masks = evens + [m ^ 1 for m in evens]
        self.bits = bits

    def onward(self, half, mask):
        order = self.orders[half]
        last = max([i for i, bit in enumerate(order) if mask & bit], default=-1)
        return order[last + 1 :]


class Gather:
    def __init__(self, links, d, t, piece, send, recv):
        self.links, self.d, self.t = links, d, t
        self.piece, self.send, self.recv = piece, send, recv

    def copy(self, half, mask, bit):
        index = self.links.masks.index(mask ^ bit)
        return mesh_copy(
            self.piece(half, mask), self.piece(half, mask ^ bit), self.send(half, index),
            self.recv(half, index), (self.d ^ bit, self.t),
        )

    def launch(self):
        for step in range(len(self.links.bits)):
            for half in (0, 1):
                self.copy(half, 0, self.links.orders[half][step]).start()
        for half in (0, 1):
            self.copy(half, 0, 1).start()

    def arrive(self, half, mask):
        bit = [b for b in self.links.orders[half] if b & mask][-1]
        self.copy(half, mask ^ bit, bit).wait_recv()
        for other in self.links.onward(half, mask):
            self.copy(half, mask, other).start()
        self.copy(half, mask, 1).start()

    def onward(self):
        for mask in self.links.evens[1:]:
            for half in (0, 1):
                if self.links.onward(half, mask):
                    self.arrive(half, mask)

    def complete(self):
        for mask in self.links.evens[1:]:
            for half in (0, 1):
                if not self.links.onward(half, mask):
                    self.arrive(half, mask)
        for mask in self.links.evens:
            for half in (0, 1):
                self.copy(half, mask, 1).wait_recv()

    def finish(self):
        for mask in self.links.masks[1:]:
            for half in (0, 1):
                self.copy(half, mask ^ 1 if mask & 1 else 0, 1 if mask & 1 else mask).wait_send()


class Relay:
    def __init__(self, d, t, line, slot, send, recv):
        self.d, self.t, self.line = d, t, line
        self.slot, self.send, self.recv = slot, send, recv
        self.inner = (t > 0) & (t < line - 1)

    def copy(self, number, source, target, to):
        return mesh_copy(
            self.slot(source), self.slot(target), self.send.at[number], self.recv.at[target],
            (self.d, to),
        )

    def moves(self):
        t = self.t
        return (
            (t > 0, (0, 0, 1, t - 1)),
            (t < self.line - 1, (1, 0, 3, t + 1)),
            (self.inner, (2, 1, 2, t - 1)),
            (self.inner, (3, 3, 2, t + 1)),
            (t == 1, (4, 2, 3, t - 1)),
            (t == 2, (5, 2, 1, t + 1)),
        )

    def start(self, *numbers):
        for number in numbers:
            condition, route = self.moves()[number]

            @pl.when(condition)
            def _(route=route):
                self.copy(*route).start()

    def wait(self, slot):
        self.copy(0, 0, slot, self.t).wait_recv()

    def finish(self):
        for condition, route in self.moves():

            @pl.when(condition)
            def _(route=route):
                self.copy(*route).wait_send()

    def first(self):
        self.start(0, 1)

    def second(self):
        t, line = self.t, self.line

        @pl.when(t < line - 1)
        def _():
            self.wait(1)

        self.start(2)

        @pl.when(t > 0)
        def _():
            self.wait(3)

        self.start(3)

    def third(self):
        self.wait(2)
        self.start(4, 5)

    def ends(self):
        @pl.when(self.t == 0)
        def _():
            self.wait(3)

        @pl.when(self.t == self.line - 1)
        def _():
            self.wait(1)


def slot_of(i, t, line):
    far = jnp.where(t < line - 1, 1, 3)
    near = jnp.where(t < line - 1, 3, 1)
    return jnp.where(i == 0, 0, jnp.where(i == 1, far, jnp.where(i == 2, 2, near)))


def greet(links, d, t, line):
    barrier = pltpu.get_barrier_semaphore()
    for bit in [1] + links.bits:
        pl.semaphore_signal(barrier, inc=1, device_id=(d ^ bit, t), device_id_type=pl.DeviceIdType.MESH)

    @pl.when(t > 0)
    def _():
        pl.semaphore_signal(barrier, inc=1, device_id=(d, t - 1), device_id_type=pl.DeviceIdType.MESH)

    @pl.when(t < line - 1)
    def _():
        pl.semaphore_signal(barrier, inc=1, device_id=(d, t + 1), device_id_type=pl.DeviceIdType.MESH)

    pl.semaphore_wait(
        barrier,
        1 + len(links.bits) + jnp.where(t > 0, 1, 0) + jnp.where(t < line - 1, 1, 0),
    )


def nt(a, b):
    return lax.dot_general(a, b, (((1,), (1,)), ((), ())), preferred_element_type=f32)


def tn(a, b):
    return lax.dot_general(a, b, (((0,), (0,)), ((), ())), preferred_element_type=f32)


def nn(a, b):
    return jnp.dot(a, b, preferred_element_type=f32)


def head_norm(values, gain):
    inverse = lax.rsqrt(jnp.mean(values * values, axis=-1, keepdims=True) + epsilon)
    return values * inverse * gain


def forward_kernel(
    size, line, head,
    shard, mlp_shard, rows_in, upstream, source, gain_q, gain_k, gain_two, cosine, sine, key_seg, query_seg,
    weights_out, mlp_out, upstream_all, proj_q, proj_k, q_out, k_out, v_out, lse_out, att_out, middle, normed_out,
    full, rows_all, acc,
    z_send, z_recv, send, recv, row_send, row_recv, keep, mlp_send, mlp_recv, up_send, up_recv, local,
):
    links = Links(size)
    d, t = lax.axis_index("dp"), lax.axis_index("tensor")
    block = shard.shape[1]
    rows, width = rows_in.shape
    span = rows_all.shape[0]
    factor = head**-0.5

    def place(mask):
        return pl.ds(links.masks.index(mask) * block, block)

    def gather(slot):
        return Gather(
            links, d, t,
            lambda half, mask: full.at[half, slot, place(mask)],
            lambda half, index: send.at[slot, half, index],
            lambda half, index: recv.at[slot, half, index],
        )

    feed = Gather(
        links, d, t,
        lambda half, mask: mlp_out.at[half, place(mask)],
        lambda half, index: mlp_send.at[half, index],
        lambda half, index: mlp_recv.at[half, index],
    )
    relay = Relay(d, t, line, lambda slot: full.at[:, slot, place(0)], z_send, z_recv)
    upward = Relay(d, t, line, lambda slot: upstream_all.at[slot], up_send, up_recv)

    own = (
        pltpu.make_async_copy(shard, full.at[:, 0, place(0)], local.at[0]),
        pltpu.make_async_copy(mlp_shard, mlp_out.at[:, place(0)], local.at[1]),
        pltpu.make_async_copy(upstream, upstream_all.at[0], local.at[2]),
    )
    for copy in own:
        copy.start()
    rows_all[pl.ds(span - rows, rows), :] = rows_in[...]

    @pl.when(t == 0)
    def _():
        rows_all[pl.ds(0, 2 * rows), :] = jnp.zeros((2 * rows, width), bf16)

    @pl.when(t == 1)
    def _():
        rows_all[pl.ds(0, rows), :] = jnp.zeros((rows, width), bf16)

    greet(links, d, t, line)
    own[0].wait()

    row_one = mesh_copy(
        rows_in, rows_all.at[pl.ds(rows, rows)], row_send.at[0], row_recv.at[0], (d, t + 1)
    )
    row_two = mesh_copy(
        rows_all.at[pl.ds(rows, rows)], rows_all.at[pl.ds(0, rows)], row_send.at[1],
        row_recv.at[1], (d, t + 1),
    )
    inner = relay.inner
    relay.first()

    @pl.when(t < line - 1)
    def _():
        row_one.start()

    gather(0).launch()
    gather(0).onward()
    relay.second()
    second = slot_of(1, t, line)

    @pl.when(t < line - 1)
    def _():
        gather(1).launch()

    @pl.when(t == line - 1)
    def _():
        gather(3).launch()

    @pl.when(t > 0)
    def _():
        row_one.wait_recv()

    @pl.when(inner)
    def _():
        row_two.start()

    relay.third()
    gather(2).launch()
    gather(second).onward()

    @pl.when(t > 1)
    def _():
        row_two.wait_recv()

    own[1].wait()
    own[2].wait()
    acc[...] = source[...]

    lane = lax.broadcasted_iota(jnp.int32, (rows, 128), 1)
    q_index = lax.broadcasted_iota(jnp.int32, (rows, span), 0) + (span - rows)
    k_index = lax.broadcasted_iota(jnp.int32, (rows, span), 1)

    def step(i, carry):
        slot = slot_of(i, t, line)

        @pl.when(i == 1)
        def _():
            relay.ends()
            gather(slot_of(3, t, line)).launch()
            upward.first()

        @pl.when(i >= 2)
        def _():
            gather(slot).onward()

        @pl.when(i == 3)
        def _():
            feed.launch()

        gather(slot).complete()
        for half in (0, 1):
            pltpu.make_async_copy(
                full.at[half, slot], weights_out.at[half, slot], keep.at[slot, half]
            ).start()

        own_rows = pl.ds(span - rows, rows)
        allowed = (query_seg[...] == key_seg[...]) & (k_index <= q_index)
        lse_acc = jnp.zeros((rows, 128), f32)
        for g in (0, 1):
            key_cols = slice(g * head, (g + 1) * head)
            if g == 0:
                for r in range(span // rows):
                    part = pl.ds(r * rows, rows)
                    both = nn(rows_all[part, :], full[1, slot, :, 0 : 4 * head])
                    if r == span // rows - 1:
                        proj_k[slot] = both[:, : 2 * head]
                    for h in (0, 1):
                        unit = head_norm(both[:, h * head : (h + 1) * head], gain_k[...])
                        turned = unit * cosine[part, :] + pltpu.roll(unit, head // 2, 1) * sine[part, :]
                        k_out[slot, part, h * head : (h + 1) * head] = turned.astype(bf16)
                    v_out[slot, part, :] = both[:, 2 * head :].astype(bf16)
            for j in (0, 1):
                h = 2 * g + j
                cols = slice(h * head, (h + 1) * head)
                raw = nn(rows_in[...], full[0, slot, :, cols])
                proj_q[slot, :, cols] = raw
                unit = head_norm(raw, gain_q[...])
                turned = unit * cosine[own_rows, :] + pltpu.roll(unit, head // 2, 1) * sine[own_rows, :]
                query = turned.astype(bf16)
                q_out[slot, :, cols] = query
                scores = nt(query, k_out[slot, :, key_cols]) * factor
                scores = jnp.where(allowed, scores, -1e30)
                top = jnp.max(scores, axis=-1, keepdims=True)
                weight = jnp.exp(scores - top)
                total = jnp.sum(weight, axis=-1, keepdims=True)
                probs = (weight / total).astype(bf16)
                att_out[slot, :, cols] = nn(probs, v_out[slot, :, key_cols]).astype(bf16)
                lse_acc = jnp.where(lane == h, top + jnp.log(total), lse_acc)
        lse_out[slot] = lse_acc
        for half in (0, 1):
            acc[...] += nt(
                att_out[slot, :, half * 2 * head : (half + 1) * 2 * head],
                full[half, slot, :, 4 * head : 6 * head],
            )
        return carry

    lax.fori_loop(0, line, step, 0)
    upward.second()
    feed.onward()
    values = acc[...]
    middle[...] = values
    normed_out[...] = head_norm(values, gain_two[...]).astype(bf16)
    upward.third()
    feed.complete()

    def finish(i, carry):
        gather(i).finish()
        for half in (0, 1):
            pltpu.make_async_copy(full.at[half, i], weights_out.at[half, i], keep.at[i, half]).wait()
        return carry

    lax.fori_loop(0, line, finish, 0)
    feed.finish()
    relay.finish()

    @pl.when(t < line - 1)
    def _():
        row_one.wait_send()

    @pl.when(inner)
    def _():
        row_two.wait_send()

    upward.ends()
    upward.finish()


def attention_forward(shard, mlp_shard, rows_one, upstream, source, gain_q, gain_k, gain_two, cosine, sine, key_seg, query_seg, size, line):
    _, block, cols = shard.shape
    rows, width = rows_one.shape
    span = cosine.shape[0]
    head = gain_q.shape[1]
    pieces = 2 * (size // 2)
    vmem = pl.BlockSpec(memory_space=pltpu.VMEM)
    hbm = pl.BlockSpec(memory_space=pl.ANY)
    shape = jax.ShapeDtypeStruct
    return pl.pallas_call(
        functools.partial(forward_kernel, size, line, head),
        out_shape=(
            shape((2, line, width, cols), bf16),
            shape((2, width, mlp_shard.shape[2]), bf16),
            shape((line, rows, width), bf16),
            shape((line, rows, 4 * head), f32),
            shape((line, rows, 2 * head), f32),
            shape((line, rows, 4 * head), bf16),
            shape((line, span, 2 * head), bf16),
            shape((line, span, 2 * head), bf16),
            shape((line, rows, 128), f32),
            shape((line, rows, 4 * head), bf16),
            shape((rows, width), f32),
            shape((rows, width), bf16),
        ),
        in_specs=[hbm, hbm, vmem, hbm] + [vmem] * 8,
        out_specs=[hbm] * 3 + [vmem] * 9,
        scratch_shapes=[
            pltpu.VMEM((2, line, width, cols), bf16),
            pltpu.VMEM((span, width), bf16),
            pltpu.VMEM((rows, width), f32),
            pltpu.SemaphoreType.DMA((6,)),
            pltpu.SemaphoreType.DMA((line,)),
            pltpu.SemaphoreType.DMA((line, 2, pieces)),
            pltpu.SemaphoreType.DMA((line, 2, pieces)),
            pltpu.SemaphoreType.DMA((2,)),
            pltpu.SemaphoreType.DMA((2,)),
            pltpu.SemaphoreType.DMA((line, 2)),
            pltpu.SemaphoreType.DMA((2, pieces)),
            pltpu.SemaphoreType.DMA((2, pieces)),
            pltpu.SemaphoreType.DMA((6,)),
            pltpu.SemaphoreType.DMA((line,)),
            pltpu.SemaphoreType.DMA((3,)),
        ],
        compiler_params=pltpu.CompilerParams(
            collective_id=0, has_side_effects=True, vmem_limit_bytes=62 << 20
        ),
        cost_estimate=pl.CostEstimate(flops=40 << 30, bytes_accessed=200 << 20, transcendentals=4 << 20),
    )(shard, mlp_shard, rows_one, upstream, source, gain_q, gain_k, gain_two, cosine, sine, key_seg, query_seg)


def feed_kernel(
    size, line,
    rows_in, upstream_in, pair_in, down_in,
    rows_out, hidden_out, gate_out, up_out, grad_out, mixed_out,
    rows_v, upstream_v, pair, down, gate_f, up_f, hidden_v, gate_v, up_v, grad_v, mixed_v,
    z_send, z_recv, send, recv, local, leave,
):
    links = Links(size)
    d, t = lax.axis_index("dp"), lax.axis_index("tensor")
    block = down_in.shape[1]
    _, rows, width = rows_v.shape
    units = hidden_v.shape[2]
    chunk = units // 4
    piece = width // 4

    def place(mask):
        return pl.ds(links.masks.index(mask) * block, block)

    gather = Gather(
        links, d, t,
        lambda half, mask: down.at[half, place(mask)],
        lambda half, index: send.at[half, index],
        lambda half, index: recv.at[half, index],
    )
    relay = Relay(d, t, line, lambda slot: rows_v.at[slot], z_send, z_recv)
    arrivals = (
        pltpu.make_async_copy(rows_in, rows_v.at[0], local.at[0]),
        pltpu.make_async_copy(down_in, down.at[:, place(0)], local.at[1]),
        pltpu.make_async_copy(pair_in, pair, local.at[2]),
        pltpu.make_async_copy(upstream_in, upstream_v, local.at[3]),
    )
    for copy in arrivals:
        copy.start()
    greet(links, d, t, line)
    arrivals[0].wait()
    relay.first()
    arrivals[1].wait()
    gather.launch()
    gather.onward()
    arrivals[2].wait()
    arrivals[3].wait()

    def departures(slot):
        position = lax.rem(slot + t, line)
        natural = pl.ds(pl.multiple_of(position * rows, rows), rows)
        return [
            pltpu.make_async_copy(rows_v.at[slot], rows_out.at[slot], leave.at[0, slot]),
            pltpu.make_async_copy(hidden_v.at[slot], hidden_out.at[slot], leave.at[1, slot]),
            pltpu.make_async_copy(gate_v.at[slot], gate_out.at[slot], leave.at[2, slot]),
            pltpu.make_async_copy(up_v.at[slot], up_out.at[slot], leave.at[3, slot]),
            pltpu.make_async_copy(grad_v.at[slot], grad_out.at[natural], leave.at[4, slot]),
            pltpu.make_async_copy(mixed_v.at[slot], mixed_out.at[natural], leave.at[5, slot]),
        ]

    def step(i, carry):
        slot = slot_of(i, t, line)
        for c in range(4):
            cols = slice(c * chunk, (c + 1) * chunk)
            gate = nn(rows_v[slot], pair[0, :, cols])
            up = nn(rows_v[slot], pair[1, :, cols])
            gate_f[:, cols] = gate
            up_f[:, cols] = up
            hidden_v[slot, :, cols] = (gate * jax.nn.sigmoid(gate) * up).astype(bf16)

        @pl.when(i == 0)
        def _():
            relay.second()
            gather.complete()

        @pl.when(i == 1)
        def _():
            relay.third()

        @pl.when(i == 2)
        def _():
            relay.ends()

        for c in range(4):
            cols = slice(c * chunk, (c + 1) * chunk)
            inner = slice((c % 2) * chunk, (c % 2 + 1) * chunk)
            grad_hidden = nn(upstream_v[slot], down[c // 2, :, inner])
            gate, up = gate_f[:, cols], up_f[:, cols]
            sigmoid = jax.nn.sigmoid(gate)
            gate_v[slot, :, cols] = (
                grad_hidden * up * sigmoid * (1.0 + gate * (1.0 - sigmoid))
            ).astype(bf16)
            up_v[slot, :, cols] = (grad_hidden * (gate * sigmoid)).astype(bf16)
        for n in range(4):
            out = slice(n * piece, (n + 1) * piece)
            grad_v[slot, :, out] = (
                nt(gate_v[slot], pair[0, out, :]) + nt(up_v[slot], pair[1, out, :])
            ).astype(bf16)
            mixed_v[slot, :, out] = (
                nt(hidden_v[slot, :, : units // 2], down[0, out, :])
                + nt(hidden_v[slot, :, units // 2 :], down[1, out, :])
            ).astype(bf16)
        for copy in departures(slot):
            copy.start()
        return carry

    lax.fori_loop(0, line, step, 0)

    def finish(i, carry):
        for copy in departures(i):
            copy.wait()
        return carry

    lax.fori_loop(0, line, finish, 0)
    gather.finish()
    relay.finish()


def feed_forward(rows_own, upstream_all, pair_full, down_shard, size, line):
    rows, width = rows_own.shape
    units = pair_full.shape[2]
    hbm = pl.BlockSpec(memory_space=pl.ANY)
    shape = jax.ShapeDtypeStruct
    dma = pltpu.SemaphoreType.DMA
    return pl.pallas_call(
        functools.partial(feed_kernel, size, line),
        out_shape=(
            shape((line, rows, width), bf16),
            shape((line, rows, units), bf16),
            shape((line, rows, units), bf16),
            shape((line, rows, units), bf16),
            shape((line * rows, width), bf16),
            shape((line * rows, width), bf16),
        ),
        in_specs=[hbm] * 4,
        out_specs=[hbm] * 6,
        scratch_shapes=[
            pltpu.VMEM((line, rows, width), bf16),
            pltpu.VMEM((line, rows, width), bf16),
            pltpu.VMEM((2, width, units), bf16),
            pltpu.VMEM((2, width, units // 2), bf16),
            pltpu.VMEM((rows, units), f32),
            pltpu.VMEM((rows, units), f32),
            pltpu.VMEM((line, rows, units), bf16),
            pltpu.VMEM((line, rows, units), bf16),
            pltpu.VMEM((line, rows, units), bf16),
            pltpu.VMEM((line, rows, width), bf16),
            pltpu.VMEM((line, rows, width), bf16),
            dma((6,)),
            dma((line,)),
            dma((2, size)),
            dma((2, size)),
            dma((4,)),
            dma((6, line)),
        ],
        compiler_params=pltpu.CompilerParams(
            collective_id=1, has_side_effects=True, vmem_limit_bytes=62 << 20
        ),
        cost_estimate=pl.CostEstimate(flops=40 << 30, bytes_accessed=60 << 20, transcendentals=3 << 20),
    )(rows_own, upstream_all, pair_full, down_shard)


class Scatter:
    def __init__(self, links, d, t, block, refs, semaphores):
        self.links, self.d, self.t, self.block = links, d, t, block
        self.odd, self.core, self.sums, self.arrived, self.out = refs
        self.core_send, self.core_recv, self.send, self.recv = semaphores

    @staticmethod
    def pieces(links):
        return max(1, len(links.evens) - 1)

    def steps(self, half):
        masks, number, found = self.links.evens, 0, []
        for bit in self.links.orders[half][::-1]:
            masks = [m for m in masks if not m & bit]
            found.append((bit, [(m, number + i) for i, m in enumerate(masks)]))
            number += len(masks)
        return found

    def rows(self, mask):
        return pl.ds(self.links.evens.index(mask) * self.block, self.block)

    def core_copy(self, j):
        return mesh_copy(
            self.odd(j), self.core(j), self.core_send(j), self.core_recv(j), (self.d ^ 1, self.t)
        )

    def piece_copy(self, j, mask, number, bit):
        return mesh_copy(
            self.sums(j, self.rows(mask ^ bit)), self.arrived(j, number), self.send(j, number),
            self.recv(j, number), (self.d ^ bit, self.t),
        )

    def launch(self, j, half, step):
        steps = self.steps(half)
        if step < len(steps):
            bit, pairs = steps[step]
            for mask, number in pairs:
                self.piece_copy(j, mask, number, bit).start()

    def add(self, j, mask, value):
        if mask == 0:
            out = self.out(j)
            out[...] = out[...] + value[...].astype(f32)
        else:
            total = self.sums(j, self.rows(mask))
            total[...] = (total[...].astype(f32) + value[...].astype(f32)).astype(bf16)

    def stage(self, j, half, stage):
        if stage == 0:
            self.core_copy(j).wait_recv()
            steps = self.steps(half)
            first = steps[0][0] if steps else 0
            for mask in sorted(self.links.evens, key=lambda m: not m & first):
                self.add(j, mask, self.core(j, self.rows(mask)))
        else:
            bit, pairs = self.steps(half)[stage - 1]
            for mask, number in pairs[::-1]:
                self.piece_copy(j, mask, number, bit).wait_recv()
                self.add(j, mask, self.arrived(j, number))
        self.launch(j, half, stage)

    def finish(self, j, half):
        self.core_copy(j).wait_send()
        for bit, pairs in self.steps(half):
            for mask, number in pairs:
                self.piece_copy(j, mask, number, bit).wait_send()


def greet_dp(links, d, t):
    barrier = pltpu.get_barrier_semaphore()
    for bit in [1] + links.bits:
        pl.semaphore_signal(barrier, inc=1, device_id=(d ^ bit, t), device_id_type=pl.DeviceIdType.MESH)
    pl.semaphore_wait(barrier, 1 + len(links.bits))


def weight_kernel(
    size, line,
    rows_in, upstream_in, gate_in, up_in, hidden_in,
    gate_out, up_out, down_out,
    raw, left, right, odd, core, sums, arrived, out,
    core_send, core_recv, send, recv, local, raw_sem, leave,
):
    links = Links(size)
    d, t = lax.axis_index("dp"), lax.axis_index("tensor")
    width = left.shape[1]
    rows = raw.shape[1]
    count, tokens, chunk = right.shape
    middle = width // 2
    block = out.shape[1]
    pairs = count // 2
    wide = gate_in.shape[1] // chunk

    def load(j):
        p, h = j // 2, j % 2
        if p < wide:
            source, at = (gate_in, up_in)[h], p
        else:
            source, at = hidden_in, p - wide + h * (wide // 2)
        return pltpu.make_async_copy(
            source.at[:, at * chunk : (at + 1) * chunk], right.at[j], local.at[j]
        )

    def store(j):
        p, h = j // 2, j % 2
        if p < wide:
            target, at = (gate_out, up_out)[h], p
        else:
            target, at = down_out, p - wide + h * (wide // 2)
        return pltpu.make_async_copy(
            out.at[j], target.at[:, at * chunk : (at + 1) * chunk], leave.at[j]
        )

    def fetch(k, r):
        source = (rows_in, upstream_in)[k]
        slot = (k * line + r) % 2
        return pltpu.make_async_copy(source.at[r], raw.at[slot], raw_sem.at[slot]), slot

    fetch(0, 0)[0].start()
    for j in range(count):
        load(j).start()
    greet_dp(links, d, t)

    def turn(k):
        for r in range(line):
            copy, slot = fetch(k, r)
            copy.wait()
            following = k * line + r + 1
            if following < 2 * line:
                fetch(following // line, following % line)[0].start()
            left[k, :, r * rows : (r + 1) * rows] = raw[slot].T

    engine = Scatter(
        links, d, t, block,
        (
            lambda j: odd.at[j],
            lambda j, at=pl.ds(0, middle): core.at[j, at],
            lambda j, at: sums.at[j, at],
            lambda j, number: arrived.at[j, number],
            lambda j: out.at[j],
        ),
        (
            lambda j: core_send.at[j],
            lambda j: core_recv.at[j],
            lambda j, number: send.at[j, number],
            lambda j, number: recv.at[j, number],
        ),
    )
    for j in range(count):
        load(j).wait()
    turn(0)

    def step(p, carry):
        @pl.when(p == wide // 2)
        def _():
            turn(1)

        @pl.when(p < pairs)
        def _():
            k = jnp.where(p < wide, 0, 1)
            for h in (0, 1):
                j = 2 * p + h
                for r in range(middle // 256):
                    at = pl.ds(middle + r * 256, 256)
                    odd[j, pl.ds(r * 256, 256), :] = nn(left[k, at, :], right[j]).astype(bf16)
                engine.core_copy(j).start()
            for h in (0, 1):
                j = 2 * p + h
                for r in range(middle // 256):
                    at = pl.ds(r * 256, 256)
                    value = nn(left[k, at, :], right[j])
                    sums[j, at, :] = value.astype(bf16)
                    if r == 0:
                        out[j] = value[:block]

        for stage in range(len(links.bits) + 1):
            @pl.when((p >= stage + 1) & (p < pairs + stage + 1))
            def _(stage=stage):
                for h in (0, 1):
                    engine.stage(2 * (p - stage - 1) + h, h, stage)

        return carry

    lax.fori_loop(0, pairs + len(links.bits) + 1, step, 0)
    for j in range(count):
        store(j).start()

    def finish(p, carry):
        for h in (0, 1):
            engine.finish(2 * p + h, h)
        return carry

    lax.fori_loop(0, pairs, finish, 0)
    for j in range(count):
        store(j).wait()


def feed_weights(rows_all, upstream_all, gate, up, hidden, size):
    line, rows, width = rows_all.shape
    tokens, units = gate.shape
    chunk = units // 4
    count = 3 * 4
    block = width // size
    middle = width // 2
    pieces = Scatter.pieces(Links(size))
    hbm = pl.BlockSpec(memory_space=pl.ANY)
    shape = jax.ShapeDtypeStruct
    dma = pltpu.SemaphoreType.DMA
    return pl.pallas_call(
        functools.partial(weight_kernel, size, line),
        out_shape=(shape((block, units), f32),) * 3,
        in_specs=[hbm] * 5,
        out_specs=[hbm] * 3,
        scratch_shapes=[
            pltpu.VMEM((2, rows, width), bf16),
            pltpu.VMEM((2, width, tokens), bf16),
            pltpu.VMEM((count, tokens, chunk), bf16),
            pltpu.VMEM((count, middle, chunk), bf16),
            pltpu.VMEM((count, middle, chunk), bf16),
            pltpu.VMEM((count, middle, chunk), bf16),
            pltpu.VMEM((count, pieces, block, chunk), bf16),
            pltpu.VMEM((count, block, chunk), f32),
            dma((count,)),
            dma((count,)),
            dma((count, pieces)),
            dma((count, pieces)),
            dma((count,)),
            dma((2,)),
            dma((count,)),
        ],
        compiler_params=pltpu.CompilerParams(
            collective_id=2, has_side_effects=True, vmem_limit_bytes=63 << 20
        ),
        cost_estimate=pl.CostEstimate(flops=20 << 30, bytes_accessed=60 << 20, transcendentals=0),
    )(rows_all, upstream_all, gate, up, hidden)


def spread_stages(engine, links, first, last, p):
    for stage in range(len(links.bits) + 1)[::-1]:
        @pl.when((p - stage >= first) & (p - stage < last))
        def _(stage=stage):
            for h in (0, 1):
                engine.stage(2 * (p - stage) + h, h, stage)


def backward_kernel(
    size, line, head,
    branch, weights, q_in, k_in, v_in, lse_in, att_in, proj_q, proj_k, gain_q, gain_k, cosine, sine,
    key_seg, query_seg,
    gq_out, gkv_out, terms_out, o_out,
    o_full, branch_t, gatt, own_kv, near_f, far_v, near_v, far_in, near_in, odd, core, sums, arrived, out,
    core_send, core_recv, send, recv, far_send, far_recv, near_send, near_recv, local,
):
    links = Links(size)
    d, t = lax.axis_index("dp"), lax.axis_index("tensor")
    rows, width = branch.shape
    span = k_in.shape[1]
    middle = width // 2
    block = out.shape[1]
    factor = head**-0.5
    loads = [
        pltpu.make_async_copy(
            weights.at[h, s, :, 4 * head : 6 * head], o_full.at[s, h], local.at[s, h]
        )
        for s in range(line)
        for h in (0, 1)
    ]
    for copy in loads:
        copy.start()
    greet(links, d, t, line)
    engine = Scatter(
        links, d, t, block,
        (
            lambda j: odd.at[j],
            lambda j, at=pl.ds(0, middle): core.at[j, at],
            lambda j, at: sums.at[j, at],
            lambda j, number: arrived.at[j, number],
            lambda j: out.at[j],
        ),
        (
            lambda j: core_send.at[j],
            lambda j: core_recv.at[j],
            lambda j, number: send.at[j, number],
            lambda j, number: recv.at[j, number],
        ),
    )
    branch_t[...] = branch[...].T

    def first(s, carry):
        for h in (0, 1):
            j = 2 * s + h
            right = att_in[s, :, h * 2 * head : (h + 1) * 2 * head]
            odd[j] = nn(branch_t[middle:, :], right).astype(bf16)
            engine.core_copy(j).start()
        for h in (0, 1):
            j = 2 * s + h
            right = att_in[s, :, h * 2 * head : (h + 1) * 2 * head]
            value = nn(branch_t[:middle, :], right)
            sums[j] = value.astype(bf16)
            out[j] = value[:block]
        return carry

    lax.fori_loop(0, line, first, 0)
    for copy in loads:
        copy.wait()

    k_index = lax.broadcasted_iota(jnp.int32, (span, rows), 0)
    q_index = lax.broadcasted_iota(jnp.int32, (span, rows), 1) + (span - rows)

    def far_copy(slot):
        return mesh_copy(
            far_v.at[slot], far_in.at[lax.rem(slot + 1, line)], far_send.at[slot],
            far_recv.at[lax.rem(slot + 1, line)], (d, t - 1),
        )

    def near_copy(slot):
        return mesh_copy(
            near_v.at[slot], near_in.at[lax.rem(slot + 1, line)], near_send.at[slot],
            near_recv.at[lax.rem(slot + 1, line)], (d, t - 1),
        )

    def arriving(copy, slot):
        return copy(lax.rem(slot + line - 1, line))

    def pass_near(slot):
        @pl.when((t > 0) & (t < line - 1))
        def _():
            arriving(far_copy, slot).wait_recv()
            near_v[slot] = (near_f[slot] + far_in[slot].astype(f32)).astype(bf16)

        @pl.when(t == line - 1)
        def _():
            near_v[slot] = near_f[slot].astype(bf16)

        @pl.when(t > 0)
        def _():
            near_copy(slot).start()

    def head_back(raw, gain, value, cos, sin):
        c = value * cos + pltpu.roll(value * sin, head // 2, 1)
        inverse = lax.rsqrt(jnp.mean(raw * raw, axis=-1, keepdims=True) + epsilon)
        normed = raw * inverse
        inner = c * gain
        grad = inverse * (inner - normed * jnp.mean(inner * normed, axis=-1, keepdims=True))
        return grad, jnp.sum(c * normed, axis=0, keepdims=True)

    terms_out[...] = jnp.zeros(terms_out.shape, f32)

    def step(s, carry):
        allowed = (key_seg[...] == query_seg[...]) & (k_index <= q_index)
        for h in (0, 1):
            gatt[:, h * 2 * head : (h + 1) * 2 * head] = nn(branch[...], o_full[s, h]).astype(bf16)
        lse = lse_in[s].T
        for g in (0, 1):
            keys = k_in[s, :, g * head : (g + 1) * head]
            values = v_in[s, :, g * head : (g + 1) * head]
            grad_k = jnp.zeros((span, head), f32)
            grad_v = jnp.zeros((span, head), f32)
            for j in (0, 1):
                h = 2 * g + j
                cols = slice(h * head, (h + 1) * head)
                query = q_in[s, :, cols]
                upward = gatt[:, cols]
                scores = nt(keys, query) * factor
                scores = jnp.where(allowed, scores, -1e30)
                probs = jnp.exp(scores - lse[h : h + 1, :])
                grad_probs = nt(values, upward)
                delta = jnp.sum(probs * grad_probs, axis=0, keepdims=True)
                grad_scores = (probs * (grad_probs - delta)).astype(bf16)
                grad_k = grad_k + nn(grad_scores, query)
                grad_v = grad_v + nn(probs.astype(bf16), upward)
                grad_q = (tn(grad_scores, keys) * factor).astype(bf16).astype(f32)
                grad, term = head_back(proj_q[s, :, cols], gain_q[...], grad_q, cosine[...], sine[...])
                gq_out[s, :, cols] = grad.astype(bf16)
                terms_out[0:1, :] += term
            grad_k = grad_k * factor
            for at, value in ((g * head, grad_k), ((2 + g) * head, grad_v)):
                far_v[s, :, at : at + head] = value[:rows].astype(bf16)
                near_f[s, :, at : at + head] = value[rows : 2 * rows]
                own_kv[s, :, at : at + head] = value[2 * rows :]

        @pl.when(t > 1)
        def _():
            far_copy(s).start()

        spread_stages(engine, links, 0, line, s)

        @pl.when(s > 0)
        def _():
            pass_near(s)

        return carry

    lax.fori_loop(0, line, step, 0)
    pass_near(0)

    def last(i, carry):
        s = lax.rem(i + 2, line)
        spread_stages(engine, links, 0, line, i + line)

        @pl.when(t < line - 1)
        def _():
            arriving(near_copy, s).wait_recv()
            own_kv[s] = own_kv[s] + near_in[s].astype(f32)

        for g in (0, 1):
            cols = slice(g * head, (g + 1) * head)
            value = own_kv[s, :, cols].astype(bf16).astype(f32)
            grad, term = head_back(proj_k[s, :, cols], gain_k[...], value, cosine[...], sine[...])
            gkv_out[s, :, cols] = grad.astype(bf16)
            terms_out[1:2, :] += term
        gkv_out[s, :, 2 * head :] = own_kv[s, :, 2 * head :].astype(bf16)
        return carry

    lax.fori_loop(0, line, last, 0)

    def finish(s, carry):
        for h in (0, 1):
            engine.finish(2 * s + h, h)
            o_out[s, :, h * 2 * head : (h + 1) * 2 * head] = out[2 * s + h]

        @pl.when(t > 1)
        def _():
            far_copy(s).wait_send()

        @pl.when(t > 0)
        def _():
            near_copy(s).wait_send()

        return carry

    lax.fori_loop(0, line, finish, 0)


def attention_backward(branch, weights, q, k, v, lse, att, proj_q, proj_k, gain_q, gain_k, cosine, sine, key_seg, query_seg, size):
    line, rows, q_cols = q.shape
    width = branch.shape[1]
    span = k.shape[1]
    head = gain_q.shape[1]
    block, middle, count, chunk = width // size, width // 2, 2 * line, 2 * head
    pieces = Scatter.pieces(Links(size))
    vmem = pl.BlockSpec(memory_space=pltpu.VMEM)
    hbm = pl.BlockSpec(memory_space=pl.ANY)
    shape = jax.ShapeDtypeStruct
    dma = pltpu.SemaphoreType.DMA
    return pl.pallas_call(
        functools.partial(backward_kernel, size, line, head),
        out_shape=(
            shape((line, rows, 4 * head), bf16),
            shape((line, rows, 4 * head), bf16),
            shape((8, head), f32),
            shape((line, block, 4 * head), f32),
        ),
        in_specs=[vmem, hbm] + [vmem] * 13,
        out_specs=[vmem] * 4,
        scratch_shapes=[
            pltpu.VMEM((line, 2, width, 2 * head), bf16),
            pltpu.VMEM((width, rows), bf16),
            pltpu.VMEM((rows, 4 * head), bf16),
            pltpu.VMEM((line, rows, 4 * head), f32),
            pltpu.VMEM((line, rows, 4 * head), f32),
            pltpu.VMEM((line, rows, 4 * head), bf16),
            pltpu.VMEM((line, rows, 4 * head), bf16),
            pltpu.VMEM((line, rows, 4 * head), bf16),
            pltpu.VMEM((line, rows, 4 * head), bf16),
            pltpu.VMEM((count, middle, chunk), bf16),
            pltpu.VMEM((count, middle, chunk), bf16),
            pltpu.VMEM((count, middle, chunk), bf16),
            pltpu.VMEM((count, pieces, block, chunk), bf16),
            pltpu.VMEM((count, block, chunk), f32),
            dma((count,)),
            dma((count,)),
            dma((count, pieces)),
            dma((count, pieces)),
            dma((line,)),
            dma((line,)),
            dma((line,)),
            dma((line,)),
            dma((line, 2)),
        ],
        compiler_params=pltpu.CompilerParams(
            collective_id=3, has_side_effects=True, vmem_limit_bytes=62 << 20
        ),
        cost_estimate=pl.CostEstimate(flops=20 << 30, bytes_accessed=40 << 20, transcendentals=4 << 20),
    )(branch, weights, q, k, v, lse, att, proj_q, proj_k, gain_q, gain_k, cosine, sine, key_seg, query_seg)


def final_kernel(
    size, line, head,
    rows_in, gq_in, gkv_in, o_in, weights, source, grad_middle, gain_one,
    q_out, kv_out, o_out, input_out, terms_out,
    rows_t, pair, acc, odd, core, sums, arrived, out, outbox, inbox,
    core_send, core_recv, send, recv, local, line_send, line_recv,
):
    links = Links(size)
    d, t = lax.axis_index("dp"), lax.axis_index("tensor")
    rows, width = rows_in.shape
    middle = width // 2
    block = out.shape[1]
    chunk = 4 * head
    last_stage = len(links.bits)
    inner = (t > 0) & (t < line - 1)
    is_end = (t == 0) | (t == line - 1)

    def slot_at(i):
        return slot_of(line - 1 - i, t, line)

    def load(i, h):
        return pltpu.make_async_copy(
            weights.at[h, slot_at(i), :, 0 : 4 * head], pair.at[h], local.at[h]
        )

    for h in (0, 1):
        load(0, h).start()
    greet(links, d, t, line)
    engine = Scatter(
        links, d, t, block,
        (
            lambda j: odd.at[j],
            lambda j, at=pl.ds(0, middle): core.at[j, at],
            lambda j, at: sums.at[j, at],
            lambda j, number: arrived.at[j, number],
            lambda j: out.at[j],
        ),
        (
            lambda j: core_send.at[j],
            lambda j: core_recv.at[j],
            lambda j, number: send.at[j, number],
            lambda j, number: recv.at[j, number],
        ),
    )
    rows_t[...] = rows_in[...].T
    acc[...] = jnp.zeros(acc.shape, f32)

    def first(i, carry):
        slot = slot_at(i)
        for h in (0, 1):
            j = 2 * i + h
            odd[j] = nn(rows_t[middle:, :], (gq_in, gkv_in)[h][slot]).astype(bf16)
            engine.core_copy(j).start()
        for h in (0, 1):
            j = 2 * i + h
            value = nn(rows_t[:middle, :], (gq_in, gkv_in)[h][slot])
            sums[j] = value.astype(bf16)
            out[j] = value[:block]
        return carry

    lax.fori_loop(0, line, first, 0)

    def content(i, c):
        return o_in[slot_at(i)] if c == 2 else out[2 * i + c]

    def each(fill):
        for c in range(3):
            fill(c, slice(c * chunk, (c + 1) * chunk))

    def post(number, to):
        box = (0, 1, 1, 3, 2)[number]
        return mesh_copy(
            outbox.at[box], inbox.at[number], line_send.at[number], line_recv.at[number], (d, to)
        )

    def first_post():
        return post(0, jnp.where(t == 0, t + 1, t - 1))

    def along(i):
        if i == 0:

            @pl.when(is_end)
            def _():
                def fill(c, at):
                    outbox[0, :, at] = content(0, c).astype(bf16)

                each(fill)
                first_post().start()

        if i == 1:

            @pl.when(inner)
            def _():
                first_post().wait_recv()

            @pl.when(is_end)
            def _():
                inbox[0] = jnp.zeros(inbox.shape[1:], bf16)

            def fill(c, at):
                outbox[1, :, at] = (content(1, c) + inbox[0, :, at].astype(f32)).astype(bf16)

            each(fill)

            @pl.when(t >= 2)
            def _():
                post(1, t - 1).start()

            @pl.when(t <= 1)
            def _():
                post(2, t + 1).start()

        if i == 2:

            @pl.when(inner)
            def _():
                post(1, t - 1).wait_recv()
                post(2, t + 1).wait_recv()

            @pl.when(is_end)
            def _():
                inbox[1] = jnp.zeros(inbox.shape[1:], bf16)
                inbox[2] = jnp.zeros(inbox.shape[1:], bf16)

            def leftward(c, at):
                three = jnp.where(t == line - 1, content(2, c), content(0, c))
                outbox[3, :, at] = (three + inbox[1, :, at].astype(f32)).astype(bf16)

            def rightward(c, at):
                outbox[2, :, at] = (content(2, c) + inbox[2, :, at].astype(f32)).astype(bf16)

            @pl.when(t > 0)
            def _():
                each(leftward)
                post(3, t - 1).start()

            @pl.when(t < line - 1)
            def _():
                each(rightward)
                post(4, t + 1).start()

    def step(i, carry):
        @pl.when(i < line)
        def _():
            for h in (0, 1):
                load(i, h).wait()
            slot = slot_at(i)
            for n in range(4):
                at = slice(n * (width // 4), (n + 1) * (width // 4))
                acc[:, at] += nt(gq_in[slot], pair[0, at, :]) + nt(gkv_in[slot], pair[1, at, :])

            @pl.when(i + 1 < line)
            def _():
                for h in (0, 1):
                    load(i + 1, h).start()

        spread_stages(engine, links, 0, line, i)
        for p in range(line - 1):

            @pl.when(i == p + last_stage)
            def _(p=p):
                along(p)

        return carry

    lax.fori_loop(0, line + last_stage, step, 0)

    part = rows // 4
    terms_out[...] = jnp.zeros(terms_out.shape, f32)

    def close(r, carry):
        at = pl.ds(pl.multiple_of(r * part, part), part)
        values = source[at, :]
        inverse = lax.rsqrt(jnp.mean(values * values, axis=-1, keepdims=True) + epsilon)
        normed = values * inverse
        c = acc[at, :]
        term = c * gain_one[...]
        grad = inverse * (term - normed * jnp.mean(term * normed, axis=-1, keepdims=True))
        input_out[at, :] = (grad_middle[at, :] + grad).astype(bf16)
        terms_out[...] += jnp.sum(c * normed, axis=0, keepdims=True)
        return carry

    lax.fori_loop(0, 4, close, 0)

    @pl.when(t < line - 1)
    def _():
        post(3, t - 1).wait_recv()

    @pl.when(t == line - 1)
    def _():
        inbox[3] = jnp.zeros(inbox.shape[1:], bf16)

    @pl.when(t > 0)
    def _():
        post(4, t + 1).wait_recv()

    @pl.when(t == 0)
    def _():
        inbox[4] = jnp.zeros(inbox.shape[1:], bf16)

    def total(c, at):
        (q_out, kv_out, o_out)[c][...] = (
            content(line - 1, c) + inbox[3, :, at].astype(f32) + inbox[4, :, at].astype(f32)
        )

    each(total)

    def finish(i, carry):
        for h in (0, 1):
            engine.finish(2 * i + h, h)
        return carry

    lax.fori_loop(0, line, finish, 0)

    @pl.when(is_end)
    def _():
        first_post().wait_send()

    @pl.when(t >= 2)
    def _():
        post(1, t - 1).wait_send()

    @pl.when(t <= 1)
    def _():
        post(2, t + 1).wait_send()

    @pl.when(t > 0)
    def _():
        post(3, t - 1).wait_send()

    @pl.when(t < line - 1)
    def _():
        post(4, t + 1).wait_send()


def attention_weights(rows_one, gq, gkv, o_sum, weights, source, grad_middle, gain_one, size, head):
    line, rows, chunk = gq.shape
    width = rows_one.shape[1]
    block, middle, count = width // size, width // 2, 2 * line
    pieces = Scatter.pieces(Links(size))
    vmem = pl.BlockSpec(memory_space=pltpu.VMEM)
    hbm = pl.BlockSpec(memory_space=pl.ANY)
    shape = jax.ShapeDtypeStruct
    dma = pltpu.SemaphoreType.DMA
    return pl.pallas_call(
        functools.partial(final_kernel, size, line, head),
        out_shape=(
            shape((block, chunk), f32),
            shape((block, chunk), f32),
            shape((block, chunk), f32),
            shape((rows, width), bf16),
            shape((1, width), f32),
        ),
        in_specs=[vmem] * 4 + [hbm] + [vmem] * 3,
        out_specs=[vmem] * 5,
        scratch_shapes=[
            pltpu.VMEM((width, rows), bf16),
            pltpu.VMEM((2, width, chunk), bf16),
            pltpu.VMEM((rows, width), f32),
            pltpu.VMEM((count, middle, chunk), bf16),
            pltpu.VMEM((count, middle, chunk), bf16),
            pltpu.VMEM((count, middle, chunk), bf16),
            pltpu.VMEM((count, pieces, block, chunk), bf16),
            pltpu.VMEM((count, block, chunk), f32),
            pltpu.VMEM((4, block, 3 * chunk), bf16),
            pltpu.VMEM((5, block, 3 * chunk), bf16),
            dma((count,)),
            dma((count,)),
            dma((count, pieces)),
            dma((count, pieces)),
            dma((2,)),
            dma((5,)),
            dma((5,)),
        ],
        compiler_params=pltpu.CompilerParams(
            collective_id=4, has_side_effects=True, vmem_limit_bytes=63 << 20
        ),
        cost_estimate=pl.CostEstimate(flops=16 << 30, bytes_accessed=40 << 20, transcendentals=0),
    )(rows_one, gq, gkv, o_sum, weights, source, grad_middle, gain_one)


def body(
    layer_input,
    first_gain,
    query_weight,
    key_matrix,
    value_matrix,
    query_gain,
    key_gain,
    output_weight,
    second_gain,
    gate_weight,
    up_weight,
    down_weight,
    segments,
    cotangent,
):
    plan = Plan()
    line, place = plan.line, plan.place
    rows, seq_count, width = layer_input.shape
    head = query_gain.shape[0]
    kv_heads = key_matrix.shape[1] // head
    query_heads = query_weight.shape[1] // head
    groups = query_heads // kv_heads
    all_kv = line * kv_heads
    half = width // 2
    hops = -(-(longest_document - 1) // rows)
    assert seq_count == 1 and hops == 2
    factor = head**-0.5

    gain_one = plan.to_masks(first_gain.astype(f32))
    gain_two = plan.to_masks(second_gain.astype(f32))
    gain_query = query_gain.astype(f32)
    gain_key = key_gain.astype(f32)
    source = plan.to_masks(layer_input[:, 0, :]).astype(f32)
    upstream = plan.to_masks(cotangent[:, 0, :])

    q_cols = query_weight.shape[1]
    kv_cols = key_matrix.shape[1]
    o_half = output_weight.shape[1] // 2
    shard = jnp.stack(
        [
            jnp.concatenate([query_weight, output_weight[:, :o_half]], axis=1),
            jnp.concatenate([key_matrix, value_matrix, output_weight[:, o_half:]], axis=1),
        ]
    )
    normed, inverse_one = rms_parts(source, gain_one)
    rows_one = normed.astype(bf16)
    span = (hops + 1) * rows
    positions = (place - hops) * rows + jnp.arange(span)
    cosine, sine = rope_tables(positions, head)
    padded = jnp.concatenate([jnp.full((hops * rows,), -1, segments.dtype), segments[0]], axis=0)
    key_segments = lax.dynamic_slice(padded, (place * rows,), (span,))
    query_segments = key_segments[hops * rows :]
    mlp_shard = jnp.stack([gate_weight, up_weight])
    (
        weights, pair_full, upstream_all, proj_query, proj_key, query_rows, key_rows, value_rows, lse, attended, middle, rows_two_own,
    ) = attention_forward(
        shard, mlp_shard, rows_one, upstream, source, gain_query[None], gain_key[None], gain_two[None], cosine, sine,
        key_segments[None, :], query_segments[:, None], plan.size, line,
    )
    inverse_two = lax.rsqrt(jnp.mean(middle * middle, axis=-1, keepdims=True) + epsilon)

    hidden_half = down_weight.shape[1] // 2
    down_shard = jnp.stack([down_weight[:, :hidden_half], down_weight[:, hidden_half:]])
    rows_two, hidden, grad_gate, grad_up, grad_two_part, mixed_part = feed_forward(
        rows_two_own, upstream_all, pair_full, down_shard, plan.size, line
    )

    def unslot(values):
        return values.reshape(-1, values.shape[2])

    hidden, grad_gate, grad_up = map(unslot, (hidden, grad_gate, grad_up))
    grad_two = lax.psum_scatter(
        grad_two_part, "tensor", scatter_dimension=0, tiled=True
    ).astype(f32)
    mixed_in = after(mixed_part, grad_two)
    mixed = lax.psum_scatter(mixed_in, "tensor", scatter_dimension=0, tiled=True).astype(f32)

    gate_grad, up_grad, down_grad = feed_weights(
        rows_two, upstream_all, grad_gate, grad_up, hidden, plan.size
    )

    grad_mid_norm, gain_two_terms = rms_back(middle, inverse_two, gain_two, grad_two)
    grad_middle = upstream.astype(f32) + grad_mid_norm
    grad_branch = grad_middle.astype(bf16)
    own_rows = slice(hops * rows, None)
    grad_query_low, grad_kv_low, head_terms, output_sum = attention_backward(
        grad_branch, weights, query_rows, key_rows, value_rows, lse, attended, proj_query, proj_key,
        gain_query[None], gain_key[None], cosine[own_rows], sine[own_rows],
        key_segments[:, None], query_segments[None, :], plan.size,
    )
    query_weight_grad, kv_grad, output_grad, input_masked, gain_one_terms = attention_weights(
        rows_one, grad_query_low, grad_kv_low, output_sum, weights, source, grad_middle, gain_one[None],
        plan.size, head,
    )
    input_grad = plan.from_masks(input_masked)[:, None, :]
    middle_late = after(middle, gain_one_terms)
    layer_output = plan.from_masks((middle_late + mixed).astype(bf16))[:, None, :]

    gains = plan.total(
        jnp.concatenate(
            [
                plan.from_masks(gain_one_terms[0]),
                plan.from_masks(jnp.sum(gain_two_terms, axis=0)),
                head_terms[0],
                head_terms[1],
            ]
        )
    )
    return (
        layer_output,
        input_grad,
        gains[:width],
        query_weight_grad,
        kv_grad[:, :kv_cols],
        kv_grad[:, kv_cols:],
        gains[2 * width : 2 * width + head],
        gains[2 * width + head :],
        output_grad,
        gains[width : 2 * width],
        gate_grad,
        up_grad,
        down_grad,
    )


def solution(mesh):
    positions = P("tensor", "dp", None)
    weight = P("dp", "tensor")
    return jax.shard_map(
        body,
        mesh=mesh,
        in_specs=(
            positions,
            P(),
            weight,
            weight,
            weight,
            P(),
            P(),
            weight,
            P(),
            weight,
            weight,
            weight,
            P("dp", None),
            positions,
        ),
        out_specs=(
            positions,
            positions,
            P(),
            weight,
            weight,
            weight,
            P(),
            P(),
            weight,
            P(),
            weight,
            weight,
            weight,
        ),
        check_vma=False,
    )
```

```python
import functools

import jax
import jax.numpy as jnp
from jax import lax
from jax.experimental import pallas as pl
from jax.experimental.pallas import tpu as pltpu
from jax.sharding import PartitionSpec as P

epsilon = 1e-06
rope_base = 1000000.0
longest_document = 512
bf16 = jnp.bfloat16
f32 = jnp.float32


def mm(eq, a, b):
    return jnp.einsum(eq, a, b, preferred_element_type=f32)


def rms_parts(values, gain):
    inverse = lax.rsqrt(jnp.mean(values * values, axis=-1, keepdims=True) + epsilon)
    return values * inverse * gain, inverse


def rms_back(values, inverse, gain, upstream):
    normed = values * inverse
    inner = upstream * gain
    grad = inverse * (inner - normed * jnp.mean(inner * normed, axis=-1, keepdims=True))
    return grad, upstream * normed


def rope_tables(positions, head_size):
    half = head_size // 2
    frequency = rope_base ** (-(2.0 * jnp.arange(half, dtype=f32)) / head_size)
    angles = positions.astype(f32)[:, None] * frequency[None, :]
    sine = jnp.sin(angles)
    return (
        jnp.concatenate([jnp.cos(angles)] * 2, axis=1),
        jnp.concatenate([-sine, sine], axis=1),
    )


def rotate_back(upstream, cosine, sine):
    half = upstream.shape[-1] // 2
    shifted = upstream * sine
    return upstream * cosine + jnp.concatenate(
        [shifted[..., half:], shifted[..., :half]], axis=-1
    )


class Plan:
    def __init__(self):
        self.size = lax.axis_size("dp")
        self.index = lax.axis_index("dp")
        self.place = lax.axis_index("tensor")
        self.line = lax.axis_size("tensor")
        assert self.line == 4
        self.others = [1 << i for i in range(1, self.size.bit_length() - 1)]
        evens = [0]
        for bit in self.others:
            evens = evens + [m ^ bit for m in evens]
        self.evens = evens
        self.masks = evens + [m ^ 1 for m in evens]
        self.forward = self.others
        self.backward = self.others[::-1]

    def swap(self, value, bit):
        return lax.ppermute(value, "dp", [(i, i ^ bit) for i in range(self.size)])

    def move(self, value, pairs):
        return lax.ppermute(value, "tensor", pairs)

    def xor_blocks(self, blocks):
        bit = 1
        while bit < self.size:
            on = (self.index & bit) != 0
            blocks = [jnp.where(on, blocks[i ^ bit], blocks[i]) for i in range(self.size)]
            bit *= 2
        return blocks

    def to_masks(self, value):
        blocks = self.xor_blocks(jnp.split(value, self.size, axis=-1))
        return jnp.concatenate([blocks[m] for m in self.masks], axis=-1)

    def from_masks(self, value):
        parts = jnp.split(value, self.size, axis=-1)
        blocks = [parts[self.masks.index(m)] for m in range(self.size)]
        return jnp.concatenate(self.xor_blocks(blocks), axis=-1)

    def gather(self, shard, order):
        rows = shard.shape[0]
        held, masks = shard, [0]
        for bit in order:
            arrived = self.swap(held, bit)
            held = jnp.concatenate([held, arrived], axis=0)
            masks = masks + [m ^ bit for m in masks]
        if masks != self.evens:
            held = jnp.concatenate(
                [lax.slice_in_dim(held, masks.index(m) * rows, (masks.index(m) + 1) * rows) for m in self.evens],
                axis=0,
            )
        return held, self.swap(held, 1)

    def reduce(self, even, odd, order):
        rows = even.shape[0] // len(self.evens)
        total = even.astype(f32) + self.swap(odd.astype(bf16), 1).astype(f32)
        pieces = {
            m: lax.slice_in_dim(total, i * rows, (i + 1) * rows) for i, m in enumerate(self.evens)
        }
        for bit in order:
            leaving = [m for m in pieces if m & bit]
            sent = jnp.concatenate([pieces[m].astype(bf16) for m in leaving], axis=0)
            arrived = self.swap(sent, bit)
            kept = {m: v for m, v in pieces.items() if not m & bit}
            for i, m in enumerate(leaving):
                kept[m ^ bit] = kept[m ^ bit] + lax.slice_in_dim(
                    arrived, i * rows, (i + 1) * rows
                ).astype(f32)
            pieces = kept
        return pieces[0]

    def gather_line(self, own):
        from_right = self.move(own, [(1, 0), (2, 1), (3, 2)])
        from_left = self.move(own, [(0, 1), (1, 2), (2, 3)])
        right_two = self.move(from_right, [(1, 0), (2, 1)])
        left_two = self.move(from_left, [(1, 2), (2, 3)])
        slot_two = jnp.where(self.place < 2, right_two, left_two)
        last = self.move(slot_two, [(1, 0), (2, 3)])
        slot_one = jnp.where(self.place < 3, from_right, last)
        slot_three = jnp.where(self.place > 0, from_left, last)
        return [own, slot_one, slot_two, slot_three]

    def scatter_line(self, slots):
        zero, one, two, three = slots
        first = self.move(
            jnp.where(self.place == 3, one, three).astype(bf16), [(3, 2), (0, 1)]
        )
        middle = (two + first.astype(f32)).astype(bf16)
        leftward = self.move(middle, [(3, 2), (2, 1)])
        rightward = self.move(middle, [(0, 1), (1, 2)])
        leftward = self.move(
            (three + leftward.astype(f32)).astype(bf16), [(3, 2), (2, 1), (1, 0)]
        )
        rightward = self.move(
            (one + rightward.astype(f32)).astype(bf16), [(0, 1), (1, 2), (2, 3)]
        )
        return zero + leftward.astype(f32) + rightward.astype(f32)

    def total(self, value):
        bit = 1
        while bit < self.size:
            value = value + self.swap(value, bit)
            bit *= 2
        for bit in (1, 2):
            value = value + self.move(value, [(i, i ^ bit) for i in range(self.line)])
        return value


def after(value, *others):
    return lax.optimization_barrier((value,) + others)[0]


def mesh_copy(src, dst, send, recv, device):
    return pltpu.make_async_remote_copy(
        src_ref=src, dst_ref=dst, send_sem=send, recv_sem=recv, device_id=device,
        device_id_type=pl.DeviceIdType.MESH,
    )


class Links:
    def __init__(self, size):
        bits = [1 << i for i in range(1, size.bit_length() - 1)]
        self.orders = (bits, bits[::-1])
        evens = [0]
        for bit in bits:
            evens = evens + [m ^ bit for m in evens]
        self.evens = evens
        self.masks = evens + [m ^ 1 for m in evens]
        self.bits = bits

    def onward(self, half, mask):
        order = self.orders[half]
        last = max([i for i, bit in enumerate(order) if mask & bit], default=-1)
        return order[last + 1 :]


class Gather:
    def __init__(self, links, d, t, piece, send, recv):
        self.links, self.d, self.t = links, d, t
        self.piece, self.send, self.recv = piece, send, recv

    def copy(self, half, mask, bit):
        index = self.links.masks.index(mask ^ bit)
        return mesh_copy(
            self.piece(half, mask), self.piece(half, mask ^ bit), self.send(half, index),
            self.recv(half, index), (self.d ^ bit, self.t),
        )

    def launch(self):
        for step in range(len(self.links.bits)):
            for half in (0, 1):
                self.copy(half, 0, self.links.orders[half][step]).start()
        for half in (0, 1):
            self.copy(half, 0, 1).start()

    def arrive(self, half, mask):
        bit = [b for b in self.links.orders[half] if b & mask][-1]
        self.copy(half, mask ^ bit, bit).wait_recv()
        for other in self.links.onward(half, mask):
            self.copy(half, mask, other).start()
        self.copy(half, mask, 1).start()

    def onward(self):
        for mask in self.links.evens[1:]:
            for half in (0, 1):
                if self.links.onward(half, mask):
                    self.arrive(half, mask)

    def complete(self):
        for mask in self.links.evens[1:]:
            for half in (0, 1):
                if not self.links.onward(half, mask):
                    self.arrive(half, mask)
        for mask in self.links.evens:
            for half in (0, 1):
                self.copy(half, mask, 1).wait_recv()

    def finish(self):
        for mask in self.links.masks[1:]:
            for half in (0, 1):
                self.copy(half, mask ^ 1 if mask & 1 else 0, 1 if mask & 1 else mask).wait_send()


class Relay:
    def __init__(self, d, t, line, slot, send, recv):
        self.d, self.t, self.line = d, t, line
        self.slot, self.send, self.recv = slot, send, recv
        self.inner = (t > 0) & (t < line - 1)

    def copy(self, number, source, target, to):
        return mesh_copy(
            self.slot(source), self.slot(target), self.send.at[number], self.recv.at[target],
            (self.d, to),
        )

    def moves(self):
        t = self.t
        return (
            (t > 0, (0, 0, 1, t - 1)),
            (t < self.line - 1, (1, 0, 3, t + 1)),
            (self.inner, (2, 1, 2, t - 1)),
            (self.inner, (3, 3, 2, t + 1)),
            (t == 1, (4, 2, 3, t - 1)),
            (t == 2, (5, 2, 1, t + 1)),
        )

    def start(self, *numbers):
        for number in numbers:
            condition, route = self.moves()[number]

            @pl.when(condition)
            def _(route=route):
                self.copy(*route).start()

    def wait(self, slot):
        self.copy(0, 0, slot, self.t).wait_recv()

    def finish(self):
        for condition, route in self.moves():

            @pl.when(condition)
            def _(route=route):
                self.copy(*route).wait_send()

    def first(self):
        self.start(0, 1)

    def second(self):
        t, line = self.t, self.line

        @pl.when(t < line - 1)
        def _():
            self.wait(1)

        self.start(2)

        @pl.when(t > 0)
        def _():
            self.wait(3)

        self.start(3)

    def third(self):
        self.wait(2)
        self.start(4, 5)

    def ends(self):
        @pl.when(self.t == 0)
        def _():
            self.wait(3)

        @pl.when(self.t == self.line - 1)
        def _():
            self.wait(1)


def slot_of(i, t, line):
    far = jnp.where(t < line - 1, 1, 3)
    near = jnp.where(t < line - 1, 3, 1)
    return jnp.where(i == 0, 0, jnp.where(i == 1, far, jnp.where(i == 2, 2, near)))


def greet(links, d, t, line, across=False):
    barrier = pltpu.get_barrier_semaphore()
    if across:
        pl.semaphore_signal(barrier, inc=1, device_id=(d, t ^ 2), device_id_type=pl.DeviceIdType.MESH)
    for bit in [1] + links.bits:
        pl.semaphore_signal(barrier, inc=1, device_id=(d ^ bit, t), device_id_type=pl.DeviceIdType.MESH)

    @pl.when(t > 0)
    def _():
        pl.semaphore_signal(barrier, inc=1, device_id=(d, t - 1), device_id_type=pl.DeviceIdType.MESH)

    @pl.when(t < line - 1)
    def _():
        pl.semaphore_signal(barrier, inc=1, device_id=(d, t + 1), device_id_type=pl.DeviceIdType.MESH)

    pl.semaphore_wait(
        barrier,
        1 + across + len(links.bits) + jnp.where(t > 0, 1, 0) + jnp.where(t < line - 1, 1, 0),
    )


def nt(a, b):
    return lax.dot_general(a, b, (((1,), (1,)), ((), ())), preferred_element_type=f32)


def tn(a, b):
    return lax.dot_general(a, b, (((0,), (0,)), ((), ())), preferred_element_type=f32)


def nn(a, b):
    return jnp.dot(a, b, preferred_element_type=f32)


def head_norm(values, gain):
    inverse = lax.rsqrt(jnp.mean(values * values, axis=-1, keepdims=True) + epsilon)
    return values * inverse * gain


def forward_kernel(
    size, line, head,
    shard, mlp_shard, rows_in, upstream, source, gain_q, gain_k, gain_two, cosine, sine, key_seg, query_seg,
    weights_out, mlp_out, upstream_all, proj_q, proj_k, q_out, k_out, v_out, lse_out, att_out, middle, normed_out,
    full, rows_all, acc,
    z_send, z_recv, send, recv, row_send, row_recv, keep, mlp_send, mlp_recv, up_send, up_recv, local,
):
    links = Links(size)
    d, t = lax.axis_index("dp"), lax.axis_index("tensor")
    block = shard.shape[1]
    rows, width = rows_in.shape
    span = rows_all.shape[0]
    factor = head**-0.5

    def place(mask):
        return pl.ds(links.masks.index(mask) * block, block)

    def gather(slot):
        return Gather(
            links, d, t,
            lambda half, mask: full.at[half, slot, place(mask)],
            lambda half, index: send.at[slot, half, index],
            lambda half, index: recv.at[slot, half, index],
        )

    feed = Gather(
        links, d, t,
        lambda half, mask: mlp_out.at[half, place(mask)],
        lambda half, index: mlp_send.at[half, index],
        lambda half, index: mlp_recv.at[half, index],
    )
    relay = Relay(d, t, line, lambda slot: full.at[:, slot, place(0)], z_send, z_recv)
    upward = Relay(d, t, line, lambda slot: upstream_all.at[slot], up_send, up_recv)

    own = (
        pltpu.make_async_copy(shard, full.at[:, 0, place(0)], local.at[0]),
        pltpu.make_async_copy(mlp_shard, mlp_out.at[:, place(0)], local.at[1]),
        pltpu.make_async_copy(upstream, upstream_all.at[0], local.at[2]),
    )
    for copy in own:
        copy.start()
    rows_all[pl.ds(span - rows, rows), :] = rows_in[...]

    @pl.when(t == 0)
    def _():
        rows_all[pl.ds(0, 2 * rows), :] = jnp.zeros((2 * rows, width), bf16)

    @pl.when(t == 1)
    def _():
        rows_all[pl.ds(0, rows), :] = jnp.zeros((rows, width), bf16)

    greet(links, d, t, line)
    own[0].wait()

    row_one = mesh_copy(
        rows_in, rows_all.at[pl.ds(rows, rows)], row_send.at[0], row_recv.at[0], (d, t + 1)
    )
    row_two = mesh_copy(
        rows_all.at[pl.ds(rows, rows)], rows_all.at[pl.ds(0, rows)], row_send.at[1],
        row_recv.at[1], (d, t + 1),
    )
    inner = relay.inner
    relay.first()

    @pl.when(t < line - 1)
    def _():
        row_one.start()

    gather(0).launch()
    gather(0).onward()
    relay.second()
    second = slot_of(1, t, line)

    @pl.when(t < line - 1)
    def _():
        gather(1).launch()

    @pl.when(t == line - 1)
    def _():
        gather(3).launch()

    @pl.when(t > 0)
    def _():
        row_one.wait_recv()

    @pl.when(inner)
    def _():
        row_two.start()

    relay.third()
    gather(2).launch()
    gather(second).onward()

    @pl.when(t > 1)
    def _():
        row_two.wait_recv()

    own[1].wait()
    own[2].wait()
    upward.first()
    acc[...] = source[...]

    lane = lax.broadcasted_iota(jnp.int32, (rows, 128), 1)
    q_index = lax.broadcasted_iota(jnp.int32, (rows, span), 0) + (span - rows)
    k_index = lax.broadcasted_iota(jnp.int32, (rows, span), 1)

    def step(i, carry):
        slot = slot_of(i, t, line)

        @pl.when(i == 1)
        def _():
            relay.ends()
            gather(slot_of(3, t, line)).launch()

        @pl.when(i >= 2)
        def _():
            gather(slot).onward()

        @pl.when((i == 2))
        def _():
            feed.launch()

        gather(slot).complete()
        for half in (0, 1):
            pltpu.make_async_copy(
                full.at[half, slot], weights_out.at[half, slot], keep.at[slot, half]
            ).start()

        own_rows = pl.ds(span - rows, rows)
        allowed = (query_seg[...] == key_seg[...]) & (k_index <= q_index)
        lse_acc = jnp.zeros((rows, 128), f32)
        for g in (0, 1):
            key_cols = slice(g * head, (g + 1) * head)
            if g == 0:
                for r in range(span // rows):
                    part = pl.ds(r * rows, rows)
                    both = nn(rows_all[part, :], full[1, slot, :, 0 : 4 * head])
                    if r == span // rows - 1:
                        proj_k[slot] = both[:, : 2 * head]
                    for h in (0, 1):
                        unit = head_norm(both[:, h * head : (h + 1) * head], gain_k[...])
                        turned = unit * cosine[part, :] + pltpu.roll(unit, head // 2, 1) * sine[part, :]
                        k_out[slot, part, h * head : (h + 1) * head] = turned.astype(bf16)
                    v_out[slot, part, :] = both[:, 2 * head :].astype(bf16)
            for j in (0, 1):
                h = 2 * g + j
                cols = slice(h * head, (h + 1) * head)
                raw = nn(rows_in[...], full[0, slot, :, cols])
                proj_q[slot, :, cols] = raw
                unit = head_norm(raw, gain_q[...])
                turned = unit * cosine[own_rows, :] + pltpu.roll(unit, head // 2, 1) * sine[own_rows, :]
                query = turned.astype(bf16)
                q_out[slot, :, cols] = query
                scores = nt(query, k_out[slot, :, key_cols]) * factor
                scores = jnp.where(allowed, scores, -1e30)
                top = jnp.max(scores, axis=-1, keepdims=True)
                weight = jnp.exp(scores - top)
                total = jnp.sum(weight, axis=-1, keepdims=True)
                probs = (weight / total).astype(bf16)
                att_out[slot, :, cols] = nn(probs, v_out[slot, :, key_cols]).astype(bf16)
                lse_acc = jnp.where(lane == h, top + jnp.log(total), lse_acc)
        lse_out[slot] = lse_acc
        for half in (0, 1):
            acc[...] += nt(
                att_out[slot, :, half * 2 * head : (half + 1) * 2 * head],
                full[half, slot, :, 4 * head : 6 * head],
            )

        @pl.when((i == 2))
        def _():
            upward.second()

        return carry

    lax.fori_loop(0, line, step, 0)
    upward.third()
    feed.onward()
    values = acc[...]
    middle[...] = values
    normed_out[...] = head_norm(values, gain_two[...]).astype(bf16)
    feed.complete()

    def finish(i, carry):
        gather(i).finish()
        for half in (0, 1):
            pltpu.make_async_copy(full.at[half, i], weights_out.at[half, i], keep.at[i, half]).wait()
        return carry

    lax.fori_loop(0, line, finish, 0)
    feed.finish()
    relay.finish()

    @pl.when(t < line - 1)
    def _():
        row_one.wait_send()

    @pl.when(inner)
    def _():
        row_two.wait_send()

    upward.ends()
    upward.finish()


def attention_forward(shard, mlp_shard, rows_one, upstream, source, gain_q, gain_k, gain_two, cosine, sine, key_seg, query_seg, size, line):
    _, block, cols = shard.shape
    rows, width = rows_one.shape
    span = cosine.shape[0]
    head = gain_q.shape[1]
    pieces = 2 * (size // 2)
    vmem = pl.BlockSpec(memory_space=pltpu.VMEM)
    hbm = pl.BlockSpec(memory_space=pl.ANY)
    shape = jax.ShapeDtypeStruct
    return pl.pallas_call(
        functools.partial(forward_kernel, size, line, head),
        out_shape=(
            shape((2, line, width, cols), bf16),
            shape((2, width, mlp_shard.shape[2]), bf16),
            shape((line, rows, width), bf16),
            shape((line, rows, 4 * head), f32),
            shape((line, rows, 2 * head), f32),
            shape((line, rows, 4 * head), bf16),
            shape((line, span, 2 * head), bf16),
            shape((line, span, 2 * head), bf16),
            shape((line, rows, 128), f32),
            shape((line, rows, 4 * head), bf16),
            shape((rows, width), f32),
            shape((rows, width), bf16),
        ),
        in_specs=[hbm] + [vmem] * 11,
        out_specs=[hbm] * 3 + [vmem] * 9,
        scratch_shapes=[
            pltpu.VMEM((2, line, width, cols), bf16),
            pltpu.VMEM((span, width), bf16),
            pltpu.VMEM((rows, width), f32),
            pltpu.SemaphoreType.DMA((6,)),
            pltpu.SemaphoreType.DMA((line,)),
            pltpu.SemaphoreType.DMA((line, 2, pieces)),
            pltpu.SemaphoreType.DMA((line, 2, pieces)),
            pltpu.SemaphoreType.DMA((2,)),
            pltpu.SemaphoreType.DMA((2,)),
            pltpu.SemaphoreType.DMA((line, 2)),
            pltpu.SemaphoreType.DMA((2, pieces)),
            pltpu.SemaphoreType.DMA((2, pieces)),
            pltpu.SemaphoreType.DMA((6,)),
            pltpu.SemaphoreType.DMA((line,)),
            pltpu.SemaphoreType.DMA((3,)),
        ],
        compiler_params=pltpu.CompilerParams(
            collective_id=0, has_side_effects=True, vmem_limit_bytes=62 << 20
        ),
        cost_estimate=pl.CostEstimate(flops=40 << 30, bytes_accessed=200 << 20, transcendentals=4 << 20),
    )(shard, mlp_shard, rows_one, upstream, source, gain_q, gain_k, gain_two, cosine, sine, key_seg, query_seg)


def feed_kernel(
    size, line,
    rows_in, upstream_in, pair_in, down_in,
    rows_out, hidden_out, gate_out, up_out, grad_out, mixed_out,
    rows_v, upstream_v, pair, down, gate_f, up_f, hidden_v, gate_v, up_v, grad_v, mixed_v,
    z_send, z_recv, send, recv, local, leave,
):
    links = Links(size)
    d, t = lax.axis_index("dp"), lax.axis_index("tensor")
    block = down_in.shape[1]
    _, rows, width = rows_v.shape
    units = hidden_v.shape[2]
    chunk = units // 4
    piece = width // 4

    def place(mask):
        return pl.ds(links.masks.index(mask) * block, block)

    gather = Gather(
        links, d, t,
        lambda half, mask: down.at[half, place(mask)],
        lambda half, index: send.at[half, index],
        lambda half, index: recv.at[half, index],
    )
    relay = Relay(d, t, line, lambda slot: rows_v.at[slot], z_send, z_recv)
    arrivals = (
        pltpu.make_async_copy(rows_in, rows_v.at[0], local.at[0]),
        pltpu.make_async_copy(down_in, down.at[:, place(0)], local.at[1]),
        pltpu.make_async_copy(pair_in, pair, local.at[2]),
        pltpu.make_async_copy(upstream_in, upstream_v, local.at[3]),
    )
    for copy in arrivals:
        copy.start()
    greet(links, d, t, line)
    arrivals[0].wait()
    relay.first()
    arrivals[1].wait()
    gather.launch()
    gather.onward()
    arrivals[2].wait()
    arrivals[3].wait()

    def departures(slot):
        position = lax.rem(slot + t, line)
        natural = pl.ds(pl.multiple_of(position * rows, rows), rows)
        return [
            pltpu.make_async_copy(rows_v.at[slot], rows_out.at[slot], leave.at[0, slot]),
            pltpu.make_async_copy(hidden_v.at[slot], hidden_out.at[slot], leave.at[1, slot]),
            pltpu.make_async_copy(gate_v.at[slot], gate_out.at[slot], leave.at[2, slot]),
            pltpu.make_async_copy(up_v.at[slot], up_out.at[slot], leave.at[3, slot]),
            pltpu.make_async_copy(grad_v.at[slot], grad_out.at[natural], leave.at[4, slot]),
            pltpu.make_async_copy(mixed_v.at[slot], mixed_out.at[natural], leave.at[5, slot]),
        ]

    def step(i, carry):
        slot = slot_of(i, t, line)
        for c in range(4):
            cols = slice(c * chunk, (c + 1) * chunk)
            gate = nn(rows_v[slot], pair[0, :, cols])
            up = nn(rows_v[slot], pair[1, :, cols])
            gate_f[:, cols] = gate
            up_f[:, cols] = up
            hidden_v[slot, :, cols] = (gate * jax.nn.sigmoid(gate) * up).astype(bf16)

        @pl.when(i == 0)
        def _():
            relay.second()
            gather.complete()

        @pl.when(i == 1)
        def _():
            relay.third()

        @pl.when(i == 2)
        def _():
            relay.ends()

        for c in range(4):
            cols = slice(c * chunk, (c + 1) * chunk)
            inner = slice((c % 2) * chunk, (c % 2 + 1) * chunk)
            grad_hidden = nn(upstream_v[slot], down[c // 2, :, inner])
            gate, up = gate_f[:, cols], up_f[:, cols]
            sigmoid = jax.nn.sigmoid(gate)
            gate_v[slot, :, cols] = (
                grad_hidden * up * sigmoid * (1.0 + gate * (1.0 - sigmoid))
            ).astype(bf16)
            up_v[slot, :, cols] = (grad_hidden * (gate * sigmoid)).astype(bf16)
        for n in range(4):
            out = slice(n * piece, (n + 1) * piece)
            grad_v[slot, :, out] = (
                nt(gate_v[slot], pair[0, out, :]) + nt(up_v[slot], pair[1, out, :])
            ).astype(bf16)
            mixed_v[slot, :, out] = (
                nt(hidden_v[slot, :, : units // 2], down[0, out, :])
                + nt(hidden_v[slot, :, units // 2 :], down[1, out, :])
            ).astype(bf16)
        for copy in departures(slot):
            copy.start()
        return carry

    lax.fori_loop(0, line, step, 0)

    def finish(i, carry):
        for copy in departures(i):
            copy.wait()
        return carry

    lax.fori_loop(0, line, finish, 0)
    gather.finish()
    relay.finish()


def feed_forward(rows_own, upstream_all, pair_full, down_shard, size, line):
    rows, width = rows_own.shape
    units = pair_full.shape[2]
    hbm = pl.BlockSpec(memory_space=pl.ANY)
    shape = jax.ShapeDtypeStruct
    dma = pltpu.SemaphoreType.DMA
    return pl.pallas_call(
        functools.partial(feed_kernel, size, line),
        out_shape=(
            shape((line, rows, width), bf16),
            shape((line, rows, units), bf16),
            shape((line, rows, units), bf16),
            shape((line, rows, units), bf16),
            shape((line * rows, width), bf16),
            shape((line * rows, width), bf16),
        ),
        in_specs=[hbm] * 4,
        out_specs=[hbm] * 6,
        scratch_shapes=[
            pltpu.VMEM((line, rows, width), bf16),
            pltpu.VMEM((line, rows, width), bf16),
            pltpu.VMEM((2, width, units), bf16),
            pltpu.VMEM((2, width, units // 2), bf16),
            pltpu.VMEM((rows, units), f32),
            pltpu.VMEM((rows, units), f32),
            pltpu.VMEM((line, rows, units), bf16),
            pltpu.VMEM((line, rows, units), bf16),
            pltpu.VMEM((line, rows, units), bf16),
            pltpu.VMEM((line, rows, width), bf16),
            pltpu.VMEM((line, rows, width), bf16),
            dma((6,)),
            dma((line,)),
            dma((2, size)),
            dma((2, size)),
            dma((4,)),
            dma((6, line)),
        ],
        compiler_params=pltpu.CompilerParams(
            collective_id=1, has_side_effects=True, vmem_limit_bytes=62 << 20
        ),
        cost_estimate=pl.CostEstimate(flops=40 << 30, bytes_accessed=60 << 20, transcendentals=3 << 20),
    )(rows_own, upstream_all, pair_full, down_shard)


class Scatter:
    def __init__(self, links, d, t, block, refs, semaphores):
        self.links, self.d, self.t, self.block = links, d, t, block
        self.odd, self.core, self.sums, self.arrived, self.out = refs
        self.core_send, self.core_recv, self.send, self.recv = semaphores

    @staticmethod
    def pieces(links):
        return max(1, len(links.evens) - 1)

    def steps(self, half):
        masks, number, found = self.links.evens, 0, []
        for bit in self.links.orders[half][::-1]:
            masks = [m for m in masks if not m & bit]
            found.append((bit, [(m, number + i) for i, m in enumerate(masks)]))
            number += len(masks)
        return found

    def rows(self, mask):
        return pl.ds(self.links.evens.index(mask) * self.block, self.block)

    def core_copy(self, j):
        return mesh_copy(
            self.odd(j), self.core(j), self.core_send(j), self.core_recv(j), (self.d ^ 1, self.t)
        )

    def piece_copy(self, j, mask, number, bit):
        return mesh_copy(
            self.sums(j, self.rows(mask ^ bit)), self.arrived(j, number), self.send(j, number),
            self.recv(j, number), (self.d ^ bit, self.t),
        )

    def launch(self, j, half, step):
        steps = self.steps(half)
        if step < len(steps):
            bit, pairs = steps[step]
            for mask, number in pairs:
                self.piece_copy(j, mask, number, bit).start()

    def add(self, j, mask, value):
        if mask == 0:
            out = self.out(j)
            out[...] = out[...] + value[...].astype(f32)
        else:
            total = self.sums(j, self.rows(mask))
            total[...] = (total[...].astype(f32) + value[...].astype(f32)).astype(bf16)

    def stage(self, j, half, stage):
        if stage == 0:
            self.core_copy(j).wait_recv()
            steps = self.steps(half)
            first = steps[0][0] if steps else 0
            for mask in sorted(self.links.evens, key=lambda m: not m & first):
                self.add(j, mask, self.core(j, self.rows(mask)))
        else:
            bit, pairs = self.steps(half)[stage - 1]
            for mask, number in pairs[::-1]:
                self.piece_copy(j, mask, number, bit).wait_recv()
                self.add(j, mask, self.arrived(j, number))
        self.launch(j, half, stage)

    def finish(self, j, half):
        self.core_copy(j).wait_send()
        for bit, pairs in self.steps(half):
            for mask, number in pairs:
                self.piece_copy(j, mask, number, bit).wait_send()


def greet_dp(links, d, t):
    barrier = pltpu.get_barrier_semaphore()
    for bit in [1] + links.bits:
        pl.semaphore_signal(barrier, inc=1, device_id=(d ^ bit, t), device_id_type=pl.DeviceIdType.MESH)
    pl.semaphore_wait(barrier, 1 + len(links.bits))


class LineSum:
    def __init__(self, d, t, line, source, ends, outbox, inbox, semaphores):
        self.d, self.t, self.line = d, t, line
        self.source, self.ends, self.outbox, self.inbox = source, ends, outbox, inbox
        self.send, self.recv, self.local = semaphores
        self.rows = outbox.shape[1]

    def block(self, position):
        return self.source.at[pl.ds(pl.multiple_of(position * self.rows, self.rows), self.rows)]

    def hop(self, number, source, target, to):
        return mesh_copy(source, target, self.send.at[number], self.recv.at[number], (self.d, to))

    def hops(self):
        t, line = self.t, self.line
        return (
            (t == 0, lambda: self.hop(0, self.block(line - 1), self.inbox.at[0], t + 1)),
            (t == line - 1, lambda: self.hop(0, self.block(0), self.inbox.at[0], t - 1)),
            (t >= 2, lambda: self.hop(1, self.outbox.at[0], self.inbox.at[1], t - 1)),
            (t <= 1, lambda: self.hop(2, self.outbox.at[0], self.inbox.at[2], t + 1)),
            (t > 0, lambda: self.hop(3, self.outbox.at[1], self.ends[0], t - 1)),
            (t < line - 1, lambda: self.hop(4, self.outbox.at[2], self.ends[1], t + 1)),
        )

    def start(self, *numbers):
        for number in numbers:
            condition, make = self.hops()[number]

            @pl.when(condition)
            def _(make=make):
                make().start()

    def own(self, box, step):
        position = lax.rem(self.t + step, self.line)
        return pltpu.make_async_copy(self.block(position), self.outbox.at[box], self.local.at[box])

    def take(self, box, number):
        @pl.when((self.t > 0) & (self.t < self.line - 1))
        def _():
            self.hop(number, self.outbox.at[0], self.inbox.at[number], self.t + 1).wait_recv()
            self.outbox[box] = (
                self.outbox[box].astype(f32) + self.inbox[number].astype(f32)
            ).astype(bf16)

    def first(self):
        self.start(0, 1)
        for box, step in ((0, 2), (1, 3), (2, 1)):
            self.own(box, step).start()

    def second(self):
        self.own(0, 2).wait()
        self.take(0, 0)
        self.start(2, 3)

    def third(self):
        self.own(1, 3).wait()
        self.own(2, 1).wait()
        self.take(1, 1)
        self.take(2, 2)
        self.start(4, 5)

    def finish(self):
        for condition, make in self.hops():

            @pl.when(condition)
            def _(make=make):
                make().wait_send()

        @pl.when(self.t < self.line - 1)
        def _():
            self.hop(3, self.outbox.at[1], self.ends[0], self.t + 1).wait_recv()

        @pl.when(self.t > 0)
        def _():
            self.hop(4, self.outbox.at[2], self.ends[1], self.t - 1).wait_recv()


def weight_kernel(
    size, line,
    rows_in, upstream_in, gate_in, up_in, hidden_in, mixed_in, grad_in,
    gate_out, up_out, down_out, mixed_out, sum_left, sum_right,
    outbox, inbox, raw, left, right, odd, core, sums, arrived, out,
    core_send, core_recv, send, recv, local, raw_sem, leave, line_send, line_recv, sum_send, sum_recv, sum_local,
):
    links = Links(size)
    d, t = lax.axis_index("dp"), lax.axis_index("tensor")
    width = left.shape[1]
    rows = raw.shape[1]
    ring, tokens, chunk = right.shape
    count = out.shape[0]
    middle = width // 2
    block = out.shape[1]
    pairs = count // 2
    wide = gate_in.shape[1] // chunk

    def load(j):
        p, h = j // 2, j % 2
        if p < wide:
            source, at = (gate_in, up_in)[h], p
        else:
            source, at = hidden_in, p - wide + h * (wide // 2)
        return pltpu.make_async_copy(
            source.at[:, at * chunk : (at + 1) * chunk], right.at[j % ring], local.at[j]
        )

    def store(j):
        p, h = j // 2, j % 2
        if p < wide:
            target, at = (gate_out, up_out)[h], p
        else:
            target, at = down_out, p - wide + h * (wide // 2)
        return pltpu.make_async_copy(
            out.at[j], target.at[:, at * chunk : (at + 1) * chunk], leave.at[j]
        )

    def fetch(k, r):
        source = (rows_in, upstream_in)[k]
        slot = (k * line + r) % 2
        return pltpu.make_async_copy(source.at[r], raw.at[slot], raw_sem.at[slot]), slot

    fetch(0, 0)[0].start()
    for j in range(ring):
        load(j).start()
    greet(links, d, t, line)
    gradient = LineSum(
        d, t, line, grad_in, (sum_left, sum_right), outbox, inbox, (sum_send, sum_recv, sum_local)
    )
    gradient.first()

    def hop(at, to):
        return mesh_copy(
            mixed_in.at[pl.ds(at * rows, rows)], mixed_out, line_send.at[0], line_recv.at[0], (d, to)
        )

    def hop_of(act):
        @pl.when(t == 0)
        def _():
            act(hop(line - 1, t + 1))

        @pl.when(t == line - 1)
        def _():
            act(hop(0, t - 1))

    def turn(k):
        for r in range(line):
            copy, slot = fetch(k, r)
            copy.wait()
            following = k * line + r + 1
            if following < 2 * line:
                fetch(following // line, following % line)[0].start()
            left[k, :, r * rows : (r + 1) * rows] = raw[slot].T

    engine = Scatter(
        links, d, t, block,
        (
            lambda j: odd.at[j],
            lambda j, at=pl.ds(0, middle): core.at[j, at],
            lambda j, at: sums.at[j, at],
            lambda j, number: arrived.at[j, number],
            lambda j: out.at[j],
        ),
        (
            lambda j: core_send.at[j],
            lambda j: core_recv.at[j],
            lambda j, number: send.at[j, number],
            lambda j, number: recv.at[j, number],
        ),
    )
    turn(0)
    gradient.second()

    def step(p, carry):
        @pl.when(p == wide // 2)
        def _():
            turn(1)

        @pl.when(p == 3)
        def _():
            gradient.third()

        @pl.when(p == wide)
        def _():
            hop_of(lambda copy: copy.start())

        for q in range(pairs):

            @pl.when(p == q)
            def _(q=q):
                load(2 * q).wait()
                load(2 * q + 1).wait()

        @pl.when(p < pairs)
        def _():
            k = jnp.where(p < wide, 0, 1)
            for h in (0, 1):
                j = 2 * p + h
                for r in range(middle // 256):
                    at = pl.ds(middle + r * 256, 256)
                    odd[j, pl.ds(r * 256, 256), :] = nn(
                        left[k, at, :], right[lax.rem(j, ring)]
                    ).astype(bf16)
                engine.core_copy(j).start()
            for h in (0, 1):
                j = 2 * p + h
                for r in range(middle // 256):
                    at = pl.ds(r * 256, 256)
                    value = nn(left[k, at, :], right[lax.rem(j, ring)])
                    sums[j, at, :] = value.astype(bf16)
                    if r == 0:
                        out[j] = value[:block]

        for q in range(pairs - ring // 2):

            @pl.when(p == q)
            def _(q=q):
                load(2 * q + ring).start()
                load(2 * q + ring + 1).start()

        for stage in range(len(links.bits) + 1):
            @pl.when((p >= stage + 1) & (p < pairs + stage + 1))
            def _(stage=stage):
                for h in (0, 1):
                    engine.stage(2 * (p - stage - 1) + h, h, stage)

        return carry

    lax.fori_loop(0, pairs + len(links.bits) + 1, step, 0)
    for j in range(count):
        store(j).start()

    def finish(p, carry):
        for h in (0, 1):
            engine.finish(2 * p + h, h)
        return carry

    lax.fori_loop(0, pairs, finish, 0)
    for j in range(count):
        store(j).wait()
    hop_of(lambda copy: copy.wait_send())

    @pl.when((t > 0) & (t < line - 1))
    def _():
        hop(0, t - 1).wait_recv()

    gradient.finish()


def feed_weights(rows_all, upstream_all, gate, up, hidden, mixed, grad, size):
    line, rows, width = rows_all.shape
    tokens, units = gate.shape
    chunk = units // 4
    count = 3 * 4
    block = width // size
    middle = width // 2
    pieces = Scatter.pieces(Links(size))
    hbm = pl.BlockSpec(memory_space=pl.ANY)
    shape = jax.ShapeDtypeStruct
    dma = pltpu.SemaphoreType.DMA
    return pl.pallas_call(
        functools.partial(weight_kernel, size, line),
        out_shape=(shape((block, units), f32),) * 3 + (shape((rows, width), bf16),) * 3,
        in_specs=[hbm] * 7,
        out_specs=[hbm] * 6,
        scratch_shapes=[
            pltpu.VMEM((3, rows, width), bf16),
            pltpu.VMEM((3, rows, width), bf16),
            pltpu.VMEM((2, rows, width), bf16),
            pltpu.VMEM((2, width, tokens), bf16),
            pltpu.VMEM((4, tokens, chunk), bf16),
            pltpu.VMEM((count, middle, chunk), bf16),
            pltpu.VMEM((count, middle, chunk), bf16),
            pltpu.VMEM((count, middle, chunk), bf16),
            pltpu.VMEM((count, pieces, block, chunk), bf16),
            pltpu.VMEM((count, block, chunk), f32),
            dma((count,)),
            dma((count,)),
            dma((count, pieces)),
            dma((count, pieces)),
            dma((count,)),
            dma((2,)),
            dma((count,)),
            dma((1,)),
            dma((1,)),
            dma((5,)),
            dma((5,)),
            dma((3,)),
        ],
        compiler_params=pltpu.CompilerParams(
            collective_id=2, has_side_effects=True, vmem_limit_bytes=63 << 20
        ),
        cost_estimate=pl.CostEstimate(flops=20 << 30, bytes_accessed=60 << 20, transcendentals=0),
    )(rows_all, upstream_all, gate, up, hidden, mixed, grad)


def spread_stages(engine, links, first, last, p):
    for stage in range(len(links.bits) + 1)[::-1]:
        @pl.when((p - stage >= first) & (p - stage < last))
        def _(stage=stage):
            for h in (0, 1):
                engine.stage(2 * (p - stage) + h, h, stage)


def backward_kernel(
    size, line, head,
    branch, weights, q_in, k_in, v_in, lse_in, att_in, proj_q, proj_k, gain_q, gain_k, cosine, sine,
    key_seg, query_seg, mixed_in,
    gq_out, gkv_out, terms_out, o_out, mixed_left, mixed_right,
    o_full, branch_t, gatt, own_kv, near_f, far_v, near_v, far_in, near_in, odd, core, sums, arrived, out,
    core_send, core_recv, send, recv, far_send, far_recv, near_send, near_recv, local,
    line_send, line_recv,
):
    links = Links(size)
    d, t = lax.axis_index("dp"), lax.axis_index("tensor")
    rows, width = branch.shape
    span = k_in.shape[1]
    middle = width // 2
    block = out.shape[1]
    factor = head**-0.5
    loads = [
        pltpu.make_async_copy(
            weights.at[h, s, :, 4 * head : 6 * head], o_full.at[s, h], local.at[s, h]
        )
        for s in range(line)
        for h in (0, 1)
    ]
    for copy in loads:
        copy.start()
    greet(links, d, t, line)

    def leftward():
        return mesh_copy(mixed_in, mixed_left, line_send.at[0], line_recv.at[0], (d, t - 1))

    def rightward():
        return mesh_copy(mixed_in, mixed_right, line_send.at[1], line_recv.at[1], (d, t + 1))

    @pl.when(t >= line // 2)
    def _():
        leftward().start()

    @pl.when(t < line // 2)
    def _():
        rightward().start()

    engine = Scatter(
        links, d, t, block,
        (
            lambda j: odd.at[j],
            lambda j, at=pl.ds(0, middle): core.at[j, at],
            lambda j, at: sums.at[j, at],
            lambda j, number: arrived.at[j, number],
            lambda j: out.at[j],
        ),
        (
            lambda j: core_send.at[j],
            lambda j: core_recv.at[j],
            lambda j, number: send.at[j, number],
            lambda j, number: recv.at[j, number],
        ),
    )
    branch_t[...] = branch[...].T

    def first(s, carry):
        for h in (0, 1):
            j = 2 * s + h
            right = att_in[s, :, h * 2 * head : (h + 1) * 2 * head]
            odd[j] = nn(branch_t[middle:, :], right).astype(bf16)
            engine.core_copy(j).start()
        for h in (0, 1):
            j = 2 * s + h
            right = att_in[s, :, h * 2 * head : (h + 1) * 2 * head]
            value = nn(branch_t[:middle, :], right)
            sums[j] = value.astype(bf16)
            out[j] = value[:block]
        return carry

    lax.fori_loop(0, line, first, 0)
    for copy in loads:
        copy.wait()

    k_index = lax.broadcasted_iota(jnp.int32, (span, rows), 0)
    q_index = lax.broadcasted_iota(jnp.int32, (span, rows), 1) + (span - rows)

    def far_copy(slot):
        return mesh_copy(
            far_v.at[slot], far_in.at[lax.rem(slot + 1, line)], far_send.at[slot],
            far_recv.at[lax.rem(slot + 1, line)], (d, t - 1),
        )

    def near_copy(slot):
        return mesh_copy(
            near_v.at[slot], near_in.at[lax.rem(slot + 1, line)], near_send.at[slot],
            near_recv.at[lax.rem(slot + 1, line)], (d, t - 1),
        )

    def arriving(copy, slot):
        return copy(lax.rem(slot + line - 1, line))

    def pass_near(slot):
        @pl.when((t > 0) & (t < line - 1))
        def _():
            arriving(far_copy, slot).wait_recv()
            near_v[slot] = (near_f[slot] + far_in[slot].astype(f32)).astype(bf16)

        @pl.when(t == line - 1)
        def _():
            near_v[slot] = near_f[slot].astype(bf16)

        @pl.when(t > 0)
        def _():
            near_copy(slot).start()

    def head_back(raw, gain, value, cos, sin):
        c = value * cos + pltpu.roll(value * sin, head // 2, 1)
        inverse = lax.rsqrt(jnp.mean(raw * raw, axis=-1, keepdims=True) + epsilon)
        normed = raw * inverse
        inner = c * gain
        grad = inverse * (inner - normed * jnp.mean(inner * normed, axis=-1, keepdims=True))
        return grad, jnp.sum(c * normed, axis=0, keepdims=True)

    terms_out[...] = jnp.zeros(terms_out.shape, f32)

    def step(s, carry):
        allowed = (key_seg[...] == query_seg[...]) & (k_index <= q_index)
        for h in (0, 1):
            gatt[:, h * 2 * head : (h + 1) * 2 * head] = nn(branch[...], o_full[s, h]).astype(bf16)
        lse = lse_in[s].T
        for g in (0, 1):
            keys = k_in[s, :, g * head : (g + 1) * head]
            values = v_in[s, :, g * head : (g + 1) * head]
            grad_k = jnp.zeros((span, head), f32)
            grad_v = jnp.zeros((span, head), f32)
            for j in (0, 1):
                h = 2 * g + j
                cols = slice(h * head, (h + 1) * head)
                query = q_in[s, :, cols]
                upward = gatt[:, cols]
                scores = nt(keys, query) * factor
                scores = jnp.where(allowed, scores, -1e30)
                probs = jnp.exp(scores - lse[h : h + 1, :])
                grad_probs = nt(values, upward)
                delta = jnp.sum(probs * grad_probs, axis=0, keepdims=True)
                grad_scores = (probs * (grad_probs - delta)).astype(bf16)
                grad_k = grad_k + nn(grad_scores, query)
                grad_v = grad_v + nn(probs.astype(bf16), upward)
                grad_q = (tn(grad_scores, keys) * factor).astype(bf16).astype(f32)
                grad, term = head_back(proj_q[s, :, cols], gain_q[...], grad_q, cosine[...], sine[...])
                gq_out[s, :, cols] = grad.astype(bf16)
                terms_out[0:1, :] += term
            grad_k = grad_k * factor
            for at, value in ((g * head, grad_k), ((2 + g) * head, grad_v)):
                far_v[s, :, at : at + head] = value[:rows].astype(bf16)
                near_f[s, :, at : at + head] = value[rows : 2 * rows]
                own_kv[s, :, at : at + head] = value[2 * rows :]

        @pl.when(t > 1)
        def _():
            far_copy(s).start()

        spread_stages(engine, links, 0, line, s)

        @pl.when(s > 0)
        def _():
            pass_near(s)

        return carry

    lax.fori_loop(0, line, step, 0)
    pass_near(0)

    def last(i, carry):
        s = lax.rem(i + 2, line)
        spread_stages(engine, links, 0, line, i + line)

        @pl.when(t < line - 1)
        def _():
            arriving(near_copy, s).wait_recv()
            own_kv[s] = own_kv[s] + near_in[s].astype(f32)

        for g in (0, 1):
            cols = slice(g * head, (g + 1) * head)
            value = own_kv[s, :, cols].astype(bf16).astype(f32)
            grad, term = head_back(proj_k[s, :, cols], gain_k[...], value, cosine[...], sine[...])
            gkv_out[s, :, cols] = grad.astype(bf16)
            terms_out[1:2, :] += term
        gkv_out[s, :, 2 * head :] = own_kv[s, :, 2 * head :].astype(bf16)
        return carry

    lax.fori_loop(0, line, last, 0)

    def finish(s, carry):
        for h in (0, 1):
            engine.finish(2 * s + h, h)
            o_out[s, :, h * 2 * head : (h + 1) * 2 * head] = out[2 * s + h]

        @pl.when(t > 1)
        def _():
            far_copy(s).wait_send()

        @pl.when(t > 0)
        def _():
            near_copy(s).wait_send()

        return carry

    lax.fori_loop(0, line, finish, 0)

    @pl.when(t >= line // 2)
    def _():
        leftward().wait_send()

    @pl.when(t < line // 2)
    def _():
        rightward().wait_send()

    @pl.when((t > 0) & (t < line - 1))
    def _():
        leftward().wait_recv()
        rightward().wait_recv()


def attention_backward(branch, weights, q, k, v, lse, att, proj_q, proj_k, gain_q, gain_k, cosine, sine, key_seg, query_seg, mixed, size):
    line, rows, q_cols = q.shape
    width = branch.shape[1]
    span = k.shape[1]
    head = gain_q.shape[1]
    block, middle, count, chunk = width // size, width // 2, 2 * line, 2 * head
    pieces = Scatter.pieces(Links(size))
    vmem = pl.BlockSpec(memory_space=pltpu.VMEM)
    hbm = pl.BlockSpec(memory_space=pl.ANY)
    shape = jax.ShapeDtypeStruct
    dma = pltpu.SemaphoreType.DMA
    return pl.pallas_call(
        functools.partial(backward_kernel, size, line, head),
        out_shape=(
            shape((line, rows, 4 * head), bf16),
            shape((line, rows, 4 * head), bf16),
            shape((8, head), f32),
            shape((line, block, 4 * head), f32),
            shape((rows, width), bf16),
            shape((rows, width), bf16),
        ),
        in_specs=[vmem, hbm] + [vmem] * 13 + [hbm],
        out_specs=[vmem] * 4 + [hbm] * 2,
        scratch_shapes=[
            pltpu.VMEM((line, 2, width, 2 * head), bf16),
            pltpu.VMEM((width, rows), bf16),
            pltpu.VMEM((rows, 4 * head), bf16),
            pltpu.VMEM((line, rows, 4 * head), f32),
            pltpu.VMEM((line, rows, 4 * head), f32),
            pltpu.VMEM((line, rows, 4 * head), bf16),
            pltpu.VMEM((line, rows, 4 * head), bf16),
            pltpu.VMEM((line, rows, 4 * head), bf16),
            pltpu.VMEM((line, rows, 4 * head), bf16),
            pltpu.VMEM((count, middle, chunk), bf16),
            pltpu.VMEM((count, middle, chunk), bf16),
            pltpu.VMEM((count, middle, chunk), bf16),
            pltpu.VMEM((count, pieces, block, chunk), bf16),
            pltpu.VMEM((count, block, chunk), f32),
            dma((count,)),
            dma((count,)),
            dma((count, pieces)),
            dma((count, pieces)),
            dma((line,)),
            dma((line,)),
            dma((line,)),
            dma((line,)),
            dma((line, 2)),
            dma((2,)),
            dma((2,)),
        ],
        compiler_params=pltpu.CompilerParams(
            collective_id=3, has_side_effects=True, vmem_limit_bytes=62 << 20
        ),
        cost_estimate=pl.CostEstimate(flops=20 << 30, bytes_accessed=40 << 20, transcendentals=4 << 20),
    )(branch, weights, q, k, v, lse, att, proj_q, proj_k, gain_q, gain_k, cosine, sine, key_seg, query_seg, mixed)


def final_kernel(
    size, line, head,
    rows_in, gq_in, gkv_in, o_in, weights, source, grad_middle, gain_one, second_terms, head_terms,
    mixed_l, mixed_r,
    q_out, kv_out, o_out, input_out, terms_out, mixed_left, mixed_right,
    rows_t, pair, acc, odd, core, sums, arrived, out, outbox, inbox, heap,
    core_send, core_recv, send, recv, local, line_send, line_recv, heap_send, heap_recv, mixed_send, mixed_recv,
):
    links = Links(size)
    d, t = lax.axis_index("dp"), lax.axis_index("tensor")
    rows, width = rows_in.shape
    middle = width // 2
    block = out.shape[1]
    chunk = 4 * head
    last_stage = len(links.bits)
    inner = (t > 0) & (t < line - 1)
    is_end = (t == 0) | (t == line - 1)

    def slot_at(i):
        return slot_of(line - 1 - i, t, line)

    def load(i, h):
        return pltpu.make_async_copy(
            weights.at[h, slot_at(i), :, 0 : 4 * head], pair.at[h], local.at[h]
        )

    for h in (0, 1):
        load(0, h).start()
    inside = block % 128 == 0
    greet(links, d, t, line, inside)

    def leftward():
        return mesh_copy(mixed_l, mixed_left, mixed_send.at[0], mixed_recv.at[0], (d, t - 1))

    def rightward():
        return mesh_copy(mixed_r, mixed_right, mixed_send.at[1], mixed_recv.at[1], (d, t + 1))

    @pl.when(t > 0)
    def _():
        leftward().start()

    @pl.when(t < line - 1)
    def _():
        rightward().start()

    engine = Scatter(
        links, d, t, block,
        (
            lambda j: odd.at[j],
            lambda j, at=pl.ds(0, middle): core.at[j, at],
            lambda j, at: sums.at[j, at],
            lambda j, number: arrived.at[j, number],
            lambda j: out.at[j],
        ),
        (
            lambda j: core_send.at[j],
            lambda j: core_recv.at[j],
            lambda j, number: send.at[j, number],
            lambda j, number: recv.at[j, number],
        ),
    )
    rows_t[...] = rows_in[...].T
    acc[...] = jnp.zeros(acc.shape, f32)

    def first(i, carry):
        slot = slot_at(i)
        for h in (0, 1):
            j = 2 * i + h
            odd[j] = nn(rows_t[middle:, :], (gq_in, gkv_in)[h][slot]).astype(bf16)
            engine.core_copy(j).start()
        for h in (0, 1):
            j = 2 * i + h
            value = nn(rows_t[:middle, :], (gq_in, gkv_in)[h][slot])
            sums[j] = value.astype(bf16)
            out[j] = value[:block]
        return carry

    lax.fori_loop(0, line, first, 0)

    def content(i, c):
        return o_in[slot_at(i)] if c == 2 else out[2 * i + c]

    def each(fill):
        for c in range(3):
            fill(c, slice(c * chunk, (c + 1) * chunk))

    def post(number, to):
        box = (0, 1, 1, 3, 2)[number]
        return mesh_copy(
            outbox.at[box], inbox.at[number], line_send.at[number], line_recv.at[number], (d, to)
        )

    def first_post():
        return post(0, jnp.where(t == 0, t + 1, t - 1))

    def along(i):
        if i == 0:

            @pl.when(is_end)
            def _():
                def fill(c, at):
                    outbox[0, :, at] = content(0, c).astype(bf16)

                each(fill)
                first_post().start()

        if i == 1:

            @pl.when(inner)
            def _():
                first_post().wait_recv()

            @pl.when(is_end)
            def _():
                inbox[0] = jnp.zeros(inbox.shape[1:], bf16)

            def fill(c, at):
                outbox[1, :, at] = (content(1, c) + inbox[0, :, at].astype(f32)).astype(bf16)

            each(fill)

            @pl.when(t >= 2)
            def _():
                post(1, t - 1).start()

            @pl.when(t <= 1)
            def _():
                post(2, t + 1).start()

        if i == 2:

            @pl.when(inner)
            def _():
                post(1, t - 1).wait_recv()
                post(2, t + 1).wait_recv()

            @pl.when(is_end)
            def _():
                inbox[1] = jnp.zeros(inbox.shape[1:], bf16)
                inbox[2] = jnp.zeros(inbox.shape[1:], bf16)

            def leftward(c, at):
                three = jnp.where(t == line - 1, content(2, c), content(0, c))
                outbox[3, :, at] = (three + inbox[1, :, at].astype(f32)).astype(bf16)

            def rightward(c, at):
                outbox[2, :, at] = (content(2, c) + inbox[2, :, at].astype(f32)).astype(bf16)

            @pl.when(t > 0)
            def _():
                each(leftward)
                post(3, t - 1).start()

            @pl.when(t < line - 1)
            def _():
                each(rightward)
                post(4, t + 1).start()

    part = rows // 4
    terms_out[...] = jnp.zeros(terms_out.shape, f32)
    terms_out[1:2, :] = second_terms[...]
    terms_out[2:3, 0:head] = head_terms[0:1, :]
    terms_out[2:3, head : 2 * head] = head_terms[1:2, :]

    def close(r, carry):
        at = pl.ds(pl.multiple_of(r * part, part), part)
        values = source[at, :]
        inverse = lax.rsqrt(jnp.mean(values * values, axis=-1, keepdims=True) + epsilon)
        normed = values * inverse
        c = acc[at, :]
        term = c * gain_one[...]
        grad = inverse * (term - normed * jnp.mean(term * normed, axis=-1, keepdims=True))
        input_out[at, :] = (grad_middle[at, :] + grad).astype(bf16)
        terms_out[0:1, :] += jnp.sum(c * normed, axis=0, keepdims=True)
        return carry

    def step(i, carry):
        @pl.when(i < line)
        def _():
            for h in (0, 1):
                load(i, h).wait()
            slot = slot_at(i)
            for n in range(4):
                at = slice(n * (width // 4), (n + 1) * (width // 4))
                acc[:, at] += nt(gq_in[slot], pair[0, at, :]) + nt(gkv_in[slot], pair[1, at, :])

            @pl.when(i + 1 < line)
            def _():
                for h in (0, 1):
                    load(i + 1, h).start()

        @pl.when(i == line)
        def _():
            lax.fori_loop(0, 4, close, 0)

        spread_stages(engine, links, 0, line, i)
        for p in range(line - 1):

            @pl.when(i == p + last_stage)
            def _(p=p):
                along(p)

        return carry

    lax.fori_loop(0, line + last_stage, step, 0)

    if inside:
        hops = [((d ^ bit, t), bit) for bit in [1] + links.bits]
        hops = hops + [((d, t ^ 1), 0), ((d, t ^ 2), 0)]
        for k, (to, bit) in enumerate(hops):
            copy = mesh_copy(terms_out, heap.at[k], heap_send.at[k], heap_recv.at[k], to)
            copy.start()
            copy.wait()
            for i, mask in enumerate(links.masks):
                other = links.masks.index(mask ^ bit)
                terms_out[0:2, i * block : (i + 1) * block] += heap[
                    k, 0:2, other * block : (other + 1) * block
                ]
            terms_out[2:3, :] += heap[k, 2:3, :]

    @pl.when(t < line - 1)
    def _():
        post(3, t - 1).wait_recv()

    @pl.when(t == line - 1)
    def _():
        inbox[3] = jnp.zeros(inbox.shape[1:], bf16)

    @pl.when(t > 0)
    def _():
        post(4, t + 1).wait_recv()

    @pl.when(t == 0)
    def _():
        inbox[4] = jnp.zeros(inbox.shape[1:], bf16)

    def total(c, at):
        (q_out, kv_out, o_out)[c][...] = (
            content(line - 1, c) + inbox[3, :, at].astype(f32) + inbox[4, :, at].astype(f32)
        )

    each(total)

    def finish(i, carry):
        for h in (0, 1):
            engine.finish(2 * i + h, h)
        return carry

    lax.fori_loop(0, line, finish, 0)

    @pl.when(t > 0)
    def _():
        leftward().wait_send()
        rightward().wait_recv()

    @pl.when(t < line - 1)
    def _():
        rightward().wait_send()
        leftward().wait_recv()

    @pl.when(is_end)
    def _():
        first_post().wait_send()

    @pl.when(t >= 2)
    def _():
        post(1, t - 1).wait_send()

    @pl.when(t <= 1)
    def _():
        post(2, t + 1).wait_send()

    @pl.when(t > 0)
    def _():
        post(3, t - 1).wait_send()

    @pl.when(t < line - 1)
    def _():
        post(4, t + 1).wait_send()


def attention_weights(rows_one, gq, gkv, o_sum, weights, source, grad_middle, gain_one, second_terms, head_terms, mixed_l, mixed_r, size, head):
    line, rows, chunk = gq.shape
    width = rows_one.shape[1]
    block, middle, count = width // size, width // 2, 2 * line
    pieces = Scatter.pieces(Links(size))
    hops = 3 + len(Links(size).bits)
    vmem = pl.BlockSpec(memory_space=pltpu.VMEM)
    hbm = pl.BlockSpec(memory_space=pl.ANY)
    shape = jax.ShapeDtypeStruct
    dma = pltpu.SemaphoreType.DMA
    return pl.pallas_call(
        functools.partial(final_kernel, size, line, head),
        out_shape=(
            shape((block, chunk), f32),
            shape((block, chunk), f32),
            shape((block, chunk), f32),
            shape((rows, width), bf16),
            shape((8, width), f32),
            shape((rows, width), bf16),
            shape((rows, width), bf16),
        ),
        in_specs=[vmem] * 4 + [hbm] + [vmem] * 5 + [hbm] * 2,
        out_specs=[vmem] * 5 + [hbm] * 2,
        scratch_shapes=[
            pltpu.VMEM((width, rows), bf16),
            pltpu.VMEM((2, width, chunk), bf16),
            pltpu.VMEM((rows, width), f32),
            pltpu.VMEM((count, middle, chunk), bf16),
            pltpu.VMEM((count, middle, chunk), bf16),
            pltpu.VMEM((count, middle, chunk), bf16),
            pltpu.VMEM((count, pieces, block, chunk), bf16),
            pltpu.VMEM((count, block, chunk), f32),
            pltpu.VMEM((4, block, 3 * chunk), bf16),
            pltpu.VMEM((5, block, 3 * chunk), bf16),
            pltpu.VMEM((hops, 8, width), f32),
            dma((count,)),
            dma((count,)),
            dma((count, pieces)),
            dma((count, pieces)),
            dma((2,)),
            dma((5,)),
            dma((5,)),
            dma((hops,)),
            dma((hops,)),
            dma((2,)),
            dma((2,)),
        ],
        compiler_params=pltpu.CompilerParams(
            collective_id=4, has_side_effects=True, vmem_limit_bytes=63 << 20
        ),
        cost_estimate=pl.CostEstimate(flops=16 << 30, bytes_accessed=40 << 20, transcendentals=0),
    )(rows_one, gq, gkv, o_sum, weights, source, grad_middle, gain_one, second_terms, head_terms, mixed_l, mixed_r)


def body(
    layer_input,
    first_gain,
    query_weight,
    key_matrix,
    value_matrix,
    query_gain,
    key_gain,
    output_weight,
    second_gain,
    gate_weight,
    up_weight,
    down_weight,
    segments,
    cotangent,
):
    plan = Plan()
    line, place = plan.line, plan.place
    rows, seq_count, width = layer_input.shape
    head = query_gain.shape[0]
    kv_heads = key_matrix.shape[1] // head
    query_heads = query_weight.shape[1] // head
    groups = query_heads // kv_heads
    all_kv = line * kv_heads
    half = width // 2
    hops = -(-(longest_document - 1) // rows)
    assert seq_count == 1 and hops == 2
    factor = head**-0.5

    gain_one = plan.to_masks(first_gain.astype(f32))
    gain_two = plan.to_masks(second_gain.astype(f32))
    gain_query = query_gain.astype(f32)
    gain_key = key_gain.astype(f32)
    source = plan.to_masks(layer_input[:, 0, :]).astype(f32)
    upstream = plan.to_masks(cotangent[:, 0, :])

    q_cols = query_weight.shape[1]
    kv_cols = key_matrix.shape[1]
    o_half = output_weight.shape[1] // 2
    shard = jnp.stack(
        [
            jnp.concatenate([query_weight, output_weight[:, :o_half]], axis=1),
            jnp.concatenate([key_matrix, value_matrix, output_weight[:, o_half:]], axis=1),
        ]
    )
    normed, inverse_one = rms_parts(source, gain_one)
    rows_one = normed.astype(bf16)
    span = (hops + 1) * rows
    positions = (place - hops) * rows + jnp.arange(span)
    cosine, sine = rope_tables(positions, head)
    padded = jnp.concatenate([jnp.full((hops * rows,), -1, segments.dtype), segments[0]], axis=0)
    key_segments = lax.dynamic_slice(padded, (place * rows,), (span,))
    query_segments = key_segments[hops * rows :]
    mlp_shard = jnp.stack([gate_weight, up_weight])
    (
        weights, pair_full, upstream_all, proj_query, proj_key, query_rows, key_rows, value_rows, lse, attended, middle, rows_two_own,
    ) = attention_forward(
        shard, mlp_shard, rows_one, upstream, source, gain_query[None], gain_key[None], gain_two[None], cosine, sine,
        key_segments[None, :], query_segments[:, None], plan.size, line,
    )
    inverse_two = lax.rsqrt(jnp.mean(middle * middle, axis=-1, keepdims=True) + epsilon)

    hidden_half = down_weight.shape[1] // 2
    down_shard = jnp.stack([down_weight[:, :hidden_half], down_weight[:, hidden_half:]])
    rows_two, hidden, grad_gate, grad_up, grad_two_part, mixed_part = feed_forward(
        rows_two_own, upstream_all, pair_full, down_shard, plan.size, line
    )

    def unslot(values):
        return values.reshape(-1, values.shape[2])

    hidden, grad_gate, grad_up = map(unslot, (hidden, grad_gate, grad_up))
    inner = (place > 0) & (place < line - 1)

    def share(step, part=mixed_part):
        return lax.dynamic_slice(part, ((place + step) % line * rows, 0), (rows, width)).astype(f32)

    def closed(part, from_right, from_left):
        return (
            share(0, part)
            + jnp.where(place < line - 1, from_right.astype(f32), 0.0)
            + jnp.where(place > 0, from_left.astype(f32), 0.0)
        )

    gate_grad, up_grad, down_grad, mixed_one, grad_left, grad_right = feed_weights(
        rows_two, upstream_all, grad_gate, grad_up, hidden, mixed_part, grad_two_part, plan.size
    )
    mixed_two = (share(2) + jnp.where(inner, mixed_one.astype(f32), 0.0)).astype(bf16)
    grad_two = closed(grad_two_part, grad_left, grad_right)

    grad_mid_norm, gain_two_terms = rms_back(middle, inverse_two, gain_two, grad_two)
    grad_middle = upstream.astype(f32) + grad_mid_norm
    grad_branch = grad_middle.astype(bf16)
    own_rows = slice(hops * rows, None)
    grad_query_low, grad_kv_low, head_terms, output_sum, mixed_left, mixed_right = attention_backward(
        grad_branch, weights, query_rows, key_rows, value_rows, lse, attended, proj_query, proj_key,
        gain_query[None], gain_key[None], cosine[own_rows], sine[own_rows],
        key_segments[:, None], query_segments[None, :], mixed_two, plan.size,
    )
    mixed_three = [
        (share(step) + jnp.where(inner, come.astype(f32), 0.0)).astype(bf16)
        for step, come in ((3, mixed_left), (1, mixed_right))
    ]
    second_terms = jnp.sum(gain_two_terms, axis=0, keepdims=True)
    query_weight_grad, kv_grad, output_grad, input_masked, terms, mixed_left, mixed_right = attention_weights(
        rows_one, grad_query_low, grad_kv_low, output_sum, weights, source, grad_middle, gain_one[None],
        second_terms, head_terms, *mixed_three, plan.size, head,
    )
    input_grad = plan.from_masks(input_masked)[:, None, :]
    middle_late = after(middle, terms)
    mixed = closed(mixed_part, mixed_left, mixed_right)
    layer_output = plan.from_masks((middle_late + mixed).astype(bf16))[:, None, :]
    gains = jnp.concatenate([plan.from_masks(terms[0]), plan.from_masks(terms[1]), terms[2, : 2 * head]])
    if width // plan.size % 128:
        gains = plan.total(gains)
    return (
        layer_output,
        input_grad,
        gains[:width],
        query_weight_grad,
        kv_grad[:, :kv_cols],
        kv_grad[:, kv_cols:],
        gains[2 * width : 2 * width + head],
        gains[2 * width + head :],
        output_grad,
        gains[width : 2 * width],
        gate_grad,
        up_grad,
        down_grad,
    )


def solution(mesh):
    positions = P("tensor", "dp", None)
    weight = P("dp", "tensor")
    return jax.shard_map(
        body,
        mesh=mesh,
        in_specs=(
            positions,
            P(),
            weight,
            weight,
            weight,
            P(),
            P(),
            weight,
            P(),
            weight,
            weight,
            weight,
            P("dp", None),
            positions,
        ),
        out_specs=(
            positions,
            positions,
            P(),
            weight,
            weight,
            weight,
            P(),
            P(),
            weight,
            P(),
            weight,
            weight,
            weight,
        ),
        check_vma=False,
    )
```

```python
import functools

import jax
import jax.numpy as jnp
import numpy as np
from jax import lax
from jax.experimental import pallas as pl
from jax.experimental.pallas import tpu as pltpu
from jax.sharding import PartitionSpec as P

epsilon = 1e-06
rope_base = 1000000.0
longest_document = 512
bf16 = jnp.bfloat16
f32 = jnp.float32


def mm(eq, a, b):
    return jnp.einsum(eq, a, b, preferred_element_type=f32)


def rms_parts(values, gain):
    inverse = lax.rsqrt(jnp.mean(values * values, axis=-1, keepdims=True) + epsilon)
    return values * inverse * gain, inverse


def rms_back(values, inverse, gain, upstream):
    normed = values * inverse
    inner = upstream * gain
    grad = inverse * (inner - normed * jnp.mean(inner * normed, axis=-1, keepdims=True))
    return grad, upstream * normed


def rope_tables(first, count, head_size):
    half = head_size // 2
    exponent = -(2.0 * np.arange(half, dtype=np.float32)) / np.float32(head_size)
    frequency = np.power(np.float32(rope_base), exponent, dtype=np.float32)
    angles = np.arange(first, first + count, dtype=np.float32)[:, None] * frequency[None, :]
    cosine = np.cos(angles.astype(np.float64)).astype(np.float32)
    sine = np.sin(angles.astype(np.float64)).astype(np.float32)
    return np.concatenate([cosine, cosine], axis=1), np.concatenate([-sine, sine], axis=1)


class Plan:
    def __init__(self):
        self.size = lax.axis_size("dp")
        self.index = lax.axis_index("dp")
        self.place = lax.axis_index("tensor")
        self.line = lax.axis_size("tensor")
        assert self.line == 4
        self.others = [1 << i for i in range(1, self.size.bit_length() - 1)]
        evens = [0]
        for bit in self.others:
            evens = evens + [m ^ bit for m in evens]
        self.evens = evens
        self.masks = evens + [m ^ 1 for m in evens]
        self.forward = self.others
        self.backward = self.others[::-1]

    def swap(self, value, bit):
        return lax.ppermute(value, "dp", [(i, i ^ bit) for i in range(self.size)])

    def move(self, value, pairs):
        return lax.ppermute(value, "tensor", pairs)

    def xor_blocks(self, blocks):
        bit = 1
        while bit < self.size:
            on = (self.index & bit) != 0
            blocks = [jnp.where(on, blocks[i ^ bit], blocks[i]) for i in range(self.size)]
            bit *= 2
        return blocks

    def to_masks(self, value):
        blocks = self.xor_blocks(jnp.split(value, self.size, axis=-1))
        return jnp.concatenate([blocks[m] for m in self.masks], axis=-1)

    def from_masks(self, value):
        parts = jnp.split(value, self.size, axis=-1)
        blocks = [parts[self.masks.index(m)] for m in range(self.size)]
        return jnp.concatenate(self.xor_blocks(blocks), axis=-1)

    def gather(self, shard, order):
        rows = shard.shape[0]
        held, masks = shard, [0]
        for bit in order:
            arrived = self.swap(held, bit)
            held = jnp.concatenate([held, arrived], axis=0)
            masks = masks + [m ^ bit for m in masks]
        if masks != self.evens:
            held = jnp.concatenate(
                [lax.slice_in_dim(held, masks.index(m) * rows, (masks.index(m) + 1) * rows) for m in self.evens],
                axis=0,
            )
        return held, self.swap(held, 1)

    def reduce(self, even, odd, order):
        rows = even.shape[0] // len(self.evens)
        total = even.astype(f32) + self.swap(odd.astype(bf16), 1).astype(f32)
        pieces = {
            m: lax.slice_in_dim(total, i * rows, (i + 1) * rows) for i, m in enumerate(self.evens)
        }
        for bit in order:
            leaving = [m for m in pieces if m & bit]
            sent = jnp.concatenate([pieces[m].astype(bf16) for m in leaving], axis=0)
            arrived = self.swap(sent, bit)
            kept = {m: v for m, v in pieces.items() if not m & bit}
            for i, m in enumerate(leaving):
                kept[m ^ bit] = kept[m ^ bit] + lax.slice_in_dim(
                    arrived, i * rows, (i + 1) * rows
                ).astype(f32)
            pieces = kept
        return pieces[0]

    def gather_line(self, own):
        from_right = self.move(own, [(1, 0), (2, 1), (3, 2)])
        from_left = self.move(own, [(0, 1), (1, 2), (2, 3)])
        right_two = self.move(from_right, [(1, 0), (2, 1)])
        left_two = self.move(from_left, [(1, 2), (2, 3)])
        slot_two = jnp.where(self.place < 2, right_two, left_two)
        last = self.move(slot_two, [(1, 0), (2, 3)])
        slot_one = jnp.where(self.place < 3, from_right, last)
        slot_three = jnp.where(self.place > 0, from_left, last)
        return [own, slot_one, slot_two, slot_three]

    def scatter_line(self, slots):
        zero, one, two, three = slots
        first = self.move(
            jnp.where(self.place == 3, one, three).astype(bf16), [(3, 2), (0, 1)]
        )
        middle = (two + first.astype(f32)).astype(bf16)
        leftward = self.move(middle, [(3, 2), (2, 1)])
        rightward = self.move(middle, [(0, 1), (1, 2)])
        leftward = self.move(
            (three + leftward.astype(f32)).astype(bf16), [(3, 2), (2, 1), (1, 0)]
        )
        rightward = self.move(
            (one + rightward.astype(f32)).astype(bf16), [(0, 1), (1, 2), (2, 3)]
        )
        return zero + leftward.astype(f32) + rightward.astype(f32)

    def total(self, value):
        bit = 1
        while bit < self.size:
            value = value + self.swap(value, bit)
            bit *= 2
        for bit in (1, 2):
            value = value + self.move(value, [(i, i ^ bit) for i in range(self.line)])
        return value


def after(value, *others):
    return lax.optimization_barrier((value,) + others)[0]


def mesh_copy(src, dst, send, recv, device):
    return pltpu.make_async_remote_copy(
        src_ref=src, dst_ref=dst, send_sem=send, recv_sem=recv, device_id=device,
        device_id_type=pl.DeviceIdType.MESH,
    )


class Links:
    def __init__(self, size):
        bits = [1 << i for i in range(1, size.bit_length() - 1)]
        self.orders = (bits, bits[::-1])
        evens = [0]
        for bit in bits:
            evens = evens + [m ^ bit for m in evens]
        self.evens = evens
        self.masks = evens + [m ^ 1 for m in evens]
        self.bits = bits

    def onward(self, half, mask):
        order = self.orders[half]
        last = max([i for i, bit in enumerate(order) if mask & bit], default=-1)
        return order[last + 1 :]


class Gather:
    def __init__(self, links, d, t, piece, send, recv):
        self.links, self.d, self.t = links, d, t
        self.piece, self.send, self.recv = piece, send, recv

    def copy(self, half, mask, bit):
        index = self.links.masks.index(mask ^ bit)
        return mesh_copy(
            self.piece(half, mask), self.piece(half, mask ^ bit), self.send(half, index),
            self.recv(half, index), (self.d ^ bit, self.t),
        )

    def launch(self):
        for step in range(len(self.links.bits)):
            for half in (0, 1):
                self.copy(half, 0, self.links.orders[half][step]).start()
        for half in (0, 1):
            self.copy(half, 0, 1).start()

    def arrive(self, half, mask):
        bit = [b for b in self.links.orders[half] if b & mask][-1]
        self.copy(half, mask ^ bit, bit).wait_recv()
        for other in self.links.onward(half, mask):
            self.copy(half, mask, other).start()
        self.copy(half, mask, 1).start()

    def onward(self):
        for mask in self.links.evens[1:]:
            for half in (0, 1):
                if self.links.onward(half, mask):
                    self.arrive(half, mask)

    def complete(self):
        for mask in self.links.evens[1:]:
            for half in (0, 1):
                if not self.links.onward(half, mask):
                    self.arrive(half, mask)
        for mask in self.links.evens:
            for half in (0, 1):
                self.copy(half, mask, 1).wait_recv()

    def finish(self):
        for mask in self.links.masks[1:]:
            for half in (0, 1):
                self.copy(half, mask ^ 1 if mask & 1 else 0, 1 if mask & 1 else mask).wait_send()


class Relay:
    def __init__(self, d, t, line, slot, send, recv):
        self.d, self.t, self.line = d, t, line
        self.slot, self.send, self.recv = slot, send, recv
        self.inner = (t > 0) & (t < line - 1)

    def copy(self, number, source, target, to):
        return mesh_copy(
            self.slot(source), self.slot(target), self.send.at[number], self.recv.at[target],
            (self.d, to),
        )

    def moves(self):
        t = self.t
        return (
            (t > 0, (0, 0, 1, t - 1)),
            (t < self.line - 1, (1, 0, 3, t + 1)),
            (self.inner, (2, 1, 2, t - 1)),
            (self.inner, (3, 3, 2, t + 1)),
            (t == 1, (4, 2, 3, t - 1)),
            (t == 2, (5, 2, 1, t + 1)),
        )

    def start(self, *numbers):
        for number in numbers:
            condition, route = self.moves()[number]

            @pl.when(condition)
            def _(route=route):
                self.copy(*route).start()

    def wait(self, slot):
        self.copy(0, 0, slot, self.t).wait_recv()

    def finish(self):
        for condition, route in self.moves():

            @pl.when(condition)
            def _(route=route):
                self.copy(*route).wait_send()

    def first(self):
        self.start(0, 1)

    def second(self):
        t, line = self.t, self.line

        @pl.when(t < line - 1)
        def _():
            self.wait(1)

        self.start(2)

        @pl.when(t > 0)
        def _():
            self.wait(3)

        self.start(3)

    def third(self):
        self.wait(2)
        self.start(4, 5)

    def ends(self):
        @pl.when(self.t == 0)
        def _():
            self.wait(3)

        @pl.when(self.t == self.line - 1)
        def _():
            self.wait(1)


def slot_of(i, t, line):
    far = jnp.where(t < line - 1, 1, 3)
    near = jnp.where(t < line - 1, 3, 1)
    return jnp.where(i == 0, 0, jnp.where(i == 1, far, jnp.where(i == 2, 2, near)))


def greet(links, d, t, line, across=False):
    barrier = pltpu.get_barrier_semaphore()
    if across:
        pl.semaphore_signal(barrier, inc=1, device_id=(d, t ^ 2), device_id_type=pl.DeviceIdType.MESH)
    for bit in [1] + links.bits:
        pl.semaphore_signal(barrier, inc=1, device_id=(d ^ bit, t), device_id_type=pl.DeviceIdType.MESH)

    @pl.when(t > 0)
    def _():
        pl.semaphore_signal(barrier, inc=1, device_id=(d, t - 1), device_id_type=pl.DeviceIdType.MESH)

    @pl.when(t < line - 1)
    def _():
        pl.semaphore_signal(barrier, inc=1, device_id=(d, t + 1), device_id_type=pl.DeviceIdType.MESH)

    pl.semaphore_wait(
        barrier,
        1 + across + len(links.bits) + jnp.where(t > 0, 1, 0) + jnp.where(t < line - 1, 1, 0),
    )


def nt(a, b):
    return lax.dot_general(a, b, (((1,), (1,)), ((), ())), preferred_element_type=f32)


def tn(a, b):
    return lax.dot_general(a, b, (((0,), (0,)), ((), ())), preferred_element_type=f32)


def nn(a, b):
    return jnp.dot(a, b, preferred_element_type=f32)


def head_norm(values, gain):
    inverse = lax.rsqrt(jnp.mean(values * values, axis=-1, keepdims=True) + epsilon)
    return values * inverse * gain


def segment_masks(segments, padded, t, rows, span):
    ahead = span - rows
    padded[...] = jnp.full(padded.shape, -1.0, f32)
    padded[0:1, ahead:] = segments[...].astype(f32)
    key_row = padded[0:1, pl.ds(pl.multiple_of(t * rows, 128), span)]
    return key_row, turned(key_row[:, ahead:])


def turned(row):
    return jnp.broadcast_to(row, (128, row.shape[1])).T[:, 0:1]


def forward_kernel(
    size, line, head,
    q_shard, k_shard, v_shard, o_shard, gate_shard, up_shard, rows_in, upstream, source, gain_qk, gain_two,
    cosine_in, sine_in, segments,
    weights_out, mlp_out, upstream_all, proj_q, proj_k, q_out, k_out, v_out, lse_out, att_out, middle, normed_out,
    full, rows_all, acc,
    z_send, z_recv, send, recv, row_send, row_recv, keep, mlp_send, mlp_recv, up_send, up_recv, local, cosine, sine, padded,
):
    links = Links(size)
    d, t = lax.axis_index("dp"), lax.axis_index("tensor")
    block = q_shard.shape[0]
    rows, width = rows_in.shape
    span = rows_all.shape[0]
    factor = head**-0.5

    def place(mask):
        return pl.ds(links.masks.index(mask) * block, block)

    def gather(slot):
        return Gather(
            links, d, t,
            lambda half, mask: full.at[half, slot, place(mask)],
            lambda half, index: send.at[slot, half, index],
            lambda half, index: recv.at[slot, half, index],
        )

    feed = Gather(
        links, d, t,
        lambda half, mask: mlp_out.at[half, place(mask)],
        lambda half, index: mlp_send.at[half, index],
        lambda half, index: mlp_recv.at[half, index],
    )
    relay = Relay(d, t, line, lambda slot: full.at[:, slot, place(0)], z_send, z_recv)
    upward = Relay(d, t, line, lambda slot: upstream_all.at[slot], up_send, up_recv)

    table = pl.ds(pl.multiple_of(t * rows, rows), span)
    o_half = 2 * head
    parts = (
        (q_shard, full.at[0, 0, place(0), 0 : 4 * head]),
        (o_shard.at[:, 0:o_half], full.at[0, 0, place(0), 4 * head : 6 * head]),
        (k_shard, full.at[1, 0, place(0), 0 : 2 * head]),
        (v_shard, full.at[1, 0, place(0), 2 * head : 4 * head]),
        (o_shard.at[:, o_half : 2 * o_half], full.at[1, 0, place(0), 4 * head : 6 * head]),
        (gate_shard, mlp_out.at[0, place(0)]),
        (up_shard, mlp_out.at[1, place(0)]),
        (upstream, upstream_all.at[0]),
        (cosine_in.at[table], cosine),
        (sine_in.at[table], sine),
    )
    own = [
        pltpu.make_async_copy(source_ref, target_ref, local.at[n])
        for n, (source_ref, target_ref) in enumerate(parts)
    ]
    for copy in own:
        copy.start()
    rows_all[pl.ds(span - rows, rows), :] = rows_in[...]

    @pl.when(t == 0)
    def _():
        rows_all[pl.ds(0, 2 * rows), :] = jnp.zeros((2 * rows, width), bf16)

    @pl.when(t == 1)
    def _():
        rows_all[pl.ds(0, rows), :] = jnp.zeros((rows, width), bf16)

    greet(links, d, t, line)
    for copy in own[:5]:
        copy.wait()

    row_one = mesh_copy(
        rows_in, rows_all.at[pl.ds(rows, rows)], row_send.at[0], row_recv.at[0], (d, t + 1)
    )
    row_two = mesh_copy(
        rows_all.at[pl.ds(rows, rows)], rows_all.at[pl.ds(0, rows)], row_send.at[1],
        row_recv.at[1], (d, t + 1),
    )
    inner = relay.inner
    relay.first()

    @pl.when(t < line - 1)
    def _():
        row_one.start()

    gather(0).launch()
    gather(0).onward()
    relay.second()
    second = slot_of(1, t, line)

    @pl.when(t < line - 1)
    def _():
        gather(1).launch()

    @pl.when(t == line - 1)
    def _():
        gather(3).launch()

    @pl.when(t > 0)
    def _():
        row_one.wait_recv()

    @pl.when(inner)
    def _():
        row_two.start()

    relay.third()
    gather(2).launch()
    gather(second).onward()

    @pl.when(t > 1)
    def _():
        row_two.wait_recv()

    for copy in own[5:]:
        copy.wait()
    key_row, query_column = segment_masks(segments, padded, t, rows, span)
    upward.first()
    acc[...] = source[...]

    lane = lax.broadcasted_iota(jnp.int32, (rows, 128), 1)
    q_index = lax.broadcasted_iota(jnp.int32, (rows, span), 0) + (span - rows)
    k_index = lax.broadcasted_iota(jnp.int32, (rows, span), 1)

    def step(i, carry):
        slot = slot_of(i, t, line)

        @pl.when(i == 1)
        def _():
            relay.ends()
            gather(slot_of(3, t, line)).launch()

        @pl.when(i >= 2)
        def _():
            gather(slot).onward()

        @pl.when((i == 2))
        def _():
            feed.launch()

        gather(slot).complete()
        for half in (0, 1):
            pltpu.make_async_copy(
                full.at[half, slot], weights_out.at[half, slot], keep.at[slot, half]
            ).start()

        own_rows = pl.ds(span - rows, rows)
        allowed = (query_column == key_row) & (k_index <= q_index)
        lse_acc = jnp.zeros((rows, 128), f32)
        for g in (0, 1):
            key_cols = slice(g * head, (g + 1) * head)
            if g == 0:
                for r in range(span // rows):
                    part = pl.ds(r * rows, rows)
                    both = nn(rows_all[part, :], full[1, slot, :, 0 : 4 * head])
                    if r == span // rows - 1:
                        proj_k[slot] = both[:, : 2 * head]
                    for h in (0, 1):
                        unit = head_norm(both[:, h * head : (h + 1) * head], gain_qk[1:2, :])
                        turned = unit * cosine[part, :] + pltpu.roll(unit, head // 2, 1) * sine[part, :]
                        k_out[slot, part, h * head : (h + 1) * head] = turned.astype(bf16)
                    v_out[slot, part, :] = both[:, 2 * head :].astype(bf16)
            for j in (0, 1):
                h = 2 * g + j
                cols = slice(h * head, (h + 1) * head)
                raw = nn(rows_in[...], full[0, slot, :, cols])
                proj_q[slot, :, cols] = raw
                unit = head_norm(raw, gain_qk[0:1, :])
                turned = unit * cosine[own_rows, :] + pltpu.roll(unit, head // 2, 1) * sine[own_rows, :]
                query = turned.astype(bf16)
                q_out[slot, :, cols] = query
                scores = nt(query, k_out[slot, :, key_cols]) * factor
                scores = jnp.where(allowed, scores, -1e30)
                top = jnp.max(scores, axis=-1, keepdims=True)
                weight = jnp.exp(scores - top)
                total = jnp.sum(weight, axis=-1, keepdims=True)
                probs = (weight / total).astype(bf16)
                att_out[slot, :, cols] = nn(probs, v_out[slot, :, key_cols]).astype(bf16)
                lse_acc = jnp.where(lane == h, top + jnp.log(total), lse_acc)
        lse_out[slot] = lse_acc
        for half in (0, 1):
            acc[...] += nt(
                att_out[slot, :, half * 2 * head : (half + 1) * 2 * head],
                full[half, slot, :, 4 * head : 6 * head],
            )

        @pl.when((i == 2))
        def _():
            upward.second()

        return carry

    lax.fori_loop(0, line, step, 0)
    upward.third()
    feed.onward()
    values = acc[...]
    middle[...] = values
    normed_out[...] = head_norm(values, gain_two[...]).astype(bf16)
    feed.complete()

    def finish(i, carry):
        gather(i).finish()
        for half in (0, 1):
            pltpu.make_async_copy(full.at[half, i], weights_out.at[half, i], keep.at[i, half]).wait()
        return carry

    lax.fori_loop(0, line, finish, 0)
    feed.finish()
    relay.finish()

    @pl.when(t < line - 1)
    def _():
        row_one.wait_send()

    @pl.when(inner)
    def _():
        row_two.wait_send()

    upward.ends()
    upward.finish()


def attention_forward(weights, mlp, rows_one, upstream, source, gain_qk, gain_two, tables, segments, size, line):
    cols = 3 * weights[0].shape[1] // 2
    rows, width = rows_one.shape
    length = segments.shape[1]
    span = tables[0].shape[0] - length + rows
    head = gain_qk.shape[1]
    pieces = 2 * (size // 2)
    vmem = pl.BlockSpec(memory_space=pltpu.VMEM)
    hbm = pl.BlockSpec(memory_space=pl.ANY)
    shape = jax.ShapeDtypeStruct
    return pl.pallas_call(
        functools.partial(forward_kernel, size, line, head),
        out_shape=(
            shape((2, line, width, cols), bf16),
            shape((2, width, mlp[0].shape[1]), bf16),
            shape((line, rows, width), bf16),
            shape((line, rows, 4 * head), f32),
            shape((line, rows, 2 * head), f32),
            shape((line, rows, 4 * head), bf16),
            shape((line, span, 2 * head), bf16),
            shape((line, span, 2 * head), bf16),
            shape((line, rows, 128), f32),
            shape((line, rows, 4 * head), bf16),
            shape((rows, width), f32),
            shape((rows, width), bf16),
        ),
        in_specs=[hbm] * 4 + [vmem] * 7 + [hbm] * 2 + [vmem],
        out_specs=[hbm] * 3 + [vmem] * 9,
        scratch_shapes=[
            pltpu.VMEM((2, line, width, cols), bf16),
            pltpu.VMEM((span, width), bf16),
            pltpu.VMEM((rows, width), f32),
            pltpu.SemaphoreType.DMA((6,)),
            pltpu.SemaphoreType.DMA((line,)),
            pltpu.SemaphoreType.DMA((line, 2, pieces)),
            pltpu.SemaphoreType.DMA((line, 2, pieces)),
            pltpu.SemaphoreType.DMA((2,)),
            pltpu.SemaphoreType.DMA((2,)),
            pltpu.SemaphoreType.DMA((line, 2)),
            pltpu.SemaphoreType.DMA((2, pieces)),
            pltpu.SemaphoreType.DMA((2, pieces)),
            pltpu.SemaphoreType.DMA((6,)),
            pltpu.SemaphoreType.DMA((line,)),
            pltpu.SemaphoreType.DMA((10,)),
            pltpu.VMEM((span, head), f32),
            pltpu.VMEM((span, head), f32),
            pltpu.VMEM((8, tables[0].shape[0]), f32),
        ],
        compiler_params=pltpu.CompilerParams(
            collective_id=0, has_side_effects=True, vmem_limit_bytes=62 << 20
        ),
        cost_estimate=pl.CostEstimate(flops=40 << 30, bytes_accessed=200 << 20, transcendentals=4 << 20),
    )(*weights, *mlp, rows_one, upstream, source, gain_qk, gain_two, *tables, segments)


def feed_kernel(
    size, line,
    rows_in, upstream_in, pair_in, down_in,
    rows_out, hidden_out, gate_out, up_out, grad_out, mixed_out,
    rows_v, upstream_v, pair, down, gate_f, up_f, hidden_v, gate_v, up_v, grad_v, mixed_v,
    z_send, z_recv, send, recv, local, leave,
):
    links = Links(size)
    d, t = lax.axis_index("dp"), lax.axis_index("tensor")
    block = down_in.shape[0]
    _, rows, width = rows_v.shape
    units = hidden_v.shape[2]
    chunk = units // 4
    piece = width // 4

    def place(mask):
        return pl.ds(links.masks.index(mask) * block, block)

    gather = Gather(
        links, d, t,
        lambda half, mask: down.at[half, place(mask)],
        lambda half, index: send.at[half, index],
        lambda half, index: recv.at[half, index],
    )
    relay = Relay(d, t, line, lambda slot: rows_v.at[slot], z_send, z_recv)
    arrivals = (
        pltpu.make_async_copy(rows_in, rows_v.at[0], local.at[0]),
        pltpu.make_async_copy(down_in.at[:, 0 : units // 2], down.at[0, place(0)], local.at[1]),
        pltpu.make_async_copy(down_in.at[:, units // 2 :], down.at[1, place(0)], local.at[4]),
        pltpu.make_async_copy(pair_in, pair, local.at[2]),
        pltpu.make_async_copy(upstream_in, upstream_v, local.at[3]),
    )
    for copy in arrivals:
        copy.start()
    greet(links, d, t, line)
    arrivals[0].wait()
    relay.first()
    arrivals[1].wait()
    arrivals[2].wait()
    gather.launch()
    gather.onward()
    arrivals[3].wait()
    arrivals[4].wait()

    def departures(slot):
        position = lax.rem(slot + t, line)
        natural = pl.ds(pl.multiple_of(position * rows, rows), rows)
        return [
            pltpu.make_async_copy(rows_v.at[slot], rows_out.at[slot], leave.at[0, slot]),
            pltpu.make_async_copy(hidden_v.at[slot], hidden_out.at[slot], leave.at[1, slot]),
            pltpu.make_async_copy(gate_v.at[slot], gate_out.at[slot], leave.at[2, slot]),
            pltpu.make_async_copy(up_v.at[slot], up_out.at[slot], leave.at[3, slot]),
            pltpu.make_async_copy(grad_v.at[slot], grad_out.at[natural], leave.at[4, slot]),
            pltpu.make_async_copy(mixed_v.at[slot], mixed_out.at[natural], leave.at[5, slot]),
        ]

    def step(i, carry):
        slot = slot_of(i, t, line)
        for c in range(4):
            cols = slice(c * chunk, (c + 1) * chunk)
            gate = nn(rows_v[slot], pair[0, :, cols])
            up = nn(rows_v[slot], pair[1, :, cols])
            gate_f[:, cols] = gate
            up_f[:, cols] = up
            hidden_v[slot, :, cols] = (gate * jax.nn.sigmoid(gate) * up).astype(bf16)

        @pl.when(i == 0)
        def _():
            relay.second()
            gather.complete()

        @pl.when(i == 1)
        def _():
            relay.third()

        @pl.when(i == 2)
        def _():
            relay.ends()

        for c in range(4):
            cols = slice(c * chunk, (c + 1) * chunk)
            inner = slice((c % 2) * chunk, (c % 2 + 1) * chunk)
            grad_hidden = nn(upstream_v[slot], down[c // 2, :, inner])
            gate, up = gate_f[:, cols], up_f[:, cols]
            sigmoid = jax.nn.sigmoid(gate)
            gate_v[slot, :, cols] = (
                grad_hidden * up * sigmoid * (1.0 + gate * (1.0 - sigmoid))
            ).astype(bf16)
            up_v[slot, :, cols] = (grad_hidden * (gate * sigmoid)).astype(bf16)
        for n in range(4):
            out = slice(n * piece, (n + 1) * piece)
            grad_v[slot, :, out] = (
                nt(gate_v[slot], pair[0, out, :]) + nt(up_v[slot], pair[1, out, :])
            ).astype(bf16)
            mixed_v[slot, :, out] = (
                nt(hidden_v[slot, :, : units // 2], down[0, out, :])
                + nt(hidden_v[slot, :, units // 2 :], down[1, out, :])
            ).astype(bf16)
        for copy in departures(slot):
            copy.start()
        return carry

    lax.fori_loop(0, line, step, 0)

    def finish(i, carry):
        for copy in departures(i):
            copy.wait()
        return carry

    lax.fori_loop(0, line, finish, 0)
    gather.finish()
    relay.finish()


def feed_forward(rows_own, upstream_all, pair_full, down_shard, size, line):
    rows, width = rows_own.shape
    units = pair_full.shape[2]
    hbm = pl.BlockSpec(memory_space=pl.ANY)
    shape = jax.ShapeDtypeStruct
    dma = pltpu.SemaphoreType.DMA
    return pl.pallas_call(
        functools.partial(feed_kernel, size, line),
        out_shape=(
            shape((line, rows, width), bf16),
            shape((line, rows, units), bf16),
            shape((line, rows, units), bf16),
            shape((line, rows, units), bf16),
            shape((line * rows, width), bf16),
            shape((line * rows, width), bf16),
        ),
        in_specs=[hbm] * 4,
        out_specs=[hbm] * 6,
        scratch_shapes=[
            pltpu.VMEM((line, rows, width), bf16),
            pltpu.VMEM((line, rows, width), bf16),
            pltpu.VMEM((2, width, units), bf16),
            pltpu.VMEM((2, width, units // 2), bf16),
            pltpu.VMEM((rows, units), f32),
            pltpu.VMEM((rows, units), f32),
            pltpu.VMEM((line, rows, units), bf16),
            pltpu.VMEM((line, rows, units), bf16),
            pltpu.VMEM((line, rows, units), bf16),
            pltpu.VMEM((line, rows, width), bf16),
            pltpu.VMEM((line, rows, width), bf16),
            dma((6,)),
            dma((line,)),
            dma((2, size)),
            dma((2, size)),
            dma((5,)),
            dma((6, line)),
        ],
        compiler_params=pltpu.CompilerParams(
            collective_id=1, has_side_effects=True, vmem_limit_bytes=62 << 20
        ),
        cost_estimate=pl.CostEstimate(flops=40 << 30, bytes_accessed=60 << 20, transcendentals=3 << 20),
    )(rows_own, upstream_all, pair_full, down_shard)


class Scatter:
    def __init__(self, links, d, t, block, refs, semaphores):
        self.links, self.d, self.t, self.block = links, d, t, block
        self.odd, self.core, self.sums, self.arrived, self.out = refs
        self.core_send, self.core_recv, self.send, self.recv = semaphores

    @staticmethod
    def pieces(links):
        return max(1, len(links.evens) - 1)

    def steps(self, half):
        masks, number, found = self.links.evens, 0, []
        for bit in self.links.orders[half][::-1]:
            masks = [m for m in masks if not m & bit]
            found.append((bit, [(m, number + i) for i, m in enumerate(masks)]))
            number += len(masks)
        return found

    def rows(self, mask):
        return pl.ds(self.links.evens.index(mask) * self.block, self.block)

    def core_copy(self, j):
        return mesh_copy(
            self.odd(j), self.core(j), self.core_send(j), self.core_recv(j), (self.d ^ 1, self.t)
        )

    def piece_copy(self, j, mask, number, bit):
        return mesh_copy(
            self.sums(j, self.rows(mask ^ bit)), self.arrived(j, number), self.send(j, number),
            self.recv(j, number), (self.d ^ bit, self.t),
        )

    def launch(self, j, half, step):
        steps = self.steps(half)
        if step < len(steps):
            bit, pairs = steps[step]
            for mask, number in pairs:
                self.piece_copy(j, mask, number, bit).start()

    def add(self, j, mask, value):
        if mask == 0:
            out = self.out(j)
            out[...] = out[...] + value[...].astype(f32)
        else:
            total = self.sums(j, self.rows(mask))
            total[...] = (total[...].astype(f32) + value[...].astype(f32)).astype(bf16)

    def stage(self, j, half, stage):
        if stage == 0:
            self.core_copy(j).wait_recv()
            steps = self.steps(half)
            first = steps[0][0] if steps else 0
            for mask in sorted(self.links.evens, key=lambda m: not m & first):
                self.add(j, mask, self.core(j, self.rows(mask)))
        else:
            bit, pairs = self.steps(half)[stage - 1]
            for mask, number in pairs[::-1]:
                self.piece_copy(j, mask, number, bit).wait_recv()
                self.add(j, mask, self.arrived(j, number))
        self.launch(j, half, stage)

    def finish(self, j, half, core=True):
        if core:
            self.core_copy(j).wait_send()
        for bit, pairs in self.steps(half):
            for mask, number in pairs:
                self.piece_copy(j, mask, number, bit).wait_send()


def greet_dp(links, d, t):
    barrier = pltpu.get_barrier_semaphore()
    for bit in [1] + links.bits:
        pl.semaphore_signal(barrier, inc=1, device_id=(d ^ bit, t), device_id_type=pl.DeviceIdType.MESH)
    pl.semaphore_wait(barrier, 1 + len(links.bits))


class LineSum:
    def __init__(self, d, t, line, source, ends, outbox, inbox, semaphores):
        self.d, self.t, self.line = d, t, line
        self.source, self.ends, self.outbox, self.inbox = source, ends, outbox, inbox
        self.send, self.recv, self.local = semaphores
        self.rows = outbox.shape[1]

    def block(self, position):
        return self.source.at[pl.ds(pl.multiple_of(position * self.rows, self.rows), self.rows)]

    def hop(self, number, source, target, to):
        return mesh_copy(source, target, self.send.at[number], self.recv.at[number], (self.d, to))

    def hops(self):
        t, line = self.t, self.line
        return (
            (t == 0, lambda: self.hop(0, self.block(line - 1), self.inbox.at[0], t + 1)),
            (t == line - 1, lambda: self.hop(0, self.block(0), self.inbox.at[0], t - 1)),
            (t >= 2, lambda: self.hop(1, self.outbox.at[0], self.inbox.at[1], t - 1)),
            (t <= 1, lambda: self.hop(2, self.outbox.at[0], self.inbox.at[2], t + 1)),
            (t > 0, lambda: self.hop(3, self.outbox.at[1], self.ends[0], t - 1)),
            (t < line - 1, lambda: self.hop(4, self.outbox.at[2], self.ends[1], t + 1)),
        )

    def start(self, *numbers):
        for number in numbers:
            condition, make = self.hops()[number]

            @pl.when(condition)
            def _(make=make):
                make().start()

    def own(self, box, step):
        position = lax.rem(self.t + step, self.line)
        return pltpu.make_async_copy(self.block(position), self.outbox.at[box], self.local.at[box])

    def take(self, box, number):
        @pl.when((self.t > 0) & (self.t < self.line - 1))
        def _():
            self.hop(number, self.outbox.at[0], self.inbox.at[number], self.t + 1).wait_recv()
            self.outbox[box] = (
                self.outbox[box].astype(f32) + self.inbox[number].astype(f32)
            ).astype(bf16)

    def first(self):
        self.start(0, 1)
        for box, step in ((0, 2), (1, 3), (2, 1)):
            self.own(box, step).start()

    def second(self):
        self.own(0, 2).wait()
        self.take(0, 0)
        self.start(2, 3)

    def third(self):
        self.own(1, 3).wait()
        self.own(2, 1).wait()
        self.take(1, 1)
        self.take(2, 2)
        self.start(4, 5)

    def finish(self):
        for condition, make in self.hops():

            @pl.when(condition)
            def _(make=make):
                make().wait_send()

        @pl.when(self.t < self.line - 1)
        def _():
            self.hop(3, self.outbox.at[1], self.ends[0], self.t + 1).wait_recv()

        @pl.when(self.t > 0)
        def _():
            self.hop(4, self.outbox.at[2], self.ends[1], self.t - 1).wait_recv()


def weight_kernel(
    size, line,
    rows_in, upstream_in, gate_in, up_in, hidden_in, grad_in,
    gate_out, up_out, down_out, sum_left, sum_right,
    outbox, inbox, raw, left, right, odd, core, sums, arrived, out,
    core_send, core_recv, send, recv, local, raw_sem, leave, sum_send, sum_recv, sum_local,
):
    links = Links(size)
    d, t = lax.axis_index("dp"), lax.axis_index("tensor")
    width = left.shape[1]
    rows = raw.shape[1]
    ring, tokens, chunk = right.shape
    count = out.shape[0]
    middle = width // 2
    block = out.shape[1]
    pairs = count // 2
    wide = gate_in.shape[1] // chunk

    def load(j):
        p, h = j // 2, j % 2
        if p < wide:
            source, at = (gate_in, up_in)[h], p
        else:
            source, at = hidden_in, p - wide + h * (wide // 2)
        return pltpu.make_async_copy(
            source.at[:, at * chunk : (at + 1) * chunk], right.at[j % ring], local.at[j]
        )

    def store(j):
        p, h = j // 2, j % 2
        if p < wide:
            target, at = (gate_out, up_out)[h], p
        else:
            target, at = down_out, p - wide + h * (wide // 2)
        return pltpu.make_async_copy(
            out.at[j], target.at[:, at * chunk : (at + 1) * chunk], leave.at[j]
        )

    def fetch(k, r):
        source = (rows_in, upstream_in)[k]
        slot = (k * line + r) % 2
        return pltpu.make_async_copy(source.at[r], raw.at[slot], raw_sem.at[slot]), slot

    fetch(0, 0)[0].start()
    for j in range(ring):
        load(j).start()
    greet(links, d, t, line)
    gradient = LineSum(
        d, t, line, grad_in, (sum_left, sum_right), outbox, inbox, (sum_send, sum_recv, sum_local)
    )
    gradient.first()

    def turn(k):
        for r in range(line):
            copy, slot = fetch(k, r)
            copy.wait()
            following = k * line + r + 1
            if following < 2 * line:
                fetch(following // line, following % line)[0].start()
            left[k, :, r * rows : (r + 1) * rows] = raw[slot].T

    engine = Scatter(
        links, d, t, block,
        (
            lambda j: odd.at[j],
            lambda j, at=pl.ds(0, middle): core.at[j, at],
            lambda j, at: sums.at[j, at],
            lambda j, number: arrived.at[j, number],
            lambda j: out.at[j],
        ),
        (
            lambda j: core_send.at[j],
            lambda j: core_recv.at[j],
            lambda j, number: send.at[j, number],
            lambda j, number: recv.at[j, number],
        ),
    )
    turn(0)

    def step(p, carry):
        @pl.when(p == wide // 2)
        def _():
            gradient.second()
            turn(1)

        @pl.when(p == 3)
        def _():
            gradient.third()

        for q in range(pairs):

            @pl.when(p == q)
            def _(q=q):
                load(2 * q).wait()
                load(2 * q + 1).wait()

        @pl.when(p < pairs)
        def _():
            k = jnp.where(p < wide, 0, 1)
            for h in (0, 1):
                j = 2 * p + h
                for r in range(middle // 256):
                    at = pl.ds(middle + r * 256, 256)
                    odd[j, pl.ds(r * 256, 256), :] = nn(
                        left[k, at, :], right[lax.rem(j, ring)]
                    ).astype(bf16)
                engine.core_copy(j).start()
            for h in (0, 1):
                j = 2 * p + h
                for r in range(middle // 256):
                    at = pl.ds(r * 256, 256)
                    value = nn(left[k, at, :], right[lax.rem(j, ring)])
                    sums[j, at, :] = value.astype(bf16)
                    if r == 0:
                        out[j] = value[:block]

        for q in range(pairs - ring // 2):

            @pl.when(p == q)
            def _(q=q):
                load(2 * q + ring).start()
                load(2 * q + ring + 1).start()

        for stage in range(len(links.bits) + 1):
            @pl.when((p >= stage + 1) & (p < pairs + stage + 1))
            def _(stage=stage):
                for h in (0, 1):
                    engine.stage(2 * (p - stage - 1) + h, h, stage)

        return carry

    lax.fori_loop(0, pairs + len(links.bits) + 1, step, 0)
    for j in range(count):
        store(j).start()

    def finish(p, carry):
        for h in (0, 1):
            engine.finish(2 * p + h, h)
        return carry

    lax.fori_loop(0, pairs, finish, 0)
    for j in range(count):
        store(j).wait()
    gradient.finish()


def feed_weights(rows_all, upstream_all, gate, up, hidden, grad, size):
    line, rows, width = rows_all.shape
    tokens, units = gate.shape
    chunk = units // 4
    count = 3 * 4
    block = width // size
    middle = width // 2
    pieces = Scatter.pieces(Links(size))
    hbm = pl.BlockSpec(memory_space=pl.ANY)
    shape = jax.ShapeDtypeStruct
    dma = pltpu.SemaphoreType.DMA
    return pl.pallas_call(
        functools.partial(weight_kernel, size, line),
        out_shape=(shape((block, units), f32),) * 3 + (shape((rows, width), bf16),) * 2,
        in_specs=[hbm] * 6,
        out_specs=[hbm] * 5,
        scratch_shapes=[
            pltpu.VMEM((3, rows, width), bf16),
            pltpu.VMEM((3, rows, width), bf16),
            pltpu.VMEM((2, rows, width), bf16),
            pltpu.VMEM((2, width, tokens), bf16),
            pltpu.VMEM((4, tokens, chunk), bf16),
            pltpu.VMEM((count, middle, chunk), bf16),
            pltpu.VMEM((count, middle, chunk), bf16),
            pltpu.VMEM((count, middle, chunk), bf16),
            pltpu.VMEM((count, pieces, block, chunk), bf16),
            pltpu.VMEM((count, block, chunk), f32),
            dma((count,)),
            dma((count,)),
            dma((count, pieces)),
            dma((count, pieces)),
            dma((count,)),
            dma((2,)),
            dma((count,)),
            dma((5,)),
            dma((5,)),
            dma((3,)),
        ],
        compiler_params=pltpu.CompilerParams(
            collective_id=2, has_side_effects=True, vmem_limit_bytes=63 << 20
        ),
        cost_estimate=pl.CostEstimate(flops=20 << 30, bytes_accessed=60 << 20, transcendentals=0),
    )(rows_all, upstream_all, gate, up, hidden, grad)


def spread_stages(engine, links, first, last, p):
    for stage in range(len(links.bits) + 1)[::-1]:
        @pl.when((p - stage >= first) & (p - stage < last))
        def _(stage=stage):
            for h in (0, 1):
                engine.stage(2 * (p - stage) + h, h, stage)


def backward_kernel(
    size, line, head,
    branch, weights, q_in, k_in, v_in, lse_in, att_in, proj_q, proj_k, gain_qk, cosine_in, sine_in,
    segments, mixed_in,
    gq_out, gkv_out, terms_out, o_out, mixed_out,
    o_full, branch_t, gatt, own_kv, near_f, far_v, near_v, far_in, near_in, odd, core, sums, arrived, out,
    core_send, core_recv, send, recv, far_send, far_recv, near_send, near_recv, local,
    line_send, line_recv, cosine, sine, padded, table_sem,
):
    links = Links(size)
    d, t = lax.axis_index("dp"), lax.axis_index("tensor")
    rows, width = branch.shape
    span = k_in.shape[1]
    middle = width // 2
    block = out.shape[1]
    factor = head**-0.5
    loads = [
        pltpu.make_async_copy(
            weights.at[h, s, :, 4 * head : 6 * head], o_full.at[s, h], local.at[s, h]
        )
        for s in range(line)
        for h in (0, 1)
    ]
    table = pl.ds(pl.multiple_of(t * rows + span - rows, rows), rows)
    loads = loads + [
        pltpu.make_async_copy(cosine_in.at[table], cosine, table_sem.at[0]),
        pltpu.make_async_copy(sine_in.at[table], sine, table_sem.at[1]),
    ]
    for copy in loads:
        copy.start()
    greet(links, d, t, line)

    def hop(at, to):
        return mesh_copy(
            mixed_in.at[pl.ds(at * rows, rows)], mixed_out, line_send.at[0], line_recv.at[0], (d, to)
        )

    def hop_of(act):
        @pl.when(t == 0)
        def _():
            act(hop(line - 1, t + 1))

        @pl.when(t == line - 1)
        def _():
            act(hop(0, t - 1))

    hop_of(lambda copy: copy.start())

    engine = Scatter(
        links, d, t, block,
        (
            lambda j: odd.at[j],
            lambda j, at=pl.ds(0, middle): core.at[j, at],
            lambda j, at: sums.at[j, at],
            lambda j, number: arrived.at[j, number],
            lambda j: out.at[j],
        ),
        (
            lambda j: core_send.at[j],
            lambda j: core_recv.at[j],
            lambda j, number: send.at[j, number],
            lambda j, number: recv.at[j, number],
        ),
    )
    branch_t[...] = branch[...].T

    def first(s, carry):
        for h in (0, 1):
            j = 2 * s + h
            right = att_in[s, :, h * 2 * head : (h + 1) * 2 * head]
            odd[j] = nn(branch_t[middle:, :], right).astype(bf16)
            engine.core_copy(j).start()
        for h in (0, 1):
            j = 2 * s + h
            right = att_in[s, :, h * 2 * head : (h + 1) * 2 * head]
            value = nn(branch_t[:middle, :], right)
            sums[j] = value.astype(bf16)
            out[j] = value[:block]
        return carry

    lax.fori_loop(0, line, first, 0)
    for copy in loads:
        copy.wait()

    key_row, _ = segment_masks(segments, padded, t, rows, span)
    key_column = turned(key_row)
    query_row = key_row[:, span - rows :]
    k_index = lax.broadcasted_iota(jnp.int32, (span, rows), 0)
    q_index = lax.broadcasted_iota(jnp.int32, (span, rows), 1) + (span - rows)

    def far_copy(slot):
        return mesh_copy(
            far_v.at[slot], far_in.at[lax.rem(slot + 1, line)], far_send.at[slot],
            far_recv.at[lax.rem(slot + 1, line)], (d, t - 1),
        )

    def near_copy(slot):
        return mesh_copy(
            near_v.at[slot], near_in.at[lax.rem(slot + 1, line)], near_send.at[slot],
            near_recv.at[lax.rem(slot + 1, line)], (d, t - 1),
        )

    def arriving(copy, slot):
        return copy(lax.rem(slot + line - 1, line))

    def pass_near(slot):
        @pl.when((t > 0) & (t < line - 1))
        def _():
            arriving(far_copy, slot).wait_recv()
            near_v[slot] = (near_f[slot] + far_in[slot].astype(f32)).astype(bf16)

        @pl.when(t == line - 1)
        def _():
            near_v[slot] = near_f[slot].astype(bf16)

        @pl.when(t > 0)
        def _():
            near_copy(slot).start()

    def head_back(raw, gain, value, cos, sin):
        c = value * cos + pltpu.roll(value * sin, head // 2, 1)
        inverse = lax.rsqrt(jnp.mean(raw * raw, axis=-1, keepdims=True) + epsilon)
        normed = raw * inverse
        inner = c * gain
        grad = inverse * (inner - normed * jnp.mean(inner * normed, axis=-1, keepdims=True))
        return grad, jnp.sum(c * normed, axis=0, keepdims=True)

    terms_out[...] = jnp.zeros(terms_out.shape, f32)

    def step(s, carry):
        allowed = (key_column == query_row) & (k_index <= q_index)
        for h in (0, 1):
            gatt[:, h * 2 * head : (h + 1) * 2 * head] = nn(branch[...], o_full[s, h]).astype(bf16)
        lse = lse_in[s].T
        for g in (0, 1):
            keys = k_in[s, :, g * head : (g + 1) * head]
            values = v_in[s, :, g * head : (g + 1) * head]
            grad_k = jnp.zeros((span, head), f32)
            grad_v = jnp.zeros((span, head), f32)
            for j in (0, 1):
                h = 2 * g + j
                cols = slice(h * head, (h + 1) * head)
                query = q_in[s, :, cols]
                upward = gatt[:, cols]
                scores = nt(keys, query) * factor
                scores = jnp.where(allowed, scores, -1e30)
                probs = jnp.exp(scores - lse[h : h + 1, :])
                grad_probs = nt(values, upward)
                delta = jnp.sum(probs * grad_probs, axis=0, keepdims=True)
                grad_scores = (probs * (grad_probs - delta)).astype(bf16)
                grad_k = grad_k + nn(grad_scores, query)
                grad_v = grad_v + nn(probs.astype(bf16), upward)
                grad_q = (tn(grad_scores, keys) * factor).astype(bf16).astype(f32)
                grad, term = head_back(proj_q[s, :, cols], gain_qk[0:1, :], grad_q, cosine[...], sine[...])
                gq_out[s, :, cols] = grad.astype(bf16)
                terms_out[0:1, :] += term
            grad_k = grad_k * factor
            for at, value in ((g * head, grad_k), ((2 + g) * head, grad_v)):
                far_v[s, :, at : at + head] = value[:rows].astype(bf16)
                near_f[s, :, at : at + head] = value[rows : 2 * rows]
                own_kv[s, :, at : at + head] = value[2 * rows :]

        @pl.when(t > 1)
        def _():
            far_copy(s).start()

        spread_stages(engine, links, 0, line, s)

        @pl.when(s > 0)
        def _():
            pass_near(s)

        return carry

    lax.fori_loop(0, line, step, 0)
    pass_near(0)

    def last(i, carry):
        s = lax.rem(i + 2, line)
        spread_stages(engine, links, 0, line, i + line)

        @pl.when(t < line - 1)
        def _():
            arriving(near_copy, s).wait_recv()
            own_kv[s] = own_kv[s] + near_in[s].astype(f32)

        for g in (0, 1):
            cols = slice(g * head, (g + 1) * head)
            value = own_kv[s, :, cols].astype(bf16).astype(f32)
            grad, term = head_back(proj_k[s, :, cols], gain_qk[1:2, :], value, cosine[...], sine[...])
            gkv_out[s, :, cols] = grad.astype(bf16)
            terms_out[1:2, :] += term
        gkv_out[s, :, 2 * head :] = own_kv[s, :, 2 * head :].astype(bf16)
        return carry

    lax.fori_loop(0, line, last, 0)

    def finish(s, carry):
        for h in (0, 1):
            engine.finish(2 * s + h, h)
            o_out[s, :, h * 2 * head : (h + 1) * 2 * head] = out[2 * s + h]

        @pl.when(t > 1)
        def _():
            far_copy(s).wait_send()

        @pl.when(t > 0)
        def _():
            near_copy(s).wait_send()

        return carry

    lax.fori_loop(0, line, finish, 0)

    hop_of(lambda copy: copy.wait_send())

    @pl.when((t > 0) & (t < line - 1))
    def _():
        hop(0, t - 1).wait_recv()


def attention_backward(branch, weights, q, k, v, lse, att, proj_q, proj_k, gain_qk, tables, segments, mixed, size):
    line, rows, q_cols = q.shape
    width = branch.shape[1]
    span = k.shape[1]
    head = gain_qk.shape[1]
    block, middle, count, chunk = width // size, width // 2, 2 * line, 2 * head
    pieces = Scatter.pieces(Links(size))
    vmem = pl.BlockSpec(memory_space=pltpu.VMEM)
    hbm = pl.BlockSpec(memory_space=pl.ANY)
    shape = jax.ShapeDtypeStruct
    dma = pltpu.SemaphoreType.DMA
    return pl.pallas_call(
        functools.partial(backward_kernel, size, line, head),
        out_shape=(
            shape((line, rows, 4 * head), bf16),
            shape((line, rows, 4 * head), bf16),
            shape((8, head), f32),
            shape((line, block, 4 * head), f32),
            shape((rows, width), bf16),
        ),
        in_specs=[vmem, hbm] + [vmem] * 8 + [hbm] * 2 + [vmem] + [hbm],
        out_specs=[vmem] * 4 + [hbm],
        scratch_shapes=[
            pltpu.VMEM((line, 2, width, 2 * head), bf16),
            pltpu.VMEM((width, rows), bf16),
            pltpu.VMEM((rows, 4 * head), bf16),
            pltpu.VMEM((line, rows, 4 * head), f32),
            pltpu.VMEM((line, rows, 4 * head), f32),
            pltpu.VMEM((line, rows, 4 * head), bf16),
            pltpu.VMEM((line, rows, 4 * head), bf16),
            pltpu.VMEM((line, rows, 4 * head), bf16),
            pltpu.VMEM((line, rows, 4 * head), bf16),
            pltpu.VMEM((count, middle, chunk), bf16),
            pltpu.VMEM((count, middle, chunk), bf16),
            pltpu.VMEM((count, middle, chunk), bf16),
            pltpu.VMEM((count, pieces, block, chunk), bf16),
            pltpu.VMEM((count, block, chunk), f32),
            dma((count,)),
            dma((count,)),
            dma((count, pieces)),
            dma((count, pieces)),
            dma((line,)),
            dma((line,)),
            dma((line,)),
            dma((line,)),
            dma((line, 2)),
            dma((1,)),
            dma((1,)),
            pltpu.VMEM((rows, head), f32),
            pltpu.VMEM((rows, head), f32),
            pltpu.VMEM((8, span - rows + line * rows), f32),
            dma((2,)),
        ],
        compiler_params=pltpu.CompilerParams(
            collective_id=3, has_side_effects=True, vmem_limit_bytes=62 << 20
        ),
        cost_estimate=pl.CostEstimate(flops=20 << 30, bytes_accessed=40 << 20, transcendentals=4 << 20),
    )(branch, weights, q, k, v, lse, att, proj_q, proj_k, gain_qk, *tables, segments, mixed)


def final_kernel(
    size, line, head,
    rows_in, gq_in, gkv_in, o_in, weights, source, grad_middle, gain_one, second_terms, head_terms,
    mixed_two, mixed_in,
    q_out, kv_out, o_out, input_out, terms_out, mixed_left, mixed_right,
    rows_t, pair, acc, odd, core, sums, arrived, out, outbox, inbox, heap, mixed_box, mixed_mail,
    core_send, core_recv, send, recv, local, line_send, line_recv, heap_send, heap_recv, mixed_send, mixed_recv, mixed_local,
):
    links = Links(size)
    d, t = lax.axis_index("dp"), lax.axis_index("tensor")
    rows, width = rows_in.shape
    middle = width // 2
    block = out.shape[1]
    chunk = 4 * head
    last_stage = len(links.bits)
    inner = (t > 0) & (t < line - 1)
    is_end = (t == 0) | (t == line - 1)

    def slot_at(i):
        return slot_of(line - 1 - i, t, line)

    def load(i, h):
        return pltpu.make_async_copy(
            weights.at[h, slot_at(i), :, 0 : 4 * head], pair.at[h], local.at[h]
        )

    for h in (0, 1):
        load(0, h).start()
    inside = block % 128 == 0
    greet(links, d, t, line, inside)

    def mixed_hop(number):
        source, target, to = (
            (mixed_two, mixed_mail.at[0], t - 1),
            (mixed_two, mixed_mail.at[1], t + 1),
            (mixed_box.at[0], mixed_left, t - 1),
            (mixed_box.at[1], mixed_right, t + 1),
        )[number]
        return mesh_copy(source, target, mixed_send.at[number], mixed_recv.at[number], (d, to))

    def mixed_own(box):
        position = lax.rem(t + (3, 1)[box], line)
        at = pl.ds(pl.multiple_of(position * rows, rows), rows)
        return pltpu.make_async_copy(mixed_in.at[at], mixed_box.at[box], mixed_local.at[box])

    @pl.when(t >= line // 2)
    def _():
        mixed_hop(0).start()

    @pl.when(t < line // 2)
    def _():
        mixed_hop(1).start()

    for box in (0, 1):
        mixed_own(box).start()

    def mixed_on():
        for box in (0, 1):
            mixed_own(box).wait()

            @pl.when(inner)
            def _(box=box):
                mixed_hop(box).wait_recv()
                mixed_box[box] = (
                    mixed_box[box].astype(f32) + mixed_mail[box].astype(f32)
                ).astype(bf16)

        @pl.when(t > 0)
        def _():
            mixed_hop(2).start()

        @pl.when(t < line - 1)
        def _():
            mixed_hop(3).start()

    engine = Scatter(
        links, d, t, block,
        (
            lambda j: odd.at[lax.rem(j, odd.shape[0])],
            lambda j, at=pl.ds(0, middle): core.at[j, at],
            lambda j, at: sums.at[j, at],
            lambda j, number: arrived.at[j, number],
            lambda j: out.at[j],
        ),
        (
            lambda j: core_send.at[j],
            lambda j: core_recv.at[j],
            lambda j, number: send.at[j, number],
            lambda j, number: recv.at[j, number],
        ),
    )
    rows_t[...] = rows_in[...].T
    acc[...] = jnp.zeros(acc.shape, f32)

    def first(i, carry):
        slot = slot_at(i)
        for h in (0, 1):
            j = 2 * i + h

            @pl.when(i >= odd.shape[0] // 2)
            def _(j=j):
                engine.core_copy(j - odd.shape[0]).wait_send()

            odd[lax.rem(j, odd.shape[0])] = nn(
                rows_t[middle:, :], (gq_in, gkv_in)[h][slot]
            ).astype(bf16)
            engine.core_copy(j).start()
        for h in (0, 1):
            j = 2 * i + h
            value = nn(rows_t[:middle, :], (gq_in, gkv_in)[h][slot])
            sums[j] = value.astype(bf16)
            out[j] = value[:block]
        return carry

    lax.fori_loop(0, line, first, 0)

    def content(i, c):
        return o_in[slot_at(i)] if c == 2 else out[2 * i + c]

    def each(fill):
        for c in range(3):
            fill(c, slice(c * chunk, (c + 1) * chunk))

    def post(number, to):
        box = (0, 1, 1, 3, 2)[number]
        return mesh_copy(
            outbox.at[box], inbox.at[number], line_send.at[number], line_recv.at[number], (d, to)
        )

    def first_post():
        return post(0, jnp.where(t == 0, t + 1, t - 1))

    def along(i):
        if i == 0:

            @pl.when(is_end)
            def _():
                def fill(c, at):
                    outbox[0, :, at] = content(0, c).astype(bf16)

                each(fill)
                first_post().start()

        if i == 1:

            @pl.when(inner)
            def _():
                first_post().wait_recv()

            @pl.when(is_end)
            def _():
                inbox[0] = jnp.zeros(inbox.shape[1:], bf16)

            def fill(c, at):
                outbox[1, :, at] = (content(1, c) + inbox[0, :, at].astype(f32)).astype(bf16)

            each(fill)

            @pl.when(t >= 2)
            def _():
                post(1, t - 1).start()

            @pl.when(t <= 1)
            def _():
                post(2, t + 1).start()

        if i == 2:

            @pl.when(inner)
            def _():
                post(1, t - 1).wait_recv()
                post(2, t + 1).wait_recv()

            @pl.when(is_end)
            def _():
                inbox[1] = jnp.zeros(inbox.shape[1:], bf16)
                inbox[2] = jnp.zeros(inbox.shape[1:], bf16)

            def leftward(c, at):
                three = jnp.where(t == line - 1, content(2, c), content(0, c))
                outbox[3, :, at] = (three + inbox[1, :, at].astype(f32)).astype(bf16)

            def rightward(c, at):
                outbox[2, :, at] = (content(2, c) + inbox[2, :, at].astype(f32)).astype(bf16)

            @pl.when(t > 0)
            def _():
                each(leftward)
                post(3, t - 1).start()

            @pl.when(t < line - 1)
            def _():
                each(rightward)
                post(4, t + 1).start()

    part = rows // 4
    terms_out[...] = jnp.zeros(terms_out.shape, f32)
    terms_out[1:2, :] = second_terms[...]
    terms_out[2:3, 0:head] = head_terms[0:1, :]
    terms_out[2:3, head : 2 * head] = head_terms[1:2, :]

    def close(r, carry):
        at = pl.ds(pl.multiple_of(r * part, part), part)
        values = source[at, :]
        inverse = lax.rsqrt(jnp.mean(values * values, axis=-1, keepdims=True) + epsilon)
        normed = values * inverse
        c = acc[at, :]
        term = c * gain_one[...]
        grad = inverse * (term - normed * jnp.mean(term * normed, axis=-1, keepdims=True))
        input_out[at, :] = (grad_middle[at, :] + grad).astype(bf16)
        terms_out[0:1, :] += jnp.sum(c * normed, axis=0, keepdims=True)
        return carry

    def double(start, stop):
        hops = [((d ^ bit, t), bit) for bit in [1] + links.bits]
        hops = hops + [((d, t ^ 1), 0), ((d, t ^ 2), 0)]
        for k in range(start, stop):
            to, bit = hops[k]
            copy = mesh_copy(terms_out, heap.at[k], heap_send.at[k], heap_recv.at[k], to)
            copy.start()
            copy.wait()
            for i, mask in enumerate(links.masks):
                other = links.masks.index(mask ^ bit)
                terms_out[0:2, i * block : (i + 1) * block] += heap[
                    k, 0:2, other * block : (other + 1) * block
                ]
            terms_out[2:3, :] += heap[k, 2:3, :]

    def step(i, carry):
        @pl.when(i < line)
        def _():
            for h in (0, 1):
                load(i, h).wait()
            slot = slot_at(i)
            for n in range(4):
                at = slice(n * (width // 4), (n + 1) * (width // 4))
                acc[:, at] += nt(gq_in[slot], pair[0, at, :]) + nt(gkv_in[slot], pair[1, at, :])

            @pl.when(i + 1 < line)
            def _():
                for h in (0, 1):
                    load(i + 1, h).start()

        @pl.when(i == 1)
        def _():
            mixed_on()

        @pl.when(i == line)
        def _():
            lax.fori_loop(0, 4, close, 0)

        spread_stages(engine, links, 0, line, i)
        for p in range(line - 1):

            @pl.when(i == p + last_stage)
            def _(p=p):
                along(p)

        if inside:

            @pl.when(i == line)
            def _():
                double(0, 3)

        return carry

    lax.fori_loop(0, line + last_stage, step, 0)

    if inside:
        double(3, 3 + len(links.bits))

    @pl.when(t < line - 1)
    def _():
        post(3, t - 1).wait_recv()

    @pl.when(t == line - 1)
    def _():
        inbox[3] = jnp.zeros(inbox.shape[1:], bf16)

    @pl.when(t > 0)
    def _():
        post(4, t + 1).wait_recv()

    @pl.when(t == 0)
    def _():
        inbox[4] = jnp.zeros(inbox.shape[1:], bf16)

    def total(c, at):
        (q_out, kv_out, o_out)[c][...] = (
            content(line - 1, c) + inbox[3, :, at].astype(f32) + inbox[4, :, at].astype(f32)
        )

    each(total)

    def finish(i, carry):
        for h in (0, 1):
            engine.finish(2 * i + h, h, False)

            @pl.when(i >= line - odd.shape[0] // 2)
            def _(h=h):
                engine.core_copy(2 * i + h).wait_send()

        return carry

    lax.fori_loop(0, line, finish, 0)

    @pl.when(t >= line // 2)
    def _():
        mixed_hop(0).wait_send()

    @pl.when(t < line // 2)
    def _():
        mixed_hop(1).wait_send()

    @pl.when(t > 0)
    def _():
        mixed_hop(2).wait_send()
        mixed_hop(3).wait_recv()

    @pl.when(t < line - 1)
    def _():
        mixed_hop(3).wait_send()
        mixed_hop(2).wait_recv()

    @pl.when(is_end)
    def _():
        first_post().wait_send()

    @pl.when(t >= 2)
    def _():
        post(1, t - 1).wait_send()

    @pl.when(t <= 1)
    def _():
        post(2, t + 1).wait_send()

    @pl.when(t > 0)
    def _():
        post(3, t - 1).wait_send()

    @pl.when(t < line - 1)
    def _():
        post(4, t + 1).wait_send()


def attention_weights(rows_one, gq, gkv, o_sum, weights, source, grad_middle, gain_one, second_terms, head_terms, mixed_two, mixed_part, size, head):
    line, rows, chunk = gq.shape
    width = rows_one.shape[1]
    block, middle, count = width // size, width // 2, 2 * line
    pieces = Scatter.pieces(Links(size))
    hops = 3 + len(Links(size).bits)
    vmem = pl.BlockSpec(memory_space=pltpu.VMEM)
    hbm = pl.BlockSpec(memory_space=pl.ANY)
    shape = jax.ShapeDtypeStruct
    dma = pltpu.SemaphoreType.DMA
    return pl.pallas_call(
        functools.partial(final_kernel, size, line, head),
        out_shape=(
            shape((block, chunk), f32),
            shape((block, chunk), f32),
            shape((block, chunk), f32),
            shape((rows, width), bf16),
            shape((8, width), f32),
            shape((rows, width), bf16),
            shape((rows, width), bf16),
        ),
        in_specs=[vmem] * 4 + [hbm] + [vmem] * 5 + [hbm] * 2,
        out_specs=[vmem] * 5 + [hbm] * 2,
        scratch_shapes=[
            pltpu.VMEM((width, rows), bf16),
            pltpu.VMEM((2, width, chunk), bf16),
            pltpu.VMEM((rows, width), f32),
            pltpu.VMEM((count // 2, middle, chunk), bf16),
            pltpu.VMEM((count, middle, chunk), bf16),
            pltpu.VMEM((count, middle, chunk), bf16),
            pltpu.VMEM((count, pieces, block, chunk), bf16),
            pltpu.VMEM((count, block, chunk), f32),
            pltpu.VMEM((4, block, 3 * chunk), bf16),
            pltpu.VMEM((5, block, 3 * chunk), bf16),
            pltpu.VMEM((hops, 8, width), f32),
            pltpu.VMEM((2, rows, width), bf16),
            pltpu.VMEM((2, rows, width), bf16),
            dma((count,)),
            dma((count,)),
            dma((count, pieces)),
            dma((count, pieces)),
            dma((2,)),
            dma((5,)),
            dma((5,)),
            dma((hops,)),
            dma((hops,)),
            dma((4,)),
            dma((4,)),
            dma((2,)),
        ],
        compiler_params=pltpu.CompilerParams(
            collective_id=4, has_side_effects=True, vmem_limit_bytes=63 << 20
        ),
        cost_estimate=pl.CostEstimate(flops=16 << 30, bytes_accessed=40 << 20, transcendentals=0),
    )(rows_one, gq, gkv, o_sum, weights, source, grad_middle, gain_one, second_terms, head_terms, mixed_two, mixed_part)


def body(
    layer_input,
    first_gain,
    query_weight,
    key_matrix,
    value_matrix,
    query_gain,
    key_gain,
    output_weight,
    second_gain,
    gate_weight,
    up_weight,
    down_weight,
    segments,
    cotangent,
):
    plan = Plan()
    line, place = plan.line, plan.place
    rows, seq_count, width = layer_input.shape
    head = query_gain.shape[0]
    kv_heads = key_matrix.shape[1] // head
    query_heads = query_weight.shape[1] // head
    groups = query_heads // kv_heads
    all_kv = line * kv_heads
    half = width // 2
    hops = -(-(longest_document - 1) // rows)
    assert seq_count == 1 and hops == 2
    factor = head**-0.5

    gain_one = plan.to_masks(first_gain.astype(f32))
    gain_two = plan.to_masks(second_gain.astype(f32))
    source = plan.to_masks(layer_input[:, 0, :]).astype(f32)
    upstream = plan.to_masks(cotangent[:, 0, :])

    normed, inverse_one = rms_parts(source, gain_one)
    rows_one = normed.astype(bf16)
    tables = rope_tables(-hops * rows, (hops + line) * rows, head)
    gain_qk = jnp.stack([query_gain, key_gain]).astype(f32)
    (
        weights, pair_full, upstream_all, proj_query, proj_key, query_rows, key_rows, value_rows, lse,
        attended, middle, rows_two_own,
    ) = attention_forward(
        (query_weight, key_matrix, value_matrix, output_weight), (gate_weight, up_weight), rows_one,
        upstream, source, gain_qk, gain_two[None], tables, segments, plan.size, line,
    )
    inverse_two = lax.rsqrt(jnp.mean(middle * middle, axis=-1, keepdims=True) + epsilon)

    rows_two, hidden, grad_gate, grad_up, grad_two_part, mixed_part = feed_forward(
        rows_two_own, upstream_all, pair_full, down_weight, plan.size, line
    )

    def unslot(values):
        return values.reshape(-1, values.shape[2])

    hidden, grad_gate, grad_up = map(unslot, (hidden, grad_gate, grad_up))
    inner = (place > 0) & (place < line - 1)

    def share(step, part=mixed_part):
        return lax.dynamic_slice(part, ((place + step) % line * rows, 0), (rows, width)).astype(f32)

    def closed(part, from_right, from_left):
        return (
            share(0, part)
            + jnp.where(place < line - 1, from_right.astype(f32), 0.0)
            + jnp.where(place > 0, from_left.astype(f32), 0.0)
        )

    gate_grad, up_grad, down_grad, grad_left, grad_right = feed_weights(
        rows_two, upstream_all, grad_gate, grad_up, hidden, grad_two_part, plan.size
    )
    grad_two = closed(grad_two_part, grad_left, grad_right)

    grad_mid_norm, gain_two_terms = rms_back(middle, inverse_two, gain_two, grad_two)
    grad_middle = upstream.astype(f32) + grad_mid_norm
    grad_branch = grad_middle.astype(bf16)
    grad_query_low, grad_kv_low, head_terms, output_sum, mixed_one = attention_backward(
        grad_branch, weights, query_rows, key_rows, value_rows, lse, attended, proj_query, proj_key,
        gain_qk, tables, segments, mixed_part, plan.size,
    )
    mixed_two = (share(2) + jnp.where(inner, mixed_one.astype(f32), 0.0)).astype(bf16)
    second_terms = jnp.sum(gain_two_terms, axis=0, keepdims=True)
    query_weight_grad, kv_grad, output_grad, input_masked, terms, mixed_left, mixed_right = attention_weights(
        rows_one, grad_query_low, grad_kv_low, output_sum, weights, source, grad_middle, gain_one[None],
        second_terms, head_terms, mixed_two, mixed_part, plan.size, head,
    )
    input_grad = plan.from_masks(input_masked)[:, None, :]
    middle_late = after(middle, terms)
    mixed = closed(mixed_part, mixed_left, mixed_right)
    layer_output = plan.from_masks((middle_late + mixed).astype(bf16))[:, None, :]
    gains = jnp.concatenate([plan.from_masks(terms[0]), plan.from_masks(terms[1]), terms[2, : 2 * head]])
    if width // plan.size % 128:
        gains = plan.total(gains)
    return (
        layer_output,
        input_grad,
        gains[:width],
        query_weight_grad,
        kv_grad[:, : key_matrix.shape[1]],
        kv_grad[:, key_matrix.shape[1] :],
        gains[2 * width : 2 * width + head],
        gains[2 * width + head :],
        output_grad,
        gains[width : 2 * width],
        gate_grad,
        up_grad,
        down_grad,
    )


def solution(mesh):
    positions = P("tensor", "dp", None)
    weight = P("dp", "tensor")
    return jax.shard_map(
        body,
        mesh=mesh,
        in_specs=(
            positions,
            P(),
            weight,
            weight,
            weight,
            P(),
            P(),
            weight,
            P(),
            weight,
            weight,
            weight,
            P("dp", None),
            positions,
        ),
        out_specs=(
            positions,
            positions,
            P(),
            weight,
            weight,
            weight,
            P(),
            P(),
            weight,
            P(),
            weight,
            weight,
            weight,
        ),
        check_vma=False,
    )
```

```python
import functools

import jax
import jax.numpy as jnp
import numpy as np
from jax import lax
from jax.experimental import pallas as pl
from jax.experimental.pallas import tpu as pltpu
from jax.sharding import PartitionSpec as P

epsilon = 1e-06
rope_base = 1000000.0
longest_document = 512
bf16 = jnp.bfloat16
f32 = jnp.float32


def mm(eq, a, b):
    return jnp.einsum(eq, a, b, preferred_element_type=f32)


def rms_parts(values, gain):
    inverse = lax.rsqrt(jnp.mean(values * values, axis=-1, keepdims=True) + epsilon)
    return values * inverse * gain, inverse


def rms_back(values, inverse, gain, upstream):
    normed = values * inverse
    inner = upstream * gain
    grad = inverse * (inner - normed * jnp.mean(inner * normed, axis=-1, keepdims=True))
    return grad, upstream * normed


def rope_tables(first, count, block, head_size):
    half = head_size // 2
    exponent = -(2.0 * np.arange(half, dtype=np.float32)) / np.float32(head_size)
    frequency = np.power(np.float32(rope_base), exponent, dtype=np.float32).astype(np.float64)
    frequency = np.concatenate([frequency, frequency])[None, :]
    inside = np.arange(block)[:, None] * frequency
    starts = (first + block * np.arange(count))[:, None] * frequency
    return tuple(f(a).astype(np.float32) for a in (inside, starts) for f in (np.cos, np.sin))


def rope_block(tables, number, head):
    cos_in, sin_in, cos_at, sin_at = tables
    cos_start, sin_start = cos_at[pl.ds(number, 1), :], sin_at[pl.ds(number, 1), :]
    cosine = cos_start * cos_in[...] - sin_start * sin_in[...]
    sine = sin_start * cos_in[...] + cos_start * sin_in[...]
    lane = lax.broadcasted_iota(jnp.int32, sine.shape, 1)
    return cosine, jnp.where(lane < head // 2, -sine, sine)


class Plan:
    def __init__(self):
        self.size = lax.axis_size("dp")
        self.index = lax.axis_index("dp")
        self.place = lax.axis_index("tensor")
        self.line = lax.axis_size("tensor")
        assert self.line == 4
        self.others = [1 << i for i in range(1, self.size.bit_length() - 1)]
        evens = [0]
        for bit in self.others:
            evens = evens + [m ^ bit for m in evens]
        self.evens = evens
        self.masks = evens + [m ^ 1 for m in evens]
        self.forward = self.others
        self.backward = self.others[::-1]

    def swap(self, value, bit):
        return lax.ppermute(value, "dp", [(i, i ^ bit) for i in range(self.size)])

    def move(self, value, pairs):
        return lax.ppermute(value, "tensor", pairs)

    def xor_blocks(self, blocks):
        bit = 1
        while bit < self.size:
            on = (self.index & bit) != 0
            blocks = [jnp.where(on, blocks[i ^ bit], blocks[i]) for i in range(self.size)]
            bit *= 2
        return blocks

    def to_masks(self, value):
        blocks = self.xor_blocks(jnp.split(value, self.size, axis=-1))
        return jnp.concatenate([blocks[m] for m in self.masks], axis=-1)

    def from_masks(self, value):
        parts = jnp.split(value, self.size, axis=-1)
        blocks = [parts[self.masks.index(m)] for m in range(self.size)]
        return jnp.concatenate(self.xor_blocks(blocks), axis=-1)

    def gather(self, shard, order):
        rows = shard.shape[0]
        held, masks = shard, [0]
        for bit in order:
            arrived = self.swap(held, bit)
            held = jnp.concatenate([held, arrived], axis=0)
            masks = masks + [m ^ bit for m in masks]
        if masks != self.evens:
            held = jnp.concatenate(
                [lax.slice_in_dim(held, masks.index(m) * rows, (masks.index(m) + 1) * rows) for m in self.evens],
                axis=0,
            )
        return held, self.swap(held, 1)

    def reduce(self, even, odd, order):
        rows = even.shape[0] // len(self.evens)
        total = even.astype(f32) + self.swap(odd.astype(bf16), 1).astype(f32)
        pieces = {
            m: lax.slice_in_dim(total, i * rows, (i + 1) * rows) for i, m in enumerate(self.evens)
        }
        for bit in order:
            leaving = [m for m in pieces if m & bit]
            sent = jnp.concatenate([pieces[m].astype(bf16) for m in leaving], axis=0)
            arrived = self.swap(sent, bit)
            kept = {m: v for m, v in pieces.items() if not m & bit}
            for i, m in enumerate(leaving):
                kept[m ^ bit] = kept[m ^ bit] + lax.slice_in_dim(
                    arrived, i * rows, (i + 1) * rows
                ).astype(f32)
            pieces = kept
        return pieces[0]

    def gather_line(self, own):
        from_right = self.move(own, [(1, 0), (2, 1), (3, 2)])
        from_left = self.move(own, [(0, 1), (1, 2), (2, 3)])
        right_two = self.move(from_right, [(1, 0), (2, 1)])
        left_two = self.move(from_left, [(1, 2), (2, 3)])
        slot_two = jnp.where(self.place < 2, right_two, left_two)
        last = self.move(slot_two, [(1, 0), (2, 3)])
        slot_one = jnp.where(self.place < 3, from_right, last)
        slot_three = jnp.where(self.place > 0, from_left, last)
        return [own, slot_one, slot_two, slot_three]

    def scatter_line(self, slots):
        zero, one, two, three = slots
        first = self.move(
            jnp.where(self.place == 3, one, three).astype(bf16), [(3, 2), (0, 1)]
        )
        middle = (two + first.astype(f32)).astype(bf16)
        leftward = self.move(middle, [(3, 2), (2, 1)])
        rightward = self.move(middle, [(0, 1), (1, 2)])
        leftward = self.move(
            (three + leftward.astype(f32)).astype(bf16), [(3, 2), (2, 1), (1, 0)]
        )
        rightward = self.move(
            (one + rightward.astype(f32)).astype(bf16), [(0, 1), (1, 2), (2, 3)]
        )
        return zero + leftward.astype(f32) + rightward.astype(f32)

    def total(self, value):
        bit = 1
        while bit < self.size:
            value = value + self.swap(value, bit)
            bit *= 2
        for bit in (1, 2):
            value = value + self.move(value, [(i, i ^ bit) for i in range(self.line)])
        return value


def after(value, *others):
    return lax.optimization_barrier((value,) + others)[0]


def mesh_copy(src, dst, send, recv, device):
    return pltpu.make_async_remote_copy(
        src_ref=src, dst_ref=dst, send_sem=send, recv_sem=recv, device_id=device,
        device_id_type=pl.DeviceIdType.MESH,
    )


class Links:
    def __init__(self, size):
        bits = [1 << i for i in range(1, size.bit_length() - 1)]
        self.orders = (bits, bits[::-1])
        evens = [0]
        for bit in bits:
            evens = evens + [m ^ bit for m in evens]
        self.evens = evens
        self.masks = evens + [m ^ 1 for m in evens]
        self.bits = bits

    def onward(self, half, mask):
        order = self.orders[half]
        last = max([i for i, bit in enumerate(order) if mask & bit], default=-1)
        return order[last + 1 :]


class Gather:
    def __init__(self, links, d, t, piece, send, recv):
        self.links, self.d, self.t = links, d, t
        self.piece, self.send, self.recv = piece, send, recv

    def copy(self, half, mask, bit):
        index = self.links.masks.index(mask ^ bit)
        return mesh_copy(
            self.piece(half, mask), self.piece(half, mask ^ bit), self.send(half, index),
            self.recv(half, index), (self.d ^ bit, self.t),
        )

    def launch(self):
        for step in range(len(self.links.bits)):
            for half in (0, 1):
                self.copy(half, 0, self.links.orders[half][step]).start()
        for half in (0, 1):
            self.copy(half, 0, 1).start()

    def arrive(self, half, mask):
        bit = [b for b in self.links.orders[half] if b & mask][-1]
        self.copy(half, mask ^ bit, bit).wait_recv()
        for other in self.links.onward(half, mask):
            self.copy(half, mask, other).start()
        self.copy(half, mask, 1).start()

    def onward(self):
        for mask in self.links.evens[1:]:
            for half in (0, 1):
                if self.links.onward(half, mask):
                    self.arrive(half, mask)

    def complete(self):
        for mask in self.links.evens[1:]:
            for half in (0, 1):
                if not self.links.onward(half, mask):
                    self.arrive(half, mask)
        for mask in self.links.evens:
            for half in (0, 1):
                self.copy(half, mask, 1).wait_recv()

    def finish(self):
        for mask in self.links.masks[1:]:
            for half in (0, 1):
                self.copy(half, mask ^ 1 if mask & 1 else 0, 1 if mask & 1 else mask).wait_send()


class Relay:
    def __init__(self, d, t, line, slot, send, recv):
        self.d, self.t, self.line = d, t, line
        self.slot, self.send, self.recv = slot, send, recv
        self.inner = (t > 0) & (t < line - 1)

    def copy(self, number, source, target, to):
        return mesh_copy(
            self.slot(source), self.slot(target), self.send.at[number], self.recv.at[target],
            (self.d, to),
        )

    def moves(self):
        t = self.t
        return (
            (t > 0, (0, 0, 1, t - 1)),
            (t < self.line - 1, (1, 0, 3, t + 1)),
            (self.inner, (2, 1, 2, t - 1)),
            (self.inner, (3, 3, 2, t + 1)),
            (t == 1, (4, 2, 3, t - 1)),
            (t == 2, (5, 2, 1, t + 1)),
        )

    def start(self, *numbers):
        for number in numbers:
            condition, route = self.moves()[number]

            @pl.when(condition)
            def _(route=route):
                self.copy(*route).start()

    def wait(self, slot):
        self.copy(0, 0, slot, self.t).wait_recv()

    def finish(self):
        for condition, route in self.moves():

            @pl.when(condition)
            def _(route=route):
                self.copy(*route).wait_send()

    def first(self):
        self.start(0, 1)

    def second(self):
        t, line = self.t, self.line

        @pl.when(t < line - 1)
        def _():
            self.wait(1)

        self.start(2)

        @pl.when(t > 0)
        def _():
            self.wait(3)

        self.start(3)

    def third(self):
        self.wait(2)
        self.start(4, 5)

    def ends(self):
        @pl.when(self.t == 0)
        def _():
            self.wait(3)

        @pl.when(self.t == self.line - 1)
        def _():
            self.wait(1)


def slot_of(i, t, line):
    far = jnp.where(t < line - 1, 1, 3)
    near = jnp.where(t < line - 1, 3, 1)
    return jnp.where(i == 0, 0, jnp.where(i == 1, far, jnp.where(i == 2, 2, near)))


def greet(links, d, t, line, across=False):
    barrier = pltpu.get_barrier_semaphore()
    if across:
        pl.semaphore_signal(barrier, inc=1, device_id=(d, t ^ 2), device_id_type=pl.DeviceIdType.MESH)
    for bit in [1] + links.bits:
        pl.semaphore_signal(barrier, inc=1, device_id=(d ^ bit, t), device_id_type=pl.DeviceIdType.MESH)

    @pl.when(t > 0)
    def _():
        pl.semaphore_signal(barrier, inc=1, device_id=(d, t - 1), device_id_type=pl.DeviceIdType.MESH)

    @pl.when(t < line - 1)
    def _():
        pl.semaphore_signal(barrier, inc=1, device_id=(d, t + 1), device_id_type=pl.DeviceIdType.MESH)

    pl.semaphore_wait(
        barrier,
        1 + across + len(links.bits) + jnp.where(t > 0, 1, 0) + jnp.where(t < line - 1, 1, 0),
    )


def nt(a, b):
    return lax.dot_general(a, b, (((1,), (1,)), ((), ())), preferred_element_type=f32)


def tn(a, b):
    return lax.dot_general(a, b, (((0,), (0,)), ((), ())), preferred_element_type=f32)


def nn(a, b):
    return jnp.dot(a, b, preferred_element_type=f32)


def head_norm(values, gain):
    inverse = lax.rsqrt(jnp.mean(values * values, axis=-1, keepdims=True) + epsilon)
    return values * inverse * gain


def segment_masks(segments, padded, t, rows, span):
    ahead = span - rows
    padded[...] = jnp.full(padded.shape, -1.0, f32)
    padded[0:1, ahead:] = segments[...].astype(f32)
    key_row = padded[0:1, pl.ds(pl.multiple_of(t * rows, 128), span)]
    return key_row, turned(key_row[:, ahead:])


def turned(row):
    return jnp.broadcast_to(row, (128, row.shape[1])).T[:, 0:1]


def forward_kernel(
    size, line, head,
    q_shard, k_shard, v_shard, o_shard, gate_shard, up_shard, rows_in, upstream, source, gain_qk, gain_two,
    cos_in, sin_in, cos_at, sin_at, segments,
    weights_out, mlp_out, upstream_all, proj_q, proj_k, q_out, k_out, v_out, lse_out, att_out, middle, normed_out,
    full, rows_all, acc,
    z_send, z_recv, send, recv, row_send, row_recv, keep, mlp_send, mlp_recv, up_send, up_recv, local, cosine, sine, padded,
):
    links = Links(size)
    d, t = lax.axis_index("dp"), lax.axis_index("tensor")
    block = q_shard.shape[0]
    rows, width = rows_in.shape
    span = rows_all.shape[0]
    factor = head**-0.5

    def place(mask):
        return pl.ds(links.masks.index(mask) * block, block)

    def gather(slot):
        return Gather(
            links, d, t,
            lambda half, mask: full.at[half, slot, place(mask)],
            lambda half, index: send.at[slot, half, index],
            lambda half, index: recv.at[slot, half, index],
        )

    feed = Gather(
        links, d, t,
        lambda half, mask: mlp_out.at[half, place(mask)],
        lambda half, index: mlp_send.at[half, index],
        lambda half, index: mlp_recv.at[half, index],
    )
    relay = Relay(d, t, line, lambda slot: full.at[:, slot, place(0)], z_send, z_recv)
    upward = Relay(d, t, line, lambda slot: upstream_all.at[slot], up_send, up_recv)

    o_half = 2 * head
    parts = (
        (q_shard, full.at[0, 0, place(0), 0 : 4 * head]),
        (o_shard.at[:, 0:o_half], full.at[0, 0, place(0), 4 * head : 6 * head]),
        (k_shard, full.at[1, 0, place(0), 0 : 2 * head]),
        (v_shard, full.at[1, 0, place(0), 2 * head : 4 * head]),
        (o_shard.at[:, o_half : 2 * o_half], full.at[1, 0, place(0), 4 * head : 6 * head]),
        (gate_shard, mlp_out.at[0, place(0)]),
        (up_shard, mlp_out.at[1, place(0)]),
        (upstream, upstream_all.at[0]),
    )
    own = [
        pltpu.make_async_copy(source_ref, target_ref, local.at[n])
        for n, (source_ref, target_ref) in enumerate(parts)
    ]
    for copy in own:
        copy.start()
    rows_all[pl.ds(span - rows, rows), :] = rows_in[...]

    @pl.when(t == 0)
    def _():
        rows_all[pl.ds(0, 2 * rows), :] = jnp.zeros((2 * rows, width), bf16)

    @pl.when(t == 1)
    def _():
        rows_all[pl.ds(0, rows), :] = jnp.zeros((rows, width), bf16)

    greet(links, d, t, line)
    for copy in own[:5]:
        copy.wait()

    row_one = mesh_copy(
        rows_in, rows_all.at[pl.ds(rows, rows)], row_send.at[0], row_recv.at[0], (d, t + 1)
    )
    row_two = mesh_copy(
        rows_all.at[pl.ds(rows, rows)], rows_all.at[pl.ds(0, rows)], row_send.at[1],
        row_recv.at[1], (d, t + 1),
    )
    inner = relay.inner
    relay.first()

    @pl.when(t < line - 1)
    def _():
        row_one.start()

    gather(0).launch()
    gather(0).onward()
    relay.second()
    second = slot_of(1, t, line)

    @pl.when(t < line - 1)
    def _():
        gather(1).launch()

    @pl.when(t == line - 1)
    def _():
        gather(3).launch()

    @pl.when(t > 0)
    def _():
        row_one.wait_recv()

    @pl.when(inner)
    def _():
        row_two.start()

    relay.third()
    gather(2).launch()
    gather(second).onward()

    @pl.when(t > 1)
    def _():
        row_two.wait_recv()

    for copy in own[5:]:
        copy.wait()
    key_row, query_column = segment_masks(segments, padded, t, rows, span)
    for n in range(span // rows):
        at = pl.ds(n * rows, rows)
        cosine[at, :], sine[at, :] = rope_block((cos_in, sin_in, cos_at, sin_at), t + n, head)
    upward.first()
    acc[...] = source[...]

    lane = lax.broadcasted_iota(jnp.int32, (rows, 128), 1)
    q_index = lax.broadcasted_iota(jnp.int32, (rows, span), 0) + (span - rows)
    k_index = lax.broadcasted_iota(jnp.int32, (rows, span), 1)

    def step(i, carry):
        slot = slot_of(i, t, line)

        @pl.when(i == 1)
        def _():
            relay.ends()
            gather(slot_of(3, t, line)).launch()

        @pl.when(i >= 2)
        def _():
            gather(slot).onward()

        @pl.when((i == 2))
        def _():
            feed.launch()

        gather(slot).complete()
        for half in (0, 1):
            pltpu.make_async_copy(
                full.at[half, slot], weights_out.at[half, slot], keep.at[slot, half]
            ).start()

        own_rows = pl.ds(span - rows, rows)
        allowed = (query_column == key_row) & (k_index <= q_index)
        lse_acc = jnp.zeros((rows, 128), f32)
        for g in (0, 1):
            key_cols = slice(g * head, (g + 1) * head)
            if g == 0:
                for r in range(span // rows):
                    part = pl.ds(r * rows, rows)
                    both = nn(rows_all[part, :], full[1, slot, :, 0 : 4 * head])
                    if r == span // rows - 1:
                        proj_k[slot] = both[:, : 2 * head]
                    for h in (0, 1):
                        unit = head_norm(both[:, h * head : (h + 1) * head], gain_qk[1:2, :])
                        turned = unit * cosine[part, :] + pltpu.roll(unit, head // 2, 1) * sine[part, :]
                        k_out[slot, part, h * head : (h + 1) * head] = turned.astype(bf16)
                    v_out[slot, part, :] = both[:, 2 * head :].astype(bf16)
            for j in (0, 1):
                h = 2 * g + j
                cols = slice(h * head, (h + 1) * head)
                raw = nn(rows_in[...], full[0, slot, :, cols])
                proj_q[slot, :, cols] = raw
                unit = head_norm(raw, gain_qk[0:1, :])
                turned = unit * cosine[own_rows, :] + pltpu.roll(unit, head // 2, 1) * sine[own_rows, :]
                query = turned.astype(bf16)
                q_out[slot, :, cols] = query
                scores = nt(query, k_out[slot, :, key_cols]) * factor
                scores = jnp.where(allowed, scores, -1e30)
                top = jnp.max(scores, axis=-1, keepdims=True)
                weight = jnp.exp(scores - top)
                total = jnp.sum(weight, axis=-1, keepdims=True)
                probs = (weight / total).astype(bf16)
                att_out[slot, :, cols] = nn(probs, v_out[slot, :, key_cols]).astype(bf16)
                lse_acc = jnp.where(lane == h, top + jnp.log(total), lse_acc)
        lse_out[slot] = lse_acc
        for half in (0, 1):
            acc[...] += nt(
                att_out[slot, :, half * 2 * head : (half + 1) * 2 * head],
                full[half, slot, :, 4 * head : 6 * head],
            )

        @pl.when((i == 2))
        def _():
            upward.second()

        return carry

    lax.fori_loop(0, line, step, 0)
    upward.third()
    feed.onward()
    values = acc[...]
    middle[...] = values
    normed_out[...] = head_norm(values, gain_two[...]).astype(bf16)
    feed.complete()

    def finish(i, carry):
        gather(i).finish()
        for half in (0, 1):
            pltpu.make_async_copy(full.at[half, i], weights_out.at[half, i], keep.at[i, half]).wait()
        return carry

    lax.fori_loop(0, line, finish, 0)
    feed.finish()
    relay.finish()

    @pl.when(t < line - 1)
    def _():
        row_one.wait_send()

    @pl.when(inner)
    def _():
        row_two.wait_send()

    upward.ends()
    upward.finish()


def attention_forward(weights, mlp, rows_one, upstream, source, gain_qk, gain_two, tables, segments, size, line):
    cols = 3 * weights[0].shape[1] // 2
    rows, width = rows_one.shape
    length = segments.shape[1]
    span = rows * (1 - (1 - longest_document) // rows)
    head = gain_qk.shape[1]
    pieces = 2 * (size // 2)
    vmem = pl.BlockSpec(memory_space=pltpu.VMEM)
    hbm = pl.BlockSpec(memory_space=pl.ANY)
    shape = jax.ShapeDtypeStruct
    return pl.pallas_call(
        functools.partial(forward_kernel, size, line, head),
        out_shape=(
            shape((2, line, width, cols), bf16),
            shape((2, width, mlp[0].shape[1]), bf16),
            shape((line, rows, width), bf16),
            shape((line, rows, 4 * head), f32),
            shape((line, rows, 2 * head), f32),
            shape((line, rows, 4 * head), bf16),
            shape((line, span, 2 * head), bf16),
            shape((line, span, 2 * head), bf16),
            shape((line, rows, 128), f32),
            shape((line, rows, 4 * head), bf16),
            shape((rows, width), f32),
            shape((rows, width), bf16),
        ),
        in_specs=[hbm] * 4 + [vmem] * 12,
        out_specs=[hbm] * 3 + [vmem] * 9,
        scratch_shapes=[
            pltpu.VMEM((2, line, width, cols), bf16),
            pltpu.VMEM((span, width), bf16),
            pltpu.VMEM((rows, width), f32),
            pltpu.SemaphoreType.DMA((6,)),
            pltpu.SemaphoreType.DMA((line,)),
            pltpu.SemaphoreType.DMA((line, 2, pieces)),
            pltpu.SemaphoreType.DMA((line, 2, pieces)),
            pltpu.SemaphoreType.DMA((2,)),
            pltpu.SemaphoreType.DMA((2,)),
            pltpu.SemaphoreType.DMA((line, 2)),
            pltpu.SemaphoreType.DMA((2, pieces)),
            pltpu.SemaphoreType.DMA((2, pieces)),
            pltpu.SemaphoreType.DMA((6,)),
            pltpu.SemaphoreType.DMA((line,)),
            pltpu.SemaphoreType.DMA((8,)),
            pltpu.VMEM((span, head), f32),
            pltpu.VMEM((span, head), f32),
            pltpu.VMEM((8, span - rows + length), f32),
        ],
        compiler_params=pltpu.CompilerParams(
            collective_id=0, has_side_effects=True, vmem_limit_bytes=62 << 20
        ),
        cost_estimate=pl.CostEstimate(flops=40 << 30, bytes_accessed=200 << 20, transcendentals=4 << 20),
    )(*weights, *mlp, rows_one, upstream, source, gain_qk, gain_two, *tables, segments)


def feed_kernel(
    size, line,
    rows_in, upstream_in, pair_in, down_in,
    rows_out, hidden_out, gate_out, up_out, grad_out, mixed_out,
    rows_v, upstream_v, pair, down, gate_f, up_f, hidden_v, gate_v, up_v, grad_v, mixed_v,
    z_send, z_recv, send, recv, local, leave,
):
    links = Links(size)
    d, t = lax.axis_index("dp"), lax.axis_index("tensor")
    block = down_in.shape[0]
    _, rows, width = rows_v.shape
    units = hidden_v.shape[2]
    chunk = units // 4
    piece = width // 4

    def place(mask):
        return pl.ds(links.masks.index(mask) * block, block)

    gather = Gather(
        links, d, t,
        lambda half, mask: down.at[half, place(mask)],
        lambda half, index: send.at[half, index],
        lambda half, index: recv.at[half, index],
    )
    relay = Relay(d, t, line, lambda slot: rows_v.at[slot], z_send, z_recv)
    arrivals = (
        pltpu.make_async_copy(rows_in, rows_v.at[0], local.at[0]),
        pltpu.make_async_copy(down_in.at[:, 0 : units // 2], down.at[0, place(0)], local.at[1]),
        pltpu.make_async_copy(down_in.at[:, units // 2 :], down.at[1, place(0)], local.at[4]),
        pltpu.make_async_copy(pair_in, pair, local.at[2]),
        pltpu.make_async_copy(upstream_in, upstream_v, local.at[3]),
    )
    for copy in arrivals:
        copy.start()
    greet(links, d, t, line)
    arrivals[0].wait()
    relay.first()
    arrivals[1].wait()
    arrivals[2].wait()
    gather.launch()
    gather.onward()
    arrivals[3].wait()
    arrivals[4].wait()

    def departures(slot):
        position = lax.rem(slot + t, line)
        natural = pl.ds(pl.multiple_of(position * rows, rows), rows)
        return [
            pltpu.make_async_copy(rows_v.at[slot], rows_out.at[slot], leave.at[0, slot]),
            pltpu.make_async_copy(hidden_v.at[slot], hidden_out.at[slot], leave.at[1, slot]),
            pltpu.make_async_copy(gate_v.at[slot], gate_out.at[slot], leave.at[2, slot]),
            pltpu.make_async_copy(up_v.at[slot], up_out.at[slot], leave.at[3, slot]),
            pltpu.make_async_copy(grad_v.at[slot], grad_out.at[natural], leave.at[4, slot]),
            pltpu.make_async_copy(mixed_v.at[slot], mixed_out.at[natural], leave.at[5, slot]),
        ]

    def step(i, carry):
        slot = slot_of(i, t, line)
        for c in range(4):
            cols = slice(c * chunk, (c + 1) * chunk)
            gate = nn(rows_v[slot], pair[0, :, cols])
            up = nn(rows_v[slot], pair[1, :, cols])
            gate_f[:, cols] = gate
            up_f[:, cols] = up
            hidden_v[slot, :, cols] = (gate * jax.nn.sigmoid(gate) * up).astype(bf16)

        @pl.when(i == 0)
        def _():
            relay.second()
            gather.complete()

        @pl.when(i == 1)
        def _():
            relay.third()

        @pl.when(i == 2)
        def _():
            relay.ends()

        for c in range(4):
            cols = slice(c * chunk, (c + 1) * chunk)
            inner = slice((c % 2) * chunk, (c % 2 + 1) * chunk)
            grad_hidden = nn(upstream_v[slot], down[c // 2, :, inner])
            gate, up = gate_f[:, cols], up_f[:, cols]
            sigmoid = jax.nn.sigmoid(gate)
            gate_v[slot, :, cols] = (
                grad_hidden * up * sigmoid * (1.0 + gate * (1.0 - sigmoid))
            ).astype(bf16)
            up_v[slot, :, cols] = (grad_hidden * (gate * sigmoid)).astype(bf16)
        for n in range(4):
            out = slice(n * piece, (n + 1) * piece)
            grad_v[slot, :, out] = (
                nt(gate_v[slot], pair[0, out, :]) + nt(up_v[slot], pair[1, out, :])
            ).astype(bf16)
            mixed_v[slot, :, out] = (
                nt(hidden_v[slot, :, : units // 2], down[0, out, :])
                + nt(hidden_v[slot, :, units // 2 :], down[1, out, :])
            ).astype(bf16)
        for copy in departures(slot):
            copy.start()
        return carry

    lax.fori_loop(0, line, step, 0)

    def finish(i, carry):
        for copy in departures(i):
            copy.wait()
        return carry

    lax.fori_loop(0, line, finish, 0)
    gather.finish()
    relay.finish()


def feed_forward(rows_own, upstream_all, pair_full, down_shard, size, line):
    rows, width = rows_own.shape
    units = pair_full.shape[2]
    hbm = pl.BlockSpec(memory_space=pl.ANY)
    shape = jax.ShapeDtypeStruct
    dma = pltpu.SemaphoreType.DMA
    return pl.pallas_call(
        functools.partial(feed_kernel, size, line),
        out_shape=(
            shape((line, rows, width), bf16),
            shape((line, rows, units), bf16),
            shape((line, rows, units), bf16),
            shape((line, rows, units), bf16),
            shape((line * rows, width), bf16),
            shape((line * rows, width), bf16),
        ),
        in_specs=[hbm] * 4,
        out_specs=[hbm] * 6,
        scratch_shapes=[
            pltpu.VMEM((line, rows, width), bf16),
            pltpu.VMEM((line, rows, width), bf16),
            pltpu.VMEM((2, width, units), bf16),
            pltpu.VMEM((2, width, units // 2), bf16),
            pltpu.VMEM((rows, units), f32),
            pltpu.VMEM((rows, units), f32),
            pltpu.VMEM((line, rows, units), bf16),
            pltpu.VMEM((line, rows, units), bf16),
            pltpu.VMEM((line, rows, units), bf16),
            pltpu.VMEM((line, rows, width), bf16),
            pltpu.VMEM((line, rows, width), bf16),
            dma((6,)),
            dma((line,)),
            dma((2, size)),
            dma((2, size)),
            dma((5,)),
            dma((6, line)),
        ],
        compiler_params=pltpu.CompilerParams(
            collective_id=1, has_side_effects=True, vmem_limit_bytes=62 << 20
        ),
        cost_estimate=pl.CostEstimate(flops=40 << 30, bytes_accessed=60 << 20, transcendentals=3 << 20),
    )(rows_own, upstream_all, pair_full, down_shard)


class Scatter:
    def __init__(self, links, d, t, block, refs, semaphores):
        self.links, self.d, self.t, self.block = links, d, t, block
        self.odd, self.core, self.sums, self.arrived, self.out = refs
        self.core_send, self.core_recv, self.send, self.recv = semaphores

    @staticmethod
    def pieces(links):
        return max(1, len(links.evens) - 1)

    def steps(self, half):
        masks, number, found = self.links.evens, 0, []
        for bit in self.links.orders[half][::-1]:
            masks = [m for m in masks if not m & bit]
            found.append((bit, [(m, number + i) for i, m in enumerate(masks)]))
            number += len(masks)
        return found

    def rows(self, mask):
        return pl.ds(self.links.evens.index(mask) * self.block, self.block)

    def core_copy(self, j):
        return mesh_copy(
            self.odd(j), self.core(j), self.core_send(j), self.core_recv(j), (self.d ^ 1, self.t)
        )

    def piece_copy(self, j, mask, number, bit):
        return mesh_copy(
            self.sums(j, self.rows(mask ^ bit)), self.arrived(j, number), self.send(j, number),
            self.recv(j, number), (self.d ^ bit, self.t),
        )

    def launch(self, j, half, step):
        steps = self.steps(half)
        if step < len(steps):
            bit, pairs = steps[step]
            for mask, number in pairs:
                self.piece_copy(j, mask, number, bit).start()

    def add(self, j, mask, value):
        if mask == 0:
            out = self.out(j)
            out[...] = out[...] + value[...].astype(f32)
        else:
            total = self.sums(j, self.rows(mask))
            total[...] = (total[...].astype(f32) + value[...].astype(f32)).astype(bf16)

    def stage(self, j, half, stage):
        if stage == 0:
            self.core_copy(j).wait_recv()
            steps = self.steps(half)
            first = steps[0][0] if steps else 0
            for mask in sorted(self.links.evens, key=lambda m: not m & first):
                self.add(j, mask, self.core(j, self.rows(mask)))
        else:
            bit, pairs = self.steps(half)[stage - 1]
            for mask, number in pairs[::-1]:
                self.piece_copy(j, mask, number, bit).wait_recv()
                self.add(j, mask, self.arrived(j, number))
        self.launch(j, half, stage)

    def finish(self, j, half, core=True):
        if core:
            self.core_copy(j).wait_send()
        for bit, pairs in self.steps(half):
            for mask, number in pairs:
                self.piece_copy(j, mask, number, bit).wait_send()


def greet_dp(links, d, t):
    barrier = pltpu.get_barrier_semaphore()
    for bit in [1] + links.bits:
        pl.semaphore_signal(barrier, inc=1, device_id=(d ^ bit, t), device_id_type=pl.DeviceIdType.MESH)
    pl.semaphore_wait(barrier, 1 + len(links.bits))


class LineSum:
    def __init__(self, d, t, line, source, ends, outbox, inbox, semaphores):
        self.d, self.t, self.line = d, t, line
        self.source, self.ends, self.outbox, self.inbox = source, ends, outbox, inbox
        self.send, self.recv, self.local = semaphores
        self.rows = outbox.shape[1]

    def block(self, position):
        return self.source.at[pl.ds(pl.multiple_of(position * self.rows, self.rows), self.rows)]

    def hop(self, number, source, target, to):
        return mesh_copy(source, target, self.send.at[number], self.recv.at[number], (self.d, to))

    def hops(self):
        t, line = self.t, self.line
        return (
            (t == 0, lambda: self.hop(0, self.block(line - 1), self.inbox.at[0], t + 1)),
            (t == line - 1, lambda: self.hop(0, self.block(0), self.inbox.at[0], t - 1)),
            (t >= 2, lambda: self.hop(1, self.outbox.at[0], self.inbox.at[1], t - 1)),
            (t <= 1, lambda: self.hop(2, self.outbox.at[0], self.inbox.at[2], t + 1)),
            (t > 0, lambda: self.hop(3, self.outbox.at[1], self.ends[0], t - 1)),
            (t < line - 1, lambda: self.hop(4, self.outbox.at[2], self.ends[1], t + 1)),
        )

    def start(self, *numbers):
        for number in numbers:
            condition, make = self.hops()[number]

            @pl.when(condition)
            def _(make=make):
                make().start()

    def own(self, box, step):
        position = lax.rem(self.t + step, self.line)
        return pltpu.make_async_copy(self.block(position), self.outbox.at[box], self.local.at[box])

    def take(self, box, number):
        @pl.when((self.t > 0) & (self.t < self.line - 1))
        def _():
            self.hop(number, self.outbox.at[0], self.inbox.at[number], self.t + 1).wait_recv()
            self.outbox[box] = (
                self.outbox[box].astype(f32) + self.inbox[number].astype(f32)
            ).astype(bf16)

    def first(self):
        self.start(0, 1)
        for box, step in ((0, 2), (1, 3), (2, 1)):
            self.own(box, step).start()

    def second(self):
        self.own(0, 2).wait()
        self.take(0, 0)
        self.start(2, 3)

    def third(self):
        self.own(1, 3).wait()
        self.own(2, 1).wait()
        self.take(1, 1)
        self.take(2, 2)
        self.start(4, 5)

    def finish(self):
        for condition, make in self.hops():

            @pl.when(condition)
            def _(make=make):
                make().wait_send()

        @pl.when(self.t < self.line - 1)
        def _():
            self.hop(3, self.outbox.at[1], self.ends[0], self.t + 1).wait_recv()

        @pl.when(self.t > 0)
        def _():
            self.hop(4, self.outbox.at[2], self.ends[1], self.t - 1).wait_recv()


def weight_kernel(
    size, line,
    rows_in, upstream_in, gate_in, up_in, hidden_in, grad_in,
    gate_out, up_out, down_out, sum_left, sum_right,
    outbox, inbox, raw, left, right, odd, core, sums, arrived, out,
    core_send, core_recv, send, recv, local, raw_sem, leave, sum_send, sum_recv, sum_local,
):
    links = Links(size)
    d, t = lax.axis_index("dp"), lax.axis_index("tensor")
    width = left.shape[1]
    rows = raw.shape[1]
    ring, tokens, chunk = right.shape
    count = out.shape[0]
    middle = width // 2
    block = out.shape[1]
    pairs = count // 2
    wide = gate_in.shape[1] // chunk

    def load(j):
        p, h = j // 2, j % 2
        if p < wide:
            source, at = (gate_in, up_in)[h], p
        else:
            source, at = hidden_in, p - wide + h * (wide // 2)
        return pltpu.make_async_copy(
            source.at[:, at * chunk : (at + 1) * chunk], right.at[j % ring], local.at[j]
        )

    def store(j):
        p, h = j // 2, j % 2
        if p < wide:
            target, at = (gate_out, up_out)[h], p
        else:
            target, at = down_out, p - wide + h * (wide // 2)
        return pltpu.make_async_copy(
            out.at[j], target.at[:, at * chunk : (at + 1) * chunk], leave.at[j]
        )

    def fetch(k, r):
        source = (rows_in, upstream_in)[k]
        slot = (k * line + r) % 2
        return pltpu.make_async_copy(source.at[r], raw.at[slot], raw_sem.at[slot]), slot

    fetch(0, 0)[0].start()
    for j in range(ring):
        load(j).start()
    greet(links, d, t, line)
    gradient = LineSum(
        d, t, line, grad_in, (sum_left, sum_right), outbox, inbox, (sum_send, sum_recv, sum_local)
    )
    gradient.first()

    def turn(k):
        for r in range(line):
            copy, slot = fetch(k, r)
            copy.wait()
            following = k * line + r + 1
            if following < 2 * line:
                fetch(following // line, following % line)[0].start()
            left[k, :, r * rows : (r + 1) * rows] = raw[slot].T

    engine = Scatter(
        links, d, t, block,
        (
            lambda j: odd.at[j],
            lambda j, at=pl.ds(0, middle): core.at[j, at],
            lambda j, at: sums.at[j, at],
            lambda j, number: arrived.at[j, number],
            lambda j: out.at[j],
        ),
        (
            lambda j: core_send.at[j],
            lambda j: core_recv.at[j],
            lambda j, number: send.at[j, number],
            lambda j, number: recv.at[j, number],
        ),
    )
    turn(0)

    def step(p, carry):
        @pl.when(p == wide // 2)
        def _():
            gradient.second()
            turn(1)

        @pl.when(p == wide)
        def _():
            gradient.third()

        for q in range(pairs):

            @pl.when(p == q)
            def _(q=q):
                load(2 * q).wait()
                load(2 * q + 1).wait()

        @pl.when(p < pairs)
        def _():
            k = jnp.where(p < wide, 0, 1)
            for h in (0, 1):
                j = 2 * p + h
                for r in range(middle // 256):
                    at = pl.ds(middle + r * 256, 256)
                    odd[j, pl.ds(r * 256, 256), :] = nn(
                        left[k, at, :], right[lax.rem(j, ring)]
                    ).astype(bf16)
                engine.core_copy(j).start()
            for h in (0, 1):
                j = 2 * p + h
                for r in range(middle // 256):
                    at = pl.ds(r * 256, 256)
                    value = nn(left[k, at, :], right[lax.rem(j, ring)])
                    sums[j, at, :] = value.astype(bf16)
                    if r == 0:
                        out[j] = value[:block]

        for q in range(pairs - ring // 2):

            @pl.when(p == q)
            def _(q=q):
                load(2 * q + ring).start()
                load(2 * q + ring + 1).start()

        for stage in range(len(links.bits) + 1):
            @pl.when((p >= stage + 1) & (p < pairs + stage + 1))
            def _(stage=stage):
                for h in (0, 1):
                    engine.stage(2 * (p - stage - 1) + h, h, stage)

        return carry

    lax.fori_loop(0, pairs + len(links.bits) + 1, step, 0)
    for j in range(count):
        store(j).start()

    def finish(p, carry):
        for h in (0, 1):
            engine.finish(2 * p + h, h)
        return carry

    lax.fori_loop(0, pairs, finish, 0)
    for j in range(count):
        store(j).wait()
    gradient.finish()


def feed_weights(rows_all, upstream_all, gate, up, hidden, grad, size):
    line, rows, width = rows_all.shape
    tokens, units = gate.shape
    chunk = units // 4
    count = 3 * 4
    block = width // size
    middle = width // 2
    pieces = Scatter.pieces(Links(size))
    hbm = pl.BlockSpec(memory_space=pl.ANY)
    shape = jax.ShapeDtypeStruct
    dma = pltpu.SemaphoreType.DMA
    return pl.pallas_call(
        functools.partial(weight_kernel, size, line),
        out_shape=(shape((block, units), f32),) * 3 + (shape((rows, width), bf16),) * 2,
        in_specs=[hbm] * 6,
        out_specs=[hbm] * 5,
        scratch_shapes=[
            pltpu.VMEM((3, rows, width), bf16),
            pltpu.VMEM((3, rows, width), bf16),
            pltpu.VMEM((2, rows, width), bf16),
            pltpu.VMEM((2, width, tokens), bf16),
            pltpu.VMEM((4, tokens, chunk), bf16),
            pltpu.VMEM((count, middle, chunk), bf16),
            pltpu.VMEM((count, middle, chunk), bf16),
            pltpu.VMEM((count, middle, chunk), bf16),
            pltpu.VMEM((count, pieces, block, chunk), bf16),
            pltpu.VMEM((count, block, chunk), f32),
            dma((count,)),
            dma((count,)),
            dma((count, pieces)),
            dma((count, pieces)),
            dma((count,)),
            dma((2,)),
            dma((count,)),
            dma((5,)),
            dma((5,)),
            dma((3,)),
        ],
        compiler_params=pltpu.CompilerParams(
            collective_id=2, has_side_effects=True, vmem_limit_bytes=63 << 20
        ),
        cost_estimate=pl.CostEstimate(flops=20 << 30, bytes_accessed=60 << 20, transcendentals=0),
    )(rows_all, upstream_all, gate, up, hidden, grad)


def spread_stages(engine, links, first, last, p):
    for stage in range(len(links.bits) + 1)[::-1]:
        @pl.when((p - stage >= first) & (p - stage < last))
        def _(stage=stage):
            for h in (0, 1):
                engine.stage(2 * (p - stage) + h, h, stage)


def backward_kernel(
    size, line, head,
    branch, weights, q_in, k_in, v_in, lse_in, att_in, proj_q, proj_k, gain_qk, cos_in, sin_in, cos_at, sin_at,
    segments, mixed_in,
    gq_out, gkv_out, terms_out, o_out, mixed_out,
    o_full, branch_t, gatt, own_kv, near_f, far_v, near_v, far_in, near_in, odd, core, sums, arrived, out,
    core_send, core_recv, send, recv, far_send, far_recv, near_send, near_recv, local,
    line_send, line_recv, cosine, sine, padded,
):
    links = Links(size)
    d, t = lax.axis_index("dp"), lax.axis_index("tensor")
    rows, width = branch.shape
    span = k_in.shape[1]
    middle = width // 2
    block = out.shape[1]
    factor = head**-0.5
    loads = [
        pltpu.make_async_copy(
            weights.at[h, s, :, 4 * head : 6 * head], o_full.at[s, h], local.at[s, h]
        )
        for s in range(line)
        for h in (0, 1)
    ]
    for copy in loads:
        copy.start()
    greet(links, d, t, line)

    def hop(at, to):
        return mesh_copy(
            mixed_in.at[pl.ds(at * rows, rows)], mixed_out, line_send.at[0], line_recv.at[0], (d, to)
        )

    def hop_of(act):
        @pl.when(t == 0)
        def _():
            act(hop(line - 1, t + 1))

        @pl.when(t == line - 1)
        def _():
            act(hop(0, t - 1))

    hop_of(lambda copy: copy.start())

    engine = Scatter(
        links, d, t, block,
        (
            lambda j: odd.at[j],
            lambda j, at=pl.ds(0, middle): core.at[j, at],
            lambda j, at: sums.at[j, at],
            lambda j, number: arrived.at[j, number],
            lambda j: out.at[j],
        ),
        (
            lambda j: core_send.at[j],
            lambda j: core_recv.at[j],
            lambda j, number: send.at[j, number],
            lambda j, number: recv.at[j, number],
        ),
    )
    branch_t[...] = branch[...].T

    def first(s, carry):
        for h in (0, 1):
            j = 2 * s + h
            right = att_in[s, :, h * 2 * head : (h + 1) * 2 * head]
            odd[j] = nn(branch_t[middle:, :], right).astype(bf16)
            engine.core_copy(j).start()
        for h in (0, 1):
            j = 2 * s + h
            right = att_in[s, :, h * 2 * head : (h + 1) * 2 * head]
            value = nn(branch_t[:middle, :], right)
            sums[j] = value.astype(bf16)
            out[j] = value[:block]
        return carry

    lax.fori_loop(0, line, first, 0)
    for copy in loads:
        copy.wait()

    cosine[...], sine[...] = rope_block((cos_in, sin_in, cos_at, sin_at), t + span // rows - 1, head)
    key_row, _ = segment_masks(segments, padded, t, rows, span)
    key_column = turned(key_row)
    query_row = key_row[:, span - rows :]
    k_index = lax.broadcasted_iota(jnp.int32, (span, rows), 0)
    q_index = lax.broadcasted_iota(jnp.int32, (span, rows), 1) + (span - rows)

    def far_copy(slot):
        return mesh_copy(
            far_v.at[slot], far_in.at[lax.rem(slot + 1, line)], far_send.at[slot],
            far_recv.at[lax.rem(slot + 1, line)], (d, t - 1),
        )

    def near_copy(slot):
        return mesh_copy(
            near_v.at[slot], near_in.at[lax.rem(slot + 1, line)], near_send.at[slot],
            near_recv.at[lax.rem(slot + 1, line)], (d, t - 1),
        )

    def arriving(copy, slot):
        return copy(lax.rem(slot + line - 1, line))

    def pass_near(slot):
        @pl.when((t > 0) & (t < line - 1))
        def _():
            arriving(far_copy, slot).wait_recv()
            near_v[slot] = (near_f[slot] + far_in[slot].astype(f32)).astype(bf16)

        @pl.when(t == line - 1)
        def _():
            near_v[slot] = near_f[slot].astype(bf16)

        @pl.when(t > 0)
        def _():
            near_copy(slot).start()

    def head_back(raw, gain, value, cos, sin):
        c = value * cos + pltpu.roll(value * sin, head // 2, 1)
        inverse = lax.rsqrt(jnp.mean(raw * raw, axis=-1, keepdims=True) + epsilon)
        normed = raw * inverse
        inner = c * gain
        grad = inverse * (inner - normed * jnp.mean(inner * normed, axis=-1, keepdims=True))
        return grad, jnp.sum(c * normed, axis=0, keepdims=True)

    terms_out[...] = jnp.zeros(terms_out.shape, f32)

    def step(s, carry):
        allowed = (key_column == query_row) & (k_index <= q_index)
        for h in (0, 1):
            gatt[:, h * 2 * head : (h + 1) * 2 * head] = nn(branch[...], o_full[s, h]).astype(bf16)
        lse = lse_in[s].T
        for g in (0, 1):
            keys = k_in[s, :, g * head : (g + 1) * head]
            values = v_in[s, :, g * head : (g + 1) * head]
            grad_k = jnp.zeros((span, head), f32)
            grad_v = jnp.zeros((span, head), f32)
            for j in (0, 1):
                h = 2 * g + j
                cols = slice(h * head, (h + 1) * head)
                query = q_in[s, :, cols]
                upward = gatt[:, cols]
                scores = nt(keys, query) * factor
                scores = jnp.where(allowed, scores, -1e30)
                probs = jnp.exp(scores - lse[h : h + 1, :])
                grad_probs = nt(values, upward)
                delta = jnp.sum(probs * grad_probs, axis=0, keepdims=True)
                grad_scores = (probs * (grad_probs - delta)).astype(bf16)
                grad_k = grad_k + nn(grad_scores, query)
                grad_v = grad_v + nn(probs.astype(bf16), upward)
                grad_q = (tn(grad_scores, keys) * factor).astype(bf16).astype(f32)
                grad, term = head_back(proj_q[s, :, cols], gain_qk[0:1, :], grad_q, cosine[...], sine[...])
                gq_out[s, :, cols] = grad.astype(bf16)
                terms_out[0:1, :] += term
            grad_k = grad_k * factor
            for at, value in ((g * head, grad_k), ((2 + g) * head, grad_v)):
                far_v[s, :, at : at + head] = value[:rows].astype(bf16)
                near_f[s, :, at : at + head] = value[rows : 2 * rows]
                own_kv[s, :, at : at + head] = value[2 * rows :]

        @pl.when(t > 1)
        def _():
            far_copy(s).start()

        spread_stages(engine, links, 0, line, s)

        @pl.when(s > 0)
        def _():
            pass_near(s)

        return carry

    lax.fori_loop(0, line, step, 0)
    pass_near(0)

    def last(i, carry):
        s = lax.rem(i + 2, line)
        spread_stages(engine, links, 0, line, i + line)

        @pl.when(t < line - 1)
        def _():
            arriving(near_copy, s).wait_recv()
            own_kv[s] = own_kv[s] + near_in[s].astype(f32)

        for g in (0, 1):
            cols = slice(g * head, (g + 1) * head)
            value = own_kv[s, :, cols].astype(bf16).astype(f32)
            grad, term = head_back(proj_k[s, :, cols], gain_qk[1:2, :], value, cosine[...], sine[...])
            gkv_out[s, :, cols] = grad.astype(bf16)
            terms_out[1:2, :] += term
        gkv_out[s, :, 2 * head :] = own_kv[s, :, 2 * head :].astype(bf16)
        return carry

    lax.fori_loop(0, line, last, 0)

    def finish(s, carry):
        for h in (0, 1):
            engine.finish(2 * s + h, h)
            o_out[s, :, h * 2 * head : (h + 1) * 2 * head] = out[2 * s + h]

        @pl.when(t > 1)
        def _():
            far_copy(s).wait_send()

        @pl.when(t > 0)
        def _():
            near_copy(s).wait_send()

        return carry

    lax.fori_loop(0, line, finish, 0)

    hop_of(lambda copy: copy.wait_send())

    @pl.when((t > 0) & (t < line - 1))
    def _():
        hop(0, t - 1).wait_recv()


def attention_backward(branch, weights, q, k, v, lse, att, proj_q, proj_k, gain_qk, tables, segments, mixed, size):
    line, rows, q_cols = q.shape
    width = branch.shape[1]
    span = k.shape[1]
    head = gain_qk.shape[1]
    block, middle, count, chunk = width // size, width // 2, 2 * line, 2 * head
    pieces = Scatter.pieces(Links(size))
    vmem = pl.BlockSpec(memory_space=pltpu.VMEM)
    hbm = pl.BlockSpec(memory_space=pl.ANY)
    shape = jax.ShapeDtypeStruct
    dma = pltpu.SemaphoreType.DMA
    return pl.pallas_call(
        functools.partial(backward_kernel, size, line, head),
        out_shape=(
            shape((line, rows, 4 * head), bf16),
            shape((line, rows, 4 * head), bf16),
            shape((8, head), f32),
            shape((line, block, 4 * head), f32),
            shape((rows, width), bf16),
        ),
        in_specs=[vmem, hbm] + [vmem] * 13 + [hbm],
        out_specs=[vmem] * 4 + [hbm],
        scratch_shapes=[
            pltpu.VMEM((line, 2, width, 2 * head), bf16),
            pltpu.VMEM((width, rows), bf16),
            pltpu.VMEM((rows, 4 * head), bf16),
            pltpu.VMEM((line, rows, 4 * head), f32),
            pltpu.VMEM((line, rows, 4 * head), f32),
            pltpu.VMEM((line, rows, 4 * head), bf16),
            pltpu.VMEM((line, rows, 4 * head), bf16),
            pltpu.VMEM((line, rows, 4 * head), bf16),
            pltpu.VMEM((line, rows, 4 * head), bf16),
            pltpu.VMEM((count, middle, chunk), bf16),
            pltpu.VMEM((count, middle, chunk), bf16),
            pltpu.VMEM((count, middle, chunk), bf16),
            pltpu.VMEM((count, pieces, block, chunk), bf16),
            pltpu.VMEM((count, block, chunk), f32),
            dma((count,)),
            dma((count,)),
            dma((count, pieces)),
            dma((count, pieces)),
            dma((line,)),
            dma((line,)),
            dma((line,)),
            dma((line,)),
            dma((line, 2)),
            dma((1,)),
            dma((1,)),
            pltpu.VMEM((rows, head), f32),
            pltpu.VMEM((rows, head), f32),
            pltpu.VMEM((8, span - rows + line * rows), f32),
        ],
        compiler_params=pltpu.CompilerParams(
            collective_id=3, has_side_effects=True, vmem_limit_bytes=62 << 20
        ),
        cost_estimate=pl.CostEstimate(flops=20 << 30, bytes_accessed=40 << 20, transcendentals=4 << 20),
    )(branch, weights, q, k, v, lse, att, proj_q, proj_k, gain_qk, *tables, segments, mixed)


def final_kernel(
    size, line, head,
    rows_in, gq_in, gkv_in, o_in, weights, source, grad_middle, gain_one, second_terms, head_terms,
    mixed_two, mixed_in,
    q_out, kv_out, o_out, input_out, terms_out, mixed_left, mixed_right,
    rows_t, pair, acc, odd, core, sums, arrived, out, outbox, inbox, heap, mixed_box, mixed_mail,
    core_send, core_recv, send, recv, local, line_send, line_recv, heap_send, heap_recv, mixed_send, mixed_recv, mixed_local,
):
    links = Links(size)
    d, t = lax.axis_index("dp"), lax.axis_index("tensor")
    rows, width = rows_in.shape
    middle = width // 2
    block = out.shape[1]
    chunk = 4 * head
    last_stage = len(links.bits)
    inner = (t > 0) & (t < line - 1)
    is_end = (t == 0) | (t == line - 1)

    def slot_at(i):
        return slot_of(line - 1 - i, t, line)

    def load(i, h):
        return pltpu.make_async_copy(
            weights.at[h, slot_at(i), :, 0 : 4 * head], pair.at[h], local.at[h]
        )

    for h in (0, 1):
        load(0, h).start()
    inside = block % 128 == 0
    greet(links, d, t, line, inside)

    def mixed_hop(number):
        source, target, to = (
            (mixed_two, mixed_mail.at[0], t - 1),
            (mixed_two, mixed_mail.at[1], t + 1),
            (mixed_box.at[0], mixed_left, t - 1),
            (mixed_box.at[1], mixed_right, t + 1),
        )[number]
        return mesh_copy(source, target, mixed_send.at[number], mixed_recv.at[number], (d, to))

    def mixed_own(box):
        position = lax.rem(t + (3, 1)[box], line)
        at = pl.ds(pl.multiple_of(position * rows, rows), rows)
        return pltpu.make_async_copy(mixed_in.at[at], mixed_box.at[box], mixed_local.at[box])

    @pl.when(t >= line // 2)
    def _():
        mixed_hop(0).start()

    @pl.when(t < line // 2)
    def _():
        mixed_hop(1).start()

    for box in (0, 1):
        mixed_own(box).start()

    def mixed_on():
        for box in (0, 1):
            mixed_own(box).wait()

            @pl.when(inner)
            def _(box=box):
                mixed_hop(box).wait_recv()
                mixed_box[box] = (
                    mixed_box[box].astype(f32) + mixed_mail[box].astype(f32)
                ).astype(bf16)

        @pl.when(t > 0)
        def _():
            mixed_hop(2).start()

        @pl.when(t < line - 1)
        def _():
            mixed_hop(3).start()

    engine = Scatter(
        links, d, t, block,
        (
            lambda j: odd.at[lax.rem(j, odd.shape[0])],
            lambda j, at=pl.ds(0, middle): core.at[j, at],
            lambda j, at: sums.at[j, at],
            lambda j, number: arrived.at[j, number],
            lambda j: out.at[j],
        ),
        (
            lambda j: core_send.at[j],
            lambda j: core_recv.at[j],
            lambda j, number: send.at[j, number],
            lambda j, number: recv.at[j, number],
        ),
    )
    rows_t[...] = rows_in[...].T
    acc[...] = jnp.zeros(acc.shape, f32)

    def first(i, carry):
        slot = slot_at(i)
        for h in (0, 1):
            j = 2 * i + h

            @pl.when(i >= odd.shape[0] // 2)
            def _(j=j):
                engine.core_copy(j - odd.shape[0]).wait_send()

            odd[lax.rem(j, odd.shape[0])] = nn(
                rows_t[middle:, :], (gq_in, gkv_in)[h][slot]
            ).astype(bf16)
            engine.core_copy(j).start()
        for h in (0, 1):
            j = 2 * i + h
            value = nn(rows_t[:middle, :], (gq_in, gkv_in)[h][slot])
            sums[j] = value.astype(bf16)
            out[j] = value[:block]
        return carry

    lax.fori_loop(0, line, first, 0)

    def content(i, c):
        return o_in[slot_at(i)] if c == 2 else out[2 * i + c]

    def each(fill):
        for c in range(3):
            fill(c, slice(c * chunk, (c + 1) * chunk))

    def post(number, to):
        box = (0, 1, 1, 3, 2)[number]
        return mesh_copy(
            outbox.at[box], inbox.at[number], line_send.at[number], line_recv.at[number], (d, to)
        )

    def first_post():
        return post(0, jnp.where(t == 0, t + 1, t - 1))

    def along(i):
        if i == 0:

            @pl.when(is_end)
            def _():
                def fill(c, at):
                    outbox[0, :, at] = content(0, c).astype(bf16)

                each(fill)
                first_post().start()

        if i == 1:

            @pl.when(inner)
            def _():
                first_post().wait_recv()

            @pl.when(is_end)
            def _():
                inbox[0] = jnp.zeros(inbox.shape[1:], bf16)

            def fill(c, at):
                outbox[1, :, at] = (content(1, c) + inbox[0, :, at].astype(f32)).astype(bf16)

            each(fill)

            @pl.when(t >= 2)
            def _():
                post(1, t - 1).start()

            @pl.when(t <= 1)
            def _():
                post(2, t + 1).start()

        if i == 2:

            @pl.when(inner)
            def _():
                post(1, t - 1).wait_recv()
                post(2, t + 1).wait_recv()

            @pl.when(is_end)
            def _():
                inbox[1] = jnp.zeros(inbox.shape[1:], bf16)
                inbox[2] = jnp.zeros(inbox.shape[1:], bf16)

            def leftward(c, at):
                three = jnp.where(t == line - 1, content(2, c), content(0, c))
                outbox[3, :, at] = (three + inbox[1, :, at].astype(f32)).astype(bf16)

            def rightward(c, at):
                outbox[2, :, at] = (content(2, c) + inbox[2, :, at].astype(f32)).astype(bf16)

            @pl.when(t > 0)
            def _():
                each(leftward)
                post(3, t - 1).start()

            @pl.when(t < line - 1)
            def _():
                each(rightward)
                post(4, t + 1).start()

    part = rows // 4
    terms_out[...] = jnp.zeros(terms_out.shape, f32)
    terms_out[1:2, :] = second_terms[...]
    terms_out[2:3, 0:head] = head_terms[0:1, :]
    terms_out[2:3, head : 2 * head] = head_terms[1:2, :]

    def close(r, carry):
        at = pl.ds(pl.multiple_of(r * part, part), part)
        values = source[at, :]
        inverse = lax.rsqrt(jnp.mean(values * values, axis=-1, keepdims=True) + epsilon)
        normed = values * inverse
        c = acc[at, :]
        term = c * gain_one[...]
        grad = inverse * (term - normed * jnp.mean(term * normed, axis=-1, keepdims=True))
        input_out[at, :] = (grad_middle[at, :] + grad).astype(bf16)
        terms_out[0:1, :] += jnp.sum(c * normed, axis=0, keepdims=True)
        return carry

    def double(start, stop):
        hops = [((d ^ bit, t), bit) for bit in [1] + links.bits]
        hops = hops + [((d, t ^ 1), 0), ((d, t ^ 2), 0)]
        for k in range(start, stop):
            to, bit = hops[k]
            copy = mesh_copy(terms_out, heap.at[k], heap_send.at[k], heap_recv.at[k], to)
            copy.start()
            copy.wait()
            for i, mask in enumerate(links.masks):
                other = links.masks.index(mask ^ bit)
                terms_out[0:2, i * block : (i + 1) * block] += heap[
                    k, 0:2, other * block : (other + 1) * block
                ]
            terms_out[2:3, :] += heap[k, 2:3, :]

    def step(i, carry):
        @pl.when(i < line)
        def _():
            for h in (0, 1):
                load(i, h).wait()
            slot = slot_at(i)
            for n in range(4):
                at = slice(n * (width // 4), (n + 1) * (width // 4))
                acc[:, at] += nt(gq_in[slot], pair[0, at, :]) + nt(gkv_in[slot], pair[1, at, :])

            @pl.when(i + 1 < line)
            def _():
                for h in (0, 1):
                    load(i + 1, h).start()

        @pl.when(i == 1)
        def _():
            mixed_on()

        @pl.when(i == line)
        def _():
            lax.fori_loop(0, 4, close, 0)

        spread_stages(engine, links, 0, line, i)
        for p in range(line - 1):

            @pl.when(i == p + last_stage)
            def _(p=p):
                along(p)

        if inside:

            @pl.when(i == line)
            def _():
                double(0, 3)

        return carry

    lax.fori_loop(0, line + last_stage, step, 0)

    if inside:
        double(3, 3 + len(links.bits))

    @pl.when(t < line - 1)
    def _():
        post(3, t - 1).wait_recv()

    @pl.when(t == line - 1)
    def _():
        inbox[3] = jnp.zeros(inbox.shape[1:], bf16)

    @pl.when(t > 0)
    def _():
        post(4, t + 1).wait_recv()

    @pl.when(t == 0)
    def _():
        inbox[4] = jnp.zeros(inbox.shape[1:], bf16)

    def total(c, at):
        (q_out, kv_out, o_out)[c][...] = (
            content(line - 1, c) + inbox[3, :, at].astype(f32) + inbox[4, :, at].astype(f32)
        )

    each(total)

    def finish(i, carry):
        for h in (0, 1):
            engine.finish(2 * i + h, h, False)

            @pl.when(i >= line - odd.shape[0] // 2)
            def _(h=h):
                engine.core_copy(2 * i + h).wait_send()

        return carry

    lax.fori_loop(0, line, finish, 0)

    @pl.when(t >= line // 2)
    def _():
        mixed_hop(0).wait_send()

    @pl.when(t < line // 2)
    def _():
        mixed_hop(1).wait_send()

    @pl.when(t > 0)
    def _():
        mixed_hop(2).wait_send()
        mixed_hop(3).wait_recv()

    @pl.when(t < line - 1)
    def _():
        mixed_hop(3).wait_send()
        mixed_hop(2).wait_recv()

    @pl.when(is_end)
    def _():
        first_post().wait_send()

    @pl.when(t >= 2)
    def _():
        post(1, t - 1).wait_send()

    @pl.when(t <= 1)
    def _():
        post(2, t + 1).wait_send()

    @pl.when(t > 0)
    def _():
        post(3, t - 1).wait_send()

    @pl.when(t < line - 1)
    def _():
        post(4, t + 1).wait_send()


def attention_weights(rows_one, gq, gkv, o_sum, weights, source, grad_middle, gain_one, second_terms, head_terms, mixed_two, mixed_part, size, head):
    line, rows, chunk = gq.shape
    width = rows_one.shape[1]
    block, middle, count = width // size, width // 2, 2 * line
    pieces = Scatter.pieces(Links(size))
    hops = 3 + len(Links(size).bits)
    vmem = pl.BlockSpec(memory_space=pltpu.VMEM)
    hbm = pl.BlockSpec(memory_space=pl.ANY)
    shape = jax.ShapeDtypeStruct
    dma = pltpu.SemaphoreType.DMA
    return pl.pallas_call(
        functools.partial(final_kernel, size, line, head),
        out_shape=(
            shape((block, chunk), f32),
            shape((block, chunk), f32),
            shape((block, chunk), f32),
            shape((rows, width), bf16),
            shape((8, width), f32),
            shape((rows, width), bf16),
            shape((rows, width), bf16),
        ),
        in_specs=[vmem] * 4 + [hbm] + [vmem] * 5 + [hbm] * 2,
        out_specs=[vmem] * 5 + [hbm] * 2,
        scratch_shapes=[
            pltpu.VMEM((width, rows), bf16),
            pltpu.VMEM((2, width, chunk), bf16),
            pltpu.VMEM((rows, width), f32),
            pltpu.VMEM((count // 2, middle, chunk), bf16),
            pltpu.VMEM((count, middle, chunk), bf16),
            pltpu.VMEM((count, middle, chunk), bf16),
            pltpu.VMEM((count, pieces, block, chunk), bf16),
            pltpu.VMEM((count, block, chunk), f32),
            pltpu.VMEM((4, block, 3 * chunk), bf16),
            pltpu.VMEM((5, block, 3 * chunk), bf16),
            pltpu.VMEM((hops, 8, width), f32),
            pltpu.VMEM((2, rows, width), bf16),
            pltpu.VMEM((2, rows, width), bf16),
            dma((count,)),
            dma((count,)),
            dma((count, pieces)),
            dma((count, pieces)),
            dma((2,)),
            dma((5,)),
            dma((5,)),
            dma((hops,)),
            dma((hops,)),
            dma((4,)),
            dma((4,)),
            dma((2,)),
        ],
        compiler_params=pltpu.CompilerParams(
            collective_id=4, has_side_effects=True, vmem_limit_bytes=63 << 20
        ),
        cost_estimate=pl.CostEstimate(flops=16 << 30, bytes_accessed=40 << 20, transcendentals=0),
    )(rows_one, gq, gkv, o_sum, weights, source, grad_middle, gain_one, second_terms, head_terms, mixed_two, mixed_part)


def body(
    layer_input,
    first_gain,
    query_weight,
    key_matrix,
    value_matrix,
    query_gain,
    key_gain,
    output_weight,
    second_gain,
    gate_weight,
    up_weight,
    down_weight,
    segments,
    cotangent,
):
    plan = Plan()
    line, place = plan.line, plan.place
    rows, seq_count, width = layer_input.shape
    head = query_gain.shape[0]
    kv_heads = key_matrix.shape[1] // head
    query_heads = query_weight.shape[1] // head
    groups = query_heads // kv_heads
    all_kv = line * kv_heads
    half = width // 2
    hops = -(-(longest_document - 1) // rows)
    assert seq_count == 1 and hops == 2
    factor = head**-0.5

    gain_one = plan.to_masks(first_gain.astype(f32))
    gain_two = plan.to_masks(second_gain.astype(f32))
    source = plan.to_masks(layer_input[:, 0, :]).astype(f32)
    upstream = plan.to_masks(cotangent[:, 0, :])

    normed, inverse_one = rms_parts(source, gain_one)
    rows_one = normed.astype(bf16)
    tables = rope_tables(-hops * rows, 8, rows, head)
    gain_qk = jnp.stack([query_gain, key_gain]).astype(f32)
    (
        weights, pair_full, upstream_all, proj_query, proj_key, query_rows, key_rows, value_rows, lse,
        attended, middle, rows_two_own,
    ) = attention_forward(
        (query_weight, key_matrix, value_matrix, output_weight), (gate_weight, up_weight), rows_one,
        upstream, source, gain_qk, gain_two[None], tables, segments, plan.size, line,
    )
    inverse_two = lax.rsqrt(jnp.mean(middle * middle, axis=-1, keepdims=True) + epsilon)

    rows_two, hidden, grad_gate, grad_up, grad_two_part, mixed_part = feed_forward(
        rows_two_own, upstream_all, pair_full, down_weight, plan.size, line
    )

    def unslot(values):
        return values.reshape(-1, values.shape[2])

    hidden, grad_gate, grad_up = map(unslot, (hidden, grad_gate, grad_up))
    inner = (place > 0) & (place < line - 1)

    def share(step, part=mixed_part):
        return lax.dynamic_slice(part, ((place + step) % line * rows, 0), (rows, width)).astype(f32)

    def closed(part, from_right, from_left):
        return (
            share(0, part)
            + jnp.where(place < line - 1, from_right.astype(f32), 0.0)
            + jnp.where(place > 0, from_left.astype(f32), 0.0)
        )

    gate_grad, up_grad, down_grad, grad_left, grad_right = feed_weights(
        rows_two, upstream_all, grad_gate, grad_up, hidden, grad_two_part, plan.size
    )
    grad_two = closed(grad_two_part, grad_left, grad_right)

    grad_mid_norm, gain_two_terms = rms_back(middle, inverse_two, gain_two, grad_two)
    grad_middle = upstream.astype(f32) + grad_mid_norm
    grad_branch = grad_middle.astype(bf16)
    grad_query_low, grad_kv_low, head_terms, output_sum, mixed_one = attention_backward(
        grad_branch, weights, query_rows, key_rows, value_rows, lse, attended, proj_query, proj_key,
        gain_qk, tables, segments, mixed_part, plan.size,
    )
    mixed_two = (share(2) + jnp.where(inner, mixed_one.astype(f32), 0.0)).astype(bf16)
    second_terms = jnp.sum(gain_two_terms, axis=0, keepdims=True)
    query_weight_grad, kv_grad, output_grad, input_masked, terms, mixed_left, mixed_right = attention_weights(
        rows_one, grad_query_low, grad_kv_low, output_sum, weights, source, grad_middle, gain_one[None],
        second_terms, head_terms, mixed_two, mixed_part, plan.size, head,
    )
    input_grad = plan.from_masks(input_masked)[:, None, :]
    middle_late = after(middle, terms)
    mixed = closed(mixed_part, mixed_left, mixed_right)
    layer_output = plan.from_masks((middle_late + mixed).astype(bf16))[:, None, :]
    gains = jnp.concatenate([plan.from_masks(terms[0]), plan.from_masks(terms[1]), terms[2, : 2 * head]])
    if width // plan.size % 128:
        gains = plan.total(gains)
    return (
        layer_output,
        input_grad,
        gains[:width],
        query_weight_grad,
        kv_grad[:, : key_matrix.shape[1]],
        kv_grad[:, key_matrix.shape[1] :],
        gains[2 * width : 2 * width + head],
        gains[2 * width + head :],
        output_grad,
        gains[width : 2 * width],
        gate_grad,
        up_grad,
        down_grad,
    )


def solution(mesh):
    positions = P("tensor", "dp", None)
    weight = P("dp", "tensor")
    return jax.shard_map(
        body,
        mesh=mesh,
        in_specs=(
            positions,
            P(),
            weight,
            weight,
            weight,
            P(),
            P(),
            weight,
            P(),
            weight,
            weight,
            weight,
            P("dp", None),
            positions,
        ),
        out_specs=(
            positions,
            positions,
            P(),
            weight,
            weight,
            weight,
            P(),
            P(),
            weight,
            P(),
            weight,
            weight,
            weight,
        ),
        check_vma=False,
    )
```

```python
import functools

import jax
import jax.numpy as jnp
import numpy as np
from jax import lax
from jax.experimental import pallas as pl
from jax.experimental.pallas import tpu as pltpu
from jax.sharding import PartitionSpec as P

epsilon = 1e-06
rope_base = 1000000.0
longest_document = 512
bf16 = jnp.bfloat16
f32 = jnp.float32


def mm(eq, a, b):
    return jnp.einsum(eq, a, b, preferred_element_type=f32)


def rms_parts(values, gain):
    inverse = lax.rsqrt(jnp.mean(values * values, axis=-1, keepdims=True) + epsilon)
    return values * inverse * gain, inverse


def rms_back(values, inverse, gain, upstream):
    normed = values * inverse
    inner = upstream * gain
    grad = inverse * (inner - normed * jnp.mean(inner * normed, axis=-1, keepdims=True))
    return grad, upstream * normed


def rope_tables(first, count, block, head_size):
    half = head_size // 2
    exponent = -(2.0 * np.arange(half, dtype=np.float32)) / np.float32(head_size)
    frequency = np.power(np.float32(rope_base), exponent, dtype=np.float32).astype(np.float64)
    frequency = np.concatenate([frequency, frequency])[None, :]
    inside = np.arange(block)[:, None] * frequency
    starts = (first + block * np.arange(count))[:, None] * frequency
    return tuple(f(a).astype(np.float32) for a in (inside, starts) for f in (np.cos, np.sin))


def rope_block(tables, number, head):
    cos_in, sin_in, cos_at, sin_at = tables
    cos_start, sin_start = cos_at[pl.ds(number, 1), :], sin_at[pl.ds(number, 1), :]
    cosine = cos_start * cos_in[...] - sin_start * sin_in[...]
    sine = sin_start * cos_in[...] + cos_start * sin_in[...]
    lane = lax.broadcasted_iota(jnp.int32, sine.shape, 1)
    return cosine, jnp.where(lane < head // 2, -sine, sine)


class Plan:
    def __init__(self):
        self.size = lax.axis_size("dp")
        self.index = lax.axis_index("dp")
        self.place = lax.axis_index("tensor")
        self.line = lax.axis_size("tensor")
        assert self.line == 4
        self.others = [1 << i for i in range(1, self.size.bit_length() - 1)]
        evens = [0]
        for bit in self.others:
            evens = evens + [m ^ bit for m in evens]
        self.evens = evens
        self.masks = evens + [m ^ 1 for m in evens]
        self.forward = self.others
        self.backward = self.others[::-1]

    def swap(self, value, bit):
        return lax.ppermute(value, "dp", [(i, i ^ bit) for i in range(self.size)])

    def move(self, value, pairs):
        return lax.ppermute(value, "tensor", pairs)

    def xor_blocks(self, blocks):
        bit = 1
        while bit < self.size:
            on = (self.index & bit) != 0
            blocks = [jnp.where(on, blocks[i ^ bit], blocks[i]) for i in range(self.size)]
            bit *= 2
        return blocks

    def to_masks(self, value):
        blocks = self.xor_blocks(jnp.split(value, self.size, axis=-1))
        return jnp.concatenate([blocks[m] for m in self.masks], axis=-1)

    def from_masks(self, value):
        parts = jnp.split(value, self.size, axis=-1)
        blocks = [parts[self.masks.index(m)] for m in range(self.size)]
        return jnp.concatenate(self.xor_blocks(blocks), axis=-1)

    def gather(self, shard, order):
        rows = shard.shape[0]
        held, masks = shard, [0]
        for bit in order:
            arrived = self.swap(held, bit)
            held = jnp.concatenate([held, arrived], axis=0)
            masks = masks + [m ^ bit for m in masks]
        if masks != self.evens:
            held = jnp.concatenate(
                [lax.slice_in_dim(held, masks.index(m) * rows, (masks.index(m) + 1) * rows) for m in self.evens],
                axis=0,
            )
        return held, self.swap(held, 1)

    def reduce(self, even, odd, order):
        rows = even.shape[0] // len(self.evens)
        total = even.astype(f32) + self.swap(odd.astype(bf16), 1).astype(f32)
        pieces = {
            m: lax.slice_in_dim(total, i * rows, (i + 1) * rows) for i, m in enumerate(self.evens)
        }
        for bit in order:
            leaving = [m for m in pieces if m & bit]
            sent = jnp.concatenate([pieces[m].astype(bf16) for m in leaving], axis=0)
            arrived = self.swap(sent, bit)
            kept = {m: v for m, v in pieces.items() if not m & bit}
            for i, m in enumerate(leaving):
                kept[m ^ bit] = kept[m ^ bit] + lax.slice_in_dim(
                    arrived, i * rows, (i + 1) * rows
                ).astype(f32)
            pieces = kept
        return pieces[0]

    def gather_line(self, own):
        from_right = self.move(own, [(1, 0), (2, 1), (3, 2)])
        from_left = self.move(own, [(0, 1), (1, 2), (2, 3)])
        right_two = self.move(from_right, [(1, 0), (2, 1)])
        left_two = self.move(from_left, [(1, 2), (2, 3)])
        slot_two = jnp.where(self.place < 2, right_two, left_two)
        last = self.move(slot_two, [(1, 0), (2, 3)])
        slot_one = jnp.where(self.place < 3, from_right, last)
        slot_three = jnp.where(self.place > 0, from_left, last)
        return [own, slot_one, slot_two, slot_three]

    def scatter_line(self, slots):
        zero, one, two, three = slots
        first = self.move(
            jnp.where(self.place == 3, one, three).astype(bf16), [(3, 2), (0, 1)]
        )
        middle = (two + first.astype(f32)).astype(bf16)
        leftward = self.move(middle, [(3, 2), (2, 1)])
        rightward = self.move(middle, [(0, 1), (1, 2)])
        leftward = self.move(
            (three + leftward.astype(f32)).astype(bf16), [(3, 2), (2, 1), (1, 0)]
        )
        rightward = self.move(
            (one + rightward.astype(f32)).astype(bf16), [(0, 1), (1, 2), (2, 3)]
        )
        return zero + leftward.astype(f32) + rightward.astype(f32)

    def total(self, value):
        bit = 1
        while bit < self.size:
            value = value + self.swap(value, bit)
            bit *= 2
        for bit in (1, 2):
            value = value + self.move(value, [(i, i ^ bit) for i in range(self.line)])
        return value


def after(value, *others):
    return lax.optimization_barrier((value,) + others)[0]


def mesh_copy(src, dst, send, recv, device):
    return pltpu.make_async_remote_copy(
        src_ref=src, dst_ref=dst, send_sem=send, recv_sem=recv, device_id=device,
        device_id_type=pl.DeviceIdType.MESH,
    )


class Links:
    def __init__(self, size):
        bits = [1 << i for i in range(1, size.bit_length() - 1)]
        self.orders = (bits, bits[::-1])
        evens = [0]
        for bit in bits:
            evens = evens + [m ^ bit for m in evens]
        self.evens = evens
        self.masks = evens + [m ^ 1 for m in evens]
        self.bits = bits

    def onward(self, half, mask):
        order = self.orders[half]
        last = max([i for i, bit in enumerate(order) if mask & bit], default=-1)
        return order[last + 1 :]


class Gather:
    def __init__(self, links, d, t, piece, send, recv):
        self.links, self.d, self.t = links, d, t
        self.piece, self.send, self.recv = piece, send, recv

    def copy(self, half, mask, bit):
        index = self.links.masks.index(mask ^ bit)
        return mesh_copy(
            self.piece(half, mask), self.piece(half, mask ^ bit), self.send(half, index),
            self.recv(half, index), (self.d ^ bit, self.t),
        )

    def launch(self):
        for step in range(len(self.links.bits)):
            for half in (0, 1):
                self.copy(half, 0, self.links.orders[half][step]).start()
        for half in (0, 1):
            self.copy(half, 0, 1).start()

    def arrive(self, half, mask):
        bit = [b for b in self.links.orders[half] if b & mask][-1]
        self.copy(half, mask ^ bit, bit).wait_recv()
        for other in self.links.onward(half, mask):
            self.copy(half, mask, other).start()
        self.copy(half, mask, 1).start()

    def onward(self):
        for mask in self.links.evens[1:]:
            for half in (0, 1):
                if self.links.onward(half, mask):
                    self.arrive(half, mask)

    def complete(self):
        for mask in self.links.evens[1:]:
            for half in (0, 1):
                if not self.links.onward(half, mask):
                    self.arrive(half, mask)
        for mask in self.links.evens:
            for half in (0, 1):
                self.copy(half, mask, 1).wait_recv()

    def finish(self):
        for mask in self.links.masks[1:]:
            for half in (0, 1):
                self.copy(half, mask ^ 1 if mask & 1 else 0, 1 if mask & 1 else mask).wait_send()


class Relay:
    def __init__(self, d, t, line, slot, send, recv):
        self.d, self.t, self.line = d, t, line
        self.slot, self.send, self.recv = slot, send, recv
        self.inner = (t > 0) & (t < line - 1)

    def copy(self, number, source, target, to):
        return mesh_copy(
            self.slot(source), self.slot(target), self.send.at[number], self.recv.at[target],
            (self.d, to),
        )

    def moves(self):
        t = self.t
        return (
            (t > 0, (0, 0, 1, t - 1)),
            (t < self.line - 1, (1, 0, 3, t + 1)),
            (self.inner, (2, 1, 2, t - 1)),
            (self.inner, (3, 3, 2, t + 1)),
            (t == 1, (4, 2, 3, t - 1)),
            (t == 2, (5, 2, 1, t + 1)),
        )

    def start(self, *numbers):
        for number in numbers:
            condition, route = self.moves()[number]

            @pl.when(condition)
            def _(route=route):
                self.copy(*route).start()

    def wait(self, slot):
        self.copy(0, 0, slot, self.t).wait_recv()

    def finish(self):
        for condition, route in self.moves():

            @pl.when(condition)
            def _(route=route):
                self.copy(*route).wait_send()

    def first(self):
        self.start(0, 1)

    def second(self):
        t, line = self.t, self.line

        @pl.when(t < line - 1)
        def _():
            self.wait(1)

        self.start(2)

        @pl.when(t > 0)
        def _():
            self.wait(3)

        self.start(3)

    def third(self):
        self.wait(2)
        self.start(4, 5)

    def ends(self):
        @pl.when(self.t == 0)
        def _():
            self.wait(3)

        @pl.when(self.t == self.line - 1)
        def _():
            self.wait(1)


def slot_of(i, t, line):
    far = jnp.where(t < line - 1, 1, 3)
    near = jnp.where(t < line - 1, 3, 1)
    return jnp.where(i == 0, 0, jnp.where(i == 1, far, jnp.where(i == 2, 2, near)))


def greet(links, d, t, line, across=False):
    barrier = pltpu.get_barrier_semaphore()
    if across:
        pl.semaphore_signal(barrier, inc=1, device_id=(d, t ^ 2), device_id_type=pl.DeviceIdType.MESH)
    for bit in [1] + links.bits:
        pl.semaphore_signal(barrier, inc=1, device_id=(d ^ bit, t), device_id_type=pl.DeviceIdType.MESH)

    @pl.when(t > 0)
    def _():
        pl.semaphore_signal(barrier, inc=1, device_id=(d, t - 1), device_id_type=pl.DeviceIdType.MESH)

    @pl.when(t < line - 1)
    def _():
        pl.semaphore_signal(barrier, inc=1, device_id=(d, t + 1), device_id_type=pl.DeviceIdType.MESH)

    pl.semaphore_wait(
        barrier,
        1 + across + len(links.bits) + jnp.where(t > 0, 1, 0) + jnp.where(t < line - 1, 1, 0),
    )


def nt(a, b):
    return lax.dot_general(a, b, (((1,), (1,)), ((), ())), preferred_element_type=f32)


def tn(a, b):
    return lax.dot_general(a, b, (((0,), (0,)), ((), ())), preferred_element_type=f32)


def nn(a, b):
    return jnp.dot(a, b, preferred_element_type=f32)


def head_norm(values, gain):
    inverse = lax.rsqrt(jnp.mean(values * values, axis=-1, keepdims=True) + epsilon)
    return values * inverse * gain


def segment_masks(segments, padded, t, rows, span):
    ahead = span - rows
    padded[...] = jnp.full(padded.shape, -1.0, f32)
    padded[0:1, ahead:] = segments[...].astype(f32)
    key_row = padded[0:1, pl.ds(pl.multiple_of(t * rows, 128), span)]
    return key_row, turned(key_row[:, ahead:])


def turned(row):
    return jnp.broadcast_to(row, (128, row.shape[1])).T[:, 0:1]


def forward_kernel(
    size, line, head,
    q_shard, k_shard, v_shard, o_shard, gate_shard, up_shard, rows_in, upstream, source, gain_qk, gain_two,
    cos_in, sin_in, cos_at, sin_at, segments,
    weights_out, mlp_out, upstream_all, proj_q, proj_k, q_out, k_out, v_out, lse_out, att_out, middle, normed_out,
    full, rows_all, acc,
    z_send, z_recv, send, recv, row_send, row_recv, keep, mlp_send, mlp_recv, up_send, up_recv, local, cosine, sine, padded,
):
    links = Links(size)
    d, t = lax.axis_index("dp"), lax.axis_index("tensor")
    block = q_shard.shape[0]
    rows, width = rows_in.shape
    span = rows_all.shape[0]
    factor = head**-0.5

    def place(mask):
        return pl.ds(links.masks.index(mask) * block, block)

    def gather(slot):
        return Gather(
            links, d, t,
            lambda half, mask: full.at[half, slot, place(mask)],
            lambda half, index: send.at[slot, half, index],
            lambda half, index: recv.at[slot, half, index],
        )

    feed = Gather(
        links, d, t,
        lambda half, mask: mlp_out.at[half, place(mask)],
        lambda half, index: mlp_send.at[half, index],
        lambda half, index: mlp_recv.at[half, index],
    )
    relay = Relay(d, t, line, lambda slot: full.at[:, slot, place(0)], z_send, z_recv)
    upward = Relay(d, t, line, lambda slot: upstream_all.at[slot], up_send, up_recv)

    o_half = 2 * head
    parts = (
        (q_shard, full.at[0, 0, place(0), 0 : 4 * head]),
        (o_shard.at[:, 0:o_half], full.at[0, 0, place(0), 4 * head : 6 * head]),
        (k_shard, full.at[1, 0, place(0), 0 : 2 * head]),
        (v_shard, full.at[1, 0, place(0), 2 * head : 4 * head]),
        (o_shard.at[:, o_half : 2 * o_half], full.at[1, 0, place(0), 4 * head : 6 * head]),
        (gate_shard, mlp_out.at[0, place(0)]),
        (up_shard, mlp_out.at[1, place(0)]),
        (upstream, upstream_all.at[0]),
    )
    own = [
        pltpu.make_async_copy(source_ref, target_ref, local.at[n])
        for n, (source_ref, target_ref) in enumerate(parts)
    ]
    for copy in own:
        copy.start()
    rows_all[pl.ds(span - rows, rows), :] = rows_in[...]

    @pl.when(t == 0)
    def _():
        rows_all[pl.ds(0, 2 * rows), :] = jnp.zeros((2 * rows, width), bf16)

    @pl.when(t == 1)
    def _():
        rows_all[pl.ds(0, rows), :] = jnp.zeros((rows, width), bf16)

    greet(links, d, t, line)
    for copy in own[:5]:
        copy.wait()

    row_one = mesh_copy(
        rows_in, rows_all.at[pl.ds(rows, rows)], row_send.at[0], row_recv.at[0], (d, t + 1)
    )
    row_two = mesh_copy(
        rows_all.at[pl.ds(rows, rows)], rows_all.at[pl.ds(0, rows)], row_send.at[1],
        row_recv.at[1], (d, t + 1),
    )
    inner = relay.inner
    relay.first()

    @pl.when(t < line - 1)
    def _():
        row_one.start()

    gather(0).launch()
    gather(0).onward()
    relay.second()
    second = slot_of(1, t, line)

    @pl.when(t < line - 1)
    def _():
        gather(1).launch()

    @pl.when(t == line - 1)
    def _():
        gather(3).launch()

    @pl.when(t > 0)
    def _():
        row_one.wait_recv()

    @pl.when(inner)
    def _():
        row_two.start()

    relay.third()
    gather(2).launch()
    gather(second).onward()

    @pl.when(t > 1)
    def _():
        row_two.wait_recv()

    for copy in own[5:]:
        copy.wait()
    key_row, query_column = segment_masks(segments, padded, t, rows, span)
    for n in range(span // rows):
        at = pl.ds(n * rows, rows)
        cosine[at, :], sine[at, :] = rope_block((cos_in, sin_in, cos_at, sin_at), t + n, head)
    upward.first()
    acc[...] = source[...].astype(f32)

    lane = lax.broadcasted_iota(jnp.int32, (rows, 128), 1)
    q_index = lax.broadcasted_iota(jnp.int32, (rows, span), 0) + (span - rows)
    k_index = lax.broadcasted_iota(jnp.int32, (rows, span), 1)

    def step(i, carry):
        slot = slot_of(i, t, line)

        @pl.when(i == 1)
        def _():
            relay.ends()
            gather(slot_of(3, t, line)).launch()

        @pl.when(i >= 2)
        def _():
            gather(slot).onward()

        @pl.when((i == 2))
        def _():
            feed.launch()

        gather(slot).complete()
        for half in (0, 1):
            pltpu.make_async_copy(
                full.at[half, slot], weights_out.at[half, slot], keep.at[slot, half]
            ).start()

        own_rows = pl.ds(span - rows, rows)
        allowed = (query_column == key_row) & (k_index <= q_index)
        lse_acc = jnp.zeros((rows, 128), f32)
        for g in (0, 1):
            key_cols = slice(g * head, (g + 1) * head)
            if g == 0:
                for r in range(span // rows):
                    part = pl.ds(r * rows, rows)
                    both = nn(rows_all[part, :], full[1, slot, :, 0 : 4 * head])
                    if r == span // rows - 1:
                        proj_k[slot] = both[:, : 2 * head]
                    for h in (0, 1):
                        unit = head_norm(both[:, h * head : (h + 1) * head], gain_qk[1:2, :])
                        turned = unit * cosine[part, :] + pltpu.roll(unit, head // 2, 1) * sine[part, :]
                        k_out[slot, part, h * head : (h + 1) * head] = turned.astype(bf16)
                    v_out[slot, part, :] = both[:, 2 * head :].astype(bf16)
            for j in (0, 1):
                h = 2 * g + j
                cols = slice(h * head, (h + 1) * head)
                raw = nn(rows_in[...], full[0, slot, :, cols])
                proj_q[slot, :, cols] = raw
                unit = head_norm(raw, gain_qk[0:1, :])
                turned = unit * cosine[own_rows, :] + pltpu.roll(unit, head // 2, 1) * sine[own_rows, :]
                query = turned.astype(bf16)
                q_out[slot, :, cols] = query
                scores = nt(query, k_out[slot, :, key_cols]) * factor
                scores = jnp.where(allowed, scores, -1e30)
                top = jnp.max(scores, axis=-1, keepdims=True)
                weight = jnp.exp(scores - top)
                total = jnp.sum(weight, axis=-1, keepdims=True)
                probs = (weight / total).astype(bf16)
                att_out[slot, :, cols] = nn(probs, v_out[slot, :, key_cols]).astype(bf16)
                lse_acc = jnp.where(lane == h, top + jnp.log(total), lse_acc)
        lse_out[slot] = lse_acc
        for half in (0, 1):
            acc[...] += nt(
                att_out[slot, :, half * 2 * head : (half + 1) * 2 * head],
                full[half, slot, :, 4 * head : 6 * head],
            )

        @pl.when((i == 2))
        def _():
            upward.second()

        return carry

    lax.fori_loop(0, line, step, 0)
    upward.third()
    feed.onward()
    values = acc[...]
    middle[...] = values
    normed_out[...] = head_norm(values, gain_two[...]).astype(bf16)
    feed.complete()

    def finish(i, carry):
        gather(i).finish()
        for half in (0, 1):
            pltpu.make_async_copy(full.at[half, i], weights_out.at[half, i], keep.at[i, half]).wait()
        return carry

    lax.fori_loop(0, line, finish, 0)
    feed.finish()
    relay.finish()

    @pl.when(t < line - 1)
    def _():
        row_one.wait_send()

    @pl.when(inner)
    def _():
        row_two.wait_send()

    upward.ends()
    upward.finish()


def attention_forward(weights, mlp, rows_one, upstream, source, gain_qk, gain_two, tables, segments, size, line):
    cols = 3 * weights[0].shape[1] // 2
    rows, width = rows_one.shape
    length = segments.shape[1]
    span = rows * (1 - (1 - longest_document) // rows)
    head = gain_qk.shape[1]
    pieces = 2 * (size // 2)
    vmem = pl.BlockSpec(memory_space=pltpu.VMEM)
    hbm = pl.BlockSpec(memory_space=pl.ANY)
    shape = jax.ShapeDtypeStruct
    return pl.pallas_call(
        functools.partial(forward_kernel, size, line, head),
        out_shape=(
            shape((2, line, width, cols), bf16),
            shape((2, width, mlp[0].shape[1]), bf16),
            shape((line, rows, width), bf16),
            shape((line, rows, 4 * head), f32),
            shape((line, rows, 2 * head), f32),
            shape((line, rows, 4 * head), bf16),
            shape((line, span, 2 * head), bf16),
            shape((line, span, 2 * head), bf16),
            shape((line, rows, 128), f32),
            shape((line, rows, 4 * head), bf16),
            shape((rows, width), f32),
            shape((rows, width), bf16),
        ),
        in_specs=[hbm] * 4 + [vmem] * 12,
        out_specs=[hbm] * 3 + [vmem] * 9,
        scratch_shapes=[
            pltpu.VMEM((2, line, width, cols), bf16),
            pltpu.VMEM((span, width), bf16),
            pltpu.VMEM((rows, width), f32),
            pltpu.SemaphoreType.DMA((6,)),
            pltpu.SemaphoreType.DMA((line,)),
            pltpu.SemaphoreType.DMA((line, 2, pieces)),
            pltpu.SemaphoreType.DMA((line, 2, pieces)),
            pltpu.SemaphoreType.DMA((2,)),
            pltpu.SemaphoreType.DMA((2,)),
            pltpu.SemaphoreType.DMA((line, 2)),
            pltpu.SemaphoreType.DMA((2, pieces)),
            pltpu.SemaphoreType.DMA((2, pieces)),
            pltpu.SemaphoreType.DMA((6,)),
            pltpu.SemaphoreType.DMA((line,)),
            pltpu.SemaphoreType.DMA((8,)),
            pltpu.VMEM((span, head), f32),
            pltpu.VMEM((span, head), f32),
            pltpu.VMEM((8, span - rows + length), f32),
        ],
        compiler_params=pltpu.CompilerParams(
            collective_id=0, has_side_effects=True, vmem_limit_bytes=62 << 20
        ),
        cost_estimate=pl.CostEstimate(flops=40 << 30, bytes_accessed=200 << 20, transcendentals=4 << 20),
    )(*weights, *mlp, rows_one, upstream, source, gain_qk, gain_two, *tables, segments)


def feed_kernel(
    size, line,
    rows_in, upstream_in, pair_in, down_in,
    rows_out, hidden_out, gate_out, up_out, grad_out, mixed_out,
    rows_v, upstream_v, pair, down, gate_f, up_f, hidden_v, gate_v, up_v, grad_v, mixed_v,
    z_send, z_recv, send, recv, local, leave,
):
    links = Links(size)
    d, t = lax.axis_index("dp"), lax.axis_index("tensor")
    block = down_in.shape[0]
    _, rows, width = rows_v.shape
    units = hidden_v.shape[2]
    chunk = units // 4
    piece = width // 4

    def place(mask):
        return pl.ds(links.masks.index(mask) * block, block)

    gather = Gather(
        links, d, t,
        lambda half, mask: down.at[half, place(mask)],
        lambda half, index: send.at[half, index],
        lambda half, index: recv.at[half, index],
    )
    relay = Relay(d, t, line, lambda slot: rows_v.at[slot], z_send, z_recv)
    arrivals = (
        pltpu.make_async_copy(rows_in, rows_v.at[0], local.at[0]),
        pltpu.make_async_copy(down_in.at[:, 0 : units // 2], down.at[0, place(0)], local.at[1]),
        pltpu.make_async_copy(down_in.at[:, units // 2 :], down.at[1, place(0)], local.at[4]),
        pltpu.make_async_copy(pair_in, pair, local.at[2]),
        pltpu.make_async_copy(upstream_in, upstream_v, local.at[3]),
    )
    for copy in arrivals:
        copy.start()
    greet(links, d, t, line)
    arrivals[0].wait()
    relay.first()
    arrivals[1].wait()
    arrivals[2].wait()
    gather.launch()
    gather.onward()
    arrivals[3].wait()
    arrivals[4].wait()

    def departures(slot):
        position = lax.rem(slot + t, line)
        natural = pl.ds(pl.multiple_of(position * rows, rows), rows)
        return [
            pltpu.make_async_copy(rows_v.at[slot], rows_out.at[slot], leave.at[0, slot]),
            pltpu.make_async_copy(hidden_v.at[slot], hidden_out.at[slot], leave.at[1, slot]),
            pltpu.make_async_copy(gate_v.at[slot], gate_out.at[slot], leave.at[2, slot]),
            pltpu.make_async_copy(up_v.at[slot], up_out.at[slot], leave.at[3, slot]),
            pltpu.make_async_copy(grad_v.at[slot], grad_out.at[natural], leave.at[4, slot]),
            pltpu.make_async_copy(mixed_v.at[slot], mixed_out.at[natural], leave.at[5, slot]),
        ]

    def step(i, carry):
        slot = slot_of(i, t, line)
        for c in range(4):
            cols = slice(c * chunk, (c + 1) * chunk)
            gate = nn(rows_v[slot], pair[0, :, cols])
            up = nn(rows_v[slot], pair[1, :, cols])
            gate_f[:, cols] = gate
            up_f[:, cols] = up
            hidden_v[slot, :, cols] = (gate * jax.nn.sigmoid(gate) * up).astype(bf16)

        @pl.when(i == 0)
        def _():
            relay.second()
            gather.complete()

        @pl.when(i == 1)
        def _():
            relay.third()

        @pl.when(i == 2)
        def _():
            relay.ends()

        for c in range(4):
            cols = slice(c * chunk, (c + 1) * chunk)
            inner = slice((c % 2) * chunk, (c % 2 + 1) * chunk)
            grad_hidden = nn(upstream_v[slot], down[c // 2, :, inner])
            gate, up = gate_f[:, cols], up_f[:, cols]
            sigmoid = jax.nn.sigmoid(gate)
            gate_v[slot, :, cols] = (
                grad_hidden * up * sigmoid * (1.0 + gate * (1.0 - sigmoid))
            ).astype(bf16)
            up_v[slot, :, cols] = (grad_hidden * (gate * sigmoid)).astype(bf16)
        for n in range(4):
            out = slice(n * piece, (n + 1) * piece)
            grad_v[slot, :, out] = (
                nt(gate_v[slot], pair[0, out, :]) + nt(up_v[slot], pair[1, out, :])
            ).astype(bf16)
            mixed_v[slot, :, out] = (
                nt(hidden_v[slot, :, : units // 2], down[0, out, :])
                + nt(hidden_v[slot, :, units // 2 :], down[1, out, :])
            ).astype(bf16)
        for copy in departures(slot):
            copy.start()
        return carry

    lax.fori_loop(0, line, step, 0)

    def finish(i, carry):
        for copy in departures(i):
            copy.wait()
        return carry

    lax.fori_loop(0, line, finish, 0)
    gather.finish()
    relay.finish()


def feed_forward(rows_own, upstream_all, pair_full, down_shard, size, line):
    rows, width = rows_own.shape
    units = pair_full.shape[2]
    hbm = pl.BlockSpec(memory_space=pl.ANY)
    shape = jax.ShapeDtypeStruct
    dma = pltpu.SemaphoreType.DMA
    return pl.pallas_call(
        functools.partial(feed_kernel, size, line),
        out_shape=(
            shape((line, rows, width), bf16),
            shape((line, rows, units), bf16),
            shape((line, rows, units), bf16),
            shape((line, rows, units), bf16),
            shape((line * rows, width), bf16),
            shape((line * rows, width), bf16),
        ),
        in_specs=[hbm] * 4,
        out_specs=[hbm] * 6,
        scratch_shapes=[
            pltpu.VMEM((line, rows, width), bf16),
            pltpu.VMEM((line, rows, width), bf16),
            pltpu.VMEM((2, width, units), bf16),
            pltpu.VMEM((2, width, units // 2), bf16),
            pltpu.VMEM((rows, units), f32),
            pltpu.VMEM((rows, units), f32),
            pltpu.VMEM((line, rows, units), bf16),
            pltpu.VMEM((line, rows, units), bf16),
            pltpu.VMEM((line, rows, units), bf16),
            pltpu.VMEM((line, rows, width), bf16),
            pltpu.VMEM((line, rows, width), bf16),
            dma((6,)),
            dma((line,)),
            dma((2, size)),
            dma((2, size)),
            dma((5,)),
            dma((6, line)),
        ],
        compiler_params=pltpu.CompilerParams(
            collective_id=1, has_side_effects=True, vmem_limit_bytes=62 << 20
        ),
        cost_estimate=pl.CostEstimate(flops=40 << 30, bytes_accessed=60 << 20, transcendentals=3 << 20),
    )(rows_own, upstream_all, pair_full, down_shard)


class Scatter:
    def __init__(self, links, d, t, block, refs, semaphores):
        self.links, self.d, self.t, self.block = links, d, t, block
        self.odd, self.core, self.sums, self.arrived, self.out = refs
        self.core_send, self.core_recv, self.send, self.recv = semaphores

    @staticmethod
    def pieces(links):
        return max(1, len(links.evens) - 1)

    def steps(self, half):
        masks, number, found = self.links.evens, 0, []
        for bit in self.links.orders[half][::-1]:
            masks = [m for m in masks if not m & bit]
            found.append((bit, [(m, number + i) for i, m in enumerate(masks)]))
            number += len(masks)
        return found

    def rows(self, mask):
        return pl.ds(self.links.evens.index(mask) * self.block, self.block)

    def core_copy(self, j):
        return mesh_copy(
            self.odd(j), self.core(j), self.core_send(j), self.core_recv(j), (self.d ^ 1, self.t)
        )

    def piece_copy(self, j, mask, number, bit):
        return mesh_copy(
            self.sums(j, self.rows(mask ^ bit)), self.arrived(j, number), self.send(j, number),
            self.recv(j, number), (self.d ^ bit, self.t),
        )

    def launch(self, j, half, step):
        steps = self.steps(half)
        if step < len(steps):
            bit, pairs = steps[step]
            for mask, number in pairs:
                self.piece_copy(j, mask, number, bit).start()

    def add(self, j, mask, value):
        if mask == 0:
            out = self.out(j)
            out[...] = out[...] + value[...].astype(f32)
        else:
            total = self.sums(j, self.rows(mask))
            total[...] = (total[...].astype(f32) + value[...].astype(f32)).astype(bf16)

    def stage(self, j, half, stage):
        if stage == 0:
            self.core_copy(j).wait_recv()
            steps = self.steps(half)
            first = steps[0][0] if steps else 0
            for mask in sorted(self.links.evens, key=lambda m: not m & first):
                self.add(j, mask, self.core(j, self.rows(mask)))
        else:
            bit, pairs = self.steps(half)[stage - 1]
            for mask, number in pairs[::-1]:
                self.piece_copy(j, mask, number, bit).wait_recv()
                self.add(j, mask, self.arrived(j, number))
        self.launch(j, half, stage)

    def finish(self, j, half, core=True):
        if core:
            self.core_copy(j).wait_send()
        for bit, pairs in self.steps(half):
            for mask, number in pairs:
                self.piece_copy(j, mask, number, bit).wait_send()


def greet_dp(links, d, t):
    barrier = pltpu.get_barrier_semaphore()
    for bit in [1] + links.bits:
        pl.semaphore_signal(barrier, inc=1, device_id=(d ^ bit, t), device_id_type=pl.DeviceIdType.MESH)
    pl.semaphore_wait(barrier, 1 + len(links.bits))


class LineSum:
    def __init__(self, d, t, line, source, ends, outbox, inbox, semaphores):
        self.d, self.t, self.line = d, t, line
        self.source, self.ends, self.outbox, self.inbox = source, ends, outbox, inbox
        self.send, self.recv, self.local = semaphores
        self.rows = outbox.shape[1]

    def block(self, position):
        return self.source.at[pl.ds(pl.multiple_of(position * self.rows, self.rows), self.rows)]

    def hop(self, number, source, target, to):
        return mesh_copy(source, target, self.send.at[number], self.recv.at[number], (self.d, to))

    def hops(self):
        t, line = self.t, self.line
        return (
            (t == 0, lambda: self.hop(0, self.block(line - 1), self.inbox.at[0], t + 1)),
            (t == line - 1, lambda: self.hop(0, self.block(0), self.inbox.at[0], t - 1)),
            (t >= 2, lambda: self.hop(1, self.outbox.at[0], self.inbox.at[1], t - 1)),
            (t <= 1, lambda: self.hop(2, self.outbox.at[0], self.inbox.at[2], t + 1)),
            (t > 0, lambda: self.hop(3, self.outbox.at[1], self.ends[0], t - 1)),
            (t < line - 1, lambda: self.hop(4, self.outbox.at[2], self.ends[1], t + 1)),
        )

    def start(self, *numbers):
        for number in numbers:
            condition, make = self.hops()[number]

            @pl.when(condition)
            def _(make=make):
                make().start()

    def own(self, box, step):
        position = lax.rem(self.t + step, self.line)
        return pltpu.make_async_copy(self.block(position), self.outbox.at[box], self.local.at[box])

    def take(self, box, number):
        @pl.when((self.t > 0) & (self.t < self.line - 1))
        def _():
            self.hop(number, self.outbox.at[0], self.inbox.at[number], self.t + 1).wait_recv()
            self.outbox[box] = (
                self.outbox[box].astype(f32) + self.inbox[number].astype(f32)
            ).astype(bf16)

    def first(self):
        self.start(0, 1)
        for box, step in ((0, 2), (1, 3), (2, 1)):
            self.own(box, step).start()

    def second(self):
        self.own(0, 2).wait()
        self.take(0, 0)
        self.start(2, 3)

    def third(self):
        self.own(1, 3).wait()
        self.own(2, 1).wait()
        self.take(1, 1)
        self.take(2, 2)
        self.start(4, 5)

    def finish(self):
        for condition, make in self.hops():

            @pl.when(condition)
            def _(make=make):
                make().wait_send()

        @pl.when(self.t < self.line - 1)
        def _():
            self.hop(3, self.outbox.at[1], self.ends[0], self.t + 1).wait_recv()

        @pl.when(self.t > 0)
        def _():
            self.hop(4, self.outbox.at[2], self.ends[1], self.t - 1).wait_recv()


def weight_kernel(
    size, line,
    rows_in, upstream_in, gate_in, up_in, hidden_in, grad_in,
    gate_out, up_out, down_out, sum_left, sum_right,
    outbox, inbox, raw, left, right, odd, core, sums, arrived, out,
    core_send, core_recv, send, recv, local, raw_sem, leave, sum_send, sum_recv, sum_local,
):
    links = Links(size)
    d, t = lax.axis_index("dp"), lax.axis_index("tensor")
    width = left.shape[1]
    rows = raw.shape[1]
    ring, tokens, chunk = right.shape
    count = out.shape[0]
    middle = width // 2
    block = out.shape[1]
    pairs = count // 2
    wide = gate_in.shape[1] // chunk

    def load(j):
        p, h = j // 2, j % 2
        if p < wide:
            source, at = (gate_in, up_in)[h], p
        else:
            source, at = hidden_in, p - wide + h * (wide // 2)
        return pltpu.make_async_copy(
            source.at[:, at * chunk : (at + 1) * chunk], right.at[j % ring], local.at[j]
        )

    def store(j):
        p, h = j // 2, j % 2
        if p < wide:
            target, at = (gate_out, up_out)[h], p
        else:
            target, at = down_out, p - wide + h * (wide // 2)
        return pltpu.make_async_copy(
            out.at[j], target.at[:, at * chunk : (at + 1) * chunk], leave.at[j]
        )

    def fetch(k, r):
        source = (rows_in, upstream_in)[k]
        slot = (k * line + r) % 2
        return pltpu.make_async_copy(source.at[r], raw.at[slot], raw_sem.at[slot]), slot

    fetch(0, 0)[0].start()
    for j in range(ring):
        load(j).start()
    greet(links, d, t, line)
    gradient = LineSum(
        d, t, line, grad_in, (sum_left, sum_right), outbox, inbox, (sum_send, sum_recv, sum_local)
    )
    gradient.first()

    def turn(k):
        for r in range(line):
            copy, slot = fetch(k, r)
            copy.wait()
            following = k * line + r + 1
            if following < 2 * line:
                fetch(following // line, following % line)[0].start()
            left[k, :, r * rows : (r + 1) * rows] = raw[slot].T

    engine = Scatter(
        links, d, t, block,
        (
            lambda j: odd.at[j],
            lambda j, at=pl.ds(0, middle): core.at[j, at],
            lambda j, at: sums.at[j, at],
            lambda j, number: arrived.at[j, number],
            lambda j: out.at[j],
        ),
        (
            lambda j: core_send.at[j],
            lambda j: core_recv.at[j],
            lambda j, number: send.at[j, number],
            lambda j, number: recv.at[j, number],
        ),
    )
    turn(0)

    def step(p, carry):
        @pl.when(p == wide // 2)
        def _():
            gradient.second()
            turn(1)

        @pl.when(p == wide)
        def _():
            gradient.third()

        for q in range(pairs):

            @pl.when(p == q)
            def _(q=q):
                load(2 * q).wait()
                load(2 * q + 1).wait()

        @pl.when(p < pairs)
        def _():
            k = jnp.where(p < wide, 0, 1)
            for h in (0, 1):
                j = 2 * p + h
                for r in range(middle // 256):
                    at = pl.ds(middle + r * 256, 256)
                    odd[j, pl.ds(r * 256, 256), :] = nn(
                        left[k, at, :], right[lax.rem(j, ring)]
                    ).astype(bf16)
                engine.core_copy(j).start()
            for h in (0, 1):
                j = 2 * p + h
                for r in range(middle // 256):
                    at = pl.ds(r * 256, 256)
                    value = nn(left[k, at, :], right[lax.rem(j, ring)])
                    sums[j, at, :] = value.astype(bf16)
                    if r == 0:
                        out[j] = value[:block]

        for q in range(pairs - ring // 2):

            @pl.when(p == q)
            def _(q=q):
                load(2 * q + ring).start()
                load(2 * q + ring + 1).start()

        for stage in range(len(links.bits) + 1):
            @pl.when((p >= stage + 1) & (p < pairs + stage + 1))
            def _(stage=stage):
                for h in (0, 1):
                    engine.stage(2 * (p - stage - 1) + h, h, stage)

        return carry

    lax.fori_loop(0, pairs + len(links.bits) + 1, step, 0)
    for j in range(count):
        store(j).start()

    def finish(p, carry):
        for h in (0, 1):
            engine.finish(2 * p + h, h)
        return carry

    lax.fori_loop(0, pairs, finish, 0)
    for j in range(count):
        store(j).wait()
    gradient.finish()


def feed_weights(rows_all, upstream_all, gate, up, hidden, grad, size):
    line, rows, width = rows_all.shape
    tokens, units = gate.shape
    chunk = units // 4
    count = 3 * 4
    block = width // size
    middle = width // 2
    pieces = Scatter.pieces(Links(size))
    hbm = pl.BlockSpec(memory_space=pl.ANY)
    shape = jax.ShapeDtypeStruct
    dma = pltpu.SemaphoreType.DMA
    return pl.pallas_call(
        functools.partial(weight_kernel, size, line),
        out_shape=(shape((block, units), f32),) * 3 + (shape((rows, width), bf16),) * 2,
        in_specs=[hbm] * 6,
        out_specs=[hbm] * 5,
        scratch_shapes=[
            pltpu.VMEM((3, rows, width), bf16),
            pltpu.VMEM((3, rows, width), bf16),
            pltpu.VMEM((2, rows, width), bf16),
            pltpu.VMEM((2, width, tokens), bf16),
            pltpu.VMEM((4, tokens, chunk), bf16),
            pltpu.VMEM((count, middle, chunk), bf16),
            pltpu.VMEM((count, middle, chunk), bf16),
            pltpu.VMEM((count, middle, chunk), bf16),
            pltpu.VMEM((count, pieces, block, chunk), bf16),
            pltpu.VMEM((count, block, chunk), f32),
            dma((count,)),
            dma((count,)),
            dma((count, pieces)),
            dma((count, pieces)),
            dma((count,)),
            dma((2,)),
            dma((count,)),
            dma((5,)),
            dma((5,)),
            dma((3,)),
        ],
        compiler_params=pltpu.CompilerParams(
            collective_id=2, has_side_effects=True, vmem_limit_bytes=63 << 20
        ),
        cost_estimate=pl.CostEstimate(flops=20 << 30, bytes_accessed=60 << 20, transcendentals=0),
    )(rows_all, upstream_all, gate, up, hidden, grad)


def spread_stages(engine, links, first, last, p):
    for stage in range(len(links.bits) + 1)[::-1]:
        @pl.when((p - stage >= first) & (p - stage < last))
        def _(stage=stage):
            for h in (0, 1):
                engine.stage(2 * (p - stage) + h, h, stage)


def backward_kernel(
    size, line, head,
    branch, weights, q_in, k_in, v_in, lse_in, att_in, proj_q, proj_k, gain_qk, cos_in, sin_in, cos_at, sin_at,
    segments, mixed_in,
    gq_out, gkv_out, terms_out, o_out, mixed_out,
    o_full, branch_t, gatt, own_kv, near_f, far_v, near_v, far_in, near_in, odd, core, sums, arrived, out,
    core_send, core_recv, send, recv, far_send, far_recv, near_send, near_recv, local,
    line_send, line_recv, cosine, sine, padded,
):
    links = Links(size)
    d, t = lax.axis_index("dp"), lax.axis_index("tensor")
    rows, width = branch.shape
    span = k_in.shape[1]
    middle = width // 2
    block = out.shape[1]
    factor = head**-0.5
    loads = [
        pltpu.make_async_copy(
            weights.at[h, s, :, 4 * head : 6 * head], o_full.at[s, h], local.at[s, h]
        )
        for s in range(line)
        for h in (0, 1)
    ]
    for copy in loads:
        copy.start()
    greet(links, d, t, line)

    def hop(at, to):
        return mesh_copy(
            mixed_in.at[pl.ds(at * rows, rows)], mixed_out, line_send.at[0], line_recv.at[0], (d, to)
        )

    def hop_of(act):
        @pl.when(t == 0)
        def _():
            act(hop(line - 1, t + 1))

        @pl.when(t == line - 1)
        def _():
            act(hop(0, t - 1))

    hop_of(lambda copy: copy.start())

    engine = Scatter(
        links, d, t, block,
        (
            lambda j: odd.at[j],
            lambda j, at=pl.ds(0, middle): core.at[j, at],
            lambda j, at: sums.at[j, at],
            lambda j, number: arrived.at[j, number],
            lambda j: out.at[j],
        ),
        (
            lambda j: core_send.at[j],
            lambda j: core_recv.at[j],
            lambda j, number: send.at[j, number],
            lambda j, number: recv.at[j, number],
        ),
    )
    branch_t[...] = branch[...].T

    def first(s, carry):
        for h in (0, 1):
            j = 2 * s + h
            right = att_in[s, :, h * 2 * head : (h + 1) * 2 * head]
            odd[j] = nn(branch_t[middle:, :], right).astype(bf16)
            engine.core_copy(j).start()
        for h in (0, 1):
            j = 2 * s + h
            right = att_in[s, :, h * 2 * head : (h + 1) * 2 * head]
            value = nn(branch_t[:middle, :], right)
            sums[j] = value.astype(bf16)
            out[j] = value[:block]
        return carry

    lax.fori_loop(0, line, first, 0)
    for copy in loads:
        copy.wait()

    cosine[...], sine[...] = rope_block((cos_in, sin_in, cos_at, sin_at), t + span // rows - 1, head)
    key_row, _ = segment_masks(segments, padded, t, rows, span)
    key_column = turned(key_row)
    query_row = key_row[:, span - rows :]
    k_index = lax.broadcasted_iota(jnp.int32, (span, rows), 0)
    q_index = lax.broadcasted_iota(jnp.int32, (span, rows), 1) + (span - rows)

    def far_copy(slot):
        return mesh_copy(
            far_v.at[slot], far_in.at[lax.rem(slot + 1, line)], far_send.at[slot],
            far_recv.at[lax.rem(slot + 1, line)], (d, t - 1),
        )

    def near_copy(slot):
        return mesh_copy(
            near_v.at[slot], near_in.at[lax.rem(slot + 1, line)], near_send.at[slot],
            near_recv.at[lax.rem(slot + 1, line)], (d, t - 1),
        )

    def arriving(copy, slot):
        return copy(lax.rem(slot + line - 1, line))

    def pass_near(slot):
        @pl.when((t > 0) & (t < line - 1))
        def _():
            arriving(far_copy, slot).wait_recv()
            near_v[slot] = (near_f[slot] + far_in[slot].astype(f32)).astype(bf16)

        @pl.when(t == line - 1)
        def _():
            near_v[slot] = near_f[slot].astype(bf16)

        @pl.when(t > 0)
        def _():
            near_copy(slot).start()

    def head_back(raw, gain, value, cos, sin):
        c = value * cos + pltpu.roll(value * sin, head // 2, 1)
        inverse = lax.rsqrt(jnp.mean(raw * raw, axis=-1, keepdims=True) + epsilon)
        normed = raw * inverse
        inner = c * gain
        grad = inverse * (inner - normed * jnp.mean(inner * normed, axis=-1, keepdims=True))
        return grad, jnp.sum(c * normed, axis=0, keepdims=True)

    terms_out[...] = jnp.zeros(terms_out.shape, f32)

    def step(s, carry):
        allowed = (key_column == query_row) & (k_index <= q_index)
        for h in (0, 1):
            gatt[:, h * 2 * head : (h + 1) * 2 * head] = nn(branch[...], o_full[s, h]).astype(bf16)
        lse = lse_in[s].T
        for g in (0, 1):
            keys = k_in[s, :, g * head : (g + 1) * head]
            values = v_in[s, :, g * head : (g + 1) * head]
            grad_k = jnp.zeros((span, head), f32)
            grad_v = jnp.zeros((span, head), f32)
            for j in (0, 1):
                h = 2 * g + j
                cols = slice(h * head, (h + 1) * head)
                query = q_in[s, :, cols]
                upward = gatt[:, cols]
                scores = nt(keys, query) * factor
                scores = jnp.where(allowed, scores, -1e30)
                probs = jnp.exp(scores - lse[h : h + 1, :])
                grad_probs = nt(values, upward)
                delta = jnp.sum(probs * grad_probs, axis=0, keepdims=True)
                grad_scores = (probs * (grad_probs - delta)).astype(bf16)
                grad_k = grad_k + nn(grad_scores, query)
                grad_v = grad_v + nn(probs.astype(bf16), upward)
                grad_q = (tn(grad_scores, keys) * factor).astype(bf16).astype(f32)
                grad, term = head_back(proj_q[s, :, cols], gain_qk[0:1, :], grad_q, cosine[...], sine[...])
                gq_out[s, :, cols] = grad.astype(bf16)
                terms_out[0:1, :] += term
            grad_k = grad_k * factor
            for at, value in ((g * head, grad_k), ((2 + g) * head, grad_v)):
                far_v[s, :, at : at + head] = value[:rows].astype(bf16)
                near_f[s, :, at : at + head] = value[rows : 2 * rows]
                own_kv[s, :, at : at + head] = value[2 * rows :]

        @pl.when(t > 1)
        def _():
            far_copy(s).start()

        spread_stages(engine, links, 0, line, s)

        @pl.when(s > 0)
        def _():
            pass_near(s)

        return carry

    lax.fori_loop(0, line, step, 0)
    pass_near(0)

    def last(i, carry):
        s = lax.rem(i + 2, line)
        spread_stages(engine, links, 0, line, i + line)

        @pl.when(t < line - 1)
        def _():
            arriving(near_copy, s).wait_recv()
            own_kv[s] = own_kv[s] + near_in[s].astype(f32)

        for g in (0, 1):
            cols = slice(g * head, (g + 1) * head)
            value = own_kv[s, :, cols].astype(bf16).astype(f32)
            grad, term = head_back(proj_k[s, :, cols], gain_qk[1:2, :], value, cosine[...], sine[...])
            gkv_out[s, :, cols] = grad.astype(bf16)
            terms_out[1:2, :] += term
        gkv_out[s, :, 2 * head :] = own_kv[s, :, 2 * head :].astype(bf16)
        return carry

    lax.fori_loop(0, line, last, 0)

    def finish(s, carry):
        for h in (0, 1):
            engine.finish(2 * s + h, h)
            o_out[s, :, h * 2 * head : (h + 1) * 2 * head] = out[2 * s + h]

        @pl.when(t > 1)
        def _():
            far_copy(s).wait_send()

        @pl.when(t > 0)
        def _():
            near_copy(s).wait_send()

        return carry

    lax.fori_loop(0, line, finish, 0)

    hop_of(lambda copy: copy.wait_send())

    @pl.when((t > 0) & (t < line - 1))
    def _():
        hop(0, t - 1).wait_recv()


def attention_backward(branch, weights, q, k, v, lse, att, proj_q, proj_k, gain_qk, tables, segments, mixed, size):
    line, rows, q_cols = q.shape
    width = branch.shape[1]
    span = k.shape[1]
    head = gain_qk.shape[1]
    block, middle, count, chunk = width // size, width // 2, 2 * line, 2 * head
    pieces = Scatter.pieces(Links(size))
    vmem = pl.BlockSpec(memory_space=pltpu.VMEM)
    hbm = pl.BlockSpec(memory_space=pl.ANY)
    shape = jax.ShapeDtypeStruct
    dma = pltpu.SemaphoreType.DMA
    return pl.pallas_call(
        functools.partial(backward_kernel, size, line, head),
        out_shape=(
            shape((line, rows, 4 * head), bf16),
            shape((line, rows, 4 * head), bf16),
            shape((8, head), f32),
            shape((line, block, 4 * head), f32),
            shape((rows, width), bf16),
        ),
        in_specs=[vmem, hbm] + [vmem] * 13 + [hbm],
        out_specs=[vmem] * 4 + [hbm],
        scratch_shapes=[
            pltpu.VMEM((line, 2, width, 2 * head), bf16),
            pltpu.VMEM((width, rows), bf16),
            pltpu.VMEM((rows, 4 * head), bf16),
            pltpu.VMEM((line, rows, 4 * head), f32),
            pltpu.VMEM((line, rows, 4 * head), f32),
            pltpu.VMEM((line, rows, 4 * head), bf16),
            pltpu.VMEM((line, rows, 4 * head), bf16),
            pltpu.VMEM((line, rows, 4 * head), bf16),
            pltpu.VMEM((line, rows, 4 * head), bf16),
            pltpu.VMEM((count, middle, chunk), bf16),
            pltpu.VMEM((count, middle, chunk), bf16),
            pltpu.VMEM((count, middle, chunk), bf16),
            pltpu.VMEM((count, pieces, block, chunk), bf16),
            pltpu.VMEM((count, block, chunk), f32),
            dma((count,)),
            dma((count,)),
            dma((count, pieces)),
            dma((count, pieces)),
            dma((line,)),
            dma((line,)),
            dma((line,)),
            dma((line,)),
            dma((line, 2)),
            dma((1,)),
            dma((1,)),
            pltpu.VMEM((rows, head), f32),
            pltpu.VMEM((rows, head), f32),
            pltpu.VMEM((8, span - rows + line * rows), f32),
        ],
        compiler_params=pltpu.CompilerParams(
            collective_id=3, has_side_effects=True, vmem_limit_bytes=62 << 20
        ),
        cost_estimate=pl.CostEstimate(flops=20 << 30, bytes_accessed=40 << 20, transcendentals=4 << 20),
    )(branch, weights, q, k, v, lse, att, proj_q, proj_k, gain_qk, *tables, segments, mixed)


def final_kernel(
    size, line, head,
    rows_in, gq_in, gkv_in, o_in, weights, source, grad_middle, gain_one, second_terms, head_terms,
    mixed_two, mixed_in,
    q_out, kv_out, o_out, input_out, terms_out, mixed_left, mixed_right,
    rows_t, pair, acc, odd, core, sums, arrived, out, outbox, inbox, heap, mixed_box, mixed_mail,
    core_send, core_recv, send, recv, local, line_send, line_recv, heap_send, heap_recv, mixed_send, mixed_recv, mixed_local,
):
    links = Links(size)
    d, t = lax.axis_index("dp"), lax.axis_index("tensor")
    rows, width = rows_in.shape
    middle = width // 2
    block = out.shape[1]
    chunk = 4 * head
    last_stage = len(links.bits)
    inner = (t > 0) & (t < line - 1)
    is_end = (t == 0) | (t == line - 1)

    def slot_at(i):
        return slot_of(line - 1 - i, t, line)

    def load(i, h):
        return pltpu.make_async_copy(
            weights.at[h, slot_at(i), :, 0 : 4 * head], pair.at[h], local.at[h]
        )

    for h in (0, 1):
        load(0, h).start()
    inside = block % 128 == 0
    greet(links, d, t, line, inside)

    def mixed_hop(number):
        source, target, to = (
            (mixed_two, mixed_mail.at[0], t - 1),
            (mixed_two, mixed_mail.at[1], t + 1),
            (mixed_box.at[0], mixed_left, t - 1),
            (mixed_box.at[1], mixed_right, t + 1),
        )[number]
        return mesh_copy(source, target, mixed_send.at[number], mixed_recv.at[number], (d, to))

    def mixed_own(box):
        position = lax.rem(t + (3, 1)[box], line)
        at = pl.ds(pl.multiple_of(position * rows, rows), rows)
        return pltpu.make_async_copy(mixed_in.at[at], mixed_box.at[box], mixed_local.at[box])

    @pl.when(t >= line // 2)
    def _():
        mixed_hop(0).start()

    @pl.when(t < line // 2)
    def _():
        mixed_hop(1).start()

    for box in (0, 1):
        mixed_own(box).start()

    def mixed_on():
        for box in (0, 1):
            mixed_own(box).wait()

            @pl.when(inner)
            def _(box=box):
                mixed_hop(box).wait_recv()
                mixed_box[box] = (
                    mixed_box[box].astype(f32) + mixed_mail[box].astype(f32)
                ).astype(bf16)

        @pl.when(t > 0)
        def _():
            mixed_hop(2).start()

        @pl.when(t < line - 1)
        def _():
            mixed_hop(3).start()

    engine = Scatter(
        links, d, t, block,
        (
            lambda j: odd.at[lax.rem(j, odd.shape[0])],
            lambda j, at=pl.ds(0, middle): core.at[j, at],
            lambda j, at: sums.at[j, at],
            lambda j, number: arrived.at[j, number],
            lambda j: out.at[j],
        ),
        (
            lambda j: core_send.at[j],
            lambda j: core_recv.at[j],
            lambda j, number: send.at[j, number],
            lambda j, number: recv.at[j, number],
        ),
    )
    rows_t[...] = rows_in[...].T
    acc[...] = jnp.zeros(acc.shape, f32)

    def first(i, carry):
        slot = slot_at(i)
        for h in (0, 1):
            j = 2 * i + h

            @pl.when(i >= odd.shape[0] // 2)
            def _(j=j):
                engine.core_copy(j - odd.shape[0]).wait_send()

            odd[lax.rem(j, odd.shape[0])] = nn(
                rows_t[middle:, :], (gq_in, gkv_in)[h][slot]
            ).astype(bf16)
            engine.core_copy(j).start()
        for h in (0, 1):
            j = 2 * i + h
            value = nn(rows_t[:middle, :], (gq_in, gkv_in)[h][slot])
            sums[j] = value.astype(bf16)
            out[j] = value[:block]
        return carry

    lax.fori_loop(0, line, first, 0)

    def content(i, c):
        return o_in[slot_at(i)] if c == 2 else out[2 * i + c]

    def each(fill):
        for c in range(3):
            fill(c, slice(c * chunk, (c + 1) * chunk))

    def post(number, to):
        box = (0, 1, 1, 3, 2)[number]
        return mesh_copy(
            outbox.at[box], inbox.at[number], line_send.at[number], line_recv.at[number], (d, to)
        )

    def first_post():
        return post(0, jnp.where(t == 0, t + 1, t - 1))

    def along(i):
        if i == 0:

            @pl.when(is_end)
            def _():
                def fill(c, at):
                    outbox[0, :, at] = content(0, c).astype(bf16)

                each(fill)
                first_post().start()

        if i == 1:

            @pl.when(inner)
            def _():
                first_post().wait_recv()

            @pl.when(is_end)
            def _():
                inbox[0] = jnp.zeros(inbox.shape[1:], bf16)

            def fill(c, at):
                outbox[1, :, at] = (content(1, c) + inbox[0, :, at].astype(f32)).astype(bf16)

            each(fill)

            @pl.when(t >= 2)
            def _():
                post(1, t - 1).start()

            @pl.when(t <= 1)
            def _():
                post(2, t + 1).start()

        if i == 2:

            @pl.when(inner)
            def _():
                post(1, t - 1).wait_recv()
                post(2, t + 1).wait_recv()

            @pl.when(is_end)
            def _():
                inbox[1] = jnp.zeros(inbox.shape[1:], bf16)
                inbox[2] = jnp.zeros(inbox.shape[1:], bf16)

            def leftward(c, at):
                three = jnp.where(t == line - 1, content(2, c), content(0, c))
                outbox[3, :, at] = (three + inbox[1, :, at].astype(f32)).astype(bf16)

            def rightward(c, at):
                outbox[2, :, at] = (content(2, c) + inbox[2, :, at].astype(f32)).astype(bf16)

            @pl.when(t > 0)
            def _():
                each(leftward)
                post(3, t - 1).start()

            @pl.when(t < line - 1)
            def _():
                each(rightward)
                post(4, t + 1).start()

    part = rows // 4
    terms_out[...] = jnp.zeros(terms_out.shape, f32)
    terms_out[1:2, :] = second_terms[...]
    terms_out[2:3, 0:head] = head_terms[0:1, :]
    terms_out[2:3, head : 2 * head] = head_terms[1:2, :]

    def close(r, carry):
        at = pl.ds(pl.multiple_of(r * part, part), part)
        values = source[at, :].astype(f32)
        inverse = lax.rsqrt(jnp.mean(values * values, axis=-1, keepdims=True) + epsilon)
        normed = values * inverse
        c = acc[at, :]
        term = c * gain_one[...]
        grad = inverse * (term - normed * jnp.mean(term * normed, axis=-1, keepdims=True))
        input_out[at, :] = (grad_middle[at, :] + grad).astype(bf16)
        terms_out[0:1, :] += jnp.sum(c * normed, axis=0, keepdims=True)
        return carry

    def double(start, stop):
        hops = [((d ^ bit, t), bit) for bit in [1] + links.bits]
        hops = hops + [((d, t ^ 1), 0), ((d, t ^ 2), 0)]
        for k in range(start, stop):
            to, bit = hops[k]
            copy = mesh_copy(terms_out, heap.at[k], heap_send.at[k], heap_recv.at[k], to)
            copy.start()
            copy.wait()
            for i, mask in enumerate(links.masks):
                other = links.masks.index(mask ^ bit)
                terms_out[0:2, i * block : (i + 1) * block] += heap[
                    k, 0:2, other * block : (other + 1) * block
                ]
            terms_out[2:3, :] += heap[k, 2:3, :]

    def step(i, carry):
        @pl.when(i < line)
        def _():
            for h in (0, 1):
                load(i, h).wait()
            slot = slot_at(i)
            for n in range(4):
                at = slice(n * (width // 4), (n + 1) * (width // 4))
                acc[:, at] += nt(gq_in[slot], pair[0, at, :]) + nt(gkv_in[slot], pair[1, at, :])

            @pl.when(i + 1 < line)
            def _():
                for h in (0, 1):
                    load(i + 1, h).start()

        @pl.when(i == 1)
        def _():
            mixed_on()

        @pl.when(i == line)
        def _():
            lax.fori_loop(0, 4, close, 0)

        spread_stages(engine, links, 0, line, i)
        for p in range(line - 1):

            @pl.when(i == p + last_stage)
            def _(p=p):
                along(p)

        if inside:

            @pl.when(i == line)
            def _():
                double(0, 3)

        return carry

    lax.fori_loop(0, line + last_stage, step, 0)

    if inside:
        double(3, 3 + len(links.bits))

    @pl.when(t < line - 1)
    def _():
        post(3, t - 1).wait_recv()

    @pl.when(t == line - 1)
    def _():
        inbox[3] = jnp.zeros(inbox.shape[1:], bf16)

    @pl.when(t > 0)
    def _():
        post(4, t + 1).wait_recv()

    @pl.when(t == 0)
    def _():
        inbox[4] = jnp.zeros(inbox.shape[1:], bf16)

    def total(c, at):
        (q_out, kv_out, o_out)[c][...] = (
            content(line - 1, c) + inbox[3, :, at].astype(f32) + inbox[4, :, at].astype(f32)
        )

    each(total)

    def finish(i, carry):
        for h in (0, 1):
            engine.finish(2 * i + h, h, False)

            @pl.when(i >= line - odd.shape[0] // 2)
            def _(h=h):
                engine.core_copy(2 * i + h).wait_send()

        return carry

    lax.fori_loop(0, line, finish, 0)

    @pl.when(t >= line // 2)
    def _():
        mixed_hop(0).wait_send()

    @pl.when(t < line // 2)
    def _():
        mixed_hop(1).wait_send()

    @pl.when(t > 0)
    def _():
        mixed_hop(2).wait_send()
        mixed_hop(3).wait_recv()

    @pl.when(t < line - 1)
    def _():
        mixed_hop(3).wait_send()
        mixed_hop(2).wait_recv()

    @pl.when(is_end)
    def _():
        first_post().wait_send()

    @pl.when(t >= 2)
    def _():
        post(1, t - 1).wait_send()

    @pl.when(t <= 1)
    def _():
        post(2, t + 1).wait_send()

    @pl.when(t > 0)
    def _():
        post(3, t - 1).wait_send()

    @pl.when(t < line - 1)
    def _():
        post(4, t + 1).wait_send()


def attention_weights(rows_one, gq, gkv, o_sum, weights, source, grad_middle, gain_one, second_terms, head_terms, mixed_two, mixed_part, size, head):
    line, rows, chunk = gq.shape
    width = rows_one.shape[1]
    block, middle, count = width // size, width // 2, 2 * line
    pieces = Scatter.pieces(Links(size))
    hops = 3 + len(Links(size).bits)
    vmem = pl.BlockSpec(memory_space=pltpu.VMEM)
    hbm = pl.BlockSpec(memory_space=pl.ANY)
    shape = jax.ShapeDtypeStruct
    dma = pltpu.SemaphoreType.DMA
    return pl.pallas_call(
        functools.partial(final_kernel, size, line, head),
        out_shape=(
            shape((block, chunk), f32),
            shape((block, chunk), f32),
            shape((block, chunk), f32),
            shape((rows, width), bf16),
            shape((8, width), f32),
            shape((rows, width), bf16),
            shape((rows, width), bf16),
        ),
        in_specs=[vmem] * 4 + [hbm] + [vmem] * 5 + [hbm] * 2,
        out_specs=[vmem] * 5 + [hbm] * 2,
        scratch_shapes=[
            pltpu.VMEM((width, rows), bf16),
            pltpu.VMEM((2, width, chunk), bf16),
            pltpu.VMEM((rows, width), f32),
            pltpu.VMEM((count // 2, middle, chunk), bf16),
            pltpu.VMEM((count, middle, chunk), bf16),
            pltpu.VMEM((count, middle, chunk), bf16),
            pltpu.VMEM((count, pieces, block, chunk), bf16),
            pltpu.VMEM((count, block, chunk), f32),
            pltpu.VMEM((4, block, 3 * chunk), bf16),
            pltpu.VMEM((5, block, 3 * chunk), bf16),
            pltpu.VMEM((hops, 8, width), f32),
            pltpu.VMEM((2, rows, width), bf16),
            pltpu.VMEM((2, rows, width), bf16),
            dma((count,)),
            dma((count,)),
            dma((count, pieces)),
            dma((count, pieces)),
            dma((2,)),
            dma((5,)),
            dma((5,)),
            dma((hops,)),
            dma((hops,)),
            dma((4,)),
            dma((4,)),
            dma((2,)),
        ],
        compiler_params=pltpu.CompilerParams(
            collective_id=4, has_side_effects=True, vmem_limit_bytes=63 << 20
        ),
        cost_estimate=pl.CostEstimate(flops=16 << 30, bytes_accessed=40 << 20, transcendentals=0),
    )(rows_one, gq, gkv, o_sum, weights, source, grad_middle, gain_one, second_terms, head_terms, mixed_two, mixed_part)


def body(
    layer_input,
    first_gain,
    query_weight,
    key_matrix,
    value_matrix,
    query_gain,
    key_gain,
    output_weight,
    second_gain,
    gate_weight,
    up_weight,
    down_weight,
    segments,
    cotangent,
):
    plan = Plan()
    line, place = plan.line, plan.place
    rows, seq_count, width = layer_input.shape
    head = query_gain.shape[0]
    kv_heads = key_matrix.shape[1] // head
    query_heads = query_weight.shape[1] // head
    groups = query_heads // kv_heads
    all_kv = line * kv_heads
    half = width // 2
    hops = -(-(longest_document - 1) // rows)
    assert seq_count == 1 and hops == 2
    factor = head**-0.5

    gain_one = plan.to_masks(first_gain.astype(f32))
    gain_two = plan.to_masks(second_gain.astype(f32))
    source_low = plan.to_masks(layer_input[:, 0, :])
    source = source_low.astype(f32)
    upstream = plan.to_masks(cotangent[:, 0, :])

    normed, inverse_one = rms_parts(source, gain_one)
    rows_one = normed.astype(bf16)
    tables = rope_tables(-hops * rows, 8, rows, head)
    gain_qk = jnp.stack([query_gain, key_gain]).astype(f32)
    (
        weights, pair_full, upstream_all, proj_query, proj_key, query_rows, key_rows, value_rows, lse,
        attended, middle, rows_two_own,
    ) = attention_forward(
        (query_weight, key_matrix, value_matrix, output_weight), (gate_weight, up_weight), rows_one,
        upstream, source_low, gain_qk, gain_two[None], tables, segments, plan.size, line,
    )
    inverse_two = lax.rsqrt(jnp.mean(middle * middle, axis=-1, keepdims=True) + epsilon)

    rows_two, hidden, grad_gate, grad_up, grad_two_part, mixed_part = feed_forward(
        rows_two_own, upstream_all, pair_full, down_weight, plan.size, line
    )

    def unslot(values):
        return values.reshape(-1, values.shape[2])

    hidden, grad_gate, grad_up = map(unslot, (hidden, grad_gate, grad_up))
    inner = (place > 0) & (place < line - 1)

    def share(step, part=mixed_part):
        return lax.dynamic_slice(part, ((place + step) % line * rows, 0), (rows, width)).astype(f32)

    def closed(part, from_right, from_left):
        return (
            share(0, part)
            + jnp.where(place < line - 1, from_right.astype(f32), 0.0)
            + jnp.where(place > 0, from_left.astype(f32), 0.0)
        )

    gate_grad, up_grad, down_grad, grad_left, grad_right = feed_weights(
        rows_two, upstream_all, grad_gate, grad_up, hidden, grad_two_part, plan.size
    )
    grad_two = closed(grad_two_part, grad_left, grad_right)

    grad_mid_norm, gain_two_terms = rms_back(middle, inverse_two, gain_two, grad_two)
    grad_middle = upstream.astype(f32) + grad_mid_norm
    grad_branch = grad_middle.astype(bf16)
    grad_query_low, grad_kv_low, head_terms, output_sum, mixed_one = attention_backward(
        grad_branch, weights, query_rows, key_rows, value_rows, lse, attended, proj_query, proj_key,
        gain_qk, tables, segments, mixed_part, plan.size,
    )
    mixed_two = (share(2) + jnp.where(inner, mixed_one.astype(f32), 0.0)).astype(bf16)
    second_terms = jnp.sum(gain_two_terms, axis=0, keepdims=True)
    query_weight_grad, kv_grad, output_grad, input_masked, terms, mixed_left, mixed_right = attention_weights(
        rows_one, grad_query_low, grad_kv_low, output_sum, weights, source_low, grad_middle, gain_one[None],
        second_terms, head_terms, mixed_two, mixed_part, plan.size, head,
    )
    input_grad = plan.from_masks(input_masked)[:, None, :]
    middle_late = after(middle, terms)
    mixed = closed(mixed_part, mixed_left, mixed_right)
    layer_output = plan.from_masks((middle_late + mixed).astype(bf16))[:, None, :]
    gains = jnp.concatenate([plan.from_masks(terms[0]), plan.from_masks(terms[1]), terms[2, : 2 * head]])
    if width // plan.size % 128:
        gains = plan.total(gains)
    return (
        layer_output,
        input_grad,
        gains[:width],
        query_weight_grad,
        kv_grad[:, : key_matrix.shape[1]],
        kv_grad[:, key_matrix.shape[1] :],
        gains[2 * width : 2 * width + head],
        gains[2 * width + head :],
        output_grad,
        gains[width : 2 * width],
        gate_grad,
        up_grad,
        down_grad,
    )


def solution(mesh):
    positions = P("tensor", "dp", None)
    weight = P("dp", "tensor")
    return jax.shard_map(
        body,
        mesh=mesh,
        in_specs=(
            positions,
            P(),
            weight,
            weight,
            weight,
            P(),
            P(),
            weight,
            P(),
            weight,
            weight,
            weight,
            P("dp", None),
            positions,
        ),
        out_specs=(
            positions,
            positions,
            P(),
            weight,
            weight,
            weight,
            P(),
            P(),
            weight,
            P(),
            weight,
            weight,
            weight,
        ),
        check_vma=False,
    )
```
